128 devices in a mesh: row: 16 (over y, z), col: 8 (over x, core).
Axes of the slice: x: 4, y: 4, z: 4, core: 2. Of those that a mesh axis runs over, the one named last changes fastest.
Arguments:
- load_currents: float32 [32, 2048, 1024], P(None, 'row', 'col'), may hold values from -36 to 36
- labels: int32 [2048, 1024], P('row', 'col'), may hold values from 0 to 255, as said below
- bump_height: float32 [2048, 1024], P('row', 'col'), may hold values from 0.5 to 2
- horizontal_class: int32 [2048, 1024], P('row', 'col'), may hold values from 0 to 7
- vertical_class: int32 [2048, 1024], P('row', 'col'), may hold values from 0 to 7
- pad_class: int32 [2048, 1024], P('row', 'col'), may hold values from 0 to 7
- edge_table: float32 [8], replicated, may hold values from 0.5 to 4
- pad_table: float32 [8], replicated, may hold values from 0.02 to 0.5
Outputs:
- solution: float32 [32, 2048, 1024], P(None, 'row', 'col')
- residual: float32 [32, 2048, 1024], P(None, 'row', 'col')
The draws below stay inside these ranges and needn't reach their ends.
Inputs may be any that keep to these rules, and one draw needn't show every extreme that they name: `labels`: every number from 0 to 255 is the label of some nodes; the label of node (i, j) is 16 * floor(16 * i2 / 2048) + floor(16 * j2 / 1024) for some node (i2, j2) of the grid with |i2 - i| <= 32 and |j2 - j| <= 16.
All inputs are finite; a program needn't handle non-finite values.
Results may differ from the reference program's by a relative error of at most 0.0003.
Values sent between devices are 32-bit elements; how exact they have to be, the bound alone decides.
No kernel may reach another device: no remote copies, remote signals or barrier semaphores. Data moves between devices by JAX's collectives and lax.ppermute only.
A program may use at most 128 MiB of HBM per device.

```python
import math
from functools import partial
import jax
import jax.numpy as jnp
from jax import lax

NRHS = 32
REG = 16
NCLS = 8
ITERS = 2
NX = 2048
NY = 1024


def draw_labels(key, part):
    first_key, second_key = jax.random.split(jax.random.fold_in(key, 17))
    reach_rows = NX // (4 * REG)
    reach_cols = NY // (4 * REG)
    row_shift = jax.random.randint(first_key, (NX, NY), -reach_rows, reach_rows + 1)
    col_shift = jax.random.randint(second_key, (NX, NY), -reach_cols, reach_cols + 1)
    rows_index = jnp.arange(NX, dtype=jnp.int32)[:, None] + row_shift
    columns = jnp.arange(NY, dtype=jnp.int32)[None, :] + col_shift
    row_block = jnp.clip(rows_index * REG // NX, 0, REG - 1)
    col_block = jnp.clip(columns * REG // NY, 0, REG - 1)
    return (row_block * REG + col_block).astype(jnp.int32)


def draw_load_currents(key, part):
    rows_index = jnp.arange(NX, dtype=jnp.float32)[:, None]
    rising = 1.0 + 2.0 * rows_index / max(NX - 1, 1)
    normal_part = jnp.clip(jax.random.normal(jax.random.fold_in(key, 5), (NRHS, NX, NY), jnp.float32), -6.0, 6.0)
    return 2.0 * normal_part * rising


def set_ends(entries, own_key, low, largest):
    longest = entries.shape.index(max(entries.shape))
    spots = []
    for shift in (0, 1):
        where = [jax.random.randint(jax.random.fold_in(own_key, axis), (), 0, length) for axis, length in enumerate(entries.shape)]
        where[longest] = (where[longest] + shift) % entries.shape[longest]
        spots.append(tuple(where))
    return entries.at[spots[0]].set(low).at[spots[1]].set(largest)


def steps_of(own_key, dims, pieces, smallest, top_value):
    level, own = 1.0, jax.random.fold_in(own_key, 6)
    for axis_at, parts in pieces:
        steps = jnp.exp(jax.random.uniform(jax.random.fold_in(own, axis_at), (parts,), jnp.float32, smallest / len(pieces), top_value / len(pieces)))
        level = level * jnp.repeat(steps, dims[axis_at] // parts).reshape([-1 if axis == axis_at else 1 for axis in range(len(dims))])
    return level


def setup_inputs(seed: int = 0) -> dict:
    splits = jax.random.split(jax.random.key(seed), 9)
    load_currents = draw_load_currents(jax.random.fold_in(splits[8], 71), 0)
    labels = draw_labels(jax.random.fold_in(splits[8], 71), 0)
    bump_height = jnp.clip(jnp.exp(math.log(2.0) - 1.3862944 * jax.random.uniform(splits[2], (NX, NY), jnp.float32) ** steps_of(splits[2], (NX, NY), ((0, 16), (1, 8)), -0.2, 0.2)), 0.5, 2.0)
    horizontal_class = set_ends(jax.random.randint(splits[3], (NX, NY), 0, NCLS), jax.random.fold_in(splits[3], 1), 0, NCLS - 1).astype(jnp.int32)
    vertical_class = set_ends(jax.random.randint(splits[4], (NX, NY), 0, NCLS), jax.random.fold_in(splits[4], 1), 0, NCLS - 1).astype(jnp.int32)
    pad_class = set_ends(jax.random.randint(splits[5], (NX, NY), 0, NCLS), jax.random.fold_in(splits[5], 1), 0, NCLS - 1).astype(jnp.int32)
    edge_table = jnp.clip(jnp.exp(jax.random.uniform(splits[6], (NCLS,), jnp.float32, math.log(0.5), math.log(4.0))), 0.5, 4.0)
    pad_table = jnp.clip(jnp.exp(jax.random.uniform(splits[7], (NCLS,), jnp.float32, math.log(0.02), math.log(0.5))), 0.02, 0.5)
    return {"load_currents": load_currents, "labels": labels, "bump_height": bump_height, "horizontal_class": horizontal_class, "vertical_class": vertical_class, "pad_class": pad_class, "edge_table": edge_table, "pad_table": pad_table}


precise = lax.Precision.HIGHEST

def link_fields(horizontal_class, vertical_class, edge_table):
    right_link = edge_table[horizontal_class]
    down_link = edge_table[vertical_class]
    columns = lax.broadcasted_iota(jnp.int32, horizontal_class.shape, 1)
    rows_index = lax.broadcasted_iota(jnp.int32, horizontal_class.shape, 0)
    right_link = jnp.where(columns == horizontal_class.shape[1] - 1, 0.0, right_link)
    down_link = jnp.where(rows_index == horizontal_class.shape[0] - 1, 0.0, down_link)
    left_link = jnp.pad(right_link, ((0, 0), (1, 0)))[:, :-1]
    upper_link = jnp.pad(down_link, ((1, 0), (0, 0)))[:-1, :]
    return (right_link, left_link, down_link, upper_link)

def apply_operator(field, coeffs):
    diagonal, right_link, left_link, down_link, upper_link = coeffs
    padded = jnp.pad(field, 1)
    return diagonal * field - right_link * padded[1:-1, 2:] - left_link * padded[1:-1, :-2] - down_link * padded[2:, 1:-1] - upper_link * padded[:-2, 1:-1]

def assemble_coarse(labels, bump_height, coeffs, regions):
    diagonal, right_link, left_link, down_link, upper_link = coeffs
    right_label = jnp.roll(labels, -1, axis=1)
    right_bump = jnp.roll(bump_height, -1, axis=1)
    down_label = jnp.roll(labels, -1, axis=0)
    down_bump = jnp.roll(bump_height, -1, axis=0)
    pair_ids = jnp.concatenate([(labels * regions + labels).reshape(-1), (labels * regions + right_label).reshape(-1), (right_label * regions + labels).reshape(-1), (labels * regions + down_label).reshape(-1), (down_label * regions + labels).reshape(-1)]).astype(jnp.int32)
    across = -(right_link * bump_height * right_bump)
    downward = -(down_link * bump_height * down_bump)
    weights = jnp.concatenate([(diagonal * bump_height * bump_height).reshape(-1), across.reshape(-1), across.reshape(-1), downward.reshape(-1), downward.reshape(-1)])
    summed = jax.ops.segment_sum(weights, pair_ids, num_segments=regions * regions)
    return summed.reshape(regions, regions)

def invert(matrix):
    factor = jnp.linalg.cholesky(matrix)
    identity = jnp.eye(matrix.shape[0], dtype=matrix.dtype)
    lower_solved = lax.linalg.triangular_solve(factor, identity, left_side=True, lower=True)
    return lax.linalg.triangular_solve(factor, lower_solved, left_side=True, lower=True, transpose_a=True)

def solve_single(single_load, labels, bump_height, coeffs, inverse, regions):
    flat_labels = labels.reshape(-1).astype(jnp.int32)
    diagonal = coeffs[0]

    def project(field):
        return jax.ops.segment_sum((bump_height * field).reshape(-1), flat_labels, num_segments=regions)

    def expand(coarse):
        return bump_height * jnp.take(coarse, labels, axis=0)

    def solve_coarse(projected):
        return jnp.dot(projected, inverse, precision=precise)

    def refresh(residual):
        scaled = residual / diagonal
        weighted_norm = jnp.sum(residual * scaled)
        field_image = apply_operator(scaled, coeffs)
        coarse = solve_coarse(project(field_image))
        return (scaled, weighted_norm, field_image, coarse)
    solution = expand(solve_coarse(project(single_load)))
    residual = single_load - apply_operator(solution, coeffs)
    scaled, weighted_norm, field_image, coarse = refresh(residual)
    spread = expand(coarse)
    direction = scaled - spread
    direction_image = field_image - apply_operator(spread, coeffs)
    for iteration in range(ITERS):
        step_size = weighted_norm / jnp.sum(direction * direction_image)
        solution = solution + step_size * direction
        residual = residual - step_size * direction_image
        if iteration + 1 < ITERS:
            scaled, new_norm, field_image, coarse = refresh(residual)
            spread = expand(coarse)
            beta_ratio = new_norm / weighted_norm
            direction = scaled - spread + beta_ratio * direction
            direction_image = field_image - apply_operator(spread, coeffs) + beta_ratio * direction_image
            weighted_norm = new_norm
    return (solution, residual)

def reference(load_currents, labels, bump_height, horizontal_class, vertical_class, pad_class, edge_table, pad_table):
    right_link, left_link, down_link, upper_link = link_fields(horizontal_class, vertical_class, edge_table)
    diagonal = pad_table[pad_class] + right_link + left_link + down_link + upper_link
    coeffs = (diagonal, right_link, left_link, down_link, upper_link)
    regions = REG * REG
    inverse = invert(assemble_coarse(labels, bump_height, coeffs, regions))
    worker = partial(solve_single, labels=labels, bump_height=bump_height, coeffs=coeffs, inverse=inverse, regions=regions)
    solution, residual = lax.map(worker, load_currents)
    return (solution, residual)
```

```python
import jax
import jax.numpy as jnp
from jax import lax
from jax.experimental import pallas as pl
from jax.experimental.pallas import tpu as pltpu
from jax.sharding import Mesh
from jax.sharding import PartitionSpec as P

REG = 16
ROW = ("row_0", "row_1")
COL = ("col_0", "col_1")
F32 = jnp.float32
precise = lax.Precision.HIGHEST

LAB, BUMP, RIGHT, DOWN, PAD = 32, 33, 34, 35, 36
SUB = 40
HALO = 3
EXT = 134
GROUPS = 9
ORDER = (1, 3, 5, 7, 9, 11, 13, 15, 2, 6, 10, 14, 4, 12, 8, 0)
POS = tuple(ORDER.index(p) for p in range(16))
NT = (((1,), (1,)), ((), ()))
NN = (((1,), (0,)), ((), ()))
TN = (((0,), (0,)), ((), ()))
whole = pl.BlockSpec(memory_space=pltpu.VMEM)
scalars = pl.BlockSpec(memory_space=pltpu.SMEM)


def dot(a, b, dims=NN):
    return lax.dot_general(a, b, dims, precision=precise, preferred_element_type=F32)


def lanes(shape):
    return lax.broadcasted_iota(jnp.int32, shape, len(shape) - 1)


def roll(x, shift, axis=1):
    return pltpu.roll(x, shift, axis)


def pack_kernel(x_ref, top_ref, bottom_ref, out_ref):
    lane = lanes((SUB, 128))
    for g in range(GROUPS):
        acc = jnp.zeros((SUB, 128), F32)
        for s in range(16):
            r = 16 * g - 8 + s
            if r < -HALO or r >= 128 + HALO:
                continue
            if r < 0:
                row = top_ref[r + HALO]
            elif r < 128:
                row = x_ref[r]
            else:
                row = bottom_ref[r - 128]
            acc = jnp.where(lane // 8 == s, roll(row, (8 * s + 3) % 128), acc)
        out_ref[g] = acc


def fields_kernel(
    place_ref, x_ref, top_ref, bottom_ref, own_ref, left_ref, right_ref,
    first_ref, second_ref, basis_ref, coef_ref, out_ref,
    xe, sz_o, sz_s, y0_o, y0_s, y1_s, sc, zs, y0, y1, gram,
):
    pr, pc = place_ref[0], place_ref[1]
    lane1 = lanes((1, 128))
    lane16 = lanes((16, 128))
    lane48 = lanes((48, 128))

    for i in range(HALO):
        xe[i] = top_ref[i]
        xe[EXT - HALO + i] = bottom_ref[i]

    def copy_rows(i, _):
        xe[i + HALO] = x_ref[i]
        return 0

    lax.fori_loop(0, 128, copy_rows, 0, unroll=4)

    slot = lax.broadcasted_iota(jnp.int32, (16, 128), 0)
    region_row = pr - 1 + slot // 4
    region_col = 2 * pc - 1 + slot % 4
    inside = (slot < 12) & (region_row >= 0) & (region_row < REG) & (region_col >= 0) & (region_col < REG)
    window = jnp.where(inside, region_row * REG + region_col, -1).astype(F32)

    def mixed(g):
        j = lanes((SUB, 128)) % 8
        return jnp.where(j < 3, left_ref[g], right_ref[g])

    def pair_left(o, s, lane):
        j = lane % 8
        return roll(jnp.where(j == 2, s, o), 1), roll(jnp.where(j == 2, o, s), 1)

    def pair_right(o, s, lane):
        j = lane % 8
        return roll(jnp.where(j == 3, s, o), 127), roll(jnp.where(j == 3, o, s), 127)

    def above(before, here, lane):
        return roll(jnp.where(lane >= 120, before, here), 8)

    def below(here, after, lane):
        return roll(jnp.where(lane < 8, after, here), 120)

    for g in range(GROUPS):
        o_row, s_row = own_ref[g], mixed(g)
        o_before = own_ref[g - 1] if g else jnp.zeros((SUB, 128), F32)
        s_before = mixed(g - 1) if g else jnp.zeros((SUB, 128), F32)
        lefts = pair_left(o_row[RIGHT : RIGHT + 1], s_row[RIGHT : RIGHT + 1], lane1)
        for side, (row, before, ll) in enumerate(
            ((o_row, o_before, lefts[0]), (s_row, s_before, lefts[1]))
        ):
            rl, dl = row[RIGHT : RIGHT + 1], row[DOWN : DOWN + 1]
            ul = above(before[DOWN : DOWN + 1], dl, lane1)
            diag = row[PAD : PAD + 1] + rl + ll + dl + ul
            inv = jnp.where(diag > 0, 1.0 / diag, 0.0)
            for n, value in enumerate((diag, rl, ll, dl, ul, inv)):
                sc[side, g, n : n + 1] = value
            z = jnp.where(row[LAB : LAB + 1] == window, row[BUMP : BUMP + 1], 0.0)
            (sz_s if side else sz_o)[g] = z

    def strip_image(ref_o, ref_s, g, lane, sides):
        shape = lane.shape
        o, s = ref_o[g], ref_s[g]
        lefts, rights = pair_left(o, s, lane), pair_right(o, s, lane)
        done = []
        for side in sides:
            ref, here = (ref_s, s) if side else (ref_o, o)
            zero = jnp.zeros(shape, F32)
            up = above(ref[g - 1] if g else zero, here, lane)
            down = below(here, ref[g + 1] if g + 1 < GROUPS else zero, lane)
            c = [sc[side, g, n : n + 1] for n in range(5)]
            done.append(c[0] * here - c[1] * rights[side] - c[2] * lefts[side] - c[3] * down - c[4] * up)
        return done

    for g in range(GROUPS):
        w = strip_image(sz_o, sz_s, g, lane16, (0, 1))
        loads = (own_ref[g], mixed(g))
        for side, ref in ((0, y0_o), (1, y0_s)):
            inv = sc[side, g, 5:6]
            ref[g, 0:32] = inv * loads[side][0:32]
            ref[g, 32:48] = inv * w[side]
    for g in range(GROUPS):
        (u,) = strip_image(y0_o, y0_s, g, lane48, (1,))
        y1_s[g] = sc[1, g, 5:6] * u

    def beside(i):
        k = i + 5
        return k // 16, 125 - 8 * (k % 16)

    def coefficients(i, _):
        g, shift = beside(i)
        row = xe[i, 32:40]
        other = jnp.where(lanes((8, 128)) % 8 < 3, left_ref[g, 32:40], right_ref[g, 32:40])
        other = roll(other, shift)
        rl, dl = row[2:3], row[3:4]
        ll = roll(jnp.where(lane1 == 127, other[2:3], rl), 1)
        ul = xe[jnp.maximum(i - 1, 0), DOWN : DOWN + 1]
        diag = row[4:5] + rl + ll + dl + ul
        inv = jnp.where(diag > 0, 1.0 / diag, 0.0)
        coef_ref[i] = jnp.concatenate([diag, rl, ll, dl, ul, inv, inv, inv], axis=0)
        zs[i] = jnp.where(row[0:1] == window, row[1:2], 0.0)
        return 0

    lax.fori_loop(0, EXT, coefficients, 0, unroll=2)

    def image(ref, strip, i, lane):
        g, shift = beside(i)
        here = ref[i]
        other = roll(strip[g], shift)
        left = roll(jnp.where(lane == 127, other, here), 1)
        right = roll(jnp.where(lane == 0, other, here), 127)
        c = coef_ref[i]
        return (
            c[0:1] * here
            - c[1:2] * right
            - c[2:3] * left
            - c[3:4] * ref[i + 1]
            - c[4:5] * ref[i - 1]
        ), c[5:6]

    def first_image(i, _):
        w, inv = image(zs, sz_s, i, lane16)
        basis_ref[i, 0:16] = zs[i]
        basis_ref[i, 16:32] = w
        y0[i, 0:32] = inv * xe[i, 0:32]
        y0[i, 32:48] = inv * w
        return 0

    lax.fori_loop(1, EXT - 1, first_image, 0, unroll=2)

    def second_image(i, _):
        f1, inv = image(y0, y0_s, i, lane48)
        first_ref[i] = f1
        y1[i] = inv * f1
        return 0

    lax.fori_loop(2, EXT - 2, second_image, 0, unroll=2)

    gram[...] = jnp.zeros((48, 256), F32)

    def third_image(i, sums):
        f2, _ = image(y1, y1_s, i, lane48)
        second_ref[i - HALO] = f2
        b, f1, w = xe[i, 0:32], first_ref[i], basis_ref[i, 16:32]
        y0b, y1u = y0[i, 0:32], y1[i, 0:32]
        left = jnp.concatenate([zs[i], y0[i, 32:48], y1[i, 32:48]], axis=0)
        every = jnp.concatenate([b, w, f1, f2], axis=0)
        gram[:, 0:144] += dot(left, every, NT)
        u, uu = f1[0:32], f2[0:32]
        return (sums[0] + y0b * b, sums[1] + y0b * u, sums[2] + y1u * u, sums[3] + y1u * uu)

    zero = jnp.zeros((32, 128), F32)
    sums = lax.fori_loop(HALO, EXT - HALO, third_image, (zero, zero, zero, zero))

    a0, a1 = gram[:, 0:128], gram[:, 128:256]
    half0 = a0[16:32]
    half1 = jnp.where(lane16 < 16, a1[16:32], 0.0)
    half1 = jnp.where((lane16 >= 16) & (lane16 < 64), roll(a0[0:16], 16), half1)
    half1 = jnp.where((lane16 >= 64) & (lane16 < 96), roll(a0[32:48], 96), half1)
    half1 = jnp.where((lane16 >= 96) & (lane16 < 112), roll(a1[32:48], 96), half1)

    def relative(x, zones):
        zone = jnp.zeros((16, 128), jnp.bool_)
        for z in zones:
            zone = zone | ((lane16 >= z) & (lane16 < z + 16))
        kept = jnp.where(zone, x, 0.0)
        moved = jnp.zeros((16, 128), F32)
        for s in range(12):
            moved = jnp.where(slot == s, roll(kept, (5 - s) % 128), moved)
        return jnp.where(zone, moved, x)

    half0 = relative(half0, (32, 80))
    half1 = relative(half1, (0, 48, 96))
    eye = lax.broadcasted_iota(jnp.int32, (32, 128), 0)
    for n, total in enumerate(sums):
        column = jnp.sum(total, axis=1, keepdims=True)
        for part in range(2):
            spread = jnp.where(lanes((32, 128)) - 112 == eye - 16 * part, column, 0.0)
            line = jnp.sum(spread, axis=0, keepdims=True)
            half1 = jnp.where((slot == 2 * n + part) & (lane16 >= 112), line, half1)
    out_ref[0:12] = half0[0:12]
    out_ref[12:24] = half1[0:12]


def combine_kernel(in_ref, out_ref):
    c = lax.broadcasted_iota(jnp.int32, (8, 128), 0)
    lane = lanes((8, 128))
    for half in range(2):
        for dr in range(3):
            at = [in_ref[pl.ds(half * 12 + dr * 4 + dq, 8, stride=24), :] for dq in range(4)]
            even = at[1] + jnp.where(c >= 1, roll(at[3], 1, 0), 0.0)
            odd = at[2] + jnp.where(c < 7, roll(at[0], 7, 0), 0.0)
            if half:
                even = jnp.where(lane < 112, even, 0.0)
                odd = jnp.where(lane < 112, odd, 0.0)
                if dr == 1:
                    for s in range(8):
                        line = jnp.sum(in_ref[pl.ds(12 + s, 8, stride=24), :], axis=0, keepdims=True)
                        even = jnp.where((c == s) & (lane >= 112), line, even)
            base = half * 48 + dr * 8
            out_ref[base : base + 8] = even
            out_ref[base + 24 : base + 32] = odd


def batched_inverse(a, lane, row):
    base = lane - lane % 16
    for k in range(16):
        at_k = lane % 16 == k
        column = jnp.take_along_axis(a, base + k, axis=1)
        pivot = column[k : k + 1]
        line = jnp.where(at_k[0:1], 1.0, a[k : k + 1]) / pivot
        a = jnp.where(row == k, line, jnp.where(at_k, 0.0, a) - column * line)
    return a


def block_inverse(matrix, low, high):
    lane = lanes((16, 128))
    row = lax.broadcasted_iota(jnp.int32, (16, 128), 0)
    compact = jnp.where(lane % 16 == row, 1.0, 0.0)
    for n in range(low // 16, high // 16):
        compact = jnp.where(lane // 16 == n, matrix[16 * n : 16 * n + 16], compact)
    compact = batched_inverse(compact, lane, row)
    parts = []
    for n in range(8):
        active = low <= 16 * n < high
        parts.append(jnp.where(lane // 16 == n, compact, 0.0) if active else jnp.zeros((16, 128), F32))
    return jnp.concatenate(parts, axis=0)


def coarse_kernel(place_ref, in_ref, out_ref, g0, g1, e, ei, va, vb, mw, mt, ms, mz):
    pr, pc = place_ref[0], place_ref[1]
    lane8 = lanes((8, 128))
    sub8 = lax.broadcasted_iota(jnp.int32, (8, 128), 0)

    def at(p, par):
        return POS[p] * 16 + par * 8

    for half, ref in ((0, g0), (1, g1)):
        for par in range(2):
            for p in range(16):
                total = None
                for dr in range(3):
                    r = p + 1 - dr
                    if 0 <= r < 16:
                        base = half * 48 + par * 24 + dr * 8
                        piece = in_ref[r, base : base + 8]
                        total = piece if total is None else total + piece
                ref[at(p, par) : at(p, par) + 8] = total

    tally = g1[at(0, 0) : at(0, 0) + 8]
    for p in range(1, 16):
        tally = tally + g1[at(p, 0) : at(p, 0) + 8]

    def total_of(n):
        low = roll(tally[2 * n : 2 * n + 1], 16)
        high = roll(tally[2 * n + 1 : 2 * n + 2], 32)
        return jnp.where(lanes((1, 128)) < 16, low, high)

    bb, bu, uu, uuu = (total_of(n) for n in range(4))

    for p in range(16):
        for par in range(2):
            tile = g1[at(p, par) : at(p, par) + 8]
            halves = [jnp.zeros((8, 128), F32), jnp.zeros((8, 128), F32)]
            for dp in (-1, 0, 1):
                if not 0 <= p + dp < 16:
                    continue
                for dq in (-1, 0, 1):
                    l = 48 + 5 + 4 * dp + dq
                    other = par if dq == 0 else 1 - par
                    step = 0 if dq == 0 else ((dq - 1) // 2 if par == 0 else (dq + 1) // 2)
                    target = at(p + dp, other)
                    h, off = target // 128, target % 128
                    hit = (lane8 - off == sub8 + step) & (sub8 + step >= 0) & (sub8 + step < 8)
                    value = jnp.broadcast_to(tile[:, l : l + 1], (8, 128))
                    halves[h] = jnp.where(hit, value, halves[h])
            e[at(p, par) : at(p, par) + 8, 0:128] = halves[0]
            e[at(p, par) : at(p, par) + 8, 128:256] = halves[1]

    lane = lanes((128, 128))
    row = lax.broadcasted_iota(jnp.int32, (128, 128), 0)
    outer = block_inverse(e[0:128, 0:128], 0, 128)
    across = dot(outer, e[0:128, 128:256])
    schur = e[128:256, 128:256] - dot(e[128:256, 0:128], across)
    steps = []
    for low, high in ((0, 64), (64, 96), (96, 112)):
        inv = block_inverse(schur, low, high)
        link = jnp.where((row >= low) & (row < high) & (lane >= high), schur, 0.0)
        x = dot(inv, link)
        keep = jnp.where((row >= high) & (lane >= high), schur, 0.0)
        schur = keep - dot(link, x, TN)
        steps.append((inv, jnp.where((row == lane) & (row >= high), 1.0, 0.0) - x))
    inner = block_inverse(schur, 112, 128)
    for inv, y in reversed(steps):
        inner = inv + dot(dot(y, inner), y, NT)
    half = dot(across, inner)
    ei[0:128, 0:128] = outer + dot(half, across, NT)
    ei[0:128, 128:256] = -half
    ei[128:256, 0:128] = -half.T
    ei[128:256, 128:256] = inner

    def solve(z):
        return dot(ei[...], z)

    def apply(ref, zone, v_ref):
        sides = {}
        for p in range(16):
            even, odd = v_ref[at(p, 0) : at(p, 0) + 8], v_ref[at(p, 1) : at(p, 1) + 8]
            sides[p, 0] = (roll(odd, 1, 0), even, odd)
            sides[p, 1] = (even, odd, roll(even, 7, 0))
        tiles = {}
        for p in range(16):
            for par in range(2):
                tile = ref[at(p, par) : at(p, par) + 8]
                total = None
                for dp in (-1, 0, 1):
                    if not 0 <= p + dp < 16:
                        continue
                    for n in range(3):
                        l = zone + 5 + 4 * dp + n - 1
                        term = tile[:, l : l + 1] * sides[p + dp, par][n]
                        total = term if total is None else total + term
                tiles[POS[p] * 2 + par] = total
        return jnp.concatenate([tiles[n] for n in range(32)], axis=0)

    def inner_product(a, b):
        return jnp.sum(a * b, axis=0, keepdims=True)

    wb = g0[...]
    wu = roll(g0[...], 80)
    wuu = roll(g0[...], 32)
    zb = roll(g1[...], 112)
    tuu = roll(g1[...], 64)
    c0 = solve(zb)
    va[...] = c0
    f_c = apply(g0, 32, va)
    g_c = apply(g0, 80, va)
    h_c = apply(g1, 0, va)
    k_c = apply(g1, 96, va)
    grad0 = wb - f_c
    k0 = solve(grad0)
    vb[...] = k0
    f_k = apply(g0, 32, vb)
    g_k = apply(g0, 80, vb)
    rho0 = bb - 2.0 * inner_product(c0, wb) + inner_product(c0, f_c)
    energy0 = bu - 2.0 * inner_product(c0, wu) + inner_product(c0, g_c)
    curve0 = energy0 - inner_product(k0, grad0)
    a0 = rho0 / curve0
    e1 = c0 - a0 * k0
    f_e = f_c - a0 * f_k
    g_e = g_c - a0 * g_k
    grad1 = wb - f_e + a0 * (g_c - wu)
    k1 = solve(grad1)

    def second_norm(m0, m1, m2, v0, v1, v2, e_image, c_image, last):
        own = m0 - 2.0 * inner_product(e1, v0) + inner_product(e1, e_image)
        mixed = m1 - inner_product(c0, v1) - inner_product(e1, v1) + inner_product(e1, c_image)
        far = m2 - 2.0 * inner_product(c0, v2) + inner_product(c0, last)
        return own - 2.0 * a0 * mixed + a0 * a0 * far

    rho1 = second_norm(bb, bu, uu, wb, wu, wuu, f_e, g_c, h_c)
    energy1 = second_norm(bu, uu, uuu, wu, wuu, tuu, g_e, h_c, k_c)
    beta = rho1 / rho0
    cross = inner_product(e1, wu)
    s1q0 = (
        bu
        - inner_product(c0, wu)
        - cross
        + inner_product(e1, g_c)
        - a0 * (uu - 2.0 * inner_product(c0, wuu) + inner_product(c0, h_c))
        - inner_product(k0, grad1)
    )
    curve1 = energy1 - inner_product(k1, grad1) + 2.0 * beta * s1q0 + beta * beta * curve0
    a1 = rho1 / curve1

    ab = a1 * beta
    w_res = a1 * k1 + ab * k0 - e1
    t_res = (a0 + ab) * c0 + a1 * e1
    s_res = -(a1 * a0) * c0
    w_sol = -(a0 + ab) * c0 - a1 * e1
    t_sol = (a1 * a0) * c0
    z_sol = c0 - (a0 + ab) * k0 - a1 * k1
    big = lanes((256, 128))

    def joined(first, second):
        return jnp.where(big < 32, first, jnp.where(big < 64, roll(second, 32), 0.0))

    found = (
        (mz, jnp.where((big >= 64) & (big < 96), roll(z_sol, 64), 0.0)),
        (mw, joined(w_res, w_sol)),
        (mt, joined(t_res, t_sol)),
        (ms, jnp.where(big < 32, s_res, 0.0)),
    )
    for ref, value in found:
        for p in range(16):
            ref[16 * p : 16 * p + 16] = value[16 * POS[p] : 16 * POS[p] + 16]
    for n, (ref, _) in enumerate(found):
        for dr in range(3):
            p = jnp.clip(pr - 1 + dr, 0, 15)
            for dq in range(4):
                par = (dq + 1) % 2
                c = jnp.clip(pc - 1 + (dq + 1) // 2, 0, 7)
                k = 16 * n + 4 * dr + dq
                out_ref[k : k + 1] = ref[pl.ds(p * 16 + par * 8 + c, 1), :]
        out_ref[16 * n + 12 : 16 * n + 16] = jnp.zeros((4, 128), F32)
    out_ref[64:65] = -a0 - a1 - ab
    out_ref[65:66] = a1 * a0
    out_ref[66:67] = a0 + ab + a1
    out_ref[67:68] = -(a1 * a0)
    out_ref[68:72] = jnp.zeros((4, 128), F32)


def outputs_kernel(x_ref, first_ref, second_ref, basis_ref, coef_ref, m_ref, sol_ref, res_ref):
    m = jnp.concatenate([m_ref[...], jnp.zeros((56, 128), F32)], axis=0).T
    left = m[0:96, 0:64]
    shape = (32, 128)
    p1, p2, p3, p4 = (jnp.broadcast_to(m[0:32, 64 + n : 65 + n], shape) for n in range(4))

    def step(r, _):
        i = r + HALO
        b, f1, f2 = x_ref[r, 0:32], first_ref[i], second_ref[r]
        u, uu = f1[0:32], f2[0:32]
        rows = jnp.concatenate([basis_ref[i], f1[32:48], f2[32:48]], axis=0)
        d = dot(left, rows)
        inv = coef_ref[i, 5:6]
        res_ref[r] = b + p1 * u + p2 * uu + d[0:32]
        sol_ref[r] = inv * (p3 * b + p4 * u + d[32:64]) + d[64:96]
        return 0

    lax.fori_loop(0, 128, step, 0, unroll=2)


def from_everyone(value, axis):
    count = lax.axis_size(axis)
    return lax.all_to_all(jnp.broadcast_to(value[None], (count, *value.shape)), axis, 0, 0, tiled=True)


def lookup(entries, classes):
    levels = lax.broadcasted_iota(jnp.int32, (entries.shape[0],) + classes.shape, 0)
    return jnp.sum(jnp.where(classes[None] == levels, entries[:, None, None], 0.0), axis=0)


def shape_of(*dims):
    return jax.ShapeDtypeStruct(dims, F32)


def vmem(*dims):
    return pltpu.VMEM(dims, F32)


def body(load_currents, labels, bump_height, horizontal_class, vertical_class, pad_class, edge_table, pad_table):
    pr, pc = lax.axis_index(ROW), lax.axis_index(COL)
    rows, cols = lax.axis_size(ROW), lax.axis_size(COL)
    place = jnp.stack([pr, pc]).astype(jnp.int32)
    row_ids = lax.broadcasted_iota(jnp.int32, labels.shape, 0)
    col_ids = lax.broadcasted_iota(jnp.int32, labels.shape, 1)
    right_link = jnp.where((col_ids == 127) & (pc == cols - 1), 0.0, lookup(edge_table, horizontal_class))
    down_link = jnp.where((row_ids == 127) & (pr == rows - 1), 0.0, lookup(edge_table, vertical_class))
    pad = lookup(pad_table, pad_class)
    zero = jnp.zeros_like(pad)
    params = jnp.stack(
        [labels.astype(F32), bump_height, right_link, down_link, pad, zero, zero, zero], axis=1
    )
    x = jnp.concatenate([jnp.transpose(load_currents, (1, 0, 2)), params], axis=1)
    down = [(i, i + 1) for i in range(rows - 1)]
    top = lax.ppermute(x[-HALO:], ROW, down)
    bottom = lax.ppermute(x[:HALO], ROW, [(b, a) for a, b in down])
    own = pl.pallas_call(
        pack_kernel, out_shape=shape_of(GROUPS, SUB, 128), in_specs=[whole] * 3, out_specs=whole
    )(x, top, bottom)
    right = [(i, i + 1) for i in range(cols - 1)]
    beside_left = lax.ppermute(own, COL, right)
    beside_right = lax.ppermute(own, COL, [(b, a) for a, b in right])
    first, second, basis, coef, payload = pl.pallas_call(
        fields_kernel,
        out_shape=(
            shape_of(EXT, 48, 128),
            shape_of(128, 48, 128),
            shape_of(EXT, 32, 128),
            shape_of(EXT, 8, 128),
            shape_of(24, 128),
        ),
        in_specs=[scalars] + [whole] * 6,
        out_specs=(whole,) * 5,
        scratch_shapes=[
            vmem(EXT, SUB, 128),
            vmem(GROUPS, 16, 128),
            vmem(GROUPS, 16, 128),
            vmem(GROUPS, 48, 128),
            vmem(GROUPS, 48, 128),
            vmem(GROUPS, 48, 128),
            vmem(2, GROUPS, 8, 128),
            vmem(EXT, 16, 128),
            vmem(EXT, 48, 128),
            vmem(EXT, 48, 128),
            vmem(48, 256),
        ],
    )(place, x, top, bottom, own, beside_left, beside_right)
    in_row = from_everyone(payload, COL).reshape(-1, 128)
    combined = pl.pallas_call(
        combine_kernel, out_shape=shape_of(96, 128), in_specs=[whole], out_specs=whole
    )(in_row)
    everything = from_everyone(combined, ROW)
    matrix = pl.pallas_call(
        coarse_kernel,
        out_shape=shape_of(72, 128),
        in_specs=[scalars, whole],
        out_specs=whole,
        scratch_shapes=[vmem(256, 128), vmem(256, 128), vmem(256, 256), vmem(256, 256)]
        + [vmem(256, 128)] * 6,
    )(place, everything)
    solution, residual = pl.pallas_call(
        outputs_kernel,
        out_shape=(shape_of(128, 32, 128), shape_of(128, 32, 128)),
        in_specs=[whole] * 6,
        out_specs=(whole, whole),
    )(x, first, second, basis, coef, matrix)
    return jnp.transpose(solution, (1, 0, 2)), jnp.transpose(residual, (1, 0, 2))


def solution(mesh):
    finer = Mesh(mesh.devices.reshape(4, 4, 4, 2), ("row_0", "row_1", "col_0", "col_1"))
    grid = P(ROW, COL)
    return jax.shard_map(
        body,
        mesh=finer,
        in_specs=(P(None, ROW, COL), grid, grid, grid, grid, grid, P(), P()),
        out_specs=(P(None, ROW, COL), P(None, ROW, COL)),
        check_vma=False,
    )
```

```python
import jax
import jax.numpy as jnp
from jax import lax
from jax.experimental import pallas as pl
from jax.experimental.pallas import tpu as pltpu
from jax.sharding import Mesh
from jax.sharding import PartitionSpec as P

REG = 16
ROW = ("row_0", "row_1")
COL = ("col_0", "col_1")
F32 = jnp.float32
precise = lax.Precision.HIGHEST

LAB, BUMP, RIGHT, DOWN, PAD = 32, 33, 34, 35, 36
SUB = 40
HALO = 3
GROUPS = 9
ORDER = (1, 3, 5, 7, 9, 11, 13, 15, 2, 6, 10, 14, 4, 12, 8, 0)
POS = tuple(ORDER.index(p) for p in range(16))
NT = (((1,), (1,)), ((), ()))
NN = (((1,), (0,)), ((), ()))
TN = (((0,), (0,)), ((), ()))
whole = pl.BlockSpec(memory_space=pltpu.VMEM)
scalars = pl.BlockSpec(memory_space=pltpu.SMEM)


def dot(a, b, dims=NN):
    return lax.dot_general(a, b, dims, precision=precise, preferred_element_type=F32)


def parts_of(x, count):
    parts = []
    for n in range(count):
        parts.append(x.astype(jnp.bfloat16))
        if n + 1 < count:
            x = x - parts[-1].astype(F32)
    return parts


def fast_dot(a, b, dims=NN):
    return lax.dot_general(a, b, dims, preferred_element_type=F32)


def lanes(shape):
    return lax.broadcasted_iota(jnp.int32, shape, len(shape) - 1)


def roll(x, shift, axis=1):
    return pltpu.roll(x, shift, axis)


def prepare_kernel(
    place_ref, edge_ref, pad_ref, load_ref, label_ref, bump_ref, across_ref, down_ref, pad_class_ref,
    grid_ref, first_ref,
):
    pr, pc = place_ref[0], place_ref[1]
    shape = (128, 128)
    row, lane = lax.broadcasted_iota(jnp.int32, shape, 0), lanes(shape)

    def lookup(table, classes):
        found = jnp.zeros(shape, F32)
        for n in range(8):
            found = jnp.where(classes == n, table[n], found)
        return found

    right = lookup(edge_ref, across_ref[...])
    down = lookup(edge_ref, down_ref[...])
    grid_ref[0:128] = label_ref[...].astype(F32)
    grid_ref[128:256] = bump_ref[...]
    grid_ref[256:384] = jnp.where((lane == 127) & (pc == 7), 0.0, right)
    grid_ref[384:512] = jnp.where((row == 127) & (pr == 15), 0.0, down)
    grid_ref[512:640] = lookup(pad_ref, pad_class_ref[...])
    grid_ref[640:1024] = jnp.zeros((384, 128), F32)
    for n in range(HALO):
        first_ref[n, 0:32] = load_ref[pl.ds(n, 32, stride=128), :]
        first_ref[n, 32:40] = grid_ref[pl.ds(n, 8, stride=128), :]


def pack_kernel(load_ref, grid_ref, rows_ref, own_ref, last_ref):
    lane = lanes((32, 128)) // 8

    def group(g, slots):
        loads, rest = jnp.zeros((32, 128), F32), jnp.zeros((8, 128), F32)
        for s in slots:
            r = 16 * g - 8 + s
            b = load_ref[pl.ds(r, 32, stride=128), :]
            rows_ref[r] = b
            loads = jnp.where(lane == s, roll(b, (8 * s + 3) % 128), loads)
            rest = jnp.where(lane[0:8] == s, roll(grid_ref[pl.ds(r, 8, stride=128), :], (8 * s + 3) % 128), rest)
        own_ref[g, 0:32] = loads
        own_ref[g, 32:40] = rest

    group(0, range(8, 16))
    group(8, range(8))

    def step(g, _):
        group(g, range(16))
        return 0

    lax.fori_loop(1, 8, step, 0)
    for n in range(HALO):
        r = 128 - HALO + n
        last_ref[n, 0:32] = rows_ref[r]
        last_ref[n, 32:40] = grid_ref[pl.ds(r, 8, stride=128), :]


def corner_kernel(own_ref, top_ref, bottom_ref, out_ref):
    lane = lanes((SUB, 128)) // 8
    for g in range(GROUPS):
        out_ref[g] = own_ref[g]
    start, end = own_ref[0], own_ref[8]
    for n in range(HALO):
        s = 8 - HALO + n
        start = jnp.where(lane == s, roll(top_ref[n], (8 * s + 3) % 128), start)
        s = 8 + n
        end = jnp.where(lane == s, roll(bottom_ref[n], (8 * s + 3) % 128), end)
    out_ref[0] = start
    out_ref[8] = end


def fields_kernel(
    place_ref, rows_ref, grid_ref, top_ref, bottom_ref, own_ref, left_ref, right_ref,
    first_ref, second_ref, w_ref, coef_ref, out_ref,
    ext, sz_o, sz_s, y0_o, y0_s, y1_s, sc, y0, y1, gram,
):
    pr, pc = place_ref[0], place_ref[1]
    lane1 = lanes((1, 128))
    lane16 = lanes((16, 128))
    lane48 = lanes((48, 128))

    for n in range(5):
        ext[n, 0:16] = jnp.zeros((16, 128), F32)
        ext[n, 16:144] = grid_ref[128 * n : 128 * n + 128]
        ext[n, 144:160] = jnp.zeros((16, 128), F32)
        for k in range(HALO):
            ext[n, 16 - HALO + k : 17 - HALO + k] = top_ref[k, 32 + n : 33 + n]
            ext[n, 144 + k : 145 + k] = bottom_ref[k, 32 + n : 33 + n]

    slot = lax.broadcasted_iota(jnp.int32, (16, 128), 0)
    region_row = pr - 1 + slot // 4
    region_col = 2 * pc - 1 + slot % 4
    inside = (slot < 12) & (region_row >= 0) & (region_row < REG) & (region_col >= 0) & (region_col < REG)
    window = jnp.where(inside, region_row * REG + region_col, -1).astype(F32)

    def mixed(g):
        j = lanes((SUB, 128)) % 8
        return jnp.where(j < 3, left_ref[g], right_ref[g])

    def pair_left(o, s, lane):
        j = lane % 8
        return roll(jnp.where(j == 2, s, o), 1), roll(jnp.where(j == 2, o, s), 1)

    def pair_right(o, s, lane):
        j = lane % 8
        return roll(jnp.where(j == 3, s, o), 127), roll(jnp.where(j == 3, o, s), 127)

    def above(before, here, lane):
        return roll(jnp.where(lane >= 120, before, here), 8)

    def below(here, after, lane):
        return roll(jnp.where(lane < 8, after, here), 120)

    for g in range(GROUPS):
        o_row, s_row = own_ref[g], mixed(g)
        o_before = own_ref[g - 1] if g else jnp.zeros((SUB, 128), F32)
        s_before = mixed(g - 1) if g else jnp.zeros((SUB, 128), F32)
        lefts = pair_left(o_row[RIGHT : RIGHT + 1], s_row[RIGHT : RIGHT + 1], lane1)
        for side, (row, before, ll) in enumerate(
            ((o_row, o_before, lefts[0]), (s_row, s_before, lefts[1]))
        ):
            rl, dl = row[RIGHT : RIGHT + 1], row[DOWN : DOWN + 1]
            ul = above(before[DOWN : DOWN + 1], dl, lane1)
            diag = row[PAD : PAD + 1] + rl + ll + dl + ul
            inv = jnp.where(diag > 0, 1.0 / diag, 0.0)
            for n, value in enumerate((diag, rl, ll, dl, ul, inv)):
                sc[side, g, n : n + 1] = value
            z = jnp.where(row[LAB : LAB + 1] == window, row[BUMP : BUMP + 1], 0.0)
            (sz_s if side else sz_o)[g] = z

        at = 16 * g + 8
        beside = jnp.zeros((16, 128), F32)
        for s in range(16):
            beside = jnp.where(slot == s, roll(s_row[RIGHT : RIGHT + 1], 125 - 8 * s), beside)
        rl, dl = ext[2, at : at + 16], ext[3, at : at + 16]
        ll = roll(jnp.where(lane16 == 127, beside, rl), 1)
        ul = ext[3, at - 1 : at + 15]
        diag = ext[4, at : at + 16] + rl + ll + dl + ul
        inv = jnp.where(diag > 0, 1.0 / diag, 0.0)
        for n, value in enumerate((diag, rl, ll, dl, ul, inv)):
            coef_ref[n, at : at + 16] = value

    def strip_image(ref_o, ref_s, g, lane, sides):
        shape = lane.shape
        o, s = ref_o[g], ref_s[g]
        lefts, rights = pair_left(o, s, lane), pair_right(o, s, lane)
        done = []
        for side in sides:
            ref, here = (ref_s, s) if side else (ref_o, o)
            zero = jnp.zeros(shape, F32)
            up = above(ref[g - 1] if g else zero, here, lane)
            down = below(here, ref[g + 1] if g + 1 < GROUPS else zero, lane)
            c = [sc[side, g, n : n + 1] for n in range(5)]
            done.append(c[0] * here - c[1] * rights[side] - c[2] * lefts[side] - c[3] * down - c[4] * up)
        return done

    for g in range(GROUPS):
        w = strip_image(sz_o, sz_s, g, lane16, (0, 1))
        loads = (own_ref[g], mixed(g))
        for side, ref in ((0, y0_o), (1, y0_s)):
            inv = sc[side, g, 5:6]
            ref[g, 0:32] = inv * loads[side][0:32]
            ref[g, 32:48] = inv * w[side]
    for g in range(GROUPS):
        (u,) = strip_image(y0_o, y0_s, g, lane48, (1,))
        y1_s[g] = sc[1, g, 5:6] * u

    def passes(work, low, high):
        for s in range(16):
            if s - 8 >= low:
                work(0, s)

        def step(g, _):
            for s in range(16):
                work(g, s)
            return 0

        lax.fori_loop(1, 8, step, 0)
        for s in range(16):
            if 120 + s < high:
                work(8, s)

    def owned(g, s):
        return not isinstance(g, int) or 0 <= 16 * g - 8 + s < 128

    def coef(n, g, s):
        return coef_ref[n, pl.ds(16 * g + 8 + s, 1), :]

    def image(here, up, down, strip, g, s, lane):
        other = roll(strip[g], 125 - 8 * s)
        left = roll(jnp.where(lane == 127, other, here), 1)
        right = roll(jnp.where(lane == 0, other, here), 127)
        return (
            coef(0, g, s) * here
            - coef(1, g, s) * right
            - coef(2, g, s) * left
            - coef(3, g, s) * down
            - coef(4, g, s) * up
        )

    def basis(j):
        return jnp.where(ext[0, pl.ds(j, 1), :] == window, ext[1, pl.ds(j, 1), :], 0.0)

    def first_image(g, s):
        r, j = 16 * g - 8 + s, 16 * g + 8 + s
        w = image(basis(j), basis(j - 1), basis(j + 1), sz_s, g, s, lane16)
        if owned(g, s):
            b = rows_ref[r]
            w_ref[r] = w
        else:
            b = top_ref[r + HALO, 0:32] if r < 0 else bottom_ref[r - 128, 0:32]
        inv = coef(5, g, s)
        y0[16 * g + s, 0:32] = inv * b
        y0[16 * g + s, 32:48] = inv * w

    passes(first_image, -2, 130)

    def second_image(g, s):
        i = 16 * g + s
        f1 = image(y0[i], y0[i - 1], y0[i + 1], y0_s, g, s, lane48)
        if owned(g, s):
            first_ref[16 * g - 8 + s] = f1
        y1[i] = coef(5, g, s) * f1

    passes(second_image, -1, 129)

    def third_image(g, s):
        i = 16 * g + s
        second_ref[16 * g - 8 + s] = image(y1[i], y1[i - 1], y1[i + 1], y1_s, g, s, lane48)

    passes(third_image, 0, 128)

    gram[...] = jnp.zeros((96, 256), F32)

    def products(k, sums):
        left, every = [], []
        sums = list(sums)
        for n in range(16):
            r = 16 * k + n
            b, f1, f2, y0r, y1r = rows_ref[r], first_ref[r], second_ref[r], y0[r + 8], y1[r + 8]
            left.append(jnp.concatenate([basis(r + 16), y0r[32:48], y1r[32:48]], axis=0))
            every.append(jnp.concatenate([b, w_ref[r], f1, f2], axis=0))
            pairs = ((y0r, b), (y0r, f1), (y1r, f1), (y1r, f2))
            sums = [t + p[0:32] * q[0:32] for t, (p, q) in zip(sums, pairs)]
        left = jnp.concatenate(parts_of(jnp.concatenate(left, axis=1), 2), axis=0)
        high, low = parts_of(jnp.concatenate(every, axis=1), 2)
        gram[:, 0:144] += fast_dot(left, high, NT) + fast_dot(left, low, NT)
        return tuple(sums)

    zero = jnp.zeros((32, 128), F32)
    sums = lax.fori_loop(0, 8, products, (zero, zero, zero, zero))

    a0, a1 = gram[0:48, 0:128] + gram[48:96, 0:128], gram[0:48, 128:256] + gram[48:96, 128:256]
    half0 = a0[16:32]
    half1 = jnp.where(lane16 < 16, a1[16:32], 0.0)
    half1 = jnp.where((lane16 >= 16) & (lane16 < 64), roll(a0[0:16], 16), half1)
    half1 = jnp.where((lane16 >= 64) & (lane16 < 96), roll(a0[32:48], 96), half1)
    half1 = jnp.where((lane16 >= 96) & (lane16 < 112), roll(a1[32:48], 96), half1)

    def relative(x, zones):
        zone = jnp.zeros((16, 128), jnp.bool_)
        for z in zones:
            zone = zone | ((lane16 >= z) & (lane16 < z + 16))
        kept = jnp.where(zone, x, 0.0)
        moved = jnp.zeros((16, 128), F32)
        for s in range(12):
            moved = jnp.where(slot == s, roll(kept, (5 - s) % 128), moved)
        return jnp.where(zone, moved, x)

    half0 = relative(half0, (32, 80))
    half1 = relative(half1, (0, 48, 96))
    eye = lax.broadcasted_iota(jnp.int32, (32, 128), 0)
    for n, total in enumerate(sums):
        column = jnp.sum(total, axis=1, keepdims=True)
        for part in range(2):
            spread = jnp.where(lanes((32, 128)) - 112 == eye - 16 * part, column, 0.0)
            line = jnp.sum(spread, axis=0, keepdims=True)
            half1 = jnp.where((slot == 2 * n + part) & (lane16 >= 112), line, half1)
    out_ref[0:12] = half0[0:12]
    out_ref[12:24] = half1[0:12]


def combine_kernel(in_ref, out_ref):
    c = lax.broadcasted_iota(jnp.int32, (8, 128), 0)
    lane = lanes((8, 128))
    for half in range(2):
        for dr in range(3):
            at = [in_ref[pl.ds(half * 12 + dr * 4 + dq, 8, stride=24), :] for dq in range(4)]
            even = at[1] + jnp.where(c >= 1, roll(at[3], 1, 0), 0.0)
            odd = at[2] + jnp.where(c < 7, roll(at[0], 7, 0), 0.0)
            if half:
                even = jnp.where(lane < 112, even, 0.0)
                odd = jnp.where(lane < 112, odd, 0.0)
                if dr == 1:
                    for s in range(8):
                        line = jnp.sum(in_ref[pl.ds(12 + s, 8, stride=24), :], axis=0, keepdims=True)
                        even = jnp.where((c == s) & (lane >= 112), line, even)
            base = half * 48 + dr * 8
            out_ref[base : base + 8] = even
            out_ref[base + 24 : base + 32] = odd


def batched_inverse(a, lane, row):
    base = lane - lane % 16
    for k in range(16):
        at_k = lane % 16 == k
        column = jnp.take_along_axis(a, base + k, axis=1)
        pivot = column[k : k + 1]
        line = jnp.where(at_k[0:1], 1.0, a[k : k + 1]) / pivot
        a = jnp.where(row == k, line, jnp.where(at_k, 0.0, a) - column * line)
    return a


def block_inverse(matrix, low, high):
    lane = lanes((16, 128))
    row = lax.broadcasted_iota(jnp.int32, (16, 128), 0)
    compact = jnp.where(lane % 16 == row, 1.0, 0.0)
    for n in range(low // 16, high // 16):
        compact = jnp.where(lane // 16 == n, matrix[16 * n : 16 * n + 16], compact)
    compact = batched_inverse(compact, lane, row)
    parts = []
    for n in range(8):
        active = low <= 16 * n < high
        parts.append(jnp.where(lane // 16 == n, compact, 0.0) if active else jnp.zeros((16, 128), F32))
    return jnp.concatenate(parts, axis=0)


def coarse_kernel(place_ref, in_ref, out_ref, g0, g1, e, ei, va, vb, mw, mt, ms, mz):
    pr, pc = place_ref[0], place_ref[1]
    lane8 = lanes((8, 128))
    sub8 = lax.broadcasted_iota(jnp.int32, (8, 128), 0)

    def at(p, par):
        return POS[p] * 16 + par * 8

    for half, ref in ((0, g0), (1, g1)):
        for par in range(2):
            for p in range(16):
                total = None
                for dr in range(3):
                    r = p + 1 - dr
                    if 0 <= r < 16:
                        base = half * 48 + par * 24 + dr * 8
                        piece = in_ref[r, base : base + 8]
                        total = piece if total is None else total + piece
                ref[at(p, par) : at(p, par) + 8] = total

    tally = g1[at(0, 0) : at(0, 0) + 8]
    for p in range(1, 16):
        tally = tally + g1[at(p, 0) : at(p, 0) + 8]

    def total_of(n):
        low = roll(tally[2 * n : 2 * n + 1], 16)
        high = roll(tally[2 * n + 1 : 2 * n + 2], 32)
        return jnp.where(lanes((1, 128)) < 16, low, high)

    bb, bu, uu, uuu = (total_of(n) for n in range(4))

    for p in range(16):
        for par in range(2):
            tile = g1[at(p, par) : at(p, par) + 8]
            halves = [jnp.zeros((8, 128), F32), jnp.zeros((8, 128), F32)]
            for dp in (-1, 0, 1):
                if not 0 <= p + dp < 16:
                    continue
                for dq in (-1, 0, 1):
                    l = 48 + 5 + 4 * dp + dq
                    other = par if dq == 0 else 1 - par
                    step = 0 if dq == 0 else ((dq - 1) // 2 if par == 0 else (dq + 1) // 2)
                    target = at(p + dp, other)
                    h, off = target // 128, target % 128
                    hit = (lane8 - off == sub8 + step) & (sub8 + step >= 0) & (sub8 + step < 8)
                    value = jnp.broadcast_to(tile[:, l : l + 1], (8, 128))
                    halves[h] = jnp.where(hit, value, halves[h])
            e[at(p, par) : at(p, par) + 8, 0:128] = halves[0]
            e[at(p, par) : at(p, par) + 8, 128:256] = halves[1]

    lane = lanes((128, 128))
    row = lax.broadcasted_iota(jnp.int32, (128, 128), 0)
    outer = block_inverse(e[0:128, 0:128], 0, 128)
    across = dot(outer, e[0:128, 128:256])
    schur = e[128:256, 128:256] - dot(e[128:256, 0:128], across)
    steps = []
    for low, high in ((0, 64), (64, 96), (96, 112)):
        inv = block_inverse(schur, low, high)
        link = jnp.where((row >= low) & (row < high) & (lane >= high), schur, 0.0)
        x = dot(inv, link)
        keep = jnp.where((row >= high) & (lane >= high), schur, 0.0)
        schur = keep - dot(link, x, TN)
        steps.append((inv, jnp.where((row == lane) & (row >= high), 1.0, 0.0) - x))
    inner = block_inverse(schur, 112, 128)
    for inv, y in reversed(steps):
        inner = inv + dot(dot(y, inner), y, NT)
    half = dot(across, inner)
    ei[0:128, 0:128] = outer + dot(half, across, NT)
    ei[0:128, 128:256] = -half
    ei[128:256, 0:128] = -half.T
    ei[128:256, 128:256] = inner

    def solve(z):
        return dot(ei[...], z)

    def apply(ref, zone, v_ref):
        sides = {}
        for p in range(16):
            even, odd = v_ref[at(p, 0) : at(p, 0) + 8], v_ref[at(p, 1) : at(p, 1) + 8]
            sides[p, 0] = (roll(odd, 1, 0), even, odd)
            sides[p, 1] = (even, odd, roll(even, 7, 0))
        tiles = {}
        for p in range(16):
            for par in range(2):
                tile = ref[at(p, par) : at(p, par) + 8]
                total = None
                for dp in (-1, 0, 1):
                    if not 0 <= p + dp < 16:
                        continue
                    for n in range(3):
                        l = zone + 5 + 4 * dp + n - 1
                        term = tile[:, l : l + 1] * sides[p + dp, par][n]
                        total = term if total is None else total + term
                tiles[POS[p] * 2 + par] = total
        return jnp.concatenate([tiles[n] for n in range(32)], axis=0)

    def inner_product(a, b):
        return jnp.sum(a * b, axis=0, keepdims=True)

    wb = g0[...]
    wu = roll(g0[...], 80)
    wuu = roll(g0[...], 32)
    zb = roll(g1[...], 112)
    tuu = roll(g1[...], 64)
    c0 = solve(zb)
    va[...] = c0
    f_c = apply(g0, 32, va)
    g_c = apply(g0, 80, va)
    h_c = apply(g1, 0, va)
    k_c = apply(g1, 96, va)
    grad0 = wb - f_c
    k0 = solve(grad0)
    vb[...] = k0
    f_k = apply(g0, 32, vb)
    g_k = apply(g0, 80, vb)
    rho0 = bb - 2.0 * inner_product(c0, wb) + inner_product(c0, f_c)
    energy0 = bu - 2.0 * inner_product(c0, wu) + inner_product(c0, g_c)
    curve0 = energy0 - inner_product(k0, grad0)
    a0 = rho0 / curve0
    e1 = c0 - a0 * k0
    f_e = f_c - a0 * f_k
    g_e = g_c - a0 * g_k
    grad1 = wb - f_e + a0 * (g_c - wu)
    k1 = solve(grad1)

    def second_norm(m0, m1, m2, v0, v1, v2, e_image, c_image, last):
        own = m0 - 2.0 * inner_product(e1, v0) + inner_product(e1, e_image)
        mixed = m1 - inner_product(c0, v1) - inner_product(e1, v1) + inner_product(e1, c_image)
        far = m2 - 2.0 * inner_product(c0, v2) + inner_product(c0, last)
        return own - 2.0 * a0 * mixed + a0 * a0 * far

    rho1 = second_norm(bb, bu, uu, wb, wu, wuu, f_e, g_c, h_c)
    energy1 = second_norm(bu, uu, uuu, wu, wuu, tuu, g_e, h_c, k_c)
    beta = rho1 / rho0
    cross = inner_product(e1, wu)
    s1q0 = (
        bu
        - inner_product(c0, wu)
        - cross
        + inner_product(e1, g_c)
        - a0 * (uu - 2.0 * inner_product(c0, wuu) + inner_product(c0, h_c))
        - inner_product(k0, grad1)
    )
    curve1 = energy1 - inner_product(k1, grad1) + 2.0 * beta * s1q0 + beta * beta * curve0
    a1 = rho1 / curve1

    ab = a1 * beta
    w_res = a1 * k1 + ab * k0 - e1
    t_res = (a0 + ab) * c0 + a1 * e1
    s_res = -(a1 * a0) * c0
    w_sol = -(a0 + ab) * c0 - a1 * e1
    t_sol = (a1 * a0) * c0
    z_sol = c0 - (a0 + ab) * k0 - a1 * k1
    big = lanes((256, 128))

    def joined(first, second):
        return jnp.where(big < 32, first, jnp.where(big < 64, roll(second, 32), 0.0))

    found = (
        (mz, jnp.where((big >= 64) & (big < 96), roll(z_sol, 64), 0.0)),
        (mw, joined(w_res, w_sol)),
        (mt, joined(t_res, t_sol)),
        (ms, jnp.where(big < 32, s_res, 0.0)),
    )
    for ref, value in found:
        for p in range(16):
            ref[16 * p : 16 * p + 16] = value[16 * POS[p] : 16 * POS[p] + 16]
    for n, (ref, _) in enumerate(found):
        for dr in range(3):
            p = jnp.clip(pr - 1 + dr, 0, 15)
            for dq in range(4):
                par = (dq + 1) % 2
                c = jnp.clip(pc - 1 + (dq + 1) // 2, 0, 7)
                k = 16 * n + 4 * dr + dq
                out_ref[k : k + 1] = ref[pl.ds(p * 16 + par * 8 + c, 1), :]
        out_ref[16 * n + 12 : 16 * n + 16] = jnp.zeros((4, 128), F32)
    out_ref[64:65] = -a0 - a1 - ab
    out_ref[65:66] = a1 * a0
    out_ref[66:67] = a0 + ab + a1
    out_ref[67:68] = -(a1 * a0)
    out_ref[68:72] = jnp.zeros((4, 128), F32)


def outputs_kernel(rows_ref, first_ref, second_ref, w_ref, grid_ref, coef_ref, place_ref, m_ref, sol_ref, res_ref):
    pr, pc = place_ref[0], place_ref[1]
    slot = lax.broadcasted_iota(jnp.int32, (16, 128), 0)
    region_row = pr - 1 + slot // 4
    region_col = 2 * pc - 1 + slot % 4
    inside = (slot < 12) & (region_row >= 0) & (region_row < REG) & (region_col >= 0) & (region_col < REG)
    window = jnp.where(inside, region_row * REG + region_col, -1).astype(F32)
    m = jnp.concatenate([m_ref[...], jnp.zeros((56, 128), F32)], axis=0).T
    c1, c2, c3 = parts_of(m[0:96, 0:64], 3)
    left = jnp.concatenate([c1, c1, c2, c2, c1, c3], axis=1)
    shape = (32, 128)
    p1, p2, p3, p4 = (jnp.broadcast_to(m[0:32, 64 + n : 65 + n], shape) for n in range(4))

    def step(k, _):
        rows = []
        for n in range(8):
            r = 8 * k + n
            z = jnp.where(grid_ref[pl.ds(r, 1), :] == window, grid_ref[pl.ds(128 + r, 1), :], 0.0)
            rows.append(jnp.concatenate([z, w_ref[r], first_ref[r, 32:48], second_ref[r, 32:48]], axis=0))
        r1, r2, r3 = parts_of(jnp.concatenate(rows, axis=1), 3)
        d = fast_dot(left, jnp.concatenate([r1, r2, r1, r2, r3, r1], axis=0))
        for n in range(8):
            r = 8 * k + n
            b, u, uu = rows_ref[r], first_ref[r, 0:32], second_ref[r, 0:32]
            e = d[:, 128 * n : 128 * n + 128]
            inv = coef_ref[5, pl.ds(r + 16, 1), :]
            res_ref[pl.ds(r, 32, stride=128), :] = b + p1 * u + p2 * uu + e[0:32]
            sol_ref[pl.ds(r, 32, stride=128), :] = inv * (p3 * b + p4 * u + e[32:64]) + e[64:96]
        return 0

    lax.fori_loop(0, 16, step, 0)


def from_everyone(value, axis):
    count = lax.axis_size(axis)
    return lax.all_to_all(jnp.broadcast_to(value[None], (count, *value.shape)), axis, 0, 0, tiled=True)


def shape_of(*dims):
    return jax.ShapeDtypeStruct(dims, F32)


def vmem(*dims):
    return pltpu.VMEM(dims, F32)


def body(load_currents, labels, bump_height, horizontal_class, vertical_class, pad_class, edge_table, pad_table):
    pr, pc = lax.axis_index(ROW), lax.axis_index(COL)
    rows, cols = lax.axis_size(ROW), lax.axis_size(COL)
    place = jnp.stack([pr, pc]).astype(jnp.int32)
    loads = load_currents.reshape(-1, 128)
    grid, first_rows = pl.pallas_call(
        prepare_kernel,
        out_shape=(shape_of(1024, 128), shape_of(HALO, SUB, 128)),
        in_specs=[scalars] * 3 + [whole] * 6,
        out_specs=(whole, whole),
    )(place, edge_table, pad_table, loads, labels, bump_height, horizontal_class, vertical_class, pad_class)
    down = [(i, i + 1) for i in range(rows - 1)]
    bottom = lax.ppermute(first_rows, ROW, [(b, a) for a, b in down])
    by_rows, own, last_rows = pl.pallas_call(
        pack_kernel,
        out_shape=(shape_of(128, 32, 128), shape_of(GROUPS, SUB, 128), shape_of(HALO, SUB, 128)),
        in_specs=[whole] * 2,
        out_specs=(whole,) * 3,
    )(loads, grid)
    top = lax.ppermute(last_rows, ROW, down)
    own = pl.pallas_call(
        corner_kernel, out_shape=shape_of(GROUPS, SUB, 128), in_specs=[whole] * 3, out_specs=whole
    )(own, top, bottom)
    right = [(i, i + 1) for i in range(cols - 1)]
    beside_left = lax.ppermute(own, COL, right)
    beside_right = lax.ppermute(own, COL, [(b, a) for a, b in right])
    first, second, w, coef, payload = pl.pallas_call(
        fields_kernel,
        out_shape=(
            shape_of(128, 48, 128),
            shape_of(128, 48, 128),
            shape_of(128, 16, 128),
            shape_of(6, 160, 128),
            shape_of(24, 128),
        ),
        in_specs=[scalars] + [whole] * 7,
        out_specs=(whole,) * 5,
        scratch_shapes=[
            vmem(5, 160, 128),
            vmem(GROUPS, 16, 128),
            vmem(GROUPS, 16, 128),
            vmem(GROUPS, 48, 128),
            vmem(GROUPS, 48, 128),
            vmem(GROUPS, 48, 128),
            vmem(2, GROUPS, 8, 128),
            vmem(144, 48, 128),
            vmem(144, 48, 128),
            vmem(96, 256),
        ],
    )(place, by_rows, grid, top, bottom, own, beside_left, beside_right)
    in_row = from_everyone(payload, COL).reshape(-1, 128)
    combined = pl.pallas_call(
        combine_kernel, out_shape=shape_of(96, 128), in_specs=[whole], out_specs=whole
    )(in_row)
    everything = from_everyone(combined, ROW)
    matrix = pl.pallas_call(
        coarse_kernel,
        out_shape=shape_of(72, 128),
        in_specs=[scalars, whole],
        out_specs=whole,
        scratch_shapes=[vmem(256, 128), vmem(256, 128), vmem(256, 256), vmem(256, 256)]
        + [vmem(256, 128)] * 6,
    )(place, everything)
    solution, residual = pl.pallas_call(
        outputs_kernel,
        out_shape=(shape_of(4096, 128), shape_of(4096, 128)),
        in_specs=[whole] * 6 + [scalars, whole],
        out_specs=(whole, whole),
    )(by_rows, first, second, w, grid, coef, place, matrix)
    return solution.reshape(load_currents.shape), residual.reshape(load_currents.shape)


def solution(mesh):
    finer = Mesh(mesh.devices.reshape(4, 4, 4, 2), ("row_0", "row_1", "col_0", "col_1"))
    grid = P(ROW, COL)
    return jax.shard_map(
        body,
        mesh=finer,
        in_specs=(P(None, ROW, COL), grid, grid, grid, grid, grid, P(), P()),
        out_specs=(P(None, ROW, COL), P(None, ROW, COL)),
        check_vma=False,
    )
```

```python
import jax
import jax.numpy as jnp
from jax import lax
from jax.experimental import pallas as pl
from jax.experimental.pallas import tpu as pltpu
from jax.sharding import Mesh
from jax.sharding import PartitionSpec as P

REG = 16
ROW = ("row_0", "row_1")
COL = ("col_0", "col_1")
F32 = jnp.float32
precise = lax.Precision.HIGHEST

LAB, BUMP, RIGHT, DOWN, PAD = 32, 33, 34, 35, 36
SUB = 40
HALO = 3
GROUPS = 9
ORDER = (1, 3, 5, 7, 9, 11, 13, 15, 2, 6, 10, 14, 4, 12, 8, 0)
POS = tuple(ORDER.index(p) for p in range(16))
NT = (((1,), (1,)), ((), ()))
NN = (((1,), (0,)), ((), ()))
TN = (((0,), (0,)), ((), ()))
whole = pl.BlockSpec(memory_space=pltpu.VMEM)
outside = pl.BlockSpec(memory_space=pltpu.HBM)
limited = pltpu.CompilerParams(vmem_limit_bytes=32 * 2**20)
scalars = pl.BlockSpec(memory_space=pltpu.SMEM)


def dot(a, b, dims=NN):
    return lax.dot_general(a, b, dims, precision=precise, preferred_element_type=F32)


def parts_of(x, count):
    parts = []
    for n in range(count):
        parts.append(x.astype(jnp.bfloat16))
        if n + 1 < count:
            x = x - parts[-1].astype(F32)
    return parts


def fast_dot(a, b, dims=NN):
    return lax.dot_general(a, b, dims, preferred_element_type=F32)


def lanes(shape):
    return lax.broadcasted_iota(jnp.int32, shape, len(shape) - 1)


def roll(x, shift, axis=1):
    return pltpu.roll(x, shift, axis)


def prepare_kernel(
    place_ref, edge_hbm, pad_hbm, load_hbm, label_hbm, bump_hbm, across_hbm, down_hbm, pad_class_hbm,
    grid_ref, first_ref, edge_ref, pad_ref, load_ref, label_ref, across_ref, down_ref, pad_class_ref, done,
):
    copies = [
        pltpu.make_async_copy(source, target, done.at[n])
        for n, (source, target) in enumerate(
            (
                (edge_hbm, edge_ref),
                (pad_hbm, pad_ref),
                (across_hbm, across_ref),
                (down_hbm, down_ref),
                (pad_class_hbm, pad_class_ref),
                (label_hbm, label_ref),
                (bump_hbm, grid_ref.at[pl.ds(128, 128)]),
                (load_hbm.at[:, pl.ds(0, 8)], load_ref),
            )
        )
    ]
    for copy in copies:
        copy.start()
    for copy in copies:
        copy.wait()
    pr, pc = place_ref[0], place_ref[1]
    shape = (128, 128)
    row, lane = lax.broadcasted_iota(jnp.int32, shape, 0), lanes(shape)

    def lookup(table, classes):
        found = jnp.zeros(shape, F32)
        for n in range(8):
            found = jnp.where(classes == n, table[n], found)
        return found

    right = lookup(edge_ref, across_ref[...])
    down = lookup(edge_ref, down_ref[...])
    grid_ref[0:128] = label_ref[...].astype(F32)
    grid_ref[256:384] = jnp.where((lane == 127) & (pc == 7), 0.0, right)
    grid_ref[384:512] = jnp.where((row == 127) & (pr == 15), 0.0, down)
    grid_ref[512:640] = lookup(pad_ref, pad_class_ref[...])
    grid_ref[640:1024] = jnp.zeros((384, 128), F32)
    for n in range(HALO):
        first_ref[n, 0:32] = load_ref[:, n]
        first_ref[n, 32:40] = grid_ref[pl.ds(n, 8, stride=128), :]


def pack_kernel(load_ref, grid_ref, rows_ref, own_ref, last_ref):
    lane = lanes((32, 128)) // 8

    def group(g, slots):
        loads, rest = jnp.zeros((32, 128), F32), jnp.zeros((8, 128), F32)
        for s in slots:
            r = 16 * g - 8 + s
            b = load_ref[pl.ds(r, 32, stride=128), :]
            rows_ref[r] = b
            loads = jnp.where(lane == s, roll(b, (8 * s + 3) % 128), loads)
            rest = jnp.where(lane[0:8] == s, roll(grid_ref[pl.ds(r, 8, stride=128), :], (8 * s + 3) % 128), rest)
        own_ref[g, 0:32] = loads
        own_ref[g, 32:40] = rest

    group(0, range(8, 16))
    group(8, range(8))

    def step(g, _):
        group(g, range(16))
        return 0

    lax.fori_loop(1, 8, step, 0)
    for n in range(HALO):
        r = 128 - HALO + n
        last_ref[n, 0:32] = rows_ref[r]
        last_ref[n, 32:40] = grid_ref[pl.ds(r, 8, stride=128), :]


def corner_kernel(own_ref, top_ref, bottom_ref, out_ref):
    lane = lanes((SUB, 128)) // 8
    for g in range(GROUPS):
        out_ref[g] = own_ref[g]
    start, end = own_ref[0], own_ref[8]
    for n in range(HALO):
        s = 8 - HALO + n
        start = jnp.where(lane == s, roll(top_ref[n], (8 * s + 3) % 128), start)
        s = 8 + n
        end = jnp.where(lane == s, roll(bottom_ref[n], (8 * s + 3) % 128), end)
    out_ref[0] = start
    out_ref[8] = end


def fields_kernel(
    place_ref, rows_ref, grid_ref, top_ref, bottom_ref, own_ref, left_ref, right_ref,
    first_ref, second_ref, w_ref, coef_ref, out_ref,
    ext, so, ss, sz_o, sz_s, y0_o, y0_s, qz, q0, q1, sc, y0, y1, gram,
):
    pr, pc = place_ref[0], place_ref[1]
    lane1 = lanes((1, 128))
    lane16 = lanes((16, 128))
    lane48 = lanes((48, 128))

    for n in range(5):
        ext[n, 0:16] = jnp.zeros((16, 128), F32)
        ext[n, 16:144] = grid_ref[128 * n : 128 * n + 128]
        ext[n, 144:160] = jnp.zeros((16, 128), F32)
        for k in range(HALO):
            ext[n, 16 - HALO + k : 17 - HALO + k] = top_ref[k, 32 + n : 33 + n]
            ext[n, 144 + k : 145 + k] = bottom_ref[k, 32 + n : 33 + n]

    slot = lax.broadcasted_iota(jnp.int32, (16, 128), 0)
    region_row = pr - 1 + slot // 4
    region_col = 2 * pc - 1 + slot % 4
    inside = (slot < 12) & (region_row >= 0) & (region_row < REG) & (region_col >= 0) & (region_col < REG)
    window = jnp.where(inside, region_row * REG + region_col, -1).astype(F32)

    for ref in (so, ss, sz_o, sz_s, y0_o, y0_s):
        ref[0] = jnp.zeros(ref.shape[1:], F32)
        ref[GROUPS + 1] = jnp.zeros(ref.shape[1:], F32)

    def pair_left(o, s, lane):
        j = lane % 8
        return roll(jnp.where(j == 2, s, o), 1), roll(jnp.where(j == 2, o, s), 1)

    def pair_right(o, s, lane):
        j = lane % 8
        return roll(jnp.where(j == 3, s, o), 127), roll(jnp.where(j == 3, o, s), 127)

    def above(before, here, lane):
        return roll(jnp.where(lane >= 120, before, here), 8)

    def below(here, after, lane):
        return roll(jnp.where(lane < 8, after, here), 120)

    def strips(g, _):
        o_row = own_ref[g]
        s_row = jnp.where(lanes((SUB, 128)) % 8 < 3, left_ref[g], right_ref[g])
        so[g + 1], ss[g + 1] = o_row, s_row
        lefts = pair_left(o_row[RIGHT : RIGHT + 1], s_row[RIGHT : RIGHT + 1], lane1)
        for side, (row, ref, ll) in enumerate(((o_row, so, lefts[0]), (s_row, ss, lefts[1]))):
            rl, dl = row[RIGHT : RIGHT + 1], row[DOWN : DOWN + 1]
            ul = above(ref[g, DOWN : DOWN + 1], dl, lane1)
            diag = row[PAD : PAD + 1] + rl + ll + dl + ul
            inv = jnp.where(diag > 0, 1.0 / diag, 0.0)
            for n, value in enumerate((diag, rl, ll, dl, ul, inv)):
                sc[side, g, n : n + 1] = value
            z = jnp.where(row[LAB : LAB + 1] == window, row[BUMP : BUMP + 1], 0.0)
            (sz_s if side else sz_o)[g + 1] = z
            if side:
                qz[2 * g] = z
                qz[2 * g + 1] = roll(z, 64)

        at = pl.multiple_of(16 * g + 8, 8)
        beside = jnp.zeros((16, 128), F32)
        for s in range(16):
            beside = jnp.where(slot == s, roll(s_row[RIGHT : RIGHT + 1], 125 - 8 * s), beside)
        rl, dl = ext[2, pl.ds(at, 16)], ext[3, pl.ds(at, 16)]
        ll = roll(jnp.where(lane16 == 127, beside, rl), 1)
        last = ext[3, pl.ds(pl.multiple_of(at - 8, 8), 8)]
        ul = jnp.where(slot == 0, last[7:8], roll(dl, 1, 0))
        diag = ext[4, pl.ds(at, 16)] + rl + ll + dl + ul
        inv = jnp.where(diag > 0, 1.0 / diag, 0.0)
        for n, value in enumerate((diag, rl, ll, dl, ul, inv)):
            coef_ref[n, pl.ds(at, 16)] = value
        return 0

    lax.fori_loop(0, GROUPS, strips, 0)

    def strip_image(ref_o, ref_s, g, lane, sides):
        o, s = ref_o[g + 1], ref_s[g + 1]
        lefts, rights = pair_left(o, s, lane), pair_right(o, s, lane)
        done = []
        for side in sides:
            ref, here = (ref_s, s) if side else (ref_o, o)
            up = above(ref[g], here, lane)
            down = below(here, ref[g + 2], lane)
            c = [sc[side, g, n : n + 1] for n in range(5)]
            done.append(c[0] * here - c[1] * rights[side] - c[2] * lefts[side] - c[3] * down - c[4] * up)
        return done

    def strip_first(g, _):
        w = strip_image(sz_o, sz_s, g, lane16, (0, 1))
        for side, (source, ref) in enumerate(((so, y0_o), (ss, y0_s))):
            inv = sc[side, g, 5:6]
            ref[g + 1, 0:32] = inv * source[g + 1, 0:32]
            ref[g + 1, 32:48] = inv * w[side]
        y = y0_s[g + 1]
        q0[2 * g] = y
        q0[2 * g + 1] = roll(y, 64)
        return 0

    lax.fori_loop(0, GROUPS, strip_first, 0)

    def strip_second(g, _):
        (u,) = strip_image(y0_o, y0_s, g, lane48, (1,))
        y = sc[1, g, 5:6] * u
        q1[2 * g] = y
        q1[2 * g + 1] = roll(y, 64)
        return 0

    lax.fori_loop(0, GROUPS, strip_second, 0)

    def passes(work, low, high):
        for s in range(8):
            if s - 8 >= low:
                work(0, s)

        def step(g, _):
            for s in range(8):
                work(g, s)
            return 0

        lax.fori_loop(1, 17, step, 0)
        for s in range(8):
            if 128 + s < high:
                work(17, s)

    def owned(g):
        return not isinstance(g, int)

    def coef(n, g, s):
        return coef_ref[n, pl.ds(8 * g + 8 + s, 1), :]

    def image(here, up, down, strip, g, s, lane):
        other = roll(strip[g], 125 - 8 * s)
        left = roll(jnp.where(lane == 127, other, here), 1)
        right = roll(jnp.where(lane == 0, other, here), 127)
        return (
            coef(0, g, s) * here
            - coef(1, g, s) * right
            - coef(2, g, s) * left
            - coef(3, g, s) * down
            - coef(4, g, s) * up
        )

    def basis(j):
        return jnp.where(ext[0, pl.ds(j, 1), :] == window, ext[1, pl.ds(j, 1), :], 0.0)

    def first_image(g, s):
        r, j = 8 * g - 8 + s, 8 * g + 8 + s
        w = image(basis(j), basis(j - 1), basis(j + 1), qz, g, s, lane16)
        if owned(g):
            b = rows_ref[r]
            w_ref[r] = w
        else:
            b = top_ref[r + HALO, 0:32] if r < 0 else bottom_ref[r - 128, 0:32]
        inv = coef(5, g, s)
        y0[8 * g + s, 0:32] = inv * b
        y0[8 * g + s, 32:48] = inv * w

    passes(first_image, -2, 130)

    def second_image(g, s):
        i = 8 * g + s
        f1 = image(y0[i], y0[i - 1], y0[i + 1], q0, g, s, lane48)
        if owned(g):
            first_ref[8 * g - 8 + s] = f1
        y1[i] = coef(5, g, s) * f1

    passes(second_image, -1, 129)

    def third_image(g, s):
        i = 8 * g + s
        second_ref[8 * g - 8 + s] = image(y1[i], y1[i - 1], y1[i + 1], q1, g, s, lane48)

    passes(third_image, 0, 128)

    gram[...] = jnp.zeros((96, 256), F32)

    def products(k, sums):
        left, every = [], []
        sums = list(sums)
        for n in range(16):
            r = 16 * k + n
            b, f1, f2, y0r, y1r = rows_ref[r], first_ref[r], second_ref[r], y0[r + 8], y1[r + 8]
            left.append(jnp.concatenate([basis(r + 16), y0r[32:48], y1r[32:48]], axis=0))
            every.append(jnp.concatenate([b, w_ref[r], f1, f2], axis=0))
            pairs = ((y0r, b), (y0r, f1), (y1r, f1), (y1r, f2))
            sums = [t + p[0:32] * q[0:32] for t, (p, q) in zip(sums, pairs)]
        left = jnp.concatenate(parts_of(jnp.concatenate(left, axis=1), 2), axis=0)
        high, low = parts_of(jnp.concatenate(every, axis=1), 2)
        gram[:, 0:144] += fast_dot(left, high, NT) + fast_dot(left, low, NT)
        return tuple(sums)

    zero = jnp.zeros((32, 128), F32)
    sums = lax.fori_loop(0, 8, products, (zero, zero, zero, zero))

    a0, a1 = gram[0:48, 0:128] + gram[48:96, 0:128], gram[0:48, 128:256] + gram[48:96, 128:256]
    zr, w0, t0, w1, t1 = a0[0:16], a0[16:32], a0[32:48], a1[16:32], a1[32:48]
    matrices = jnp.zeros((16, 128), F32)
    for n, (x, z) in enumerate(((w0, 32), (w0, 80), (w1, 0), (zr, 32), (t1, 0))):
        start = 24 * n
        matrices = jnp.where((lane16 >= start) & (lane16 < start + 16), roll(x, (start - z) % 128), matrices)
    moved = jnp.zeros((16, 128), F32)
    for k in range(12):
        moved = jnp.where(slot == k, roll(matrices, (128 - k) % 128), moved)
    common = jnp.zeros((16, 128), F32)
    for n in range(5):
        start = 20 + 6 * n
        common = jnp.where((lane16 >= start) & (lane16 < start + 6), roll(moved, (start - 24 * n) % 128), common)
    lines = []
    diagonal = lanes((32, 128)) == lax.broadcasted_iota(jnp.int32, (32, 128), 0)
    for total in sums:
        column = jnp.sum(total, axis=1, keepdims=True)
        lines.append(jnp.sum(jnp.where(diagonal, column, 0.0), axis=0, keepdims=True))
    lane8, row8 = lanes((8, 128)), lax.broadcasted_iota(jnp.int32, (8, 128), 0)
    for d in range(8):
        message = common
        for n, (x, z) in enumerate(((w0, 0), (w0, 48), (w0, 96), (zr, 0), (t0, 96))):
            hit = (lane16 >= 4 * n) & (lane16 < 4 * n + 4)
            message = jnp.where(hit, roll(x, (4 * n - z - 4 * d) % 128), message)
        upper = roll(roll(message, 10, 0), 64)
        sent = jnp.where(lane8 < 64, message[0:8], upper[0:8])
        line = jnp.zeros((1, 128), F32)
        for n in range(4):
            line = jnp.where((lane1 >= 4 * n) & (lane1 < 4 * n + 4), roll(lines[n], (4 * n - 4 * d) % 128), line)
        out_ref[8 * d : 8 * d + 8] = jnp.where(row8 < 6, sent, jnp.where(row8 == 6, line, 0.0))


def batched_inverse(a, lane, row):
    base = lane - lane % 16
    for k in range(16):
        at_k = lane % 16 == k
        column = jnp.take_along_axis(a, base + k, axis=1)
        pivot = column[k : k + 1]
        line = jnp.where(at_k[0:1], 1.0, a[k : k + 1]) / pivot
        a = jnp.where(row == k, line, jnp.where(at_k, 0.0, a) - column * line)
    return a


def block_inverse(matrix, low, high):
    lane = lanes((16, 128))
    row = lax.broadcasted_iota(jnp.int32, (16, 128), 0)
    compact = jnp.where(lane % 16 == row, 1.0, 0.0)
    for n in range(low // 16, high // 16):
        compact = jnp.where(lane // 16 == n, matrix[16 * n : 16 * n + 16], compact)
    compact = batched_inverse(compact, lane, row)
    parts = []
    for n in range(8):
        active = low <= 16 * n < high
        parts.append(jnp.where(lane // 16 == n, compact, 0.0) if active else jnp.zeros((16, 128), F32))
    return jnp.concatenate(parts, axis=0)


def coarse_kernel(place_ref, in_ref, out_ref, g, e, ei, first, second, near):
    pr, pc = place_ref[0], place_ref[1]
    sub8 = lax.broadcasted_iota(jnp.int32, (8, 128), 0)

    for p in range(16):
        sums = {}
        for dr in range(3):
            r = p + 1 - dr
            if not 0 <= r < 16:
                continue
            for dq in range(4):
                k = 4 * dr + dq
                piece = in_ref[pl.ds(64 * r + k % 6, 8, stride=8), :]
                if dq == 0:
                    piece = jnp.where(sub8 < 7, roll(piece, 7, 0), 0.0)
                elif dq == 3:
                    piece = jnp.where(sub8 >= 1, roll(piece, 1, 0), 0.0)
                key = ((dq + 1) % 2, k >= 6)
                sums[key] = sums[key] + piece if key in sums else piece
        for par in range(2):
            total = jnp.zeros((8, 128), F32)
            if (par, False) in sums:
                total = total + sums[par, False]
            if (par, True) in sums:
                total = total + roll(sums[par, True], 64)
            g[pl.ds(16 * p + par, 8, stride=2), :] = total
    tally = jnp.sum(in_ref[pl.ds(6, 128, stride=8), :], axis=0, keepdims=True)
    tally = jnp.broadcast_to(tally, (128, 128)).T
    bb, bu, uu, uuu = (tally[4 * n : 4 * n + 4, 0:1] for n in range(4))
    by_lane = jnp.concatenate([g[0:128].T, g[128:256].T], axis=1)

    lane16, row16 = lanes((16, 128)), lax.broadcasted_iota(jnp.int32, (16, 128), 0)
    base = 20 + 6 * 3
    for p in range(16):
        own = g[16 * p : 16 * p + 16]
        terms = [(own, d, dp, dq) for d, dp, dq in ((0, 0, 0), (1, 0, 1))]
        terms.append((roll(own, 1, 0), 1, 0, -1))
        if p < 15:
            terms += [(own, d, 1, dq) for d, dq in ((3, -1), (4, 0), (5, 1))]
        if p > 0:
            last = g[16 * p - 16 : 16 * p]
            terms += [(roll(last, 15, 0), 3, -1, 1), (last, 4, -1, 0), (roll(last, 1, 0), 5, -1, -1)]
        halves = [jnp.zeros((16, 128), F32), jnp.zeros((16, 128), F32)]
        for x, d, dp, dq in terms:
            target = POS[p + dp] * 16
            h, off = target // 128, target % 128
            q = row16 + dq
            hit = (lane16 == off + q) & (q >= 0) & (q < 16)
            value = jnp.broadcast_to(x[:, base + d : base + d + 1], (16, 128))
            halves[h] = jnp.where(hit, value, halves[h])
        at = POS[p] * 16
        e[at : at + 16, 0:128] = halves[0]
        e[at : at + 16, 128:256] = halves[1]

    lane = lanes((128, 128))
    row = lax.broadcasted_iota(jnp.int32, (128, 128), 0)
    outer = block_inverse(e[0:128, 0:128], 0, 128)
    across = dot(outer, e[0:128, 128:256])
    schur = e[128:256, 128:256] - dot(e[128:256, 0:128], across)
    steps = []
    for low, high in ((0, 64), (64, 96), (96, 112)):
        inv = block_inverse(schur, low, high)
        link = jnp.where((row >= low) & (row < high) & (lane >= high), schur, 0.0)
        x = dot(inv, link)
        keep = jnp.where((row >= high) & (lane >= high), schur, 0.0)
        schur = keep - dot(link, x, TN)
        steps.append((inv, jnp.where((row == lane) & (row >= high), 1.0, 0.0) - x))
    inner = block_inverse(schur, 112, 128)
    for inv, y in reversed(steps):
        inner = inv + dot(dot(y, inner), y, NT)
    half = dot(across, inner)
    near_diag = outer + dot(half, across, NT)

    def ordered(top_half, bottom_half):
        blocks = [top_half[16 * n : 16 * n + 16] for n in range(8)]
        blocks += [bottom_half[16 * n : 16 * n + 16] for n in range(8)]
        blocks = [blocks[POS[p]] for p in range(16)]
        return jnp.concatenate(blocks[:8], axis=0), jnp.concatenate(blocks[8:], axis=0)

    left_top, left_bottom = ordered(near_diag, -half.T)
    right_top, right_bottom = ordered(-half, inner)
    top_left, bottom_left = ordered(left_top.T, right_top.T)
    top_right, bottom_right = ordered(left_bottom.T, right_bottom.T)
    ei[0:128, 0:128] = top_left
    ei[0:128, 128:256] = top_right
    ei[128:256, 0:128] = bottom_left
    ei[128:256, 128:256] = bottom_right

    def solve(z):
        return dot(z, ei[...])

    def apply(n, v):
        c = [by_lane[20 + 6 * n + d : 21 + 6 * n + d] for d in range(6)]
        total = c[0] * v
        for d, step in ((1, 1), (3, 15), (4, 16), (5, 17)):
            total = total + c[d] * roll(v, 256 - step) + roll(c[d] * v, step)
        return total

    def inner_product(a, b):
        return jnp.sum(a * b, axis=1, keepdims=True)

    wb, wu, wuu, zb, tuu = (by_lane[4 * n : 4 * n + 4] for n in range(5))
    c0 = solve(zb)
    f_c, g_c, h_c, k_c = apply(0, c0), apply(1, c0), apply(2, c0), apply(4, c0)
    grad0 = wb - f_c
    k0 = solve(grad0)
    f_k, g_k = apply(0, k0), apply(1, k0)
    rho0 = bb - 2.0 * inner_product(c0, wb) + inner_product(c0, f_c)
    energy0 = bu - 2.0 * inner_product(c0, wu) + inner_product(c0, g_c)
    curve0 = energy0 - inner_product(k0, grad0)
    a0 = rho0 / curve0
    e1 = c0 - a0 * k0
    f_e = f_c - a0 * f_k
    g_e = g_c - a0 * g_k
    grad1 = wb - f_e + a0 * (g_c - wu)
    k1 = solve(grad1)

    def second_norm(m0, m1, m2, v0, v1, v2, e_image, c_image, last):
        own = m0 - 2.0 * inner_product(e1, v0) + inner_product(e1, e_image)
        mixed = m1 - inner_product(c0, v1) - inner_product(e1, v1) + inner_product(e1, c_image)
        far = m2 - 2.0 * inner_product(c0, v2) + inner_product(c0, last)
        return own - 2.0 * a0 * mixed + a0 * a0 * far

    rho1 = second_norm(bb, bu, uu, wb, wu, wuu, f_e, g_c, h_c)
    energy1 = second_norm(bu, uu, uuu, wu, wuu, tuu, g_e, h_c, k_c)
    beta = rho1 / rho0
    cross = (
        bu
        - inner_product(c0, wu)
        - inner_product(e1, wu)
        + inner_product(e1, g_c)
        - a0 * (uu - 2.0 * inner_product(c0, wuu) + inner_product(c0, h_c))
        - inner_product(k0, grad1)
    )
    curve1 = energy1 - inner_product(k1, grad1) + 2.0 * beta * cross + beta * beta * curve0
    a1 = rho1 / curve1

    mine = lax.broadcasted_iota(jnp.int32, (32, 256), 0) // 4 == pc

    def zone(value):
        value = jnp.broadcast_to(value, (4, 256))
        return jnp.where(mine, jnp.concatenate([value] * 8, axis=0), 0.0)

    ab = a1 * beta
    stacks = (
        (
            zone(a1 * k1 + ab * k0 - e1),
            zone(-(a0 + ab) * c0 - a1 * e1),
            zone((a0 + ab) * c0 + a1 * e1),
            zone((a1 * a0) * c0),
        ),
        (
            zone(-(a1 * a0) * c0),
            zone(c0 - (a0 + ab) * k0 - a1 * k1),
            zone(-a0 - a1 - ab),
            zone(a1 * a0),
        ),
    )
    out_ref[...] = jnp.zeros((256, 128), F32)
    for n, (ref, stack) in enumerate(((first, stacks[0]), (second, stacks[1]))):
        stack = jnp.concatenate(stack, axis=0)
        ref[0:8] = jnp.zeros((8, 128), F32)
        ref[8:136] = stack[:, 0:128].T
        ref[136:264] = stack[:, 128:256].T
        ref[264:272] = jnp.zeros((8, 128), F32)
        for dr in range(3):
            p = jnp.clip(pr - 1 + dr, 0, 15)
            near[...] = ref[pl.ds(pl.multiple_of(16 * p, 16), 32), :]
            for dq in range(4):
                out_ref[pl.ds(16 * n + 4 * dr + dq, 8, stride=32), :] = near[pl.ds(7 + dq, 8, stride=2), :]


def outputs_kernel(rows_ref, first_ref, second_ref, w_ref, grid_ref, coef_ref, place_ref, m_ref, sol_ref, res_ref):
    pr, pc = place_ref[0], place_ref[1]
    slot = lax.broadcasted_iota(jnp.int32, (16, 128), 0)
    region_row = pr - 1 + slot // 4
    region_col = 2 * pc - 1 + slot % 4
    inside = (slot < 12) & (region_row >= 0) & (region_row < REG) & (region_col >= 0) & (region_col < REG)
    window = jnp.where(inside, region_row * REG + region_col, -1).astype(F32)
    total = m_ref[0:32]
    for n in range(1, 8):
        total = total + m_ref[32 * n : 32 * n + 32]
    top, bottom = total[0:16], total[16:32]
    lane = lanes((16, 128))
    steps = jnp.where(slot == 0, roll(bottom[5:6], 64), jnp.where(slot == 1, roll(bottom[5:6], 32), 0.0))
    m = jnp.concatenate(
        [
            jnp.where((lane >= 64) & (lane < 96), roll(bottom, 32), 0.0),
            jnp.where(lane < 64, top, 0.0),
            jnp.where(lane < 64, roll(top, 64), 0.0),
            jnp.where(lane < 32, bottom, 0.0),
            steps,
            jnp.zeros((48, 128), F32),
        ],
        axis=0,
    ).T
    c1, c2, c3 = parts_of(m[0:96, 0:64], 3)
    left = jnp.concatenate([c1, c1, c2, c2, c1, c3], axis=1)
    shape = (32, 128)
    p1, p2 = (jnp.broadcast_to(m[0:32, 64 + n : 65 + n], shape) for n in range(2))

    def step(k, _):
        rows = []
        for n in range(8):
            r = 8 * k + n
            z = jnp.where(grid_ref[pl.ds(r, 1), :] == window, grid_ref[pl.ds(128 + r, 1), :], 0.0)
            rows.append(jnp.concatenate([z, w_ref[r], first_ref[r, 32:48], second_ref[r, 32:48]], axis=0))
        r1, r2, r3 = parts_of(jnp.concatenate(rows, axis=1), 3)
        d = fast_dot(left, jnp.concatenate([r1, r2, r1, r2, r3, r1], axis=0))
        for n in range(8):
            r = 8 * k + n
            b, u, uu = rows_ref[r], first_ref[r, 0:32], second_ref[r, 0:32]
            e = d[:, 128 * n : 128 * n + 128]
            inv = coef_ref[5, pl.ds(r + 16, 1), :]
            res_ref[pl.ds(r, 32, stride=128), :] = b + p1 * u + p2 * uu + e[0:32]
            sol_ref[pl.ds(r, 32, stride=128), :] = inv * (e[32:64] - p1 * b - p2 * u) + e[64:96]
        return 0

    lax.fori_loop(0, 16, step, 0)


def shape_of(*dims):
    return jax.ShapeDtypeStruct(dims, F32)


def kept(*dims):
    return pltpu.VMEM(dims, F32)


def vmem(*dims):
    return pltpu.VMEM(dims, F32)


def body(load_currents, labels, bump_height, horizontal_class, vertical_class, pad_class, edge_table, pad_table):
    pr, pc = lax.axis_index(ROW), lax.axis_index(COL)
    rows, cols = lax.axis_size(ROW), lax.axis_size(COL)
    place = jnp.stack([pr, pc]).astype(jnp.int32)
    loads = load_currents.reshape(-1, 128)
    grid, first_rows = pl.pallas_call(
        prepare_kernel,
        out_shape=(kept(1024, 128), shape_of(HALO, SUB, 128)),
        compiler_params=limited,
        in_specs=[scalars] + [outside] * 8,
        out_specs=(whole, whole),
        scratch_shapes=[pltpu.SMEM((8,), F32), pltpu.SMEM((8,), F32), vmem(32, 8, 128)]
        + [pltpu.VMEM((128, 128), jnp.int32)] * 4
        + [pltpu.SemaphoreType.DMA((8,))],
    )(
        place,
        *(
            pltpu.with_memory_space_constraint(x, pltpu.HBM)
            for x in (
                edge_table, pad_table, load_currents, labels, bump_height,
                horizontal_class, vertical_class, pad_class,
            )
        ),
    )
    down = [(i, i + 1) for i in range(rows - 1)]
    bottom = lax.ppermute(first_rows, ROW, [(b, a) for a, b in down])
    by_rows, own, last_rows = pl.pallas_call(
        pack_kernel,
        out_shape=(kept(128, 32, 128), kept(GROUPS, SUB, 128), shape_of(HALO, SUB, 128)),
        compiler_params=limited,
        in_specs=[whole] * 2,
        out_specs=(whole,) * 3,
    )(loads, grid)
    top = lax.ppermute(last_rows, ROW, down)
    own = pl.pallas_call(
        corner_kernel, out_shape=shape_of(GROUPS, SUB, 128), in_specs=[whole] * 3, out_specs=whole, compiler_params=limited
    )(own, top, bottom)
    right = [(i, i + 1) for i in range(cols - 1)]
    beside_left = lax.ppermute(own, COL, right)
    beside_right = lax.ppermute(own, COL, [(b, a) for a, b in right])
    first, second, w, coef, payload = pl.pallas_call(
        fields_kernel,
        out_shape=(
            kept(128, 48, 128),
            kept(128, 48, 128),
            kept(128, 16, 128),
            kept(6, 160, 128),
            shape_of(64, 128),
        ),
        compiler_params=limited,
        in_specs=[scalars] + [whole] * 7,
        out_specs=(whole,) * 5,
        scratch_shapes=[
            vmem(5, 160, 128),
            vmem(GROUPS + 2, SUB, 128),
            vmem(GROUPS + 2, SUB, 128),
            vmem(GROUPS + 2, 16, 128),
            vmem(GROUPS + 2, 16, 128),
            vmem(GROUPS + 2, 48, 128),
            vmem(GROUPS + 2, 48, 128),
            vmem(2 * GROUPS, 16, 128),
            vmem(2 * GROUPS, 48, 128),
            vmem(2 * GROUPS, 48, 128),
            vmem(2, GROUPS, 8, 128),
            vmem(144, 48, 128),
            vmem(144, 48, 128),
            vmem(96, 256),
        ],
    )(place, by_rows, grid, top, bottom, own, beside_left, beside_right)
    sent = jnp.broadcast_to(payload.reshape(1, cols, 8, 128), (rows, cols, 8, 128)).reshape(-1, 8, 128)
    everything = lax.all_to_all(sent, ROW + COL, 0, 0, tiled=True).reshape(-1, 128)
    found = pl.pallas_call(
        coarse_kernel,
        out_shape=shape_of(256, 128),
        compiler_params=limited,
        in_specs=[scalars, whole],
        out_specs=whole,
        scratch_shapes=[
            vmem(256, 128),
            vmem(256, 256),
            vmem(256, 256),
            vmem(272, 128),
            vmem(272, 128),
            vmem(32, 128),
        ],
    )(place, everything)
    matrix = lax.all_to_all(found.reshape(cols, 32, 128), COL, 0, 0, tiled=True).reshape(-1, 128)
    solution, residual = pl.pallas_call(
        outputs_kernel,
        out_shape=(shape_of(4096, 128), shape_of(4096, 128)),
        compiler_params=limited,
        in_specs=[whole] * 6 + [scalars, whole],
        out_specs=(whole, whole),
    )(by_rows, first, second, w, grid, coef, place, matrix)
    return solution.reshape(load_currents.shape), residual.reshape(load_currents.shape)


def solution(mesh):
    finer = Mesh(mesh.devices.reshape(4, 4, 4, 2), ("row_0", "row_1", "col_0", "col_1"))
    grid = P(ROW, COL)
    return jax.shard_map(
        body,
        mesh=finer,
        in_specs=(P(None, ROW, COL), grid, grid, grid, grid, grid, P(), P()),
        out_specs=(P(None, ROW, COL), P(None, ROW, COL)),
        check_vma=False,
    )
```

```python
import jax
import jax.numpy as jnp
from jax import lax
from jax.experimental import pallas as pl
from jax.experimental.pallas import tpu as pltpu
from jax.sharding import Mesh
from jax.sharding import PartitionSpec as P

REG = 16
ROW = ("row_0", "row_1")
COL = ("col_0", "col_1")
F32 = jnp.float32
precise = lax.Precision.HIGHEST

LAB, BUMP, RIGHT, DOWN, PAD = 32, 33, 34, 35, 36
SUB = 40
HALO = 3
GROUPS = 9
ORDER = (1, 3, 5, 7, 9, 11, 13, 15, 2, 6, 10, 14, 4, 12, 8, 0)
POS = tuple(ORDER.index(p) for p in range(16))
NT = (((1,), (1,)), ((), ()))
NN = (((1,), (0,)), ((), ()))
TN = (((0,), (0,)), ((), ()))
whole = pl.BlockSpec(memory_space=pltpu.VMEM)
outside = pl.BlockSpec(memory_space=pltpu.HBM)
limited = pltpu.CompilerParams(vmem_limit_bytes=32 * 2**20)
scalars = pl.BlockSpec(memory_space=pltpu.SMEM)


def dot(a, b, dims=NN):
    return lax.dot_general(a, b, dims, precision=precise, preferred_element_type=F32)


def parts_of(x, count):
    parts = []
    for n in range(count):
        parts.append(x.astype(jnp.bfloat16))
        if n + 1 < count:
            x = x - parts[-1].astype(F32)
    return parts


def fast_dot(a, b, dims=NN):
    return lax.dot_general(a, b, dims, preferred_element_type=F32)


def lanes(shape):
    return lax.broadcasted_iota(jnp.int32, shape, len(shape) - 1)


def roll(x, shift, axis=1):
    return pltpu.roll(x, shift, axis)


def prepare_kernel(
    place_ref, edge_hbm, pad_hbm, load_hbm, label_hbm, bump_hbm, across_hbm, down_hbm, pad_class_hbm,
    grid_ref, first_ref, last_ref, edge_ref, pad_ref, load_ref, load_end_ref, label_ref, across_ref, down_ref, pad_class_ref, done,
):
    copies = [
        pltpu.make_async_copy(source, target, done.at[n])
        for n, (source, target) in enumerate(
            (
                (edge_hbm, edge_ref),
                (pad_hbm, pad_ref),
                (across_hbm, across_ref),
                (down_hbm, down_ref),
                (pad_class_hbm, pad_class_ref),
                (label_hbm, label_ref),
                (bump_hbm, grid_ref.at[pl.ds(128, 128)]),
                (load_hbm.at[:, pl.ds(0, 8)], load_ref),
                (load_hbm.at[:, pl.ds(120, 8)], load_end_ref),
            )
        )
    ]
    for copy in copies:
        copy.start()
    for copy in copies:
        copy.wait()
    pr, pc = place_ref[0], place_ref[1]
    shape = (128, 128)
    row, lane = lax.broadcasted_iota(jnp.int32, shape, 0), lanes(shape)

    def lookup(table, classes):
        found = jnp.zeros(shape, F32)
        for n in range(8):
            found = jnp.where(classes == n, table[n], found)
        return found

    right = lookup(edge_ref, across_ref[...])
    down = lookup(edge_ref, down_ref[...])
    grid_ref[0:128] = label_ref[...].astype(F32)
    grid_ref[256:384] = jnp.where((lane == 127) & (pc == 7), 0.0, right)
    grid_ref[384:512] = jnp.where((row == 127) & (pr == 15), 0.0, down)
    grid_ref[512:640] = lookup(pad_ref, pad_class_ref[...])
    grid_ref[640:1024] = jnp.zeros((384, 128), F32)
    for n in range(HALO):
        first_ref[n, 0:32] = load_ref[:, n]
        first_ref[n, 32:40] = grid_ref[pl.ds(n, 8, stride=128), :]
        last_ref[n, 0:32] = load_end_ref[:, 8 - HALO + n]
        last_ref[n, 32:40] = grid_ref[pl.ds(128 - HALO + n, 8, stride=128), :]


def pack_kernel(load_ref, grid_ref, rows_ref, own_ref):
    lane = lanes((32, 128)) // 8

    def group(g, slots):
        loads, rest = jnp.zeros((32, 128), F32), jnp.zeros((8, 128), F32)
        for s in slots:
            r = 16 * g - 8 + s
            b = load_ref[pl.ds(r, 32, stride=128), :]
            rows_ref[r] = b
            loads = jnp.where(lane == s, roll(b, (8 * s + 3) % 128), loads)
            rest = jnp.where(lane[0:8] == s, roll(grid_ref[pl.ds(r, 8, stride=128), :], (8 * s + 3) % 128), rest)
        own_ref[g, 0:32] = loads
        own_ref[g, 32:40] = rest

    group(0, range(8, 16))
    group(8, range(8))

    def step(g, _):
        group(g, range(16))
        return 0

    lax.fori_loop(1, 8, step, 0)


def corner_kernel(own_ref, top_ref, bottom_ref, out_ref):
    lane = lanes((SUB, 128)) // 8
    for g in range(GROUPS):
        out_ref[g] = own_ref[g]
    start, end = own_ref[0], own_ref[8]
    for n in range(HALO):
        s = 8 - HALO + n
        start = jnp.where(lane == s, roll(top_ref[n], (8 * s + 3) % 128), start)
        s = 8 + n
        end = jnp.where(lane == s, roll(bottom_ref[n], (8 * s + 3) % 128), end)
    out_ref[0] = start
    out_ref[8] = end


def fields_kernel(
    place_ref, rows_ref, grid_ref, top_ref, bottom_ref, own_ref, left_ref, right_ref,
    first_ref, second_ref, w_ref, coef_ref, out_ref,
    ext, so, ss, sz_o, sz_s, y0_o, y0_s, qz, q0, q1, sc, y0, y1, gram,
):
    pr, pc = place_ref[0], place_ref[1]
    lane1 = lanes((1, 128))
    lane16 = lanes((16, 128))
    lane48 = lanes((48, 128))

    for n in range(5):
        ext[n, 0:16] = jnp.zeros((16, 128), F32)
        ext[n, 16:144] = grid_ref[128 * n : 128 * n + 128]
        ext[n, 144:160] = jnp.zeros((16, 128), F32)
        for k in range(HALO):
            ext[n, 16 - HALO + k : 17 - HALO + k] = top_ref[k, 32 + n : 33 + n]
            ext[n, 144 + k : 145 + k] = bottom_ref[k, 32 + n : 33 + n]

    slot = lax.broadcasted_iota(jnp.int32, (16, 128), 0)
    region_row = pr - 1 + slot // 4
    region_col = 2 * pc - 1 + slot % 4
    inside = (slot < 12) & (region_row >= 0) & (region_row < REG) & (region_col >= 0) & (region_col < REG)
    window = jnp.where(inside, region_row * REG + region_col, -1).astype(F32)

    for ref in (so, ss, sz_o, sz_s, y0_o, y0_s):
        ref[0] = jnp.zeros(ref.shape[1:], F32)
        ref[GROUPS + 1] = jnp.zeros(ref.shape[1:], F32)

    def pair_left(o, s, lane):
        j = lane % 8
        return roll(jnp.where(j == 2, s, o), 1), roll(jnp.where(j == 2, o, s), 1)

    def pair_right(o, s, lane):
        j = lane % 8
        return roll(jnp.where(j == 3, s, o), 127), roll(jnp.where(j == 3, o, s), 127)

    def above(before, here, lane):
        return roll(jnp.where(lane >= 120, before, here), 8)

    def below(here, after, lane):
        return roll(jnp.where(lane < 8, after, here), 120)

    def strips(g, _):
        o_row = own_ref[g]
        s_row = jnp.where(lanes((SUB, 128)) % 8 < 3, left_ref[g], right_ref[g])
        so[g + 1], ss[g + 1] = o_row, s_row
        lefts = pair_left(o_row[RIGHT : RIGHT + 1], s_row[RIGHT : RIGHT + 1], lane1)
        for side, (row, ref, ll) in enumerate(((o_row, so, lefts[0]), (s_row, ss, lefts[1]))):
            rl, dl = row[RIGHT : RIGHT + 1], row[DOWN : DOWN + 1]
            ul = above(ref[g, DOWN : DOWN + 1], dl, lane1)
            diag = row[PAD : PAD + 1] + rl + ll + dl + ul
            inv = jnp.where(diag > 0, 1.0 / diag, 0.0)
            for n, value in enumerate((diag, rl, ll, dl, ul, inv)):
                sc[side, g, n : n + 1] = value
            z = jnp.where(row[LAB : LAB + 1] == window, row[BUMP : BUMP + 1], 0.0)
            (sz_s if side else sz_o)[g + 1] = z
            if side:
                qz[2 * g] = z
                qz[2 * g + 1] = roll(z, 64)

        at = pl.multiple_of(16 * g + 8, 8)
        beside = jnp.zeros((16, 128), F32)
        for s in range(16):
            beside = jnp.where(slot == s, roll(s_row[RIGHT : RIGHT + 1], 125 - 8 * s), beside)
        rl, dl = ext[2, pl.ds(at, 16)], ext[3, pl.ds(at, 16)]
        ll = roll(jnp.where(lane16 == 127, beside, rl), 1)
        last = ext[3, pl.ds(pl.multiple_of(at - 8, 8), 8)]
        ul = jnp.where(slot == 0, last[7:8], roll(dl, 1, 0))
        diag = ext[4, pl.ds(at, 16)] + rl + ll + dl + ul
        inv = jnp.where(diag > 0, 1.0 / diag, 0.0)
        for n, value in enumerate((diag, rl, ll, dl, ul, inv)):
            coef_ref[n, pl.ds(at, 16)] = value
        return 0

    lax.fori_loop(0, GROUPS, strips, 0)

    def strip_image(ref_o, ref_s, g, lane, sides):
        o, s = ref_o[g + 1], ref_s[g + 1]
        lefts, rights = pair_left(o, s, lane), pair_right(o, s, lane)
        done = []
        for side in sides:
            ref, here = (ref_s, s) if side else (ref_o, o)
            up = above(ref[g], here, lane)
            down = below(here, ref[g + 2], lane)
            c = [sc[side, g, n : n + 1] for n in range(5)]
            done.append(c[0] * here - c[1] * rights[side] - c[2] * lefts[side] - c[3] * down - c[4] * up)
        return done

    def strip_first(g, _):
        w = strip_image(sz_o, sz_s, g, lane16, (0, 1))
        for side, (source, ref) in enumerate(((so, y0_o), (ss, y0_s))):
            inv = sc[side, g, 5:6]
            ref[g + 1, 0:32] = inv * source[g + 1, 0:32]
            ref[g + 1, 32:48] = inv * w[side]
        y = y0_s[g + 1]
        q0[2 * g] = y
        q0[2 * g + 1] = roll(y, 64)
        return 0

    lax.fori_loop(0, GROUPS, strip_first, 0)

    def strip_second(g, _):
        (u,) = strip_image(y0_o, y0_s, g, lane48, (1,))
        y = sc[1, g, 5:6] * u
        q1[2 * g] = y
        q1[2 * g + 1] = roll(y, 64)
        return 0

    lax.fori_loop(0, GROUPS, strip_second, 0)

    def passes(work, low, high):
        for s in range(8):
            if s - 8 >= low:
                work(0, s)

        def step(g, _):
            for s in range(8):
                work(g, s)
            return 0

        lax.fori_loop(1, 17, step, 0)
        for s in range(8):
            if 128 + s < high:
                work(17, s)

    def owned(g):
        return not isinstance(g, int)

    def coef(n, g, s):
        return coef_ref[n, pl.ds(8 * g + 8 + s, 1), :]

    def image(here, up, down, strip, g, s, lane):
        other = roll(strip[g], 125 - 8 * s)
        left = roll(jnp.where(lane == 127, other, here), 1)
        right = roll(jnp.where(lane == 0, other, here), 127)
        return (
            coef(0, g, s) * here
            - coef(1, g, s) * right
            - coef(2, g, s) * left
            - coef(3, g, s) * down
            - coef(4, g, s) * up
        )

    def basis(j):
        return jnp.where(ext[0, pl.ds(j, 1), :] == window, ext[1, pl.ds(j, 1), :], 0.0)

    def first_image(g, s):
        r, j = 8 * g - 8 + s, 8 * g + 8 + s
        w = image(basis(j), basis(j - 1), basis(j + 1), qz, g, s, lane16)
        if owned(g):
            b = rows_ref[r]
            w_ref[r] = w
        else:
            b = top_ref[r + HALO, 0:32] if r < 0 else bottom_ref[r - 128, 0:32]
        inv = coef(5, g, s)
        y0[8 * g + s, 0:32] = inv * b
        y0[8 * g + s, 32:48] = inv * w

    passes(first_image, -2, 130)

    def second_image(g, s):
        i = 8 * g + s
        f1 = image(y0[i], y0[i - 1], y0[i + 1], q0, g, s, lane48)
        if owned(g):
            first_ref[8 * g - 8 + s] = f1
        y1[i] = coef(5, g, s) * f1

    passes(second_image, -1, 129)

    gram[...] = jnp.zeros((96, 256), F32)

    def third_image(g, sums):
        left, every = [], []
        sums = list(sums)
        for s in range(8):
            i = 8 * g + s
            r = i - 8
            y0r, y1r = y0[i], y1[i]
            f2 = image(y1r, y1[i - 1], y1[i + 1], q1, g, s, lane48)
            second_ref[r] = f2
            b, f1 = rows_ref[r], first_ref[r]
            left.append(jnp.concatenate([basis(i + 8), y0r[32:48], y1r[32:48]], axis=0))
            every.append(jnp.concatenate([b, w_ref[r], f1, f2], axis=0))
            pairs = ((y0r, b), (y0r, f1), (y1r, f1), (y1r, f2))
            sums = [t + p[0:32] * q[0:32] for t, (p, q) in zip(sums, pairs)]
        left = jnp.concatenate(parts_of(jnp.concatenate(left, axis=1), 2), axis=0)
        high, low = parts_of(jnp.concatenate(every, axis=1), 2)
        gram[:, 0:144] += fast_dot(left, high, NT) + fast_dot(left, low, NT)
        return tuple(sums)

    zero = jnp.zeros((32, 128), F32)
    sums = lax.fori_loop(1, 17, third_image, (zero, zero, zero, zero))

    a0, a1 = gram[0:48, 0:128] + gram[48:96, 0:128], gram[0:48, 128:256] + gram[48:96, 128:256]
    zr, w0, t0, w1, t1 = a0[0:16], a0[16:32], a0[32:48], a1[16:32], a1[32:48]
    matrices = jnp.zeros((16, 128), F32)
    for n, (x, z) in enumerate(((w0, 32), (w0, 80), (w1, 0), (zr, 32), (t1, 0))):
        start = 24 * n
        matrices = jnp.where((lane16 >= start) & (lane16 < start + 16), roll(x, (start - z) % 128), matrices)
    moved = jnp.zeros((16, 128), F32)
    for k in range(12):
        moved = jnp.where(slot == k, roll(matrices, (128 - k) % 128), moved)
    common = jnp.zeros((16, 128), F32)
    for n in range(5):
        start = 20 + 6 * n
        common = jnp.where((lane16 >= start) & (lane16 < start + 6), roll(moved, (start - 24 * n) % 128), common)
    lines = []
    diagonal = lanes((32, 128)) == lax.broadcasted_iota(jnp.int32, (32, 128), 0)
    for total in sums:
        column = jnp.sum(total, axis=1, keepdims=True)
        lines.append(jnp.sum(jnp.where(diagonal, column, 0.0), axis=0, keepdims=True))
    lane8, row8 = lanes((8, 128)), lax.broadcasted_iota(jnp.int32, (8, 128), 0)
    for d in range(8):
        message = common
        for n, (x, z) in enumerate(((w0, 0), (w0, 48), (w0, 96), (zr, 0), (t0, 96))):
            hit = (lane16 >= 4 * n) & (lane16 < 4 * n + 4)
            message = jnp.where(hit, roll(x, (4 * n - z - 4 * d) % 128), message)
        upper = roll(roll(message, 10, 0), 64)
        sent = jnp.where(lane8 < 64, message[0:8], upper[0:8])
        line = jnp.zeros((1, 128), F32)
        for n in range(4):
            line = jnp.where((lane1 >= 4 * n) & (lane1 < 4 * n + 4), roll(lines[n], (4 * n - 4 * d) % 128), line)
        out_ref[8 * d : 8 * d + 8] = jnp.where(row8 < 6, sent, jnp.where(row8 == 6, line, 0.0))


def batched_inverse(a, lane, row):
    base = lane - lane % 16
    for k in range(0, 16, 2):
        at_k, at_n = lane % 16 == k, lane % 16 == k + 1
        left = jnp.take_along_axis(a, base + k, axis=1)
        right = jnp.take_along_axis(a, base + k + 1, axis=1)
        p, q, r, t = left[k : k + 1], right[k : k + 1], left[k + 1 : k + 2], right[k + 1 : k + 2]
        inverse = 1.0 / (p * t - q * r)
        upper = jnp.where(at_k[0:1], 1.0, jnp.where(at_n[0:1], 0.0, a[k : k + 1]))
        lower = jnp.where(at_n[0:1], 1.0, jnp.where(at_k[0:1], 0.0, a[k + 1 : k + 2]))
        first = (t * upper - q * lower) * inverse
        second = (p * lower - r * upper) * inverse
        rest = jnp.where(at_k | at_n, 0.0, a) - left * first - right * second
        a = jnp.where(row == k, first, jnp.where(row == k + 1, second, rest))
    return a


def block_inverse(matrix, low, high):
    lane = lanes((16, 128))
    row = lax.broadcasted_iota(jnp.int32, (16, 128), 0)
    compact = jnp.where(lane % 16 == row, 1.0, 0.0)
    for n in range(low // 16, high // 16):
        compact = jnp.where(lane // 16 == n, matrix[16 * n : 16 * n + 16], compact)
    compact = batched_inverse(compact, lane, row)
    parts = []
    for n in range(8):
        active = low <= 16 * n < high
        parts.append(jnp.where(lane // 16 == n, compact, 0.0) if active else jnp.zeros((16, 128), F32))
    return jnp.concatenate(parts, axis=0)


def coarse_kernel(place_ref, in_ref, out_ref, g, e, ei, first, second, near):
    pr, pc = place_ref[0], place_ref[1]
    sub8 = lax.broadcasted_iota(jnp.int32, (8, 128), 0)

    for p in range(16):
        sums = {}
        for dr in range(3):
            r = p + 1 - dr
            if not 0 <= r < 16:
                continue
            for dq in range(4):
                k = 4 * dr + dq
                piece = in_ref[pl.ds(64 * r + k % 6, 8, stride=8), :]
                if dq == 0:
                    piece = jnp.where(sub8 < 7, roll(piece, 7, 0), 0.0)
                elif dq == 3:
                    piece = jnp.where(sub8 >= 1, roll(piece, 1, 0), 0.0)
                key = ((dq + 1) % 2, k >= 6)
                sums[key] = sums[key] + piece if key in sums else piece
        for par in range(2):
            total = jnp.zeros((8, 128), F32)
            if (par, False) in sums:
                total = total + sums[par, False]
            if (par, True) in sums:
                total = total + roll(sums[par, True], 64)
            g[pl.ds(16 * p + par, 8, stride=2), :] = total
    tally = jnp.sum(in_ref[pl.ds(6, 128, stride=8), :], axis=0, keepdims=True)
    tally = jnp.broadcast_to(tally, (128, 128)).T
    bb, bu, uu, uuu = (tally[4 * n : 4 * n + 4, 0:1] for n in range(4))
    by_lane = jnp.concatenate([g[0:128].T, g[128:256].T], axis=1)

    lane16, row16 = lanes((16, 128)), lax.broadcasted_iota(jnp.int32, (16, 128), 0)
    base = 20 + 6 * 3
    for p in range(16):
        own = g[16 * p : 16 * p + 16]
        terms = [(own, d, dp, dq) for d, dp, dq in ((0, 0, 0), (1, 0, 1))]
        terms.append((roll(own, 1, 0), 1, 0, -1))
        if p < 15:
            terms += [(own, d, 1, dq) for d, dq in ((3, -1), (4, 0), (5, 1))]
        if p > 0:
            last = g[16 * p - 16 : 16 * p]
            terms += [(roll(last, 15, 0), 3, -1, 1), (last, 4, -1, 0), (roll(last, 1, 0), 5, -1, -1)]
        halves = [jnp.zeros((16, 128), F32), jnp.zeros((16, 128), F32)]
        for x, d, dp, dq in terms:
            target = POS[p + dp] * 16
            h, off = target // 128, target % 128
            q = row16 + dq
            hit = (lane16 == off + q) & (q >= 0) & (q < 16)
            value = jnp.broadcast_to(x[:, base + d : base + d + 1], (16, 128))
            halves[h] = jnp.where(hit, value, halves[h])
        at = POS[p] * 16
        e[at : at + 16, 0:128] = halves[0]
        e[at : at + 16, 128:256] = halves[1]

    lane = lanes((128, 128))
    row = lax.broadcasted_iota(jnp.int32, (128, 128), 0)
    outer = block_inverse(e[0:128, 0:128], 0, 128)
    across = dot(outer, e[0:128, 128:256])
    schur = e[128:256, 128:256] - dot(e[128:256, 0:128], across)
    steps = []
    for low, high in ((0, 64), (64, 96), (96, 112)):
        inv = block_inverse(schur, low, high)
        link = jnp.where((row >= low) & (row < high) & (lane >= high), schur, 0.0)
        x = dot(inv, link)
        keep = jnp.where((row >= high) & (lane >= high), schur, 0.0)
        schur = keep - dot(link, x, TN)
        steps.append((inv, jnp.where((row == lane) & (row >= high), 1.0, 0.0) - x))
    inner = block_inverse(schur, 112, 128)
    for inv, y in reversed(steps):
        inner = inv + dot(dot(y, inner), y, NT)
    half = dot(across, inner)
    near_diag = outer + dot(half, across, NT)

    def ordered(top_half, bottom_half):
        blocks = [top_half[16 * n : 16 * n + 16] for n in range(8)]
        blocks += [bottom_half[16 * n : 16 * n + 16] for n in range(8)]
        blocks = [blocks[POS[p]] for p in range(16)]
        return jnp.concatenate(blocks[:8], axis=0), jnp.concatenate(blocks[8:], axis=0)

    left_top, left_bottom = ordered(near_diag, -half.T)
    right_top, right_bottom = ordered(-half, inner)
    top_left, bottom_left = ordered(left_top.T, right_top.T)
    top_right, bottom_right = ordered(left_bottom.T, right_bottom.T)
    ei[0:128, 0:128] = top_left
    ei[0:128, 128:256] = top_right
    ei[128:256, 0:128] = bottom_left
    ei[128:256, 128:256] = bottom_right

    def solve(z):
        return dot(z, ei[...])

    def apply(n, v):
        c = [by_lane[20 + 6 * n + d : 21 + 6 * n + d] for d in range(6)]
        total = c[0] * v
        for d, step in ((1, 1), (3, 15), (4, 16), (5, 17)):
            total = total + c[d] * roll(v, 256 - step) + roll(c[d] * v, step)
        return total

    def inner_product(a, b):
        return jnp.sum(a * b, axis=1, keepdims=True)

    wb, wu, wuu, zb, tuu = (by_lane[4 * n : 4 * n + 4] for n in range(5))
    c0 = solve(zb)
    f_c, g_c, h_c, k_c = apply(0, c0), apply(1, c0), apply(2, c0), apply(4, c0)
    grad0 = wb - f_c
    k0 = solve(grad0)
    f_k, g_k = apply(0, k0), apply(1, k0)
    rho0 = bb - 2.0 * inner_product(c0, wb) + inner_product(c0, f_c)
    energy0 = bu - 2.0 * inner_product(c0, wu) + inner_product(c0, g_c)
    curve0 = energy0 - inner_product(k0, grad0)
    a0 = rho0 / curve0
    e1 = c0 - a0 * k0
    f_e = f_c - a0 * f_k
    g_e = g_c - a0 * g_k
    grad1 = wb - f_e + a0 * (g_c - wu)
    k1 = solve(grad1)

    def second_norm(m0, m1, m2, v0, v1, v2, e_image, c_image, last):
        own = m0 - 2.0 * inner_product(e1, v0) + inner_product(e1, e_image)
        mixed = m1 - inner_product(c0, v1) - inner_product(e1, v1) + inner_product(e1, c_image)
        far = m2 - 2.0 * inner_product(c0, v2) + inner_product(c0, last)
        return own - 2.0 * a0 * mixed + a0 * a0 * far

    rho1 = second_norm(bb, bu, uu, wb, wu, wuu, f_e, g_c, h_c)
    energy1 = second_norm(bu, uu, uuu, wu, wuu, tuu, g_e, h_c, k_c)
    beta = rho1 / rho0
    cross = (
        bu
        - inner_product(c0, wu)
        - inner_product(e1, wu)
        + inner_product(e1, g_c)
        - a0 * (uu - 2.0 * inner_product(c0, wuu) + inner_product(c0, h_c))
        - inner_product(k0, grad1)
    )
    curve1 = energy1 - inner_product(k1, grad1) + 2.0 * beta * cross + beta * beta * curve0
    a1 = rho1 / curve1

    mine = lax.broadcasted_iota(jnp.int32, (32, 256), 0) // 4 == pc

    def zone(value):
        value = jnp.broadcast_to(value, (4, 256))
        return jnp.where(mine, jnp.concatenate([value] * 8, axis=0), 0.0)

    ab = a1 * beta
    stacks = (
        (
            zone(a1 * k1 + ab * k0 - e1),
            zone(-(a0 + ab) * c0 - a1 * e1),
            zone((a0 + ab) * c0 + a1 * e1),
            zone((a1 * a0) * c0),
        ),
        (
            zone(-(a1 * a0) * c0),
            zone(c0 - (a0 + ab) * k0 - a1 * k1),
            zone(-a0 - a1 - ab),
            zone(a1 * a0),
        ),
    )
    out_ref[...] = jnp.zeros((256, 128), F32)
    for n, (ref, stack) in enumerate(((first, stacks[0]), (second, stacks[1]))):
        stack = jnp.concatenate(stack, axis=0)
        ref[0:8] = jnp.zeros((8, 128), F32)
        ref[8:136] = stack[:, 0:128].T
        ref[136:264] = stack[:, 128:256].T
        ref[264:272] = jnp.zeros((8, 128), F32)
        for dr in range(3):
            p = jnp.clip(pr - 1 + dr, 0, 15)
            near[...] = ref[pl.ds(pl.multiple_of(16 * p, 16), 32), :]
            for dq in range(4):
                out_ref[pl.ds(16 * n + 4 * dr + dq, 8, stride=32), :] = near[pl.ds(7 + dq, 8, stride=2), :]


def outputs_kernel(
    place_ref, rows_ref, first_ref, second_ref, w_ref, grid_ref, coef_ref, m_ref, sol_ref, res_ref,
    left_ref, step_ref, window_ref,
):
    block = pl.program_id(0)

    @pl.when(block == 0)
    def _():
        pr, pc = place_ref[0], place_ref[1]
        slot = lax.broadcasted_iota(jnp.int32, (16, 128), 0)
        region_row = pr - 1 + slot // 4
        region_col = 2 * pc - 1 + slot % 4
        inside = (slot < 12) & (region_row >= 0) & (region_row < REG) & (region_col >= 0) & (region_col < REG)
        window_ref[...] = jnp.where(inside, region_row * REG + region_col, -1).astype(F32)
        total = m_ref[0:32]
        for n in range(1, 8):
            total = total + m_ref[32 * n : 32 * n + 32]
        top, bottom = total[0:16], total[16:32]
        lane = lanes((16, 128))
        steps = jnp.where(slot == 0, roll(bottom[5:6], 64), jnp.where(slot == 1, roll(bottom[5:6], 32), 0.0))
        m = jnp.concatenate(
            [
                jnp.where((lane >= 64) & (lane < 96), roll(bottom, 32), 0.0),
                jnp.where(lane < 64, top, 0.0),
                jnp.where(lane < 64, roll(top, 64), 0.0),
                jnp.where(lane < 32, bottom, 0.0),
                steps,
                jnp.zeros((48, 128), F32),
            ],
            axis=0,
        ).T
        c1, c2, c3 = parts_of(m[0:96, 0:64], 3)
        left_ref[...] = jnp.concatenate([c1, c1, c2, c2, c1, c3], axis=1)
        for n in range(2):
            step_ref[n] = jnp.broadcast_to(m[0:32, 64 + n : 65 + n], (32, 128))

    left, window = left_ref[...], window_ref[...]
    for part in range(2):
        rows = []
        for n in range(8):
            r = 16 * block + 8 * part + n
            z = jnp.where(grid_ref[pl.ds(r, 1), :] == window, grid_ref[pl.ds(128 + r, 1), :], 0.0)
            rows.append(jnp.concatenate([z, w_ref[r], first_ref[r, 32:48], second_ref[r, 32:48]], axis=0))
        r1, r2, r3 = parts_of(jnp.concatenate(rows, axis=1), 3)
        d = fast_dot(left, jnp.concatenate([r1, r2, r1, r2, r3, r1], axis=0))
        for n in range(8):
            r = 16 * block + 8 * part + n
            b, u, uu = rows_ref[r], first_ref[r, 0:32], second_ref[r, 0:32]
            e = d[:, 128 * n : 128 * n + 128]
            inv = coef_ref[5, pl.ds(r + 16, 1), :]
            p1, p2 = step_ref[0], step_ref[1]
            res_ref[:, 8 * part + n] = b + p1 * u + p2 * uu + e[0:32]
            sol_ref[:, 8 * part + n] = inv * (e[32:64] - p1 * b - p2 * u) + e[64:96]


def shape_of(*dims):
    return jax.ShapeDtypeStruct(dims, F32)


def kept(*dims):
    return pltpu.VMEM(dims, F32)


def vmem(*dims):
    return pltpu.VMEM(dims, F32)


def body(load_currents, labels, bump_height, horizontal_class, vertical_class, pad_class, edge_table, pad_table):
    pr, pc = lax.axis_index(ROW), lax.axis_index(COL)
    rows, cols = lax.axis_size(ROW), lax.axis_size(COL)
    place = jnp.stack([pr, pc]).astype(jnp.int32)
    loads = load_currents.reshape(-1, 128)
    grid, first_rows, last_rows = pl.pallas_call(
        prepare_kernel,
        out_shape=(kept(1024, 128), shape_of(HALO, SUB, 128), shape_of(HALO, SUB, 128)),
        compiler_params=limited,
        in_specs=[scalars] + [outside] * 8,
        out_specs=(whole,) * 3,
        scratch_shapes=[pltpu.SMEM((8,), F32), pltpu.SMEM((8,), F32), vmem(32, 8, 128), vmem(32, 8, 128)]
        + [pltpu.VMEM((128, 128), jnp.int32)] * 4
        + [pltpu.SemaphoreType.DMA((9,))],
    )(
        place,
        *(
            pltpu.with_memory_space_constraint(x, pltpu.HBM)
            for x in (
                edge_table, pad_table, load_currents, labels, bump_height,
                horizontal_class, vertical_class, pad_class,
            )
        ),
    )
    down = [(i, i + 1) for i in range(rows - 1)]
    bottom = lax.ppermute(first_rows, ROW, [(b, a) for a, b in down])
    top = lax.ppermute(last_rows, ROW, down)
    by_rows, own = pl.pallas_call(
        pack_kernel,
        out_shape=(kept(128, 32, 128), kept(GROUPS, SUB, 128)),
        compiler_params=limited,
        in_specs=[whole] * 2,
        out_specs=(whole,) * 2,
    )(loads, grid)
    own = pl.pallas_call(
        corner_kernel, out_shape=shape_of(GROUPS, SUB, 128), in_specs=[whole] * 3, out_specs=whole, compiler_params=limited
    )(own, top, bottom)
    right = [(i, i + 1) for i in range(cols - 1)]
    beside_left = lax.ppermute(own, COL, right)
    beside_right = lax.ppermute(own, COL, [(b, a) for a, b in right])
    first, second, w, coef, payload = pl.pallas_call(
        fields_kernel,
        out_shape=(
            kept(128, 48, 128),
            kept(128, 48, 128),
            kept(128, 16, 128),
            kept(6, 160, 128),
            shape_of(64, 128),
        ),
        compiler_params=limited,
        in_specs=[scalars] + [whole] * 7,
        out_specs=(whole,) * 5,
        scratch_shapes=[
            vmem(5, 160, 128),
            vmem(GROUPS + 2, SUB, 128),
            vmem(GROUPS + 2, SUB, 128),
            vmem(GROUPS + 2, 16, 128),
            vmem(GROUPS + 2, 16, 128),
            vmem(GROUPS + 2, 48, 128),
            vmem(GROUPS + 2, 48, 128),
            vmem(2 * GROUPS, 16, 128),
            vmem(2 * GROUPS, 48, 128),
            vmem(2 * GROUPS, 48, 128),
            vmem(2, GROUPS, 8, 128),
            vmem(144, 48, 128),
            vmem(144, 48, 128),
            vmem(96, 256),
        ],
    )(place, by_rows, grid, top, bottom, own, beside_left, beside_right)
    sent = jnp.broadcast_to(payload.reshape(1, cols, 8, 128), (rows, cols, 8, 128)).reshape(-1, 8, 128)
    everything = lax.all_to_all(sent, ROW + COL, 0, 0, tiled=True).reshape(-1, 128)
    found = pl.pallas_call(
        coarse_kernel,
        out_shape=shape_of(256, 128),
        compiler_params=limited,
        in_specs=[scalars, whole],
        out_specs=whole,
        scratch_shapes=[
            vmem(256, 128),
            vmem(256, 256),
            vmem(256, 256),
            vmem(272, 128),
            vmem(272, 128),
            vmem(32, 128),
        ],
    )(place, everything)
    matrix = lax.all_to_all(found.reshape(cols, 32, 128), COL, 0, 0, tiled=True).reshape(-1, 128)
    by_block = pl.BlockSpec((32, 16, 128), lambda k: (0, k, 0))
    return pl.pallas_call(
        outputs_kernel,
        grid=(8,),
        out_shape=(shape_of(32, 128, 128), shape_of(32, 128, 128)),
        compiler_params=limited,
        in_specs=[scalars] + [whole] * 7,
        out_specs=(by_block, by_block),
        scratch_shapes=[pltpu.VMEM((96, 384), jnp.bfloat16), vmem(2, 32, 128), vmem(16, 128)],
    )(place, by_rows, first, second, w, grid, coef, matrix)


def solution(mesh):
    finer = Mesh(mesh.devices.reshape(4, 4, 4, 2), ("row_0", "row_1", "col_0", "col_1"))
    grid = P(ROW, COL)
    return jax.shard_map(
        body,
        mesh=finer,
        in_specs=(P(None, ROW, COL), grid, grid, grid, grid, grid, P(), P()),
        out_specs=(P(None, ROW, COL), P(None, ROW, COL)),
        check_vma=False,
    )
```

```python
import jax
import jax.numpy as jnp
from jax import lax
from jax.experimental import pallas as pl
from jax.experimental.pallas import tpu as pltpu
from jax.sharding import Mesh
from jax.sharding import PartitionSpec as P

REG = 16
ROW = ("row_0", "row_1")
COL = ("col_0", "col_1")
F32 = jnp.float32
precise = lax.Precision.HIGHEST

LAB, BUMP, RIGHT, DOWN, PAD = 32, 33, 34, 35, 36
SUB = 40
HALO = 3
GROUPS = 9
ORDER = (1, 3, 5, 7, 9, 11, 13, 15, 2, 6, 10, 14, 4, 12, 8, 0)
POS = tuple(ORDER.index(p) for p in range(16))
NT = (((1,), (1,)), ((), ()))
NN = (((1,), (0,)), ((), ()))
TN = (((0,), (0,)), ((), ()))
whole = pl.BlockSpec(memory_space=pltpu.VMEM)
outside = pl.BlockSpec(memory_space=pltpu.HBM)
limited = pltpu.CompilerParams(vmem_limit_bytes=32 * 2**20)
scalars = pl.BlockSpec(memory_space=pltpu.SMEM)


def dot(a, b, dims=NN):
    return lax.dot_general(a, b, dims, precision=precise, preferred_element_type=F32)


def parts_of(x, count):
    parts = []
    for n in range(count):
        parts.append(x.astype(jnp.bfloat16))
        if n + 1 < count:
            x = x - parts[-1].astype(F32)
    return parts


def fast_dot(a, b, dims=NN):
    return lax.dot_general(a, b, dims, preferred_element_type=F32)


def lanes(shape):
    return lax.broadcasted_iota(jnp.int32, shape, len(shape) - 1)


def roll(x, shift, axis=1):
    return pltpu.roll(x, shift, axis)


def prepare_kernel(
    place_ref, edge_hbm, pad_hbm, load_hbm, label_hbm, bump_hbm, across_hbm, down_hbm, pad_class_hbm,
    grid_ref, first_ref, last_ref, edge_ref, pad_ref, load_ref, load_end_ref, label_ref, across_ref, down_ref, pad_class_ref, done,
):
    copies = [
        pltpu.make_async_copy(source, target, done.at[n])
        for n, (source, target) in enumerate(
            (
                (edge_hbm, edge_ref),
                (pad_hbm, pad_ref),
                (across_hbm, across_ref),
                (down_hbm, down_ref),
                (pad_class_hbm, pad_class_ref),
                (label_hbm, label_ref),
                (bump_hbm, grid_ref.at[pl.ds(128, 128)]),
                (load_hbm.at[:, pl.ds(0, 8)], load_ref),
                (load_hbm.at[:, pl.ds(120, 8)], load_end_ref),
            )
        )
    ]
    for copy in copies:
        copy.start()
    for copy in copies:
        copy.wait()
    pr, pc = place_ref[0], place_ref[1]
    shape = (128, 128)
    row, lane = lax.broadcasted_iota(jnp.int32, shape, 0), lanes(shape)

    def lookup(table, classes):
        found = jnp.zeros(shape, F32)
        for n in range(8):
            found = jnp.where(classes == n, table[n], found)
        return found

    right = lookup(edge_ref, across_ref[...])
    down = lookup(edge_ref, down_ref[...])
    grid_ref[0:128] = label_ref[...].astype(F32)
    grid_ref[256:384] = jnp.where((lane == 127) & (pc == 7), 0.0, right)
    grid_ref[384:512] = jnp.where((row == 127) & (pr == 15), 0.0, down)
    grid_ref[512:640] = lookup(pad_ref, pad_class_ref[...])
    grid_ref[640:1024] = jnp.zeros((384, 128), F32)
    for n in range(HALO):
        first_ref[n, 0:32] = load_ref[:, n]
        first_ref[n, 32:40] = grid_ref[pl.ds(n, 8, stride=128), :]
        last_ref[n, 0:32] = load_end_ref[:, 8 - HALO + n]
        last_ref[n, 32:40] = grid_ref[pl.ds(128 - HALO + n, 8, stride=128), :]


def pack_kernel(load_ref, grid_ref, rows_ref, own_ref):
    lane = lanes((32, 128)) // 8

    def group(g, slots):
        loads, rest = jnp.zeros((32, 128), F32), jnp.zeros((8, 128), F32)
        for s in slots:
            r = 16 * g - 8 + s
            b = load_ref[pl.ds(r, 32, stride=128), :]
            rows_ref[r] = b
            loads = jnp.where(lane == s, roll(b, (8 * s + 3) % 128), loads)
            rest = jnp.where(lane[0:8] == s, roll(grid_ref[pl.ds(r, 8, stride=128), :], (8 * s + 3) % 128), rest)
        own_ref[g, 0:32] = loads
        own_ref[g, 32:40] = rest

    group(0, range(8, 16))
    group(8, range(8))

    def step(g, _):
        group(g, range(16))
        return 0

    lax.fori_loop(1, 8, step, 0)


def corner_kernel(own_ref, top_ref, bottom_ref, out_ref):
    lane = lanes((SUB, 128)) // 8
    for g in range(GROUPS):
        out_ref[g] = own_ref[g]
    start, end = own_ref[0], own_ref[8]
    for n in range(HALO):
        s = 8 - HALO + n
        start = jnp.where(lane == s, roll(top_ref[n], (8 * s + 3) % 128), start)
        s = 8 + n
        end = jnp.where(lane == s, roll(bottom_ref[n], (8 * s + 3) % 128), end)
    out_ref[0] = start
    out_ref[8] = end


def fields_kernel(
    place_ref, rows_ref, grid_ref, top_ref, bottom_ref, own_ref, left_ref, right_ref,
    first_ref, second_ref, w_ref, coef_ref, out_ref,
    ext, so, ss, sz_o, sz_s, y0_o, y0_s, qz, q0, q1, sc, y0, y1, gram,
):
    pr, pc = place_ref[0], place_ref[1]
    lane1 = lanes((1, 128))
    lane16 = lanes((16, 128))
    lane48 = lanes((48, 128))

    for n in range(5):
        ext[n, 0:16] = jnp.zeros((16, 128), F32)
        ext[n, 16:144] = grid_ref[128 * n : 128 * n + 128]
        ext[n, 144:160] = jnp.zeros((16, 128), F32)
        for k in range(HALO):
            ext[n, 16 - HALO + k : 17 - HALO + k] = top_ref[k, 32 + n : 33 + n]
            ext[n, 144 + k : 145 + k] = bottom_ref[k, 32 + n : 33 + n]

    slot = lax.broadcasted_iota(jnp.int32, (16, 128), 0)
    region_row = pr - 1 + slot // 4
    region_col = 2 * pc - 1 + slot % 4
    inside = (slot < 12) & (region_row >= 0) & (region_row < REG) & (region_col >= 0) & (region_col < REG)
    window = jnp.where(inside, region_row * REG + region_col, -1).astype(F32)

    for ref in (so, ss, sz_o, sz_s, y0_o, y0_s):
        ref[0] = jnp.zeros(ref.shape[1:], F32)
        ref[GROUPS + 1] = jnp.zeros(ref.shape[1:], F32)

    def pair_left(o, s, lane):
        j = lane % 8
        return roll(jnp.where(j == 2, s, o), 1), roll(jnp.where(j == 2, o, s), 1)

    def pair_right(o, s, lane):
        j = lane % 8
        return roll(jnp.where(j == 3, s, o), 127), roll(jnp.where(j == 3, o, s), 127)

    def above(before, here, lane):
        return roll(jnp.where(lane >= 120, before, here), 8)

    def below(here, after, lane):
        return roll(jnp.where(lane < 8, after, here), 120)

    def strips(g, _):
        o_row = own_ref[g]
        s_row = jnp.where(lanes((SUB, 128)) % 8 < 3, left_ref[g], right_ref[g])
        so[g + 1], ss[g + 1] = o_row, s_row
        lefts = pair_left(o_row[RIGHT : RIGHT + 1], s_row[RIGHT : RIGHT + 1], lane1)
        for side, (row, ref, ll) in enumerate(((o_row, so, lefts[0]), (s_row, ss, lefts[1]))):
            rl, dl = row[RIGHT : RIGHT + 1], row[DOWN : DOWN + 1]
            ul = above(ref[g, DOWN : DOWN + 1], dl, lane1)
            diag = row[PAD : PAD + 1] + rl + ll + dl + ul
            inv = jnp.where(diag > 0, 1.0 / diag, 0.0)
            for n, value in enumerate((diag, rl, ll, dl, ul, inv)):
                sc[side, g, n : n + 1] = value
            z = jnp.where(row[LAB : LAB + 1] == window, row[BUMP : BUMP + 1], 0.0)
            (sz_s if side else sz_o)[g + 1] = z
            if side:
                qz[2 * g] = z
                qz[2 * g + 1] = roll(z, 64)

        at = pl.multiple_of(16 * g + 8, 8)
        beside = jnp.zeros((16, 128), F32)
        for s in range(16):
            beside = jnp.where(slot == s, roll(s_row[RIGHT : RIGHT + 1], 125 - 8 * s), beside)
        rl, dl = ext[2, pl.ds(at, 16)], ext[3, pl.ds(at, 16)]
        ll = roll(jnp.where(lane16 == 127, beside, rl), 1)
        last = ext[3, pl.ds(pl.multiple_of(at - 8, 8), 8)]
        ul = jnp.where(slot == 0, last[7:8], roll(dl, 1, 0))
        diag = ext[4, pl.ds(at, 16)] + rl + ll + dl + ul
        inv = jnp.where(diag > 0, 1.0 / diag, 0.0)
        for n, value in enumerate((diag, rl, ll, dl, ul, inv)):
            coef_ref[n, pl.ds(at, 16)] = value
        return 0

    lax.fori_loop(0, GROUPS, strips, 0, unroll=3)

    def strip_image(ref_o, ref_s, g, lane, sides):
        o, s = ref_o[g + 1], ref_s[g + 1]
        lefts, rights = pair_left(o, s, lane), pair_right(o, s, lane)
        done = []
        for side in sides:
            ref, here = (ref_s, s) if side else (ref_o, o)
            up = above(ref[g], here, lane)
            down = below(here, ref[g + 2], lane)
            c = [sc[side, g, n : n + 1] for n in range(5)]
            done.append(c[0] * here - c[1] * rights[side] - c[2] * lefts[side] - c[3] * down - c[4] * up)
        return done

    def strip_first(g, _):
        w = strip_image(sz_o, sz_s, g, lane16, (0, 1))
        for side, (source, ref) in enumerate(((so, y0_o), (ss, y0_s))):
            inv = sc[side, g, 5:6]
            ref[g + 1, 0:32] = inv * source[g + 1, 0:32]
            ref[g + 1, 32:48] = inv * w[side]
        y = y0_s[g + 1]
        q0[2 * g] = y
        q0[2 * g + 1] = roll(y, 64)
        return 0

    lax.fori_loop(0, GROUPS, strip_first, 0, unroll=3)

    def strip_second(g, _):
        (u,) = strip_image(y0_o, y0_s, g, lane48, (1,))
        y = sc[1, g, 5:6] * u
        q1[2 * g] = y
        q1[2 * g + 1] = roll(y, 64)
        return 0

    lax.fori_loop(0, GROUPS, strip_second, 0, unroll=3)

    def owned(g):
        return not isinstance(g, int)

    def coef(n, g, s):
        return coef_ref[n, pl.ds(8 * g + 8 + s, 1), :]

    def image(here, up, down, strip, g, s, lane):
        other = roll(strip[g], 125 - 8 * s)
        left = roll(jnp.where(lane == 127, other, here), 1)
        right = roll(jnp.where(lane == 0, other, here), 127)
        return (
            coef(0, g, s) * here
            - coef(1, g, s) * right
            - coef(2, g, s) * left
            - coef(3, g, s) * down
            - coef(4, g, s) * up
        )

    def basis(j):
        return jnp.where(ext[0, pl.ds(j, 1), :] == window, ext[1, pl.ds(j, 1), :], 0.0)

    def first_image(g, s):
        r, j = 8 * g - 8 + s, 8 * g + 8 + s
        w = image(basis(j), basis(j - 1), basis(j + 1), qz, g, s, lane16)
        if owned(g):
            b = rows_ref[r]
            w_ref[r] = w
        else:
            b = top_ref[r + HALO, 0:32] if r < 0 else bottom_ref[r - 128, 0:32]
        inv = coef(5, g, s)
        y0[8 * g + s, 0:32] = inv * b
        y0[8 * g + s, 32:48] = inv * w

    def second_image(g, s):
        i = 8 * g + s
        f1 = image(y0[i], y0[i - 1], y0[i + 1], q0, g, s, lane48)
        if owned(g):
            first_ref[8 * g - 8 + s] = f1
        y1[i] = coef(5, g, s) * f1

    def both(g, _):
        for s in range(8):
            second_image(g - 2, s)
        for s in range(8):
            first_image(g, s)
        return 0

    def only(work):
        def step(g, _):
            for s in range(8):
                work(g, s)
            return 0

        return step

    for s in (6, 7):
        first_image(0, s)
    lax.fori_loop(1, 3, only(first_image), 0)
    second_image(0, 7)
    lax.fori_loop(3, 17, both, 0)
    for s in (0, 1):
        first_image(17, s)
    lax.fori_loop(15, 17, only(second_image), 0)
    second_image(17, 0)

    gram[...] = jnp.zeros((96, 256), F32)

    def third_image(g, s):
        i = 8 * g + s
        second_ref[i - 8] = image(y1[i], y1[i - 1], y1[i + 1], q1, g, s, lane48)

    def products(g, sums):
        left, every = [], []
        sums = list(sums)
        for s in range(8):
            i = 8 * g + s
            r = i - 8
            b, f1, f2, y0r, y1r = rows_ref[r], first_ref[r], second_ref[r], y0[i], y1[i]
            left.append(jnp.concatenate([basis(i + 8), y0r[32:48], y1r[32:48]], axis=0))
            every.append(jnp.concatenate([b, w_ref[r], f1, f2], axis=0))
            pairs = ((y0r, b), (y0r, f1), (y1r, f1), (y1r, f2))
            sums = [t + p[0:32] * q[0:32] for t, (p, q) in zip(sums, pairs)]
        left = jnp.concatenate(parts_of(jnp.concatenate(left, axis=1), 2), axis=0)
        high, low = parts_of(jnp.concatenate(every, axis=1), 2)
        gram[:, 0:144] += fast_dot(left, high, NT) + fast_dot(left, low, NT)
        return tuple(sums)

    def last_stage(g, sums):
        sums = products(g - 1, sums)
        for s in range(8):
            third_image(g, s)
        return sums

    zero = jnp.zeros((32, 128), F32)
    lax.fori_loop(1, 2, only(third_image), 0)
    sums = lax.fori_loop(2, 17, last_stage, (zero, zero, zero, zero))
    sums = lax.fori_loop(16, 17, products, sums)

    a0, a1 = gram[0:48, 0:128] + gram[48:96, 0:128], gram[0:48, 128:256] + gram[48:96, 128:256]
    zr, w0, t0, w1, t1 = a0[0:16], a0[16:32], a0[32:48], a1[16:32], a1[32:48]
    matrices = jnp.zeros((16, 128), F32)
    for n, (x, z) in enumerate(((w0, 32), (w0, 80), (w1, 0), (zr, 32), (t1, 0))):
        start = 24 * n
        matrices = jnp.where((lane16 >= start) & (lane16 < start + 16), roll(x, (start - z) % 128), matrices)
    moved = jnp.zeros((16, 128), F32)
    for k in range(12):
        moved = jnp.where(slot == k, roll(matrices, (128 - k) % 128), moved)
    common = jnp.zeros((16, 128), F32)
    for n in range(5):
        start = 20 + 6 * n
        common = jnp.where((lane16 >= start) & (lane16 < start + 6), roll(moved, (start - 24 * n) % 128), common)
    lines = []
    diagonal = lanes((32, 128)) == lax.broadcasted_iota(jnp.int32, (32, 128), 0)
    for total in sums:
        column = jnp.sum(total, axis=1, keepdims=True)
        lines.append(jnp.sum(jnp.where(diagonal, column, 0.0), axis=0, keepdims=True))
    lane8, row8 = lanes((8, 128)), lax.broadcasted_iota(jnp.int32, (8, 128), 0)
    for d in range(8):
        message = common
        for n, (x, z) in enumerate(((w0, 0), (w0, 48), (w0, 96), (zr, 0), (t0, 96))):
            hit = (lane16 >= 4 * n) & (lane16 < 4 * n + 4)
            message = jnp.where(hit, roll(x, (4 * n - z - 4 * d) % 128), message)
        upper = roll(roll(message, 10, 0), 64)
        sent = jnp.where(lane8 < 64, message[0:8], upper[0:8])
        line = jnp.zeros((1, 128), F32)
        for n in range(4):
            line = jnp.where((lane1 >= 4 * n) & (lane1 < 4 * n + 4), roll(lines[n], (4 * n - 4 * d) % 128), line)
        out_ref[8 * d : 8 * d + 8] = jnp.where(row8 < 6, sent, jnp.where(row8 == 6, line, 0.0))


def batched_inverse(a, lane, row, size):
    base = lane - lane % size
    for k in range(0, size, 2):
        at_k, at_n = lane % size == k, lane % size == k + 1
        left = jnp.take_along_axis(a, base + k, axis=1)
        right = jnp.take_along_axis(a, base + k + 1, axis=1)
        p, q, r, t = left[k : k + 1], right[k : k + 1], left[k + 1 : k + 2], right[k + 1 : k + 2]
        inverse = 1.0 / (p * t - q * r)
        upper = jnp.where(at_k[0:1], 1.0, jnp.where(at_n[0:1], 0.0, a[k : k + 1]))
        lower = jnp.where(at_n[0:1], 1.0, jnp.where(at_k[0:1], 0.0, a[k + 1 : k + 2]))
        first = (t * upper - q * lower) * inverse
        second = (p * lower - r * upper) * inverse
        rest = jnp.where(at_k | at_n, 0.0, a) - left * first - right * second
        a = jnp.where(row == k, first, jnp.where(row == k + 1, second, rest))
    return a


def block_inverse(matrix, low, high, size=16):
    lane = lanes((size, 128))
    row = lax.broadcasted_iota(jnp.int32, (size, 128), 0)
    compact = jnp.where(lane % size == row, 1.0, 0.0)
    for n in range(low // size, high // size):
        compact = jnp.where(lane // size == n, matrix[size * n : size * n + size], compact)
    compact = batched_inverse(compact, lane, row, size)
    parts = []
    for n in range(128 // size):
        active = low <= size * n < high
        parts.append(jnp.where(lane // size == n, compact, 0.0) if active else jnp.zeros((size, 128), F32))
    return jnp.concatenate(parts, axis=0)


def coarse_kernel(place_ref, in_ref, out_ref, g, e, ei, first, second, near):
    pr, pc = place_ref[0], place_ref[1]
    sub8 = lax.broadcasted_iota(jnp.int32, (8, 128), 0)

    for p in range(16):
        sums = {}
        for dr in range(3):
            r = p + 1 - dr
            if not 0 <= r < 16:
                continue
            for dq in range(4):
                k = 4 * dr + dq
                piece = in_ref[pl.ds(64 * r + k % 6, 8, stride=8), :]
                if dq == 0:
                    piece = jnp.where(sub8 < 7, roll(piece, 7, 0), 0.0)
                elif dq == 3:
                    piece = jnp.where(sub8 >= 1, roll(piece, 1, 0), 0.0)
                key = ((dq + 1) % 2, k >= 6)
                sums[key] = sums[key] + piece if key in sums else piece
        for par in range(2):
            total = jnp.zeros((8, 128), F32)
            if (par, False) in sums:
                total = total + sums[par, False]
            if (par, True) in sums:
                total = total + roll(sums[par, True], 64)
            g[pl.ds(16 * p + par, 8, stride=2), :] = total
    tally = jnp.sum(in_ref[pl.ds(6, 128, stride=8), :], axis=0, keepdims=True)
    tally = jnp.broadcast_to(tally, (128, 128)).T
    bb, bu, uu, uuu = (tally[4 * n : 4 * n + 4, 0:1] for n in range(4))
    by_lane = jnp.concatenate([g[0:128].T, g[128:256].T], axis=1)

    lane16, row16 = lanes((16, 128)), lax.broadcasted_iota(jnp.int32, (16, 128), 0)
    base = 20 + 6 * 3
    for p in range(16):
        own = g[16 * p : 16 * p + 16]
        terms = [(own, d, dp, dq) for d, dp, dq in ((0, 0, 0), (1, 0, 1))]
        terms.append((roll(own, 1, 0), 1, 0, -1))
        if p < 15:
            terms += [(own, d, 1, dq) for d, dq in ((3, -1), (4, 0), (5, 1))]
        if p > 0:
            last = g[16 * p - 16 : 16 * p]
            terms += [(roll(last, 15, 0), 3, -1, 1), (last, 4, -1, 0), (roll(last, 1, 0), 5, -1, -1)]
        halves = [jnp.zeros((16, 128), F32), jnp.zeros((16, 128), F32)]
        for x, d, dp, dq in terms:
            target = POS[p + dp] * 16
            h, off = target // 128, target % 128
            q = row16 + dq
            hit = (lane16 == off + q) & (q >= 0) & (q < 16)
            value = jnp.broadcast_to(x[:, base + d : base + d + 1], (16, 128))
            halves[h] = jnp.where(hit, value, halves[h])
        at = POS[p] * 16
        e[at : at + 16, 0:128] = halves[0]
        e[at : at + 16, 128:256] = halves[1]

    lane = lanes((128, 128))
    row = lax.broadcasted_iota(jnp.int32, (128, 128), 0)
    outer = block_inverse(e[0:128, 0:128], 0, 128)
    across = dot(outer, e[0:128, 128:256])
    schur = e[128:256, 128:256] - dot(e[128:256, 0:128], across)
    steps = []
    for low, high in ((0, 64), (64, 96)):
        inv = block_inverse(schur, low, high)
        link = jnp.where((row >= low) & (row < high) & (lane >= high), schur, 0.0)
        x = dot(inv, link)
        keep = jnp.where((row >= high) & (lane >= high), schur, 0.0)
        schur = keep - dot(link, x, TN)
        steps.append((inv, jnp.where((row == lane) & (row >= high), 1.0, 0.0) - x))
    inner = block_inverse(schur, 96, 128, 32)
    for inv, y in reversed(steps):
        inner = inv + dot(dot(y, inner), y, NT)
    half = dot(across, inner)
    near_diag = outer + dot(half, across, NT)

    def ordered(top_half, bottom_half):
        blocks = [top_half[16 * n : 16 * n + 16] for n in range(8)]
        blocks += [bottom_half[16 * n : 16 * n + 16] for n in range(8)]
        blocks = [blocks[POS[p]] for p in range(16)]
        return jnp.concatenate(blocks[:8], axis=0), jnp.concatenate(blocks[8:], axis=0)

    left_top, left_bottom = ordered(near_diag, -half.T)
    right_top, right_bottom = ordered(-half, inner)
    top_left, bottom_left = ordered(left_top.T, right_top.T)
    top_right, bottom_right = ordered(left_bottom.T, right_bottom.T)
    inverse = jnp.concatenate(
        [jnp.concatenate([top_left, bottom_left], axis=0), jnp.concatenate([top_right, bottom_right], axis=0)],
        axis=1,
    )
    for n, part in enumerate(parts_of(inverse, 3)):
        ei[n] = part

    def solve(z):
        rows = [part.astype(F32) for part in parts_of(z, 3)]
        rows = jnp.concatenate(rows + [jnp.zeros_like(z)], axis=0).astype(jnp.bfloat16)
        a, b, c = (fast_dot(rows, ei[n]) for n in range(3))
        return a[0:4] + (a[4:8] + b[0:4]) + (a[8:12] + b[4:8] + c[0:4])

    def apply(n, v):
        c = [by_lane[20 + 6 * n + d : 21 + 6 * n + d] for d in range(6)]
        total = c[0] * v
        for d, step in ((1, 1), (3, 15), (4, 16), (5, 17)):
            total = total + c[d] * roll(v, 256 - step) + roll(c[d] * v, step)
        return total

    def inner_product(a, b):
        return jnp.sum(a * b, axis=1, keepdims=True)

    wb, wu, wuu, zb, tuu = (by_lane[4 * n : 4 * n + 4] for n in range(5))
    c0 = solve(zb)
    f_c, g_c, h_c, k_c = apply(0, c0), apply(1, c0), apply(2, c0), apply(4, c0)
    grad0 = wb - f_c
    k0 = solve(grad0)
    f_k, g_k = apply(0, k0), apply(1, k0)
    rho0 = bb - 2.0 * inner_product(c0, wb) + inner_product(c0, f_c)
    energy0 = bu - 2.0 * inner_product(c0, wu) + inner_product(c0, g_c)
    curve0 = energy0 - inner_product(k0, grad0)
    a0 = rho0 / curve0
    e1 = c0 - a0 * k0
    f_e = f_c - a0 * f_k
    g_e = g_c - a0 * g_k
    grad1 = wb - f_e + a0 * (g_c - wu)
    k1 = solve(grad1)

    def second_norm(m0, m1, m2, v0, v1, v2, e_image, c_image, last):
        own = m0 - 2.0 * inner_product(e1, v0) + inner_product(e1, e_image)
        mixed = m1 - inner_product(c0, v1) - inner_product(e1, v1) + inner_product(e1, c_image)
        far = m2 - 2.0 * inner_product(c0, v2) + inner_product(c0, last)
        return own - 2.0 * a0 * mixed + a0 * a0 * far

    rho1 = second_norm(bb, bu, uu, wb, wu, wuu, f_e, g_c, h_c)
    energy1 = second_norm(bu, uu, uuu, wu, wuu, tuu, g_e, h_c, k_c)
    beta = rho1 / rho0
    cross = (
        bu
        - inner_product(c0, wu)
        - inner_product(e1, wu)
        + inner_product(e1, g_c)
        - a0 * (uu - 2.0 * inner_product(c0, wuu) + inner_product(c0, h_c))
        - inner_product(k0, grad1)
    )
    curve1 = energy1 - inner_product(k1, grad1) + 2.0 * beta * cross + beta * beta * curve0
    a1 = rho1 / curve1

    mine = lax.broadcasted_iota(jnp.int32, (32, 256), 0) // 4 == pc

    def zone(value):
        value = jnp.broadcast_to(value, (4, 256))
        return jnp.where(mine, jnp.concatenate([value] * 8, axis=0), 0.0)

    ab = a1 * beta
    stacks = (
        (
            zone(a1 * k1 + ab * k0 - e1),
            zone(-(a0 + ab) * c0 - a1 * e1),
            zone((a0 + ab) * c0 + a1 * e1),
            zone((a1 * a0) * c0),
        ),
        (
            zone(-(a1 * a0) * c0),
            zone(c0 - (a0 + ab) * k0 - a1 * k1),
            zone(-a0 - a1 - ab),
            zone(a1 * a0),
        ),
    )
    out_ref[...] = jnp.zeros((256, 128), F32)
    for n, (ref, stack) in enumerate(((first, stacks[0]), (second, stacks[1]))):
        stack = jnp.concatenate(stack, axis=0)
        ref[0:8] = jnp.zeros((8, 128), F32)
        ref[8:136] = stack[:, 0:128].T
        ref[136:264] = stack[:, 128:256].T
        ref[264:272] = jnp.zeros((8, 128), F32)
        for dr in range(3):
            p = jnp.clip(pr - 1 + dr, 0, 15)
            near[...] = ref[pl.ds(pl.multiple_of(16 * p, 16), 32), :]
            for dq in range(4):
                out_ref[pl.ds(16 * n + 4 * dr + dq, 8, stride=32), :] = near[pl.ds(7 + dq, 8, stride=2), :]


def outputs_kernel(
    place_ref, rows_ref, first_ref, second_ref, w_ref, grid_ref, coef_ref, m_ref, sol_ref, res_ref,
    left_ref, step_ref, window_ref,
):
    block = pl.program_id(0)

    @pl.when(block == 0)
    def _():
        pr, pc = place_ref[0], place_ref[1]
        slot = lax.broadcasted_iota(jnp.int32, (16, 128), 0)
        region_row = pr - 1 + slot // 4
        region_col = 2 * pc - 1 + slot % 4
        inside = (slot < 12) & (region_row >= 0) & (region_row < REG) & (region_col >= 0) & (region_col < REG)
        window_ref[...] = jnp.where(inside, region_row * REG + region_col, -1).astype(F32)
        total = m_ref[0:32]
        for n in range(1, 8):
            total = total + m_ref[32 * n : 32 * n + 32]
        top, bottom = total[0:16], total[16:32]
        lane = lanes((16, 128))
        steps = jnp.where(slot == 0, roll(bottom[5:6], 64), jnp.where(slot == 1, roll(bottom[5:6], 32), 0.0))
        m = jnp.concatenate(
            [
                jnp.where((lane >= 64) & (lane < 96), roll(bottom, 32), 0.0),
                jnp.where(lane < 64, top, 0.0),
                jnp.where(lane < 64, roll(top, 64), 0.0),
                jnp.where(lane < 32, bottom, 0.0),
                steps,
                jnp.zeros((48, 128), F32),
            ],
            axis=0,
        ).T
        c1, c2, c3 = parts_of(m[0:96, 0:64], 3)
        left_ref[...] = jnp.concatenate([c1, c1, c2, c2, c1, c3], axis=1)
        for n in range(2):
            step_ref[n] = jnp.broadcast_to(m[0:32, 64 + n : 65 + n], (32, 128))

    left, window = left_ref[...], window_ref[...]
    for part in range(2):
        rows = []
        for n in range(8):
            r = 16 * block + 8 * part + n
            z = jnp.where(grid_ref[pl.ds(r, 1), :] == window, grid_ref[pl.ds(128 + r, 1), :], 0.0)
            rows.append(jnp.concatenate([z, w_ref[r], first_ref[r, 32:48], second_ref[r, 32:48]], axis=0))
        r1, r2, r3 = parts_of(jnp.concatenate(rows, axis=1), 3)
        d = fast_dot(left, jnp.concatenate([r1, r2, r1, r2, r3, r1], axis=0))
        for n in range(8):
            r = 16 * block + 8 * part + n
            b, u, uu = rows_ref[r], first_ref[r, 0:32], second_ref[r, 0:32]
            e = d[:, 128 * n : 128 * n + 128]
            inv = coef_ref[5, pl.ds(r + 16, 1), :]
            p1, p2 = step_ref[0], step_ref[1]
            res_ref[:, 8 * part + n] = b + p1 * u + p2 * uu + e[0:32]
            sol_ref[:, 8 * part + n] = inv * (e[32:64] - p1 * b - p2 * u) + e[64:96]


def shape_of(*dims):
    return jax.ShapeDtypeStruct(dims, F32)


def kept(*dims):
    return pltpu.VMEM(dims, F32)


def vmem(*dims):
    return pltpu.VMEM(dims, F32)


def body(load_currents, labels, bump_height, horizontal_class, vertical_class, pad_class, edge_table, pad_table):
    pr, pc = lax.axis_index(ROW), lax.axis_index(COL)
    rows, cols = lax.axis_size(ROW), lax.axis_size(COL)
    place = jnp.stack([pr, pc]).astype(jnp.int32)
    loads = load_currents.reshape(-1, 128)
    grid, first_rows, last_rows = pl.pallas_call(
        prepare_kernel,
        out_shape=(kept(1024, 128), shape_of(HALO, SUB, 128), shape_of(HALO, SUB, 128)),
        compiler_params=limited,
        in_specs=[scalars] + [outside] * 8,
        out_specs=(whole,) * 3,
        scratch_shapes=[pltpu.SMEM((8,), F32), pltpu.SMEM((8,), F32), vmem(32, 8, 128), vmem(32, 8, 128)]
        + [pltpu.VMEM((128, 128), jnp.int32)] * 4
        + [pltpu.SemaphoreType.DMA((9,))],
    )(
        place,
        *(
            pltpu.with_memory_space_constraint(x, pltpu.HBM)
            for x in (
                edge_table, pad_table, load_currents, labels, bump_height,
                horizontal_class, vertical_class, pad_class,
            )
        ),
    )
    down = [(i, i + 1) for i in range(rows - 1)]
    bottom = lax.ppermute(first_rows, ROW, [(b, a) for a, b in down])
    top = lax.ppermute(last_rows, ROW, down)
    by_rows, own = pl.pallas_call(
        pack_kernel,
        out_shape=(kept(128, 32, 128), kept(GROUPS, SUB, 128)),
        compiler_params=limited,
        in_specs=[whole] * 2,
        out_specs=(whole,) * 2,
    )(loads, grid)
    own = pl.pallas_call(
        corner_kernel, out_shape=shape_of(GROUPS, SUB, 128), in_specs=[whole] * 3, out_specs=whole, compiler_params=limited
    )(own, top, bottom)
    right = [(i, i + 1) for i in range(cols - 1)]
    beside_left = lax.ppermute(own, COL, right)
    beside_right = lax.ppermute(own, COL, [(b, a) for a, b in right])
    first, second, w, coef, payload = pl.pallas_call(
        fields_kernel,
        out_shape=(
            kept(128, 48, 128),
            kept(128, 48, 128),
            kept(128, 16, 128),
            kept(6, 160, 128),
            shape_of(64, 128),
        ),
        compiler_params=limited,
        in_specs=[scalars] + [whole] * 7,
        out_specs=(whole,) * 5,
        scratch_shapes=[
            vmem(5, 160, 128),
            vmem(GROUPS + 2, SUB, 128),
            vmem(GROUPS + 2, SUB, 128),
            vmem(GROUPS + 2, 16, 128),
            vmem(GROUPS + 2, 16, 128),
            vmem(GROUPS + 2, 48, 128),
            vmem(GROUPS + 2, 48, 128),
            vmem(2 * GROUPS, 16, 128),
            vmem(2 * GROUPS, 48, 128),
            vmem(2 * GROUPS, 48, 128),
            vmem(2, GROUPS, 8, 128),
            vmem(144, 48, 128),
            vmem(144, 48, 128),
            vmem(96, 256),
        ],
    )(place, by_rows, grid, top, bottom, own, beside_left, beside_right)
    sent = jnp.broadcast_to(payload.reshape(1, cols, 8, 128), (rows, cols, 8, 128)).reshape(-1, 8, 128)
    everything = lax.all_to_all(sent, ROW + COL, 0, 0, tiled=True).reshape(-1, 128)
    found = pl.pallas_call(
        coarse_kernel,
        out_shape=shape_of(256, 128),
        compiler_params=limited,
        in_specs=[scalars, whole],
        out_specs=whole,
        scratch_shapes=[
            vmem(256, 128),
            vmem(256, 256),
            pltpu.VMEM((3, 256, 256), jnp.bfloat16),
            vmem(272, 128),
            vmem(272, 128),
            vmem(32, 128),
        ],
    )(place, everything)
    matrix = lax.all_to_all(found.reshape(cols, 32, 128), COL, 0, 0, tiled=True).reshape(-1, 128)
    by_block = pl.BlockSpec((32, 16, 128), lambda k: (0, k, 0))
    return pl.pallas_call(
        outputs_kernel,
        grid=(8,),
        out_shape=(shape_of(32, 128, 128), shape_of(32, 128, 128)),
        compiler_params=limited,
        in_specs=[scalars] + [whole] * 7,
        out_specs=(by_block, by_block),
        scratch_shapes=[pltpu.VMEM((96, 384), jnp.bfloat16), vmem(2, 32, 128), vmem(16, 128)],
    )(place, by_rows, first, second, w, grid, coef, matrix)


def solution(mesh):
    finer = Mesh(mesh.devices.reshape(4, 4, 4, 2), ("row_0", "row_1", "col_0", "col_1"))
    grid = P(ROW, COL)
    return jax.shard_map(
        body,
        mesh=finer,
        in_specs=(P(None, ROW, COL), grid, grid, grid, grid, grid, P(), P()),
        out_specs=(P(None, ROW, COL), P(None, ROW, COL)),
        check_vma=False,
    )
```

```python
import jax
import jax.numpy as jnp
from jax import lax
from jax.experimental import pallas as pl
from jax.experimental.pallas import tpu as pltpu
from jax.sharding import Mesh
from jax.sharding import PartitionSpec as P

REG = 16
ROW = ("row_0", "row_1")
COL = ("col_0", "col_1")
F32 = jnp.float32
precise = lax.Precision.HIGHEST

LAB, BUMP, RIGHT, DOWN, PAD = 32, 33, 34, 35, 36
SUB = 40
HALO = 3
GROUPS = 9
ORDER = (1, 3, 5, 7, 9, 11, 13, 15, 2, 6, 10, 14, 4, 12, 8, 0)
POS = tuple(ORDER.index(p) for p in range(16))
NT = (((1,), (1,)), ((), ()))
NN = (((1,), (0,)), ((), ()))
TN = (((0,), (0,)), ((), ()))
whole = pl.BlockSpec(memory_space=pltpu.VMEM)
outside = pl.BlockSpec(memory_space=pltpu.HBM)
limited = pltpu.CompilerParams(vmem_limit_bytes=32 * 2**20)
scalars = pl.BlockSpec(memory_space=pltpu.SMEM)


def dot(a, b, dims=NN):
    return lax.dot_general(a, b, dims, precision=precise, preferred_element_type=F32)


def parts_of(x, count):
    parts = []
    for n in range(count):
        parts.append(x.astype(jnp.bfloat16))
        if n + 1 < count:
            x = x - parts[-1].astype(F32)
    return parts


def fast_dot(a, b, dims=NN):
    return lax.dot_general(a, b, dims, preferred_element_type=F32)


def lanes(shape):
    return lax.broadcasted_iota(jnp.int32, shape, len(shape) - 1)


def roll(x, shift, axis=1):
    return pltpu.roll(x, shift, axis)


def prepare_kernel(
    place_ref, edge_hbm, pad_hbm, load_hbm, label_hbm, bump_hbm, across_hbm, down_hbm, pad_class_hbm,
    grid_ref, far_ref, near_ref, edge_ref, pad_ref, load_ref, load_end_ref, label_ref, across_ref, down_ref, pad_class_ref, done,
):
    copies = [
        pltpu.make_async_copy(source, target, done.at[n])
        for n, (source, target) in enumerate(
            (
                (edge_hbm, edge_ref),
                (pad_hbm, pad_ref),
                (across_hbm, across_ref),
                (down_hbm, down_ref),
                (pad_class_hbm, pad_class_ref),
                (label_hbm, label_ref),
                (bump_hbm, grid_ref.at[pl.ds(128, 128)]),
                (load_hbm.at[:, pl.ds(0, 8)], load_ref),
                (load_hbm.at[:, pl.ds(120, 8)], load_end_ref),
            )
        )
    ]
    for copy in copies:
        copy.start()
    for copy in copies:
        copy.wait()
    pr, pc = place_ref[0], place_ref[1]
    shape = (128, 128)
    row, lane = lax.broadcasted_iota(jnp.int32, shape, 0), lanes(shape)

    def lookup(table, classes):
        found = jnp.zeros(shape, F32)
        for n in range(8):
            found = jnp.where(classes == n, table[n], found)
        return found

    right = lookup(edge_ref, across_ref[...])
    down = lookup(edge_ref, down_ref[...])
    grid_ref[0:128] = label_ref[...].astype(F32)
    grid_ref[256:384] = jnp.where((lane == 127) & (pc == 7), 0.0, right)
    grid_ref[384:512] = jnp.where((row == 127) & (pr == 15), 0.0, down)
    grid_ref[512:640] = lookup(pad_ref, pad_class_ref[...])
    grid_ref[640:1024] = jnp.zeros((384, 128), F32)
    for n in range(HALO):
        even = pr % 2 == 0
        first, last = load_ref[:, n], load_end_ref[:, 8 - HALO + n]
        far_ref[n, 0:32] = jnp.where(even, first, last)
        near_ref[n, 0:32] = jnp.where(even, last, first)
        first = grid_ref[pl.ds(n, 8, stride=128), :]
        last = grid_ref[pl.ds(128 - HALO + n, 8, stride=128), :]
        far_ref[n, 32:40] = jnp.where(even, first, last)
        near_ref[n, 32:40] = jnp.where(even, last, first)


def pack_kernel(load_ref, grid_ref, rows_ref, own_ref):
    lane = lanes((32, 128)) // 8

    def group(g, slots):
        loads, rest = jnp.zeros((32, 128), F32), jnp.zeros((8, 128), F32)
        for s in slots:
            r = 16 * g - 8 + s
            b = load_ref[pl.ds(r, 32, stride=128), :]
            rows_ref[r] = b
            loads = jnp.where(lane == s, roll(b, (8 * s + 3) % 128), loads)
            rest = jnp.where(lane[0:8] == s, roll(grid_ref[pl.ds(r, 8, stride=128), :], (8 * s + 3) % 128), rest)
        own_ref[g, 0:32] = loads
        own_ref[g, 32:40] = rest

    group(0, range(8, 16))
    group(8, range(8))

    def step(g, _):
        group(g, range(16))
        return 0

    lax.fori_loop(1, 8, step, 0)


def corner_kernel(place_ref, own_ref, far_ref, near_ref, out_ref, top_ref, bottom_ref):
    lane = lanes((SUB, 128)) // 8
    even = place_ref[0] % 2 == 0
    top_ref[...] = jnp.where(even, far_ref[...], near_ref[...])
    bottom_ref[...] = jnp.where(even, near_ref[...], far_ref[...])
    for g in range(GROUPS):
        out_ref[g] = own_ref[g]
    start, end = own_ref[0], own_ref[8]
    for n in range(HALO):
        s = 8 - HALO + n
        start = jnp.where(lane == s, roll(top_ref[n], (8 * s + 3) % 128), start)
        s = 8 + n
        end = jnp.where(lane == s, roll(bottom_ref[n], (8 * s + 3) % 128), end)
    out_ref[0] = start
    out_ref[8] = end


def fields_kernel(
    place_ref, rows_ref, grid_ref, top_ref, bottom_ref, own_ref, far_ref, near_ref,
    first_ref, second_ref, w_ref, coef_ref, out_ref,
    ext, so, ss, sz_o, sz_s, y0_o, y0_s, qz, q0, q1, sc, y0, y1, gram,
):
    pr, pc = place_ref[0], place_ref[1]
    lane1 = lanes((1, 128))
    lane16 = lanes((16, 128))
    lane48 = lanes((48, 128))

    for n in range(5):
        ext[n, 0:16] = jnp.zeros((16, 128), F32)
        ext[n, 16:144] = grid_ref[128 * n : 128 * n + 128]
        ext[n, 144:160] = jnp.zeros((16, 128), F32)
        for k in range(HALO):
            ext[n, 16 - HALO + k : 17 - HALO + k] = top_ref[k, 32 + n : 33 + n]
            ext[n, 144 + k : 145 + k] = bottom_ref[k, 32 + n : 33 + n]

    slot = lax.broadcasted_iota(jnp.int32, (16, 128), 0)
    region_row = pr - 1 + slot // 4
    region_col = 2 * pc - 1 + slot % 4
    inside = (slot < 12) & (region_row >= 0) & (region_row < REG) & (region_col >= 0) & (region_col < REG)
    window = jnp.where(inside, region_row * REG + region_col, -1).astype(F32)

    for ref in (so, ss, sz_o, sz_s, y0_o, y0_s):
        ref[0] = jnp.zeros(ref.shape[1:], F32)
        ref[GROUPS + 1] = jnp.zeros(ref.shape[1:], F32)

    def pair_left(o, s, lane):
        j = lane % 8
        return roll(jnp.where(j == 2, s, o), 1), roll(jnp.where(j == 2, o, s), 1)

    def pair_right(o, s, lane):
        j = lane % 8
        return roll(jnp.where(j == 3, s, o), 127), roll(jnp.where(j == 3, o, s), 127)

    def above(before, here, lane):
        return roll(jnp.where(lane >= 120, before, here), 8)

    def below(here, after, lane):
        return roll(jnp.where(lane < 8, after, here), 120)

    def strips(g, _):
        o_row = own_ref[g]
        on_left = (lanes((SUB, 128)) % 8 < 3) == (pc % 2 == 0)
        s_row = jnp.where(on_left, far_ref[g], near_ref[g])
        so[g + 1], ss[g + 1] = o_row, s_row
        lefts = pair_left(o_row[RIGHT : RIGHT + 1], s_row[RIGHT : RIGHT + 1], lane1)
        for side, (row, ref, ll) in enumerate(((o_row, so, lefts[0]), (s_row, ss, lefts[1]))):
            rl, dl = row[RIGHT : RIGHT + 1], row[DOWN : DOWN + 1]
            ul = above(ref[g, DOWN : DOWN + 1], dl, lane1)
            diag = row[PAD : PAD + 1] + rl + ll + dl + ul
            inv = jnp.where(diag > 0, 1.0 / diag, 0.0)
            for n, value in enumerate((diag, rl, ll, dl, ul, inv)):
                sc[side, g, n : n + 1] = value
            z = jnp.where(row[LAB : LAB + 1] == window, row[BUMP : BUMP + 1], 0.0)
            (sz_s if side else sz_o)[g + 1] = z
            if side:
                qz[2 * g] = z
                qz[2 * g + 1] = roll(z, 64)

        at = pl.multiple_of(16 * g + 8, 8)
        beside = jnp.zeros((16, 128), F32)
        for s in range(16):
            beside = jnp.where(slot == s, roll(s_row[RIGHT : RIGHT + 1], 125 - 8 * s), beside)
        rl, dl = ext[2, pl.ds(at, 16)], ext[3, pl.ds(at, 16)]
        ll = roll(jnp.where(lane16 == 127, beside, rl), 1)
        last = ext[3, pl.ds(pl.multiple_of(at - 8, 8), 8)]
        ul = jnp.where(slot == 0, last[7:8], roll(dl, 1, 0))
        diag = ext[4, pl.ds(at, 16)] + rl + ll + dl + ul
        inv = jnp.where(diag > 0, 1.0 / diag, 0.0)
        for n, value in enumerate((diag, rl, ll, dl, ul, inv)):
            coef_ref[n, pl.ds(at, 16)] = value
        return 0

    lax.fori_loop(0, GROUPS, strips, 0, unroll=3)

    def strip_image(ref_o, ref_s, g, lane, sides):
        o, s = ref_o[g + 1], ref_s[g + 1]
        lefts, rights = pair_left(o, s, lane), pair_right(o, s, lane)
        done = []
        for side in sides:
            ref, here = (ref_s, s) if side else (ref_o, o)
            up = above(ref[g], here, lane)
            down = below(here, ref[g + 2], lane)
            c = [sc[side, g, n : n + 1] for n in range(5)]
            done.append(c[0] * here - c[1] * rights[side] - c[2] * lefts[side] - c[3] * down - c[4] * up)
        return done

    def strip_first(g, _):
        w = strip_image(sz_o, sz_s, g, lane16, (0, 1))
        for side, (source, ref) in enumerate(((so, y0_o), (ss, y0_s))):
            inv = sc[side, g, 5:6]
            ref[g + 1, 0:32] = inv * source[g + 1, 0:32]
            ref[g + 1, 32:48] = inv * w[side]
        y = y0_s[g + 1]
        q0[2 * g] = y
        q0[2 * g + 1] = roll(y, 64)
        return 0

    lax.fori_loop(0, GROUPS, strip_first, 0, unroll=3)

    def strip_second(g, _):
        (u,) = strip_image(y0_o, y0_s, g, lane48, (1,))
        y = sc[1, g, 5:6] * u
        q1[2 * g] = y
        q1[2 * g + 1] = roll(y, 64)
        return 0

    lax.fori_loop(0, GROUPS, strip_second, 0, unroll=3)

    def owned(g):
        return not isinstance(g, int)

    def coef(n, g, s):
        return coef_ref[n, pl.ds(8 * g + 8 + s, 1), :]

    def image(here, up, down, strip, g, s, lane):
        other = roll(strip[g], 125 - 8 * s)
        left = roll(jnp.where(lane == 127, other, here), 1)
        right = roll(jnp.where(lane == 0, other, here), 127)
        return (
            coef(0, g, s) * here
            - coef(1, g, s) * right
            - coef(2, g, s) * left
            - coef(3, g, s) * down
            - coef(4, g, s) * up
        )

    def basis(j):
        return jnp.where(ext[0, pl.ds(j, 1), :] == window, ext[1, pl.ds(j, 1), :], 0.0)

    def first_image(g, s):
        r, j = 8 * g - 8 + s, 8 * g + 8 + s
        w = image(basis(j), basis(j - 1), basis(j + 1), qz, g, s, lane16)
        if owned(g):
            b = rows_ref[r]
            w_ref[r] = w
        else:
            b = top_ref[r + HALO, 0:32] if r < 0 else bottom_ref[r - 128, 0:32]
        inv = coef(5, g, s)
        y0[8 * g + s, 0:32] = inv * b
        y0[8 * g + s, 32:48] = inv * w

    def second_image(g, s):
        i = 8 * g + s
        f1 = image(y0[i], y0[i - 1], y0[i + 1], q0, g, s, lane48)
        if owned(g):
            first_ref[8 * g - 8 + s] = f1
        y1[i] = coef(5, g, s) * f1

    def both(g, _):
        for s in range(8):
            second_image(g - 2, s)
        for s in range(8):
            first_image(g, s)
        return 0

    def only(work):
        def step(g, _):
            for s in range(8):
                work(g, s)
            return 0

        return step

    for s in (6, 7):
        first_image(0, s)
    lax.fori_loop(1, 3, only(first_image), 0)
    second_image(0, 7)
    lax.fori_loop(3, 17, both, 0)
    for s in (0, 1):
        first_image(17, s)
    lax.fori_loop(15, 17, only(second_image), 0)
    second_image(17, 0)

    gram[...] = jnp.zeros((96, 256), F32)

    def third_image(g, s):
        i = 8 * g + s
        second_ref[i - 8] = image(y1[i], y1[i - 1], y1[i + 1], q1, g, s, lane48)

    def products(g, sums):
        left, every = [], []
        sums = list(sums)
        for s in range(8):
            i = 8 * g + s
            r = i - 8
            b, f1, f2, y0r, y1r = rows_ref[r], first_ref[r], second_ref[r], y0[i], y1[i]
            left.append(jnp.concatenate([basis(i + 8), y0r[32:48], y1r[32:48]], axis=0))
            every.append(jnp.concatenate([b, w_ref[r], f1, f2], axis=0))
            pairs = ((y0r, b), (y0r, f1), (y1r, f1), (y1r, f2))
            sums = [t + p[0:32] * q[0:32] for t, (p, q) in zip(sums, pairs)]
        left = jnp.concatenate(parts_of(jnp.concatenate(left, axis=1), 2), axis=0)
        high, low = parts_of(jnp.concatenate(every, axis=1), 2)
        gram[:, 0:144] += fast_dot(left, high, NT) + fast_dot(left, low, NT)
        return tuple(sums)

    def last_stage(g, sums):
        sums = products(g - 1, sums)
        for s in range(8):
            third_image(g, s)
        return sums

    zero = jnp.zeros((32, 128), F32)
    lax.fori_loop(1, 2, only(third_image), 0)
    sums = lax.fori_loop(2, 17, last_stage, (zero, zero, zero, zero))
    sums = lax.fori_loop(16, 17, products, sums)

    a0, a1 = gram[0:48, 0:128] + gram[48:96, 0:128], gram[0:48, 128:256] + gram[48:96, 128:256]
    zr, w0, t0, w1, t1 = a0[0:16], a0[16:32], a0[32:48], a1[16:32], a1[32:48]
    matrices = jnp.zeros((16, 128), F32)
    for n, (x, z) in enumerate(((w0, 32), (w0, 80), (w1, 0), (zr, 32), (t1, 0))):
        start = 24 * n
        matrices = jnp.where((lane16 >= start) & (lane16 < start + 16), roll(x, (start - z) % 128), matrices)
    moved = jnp.zeros((16, 128), F32)
    for k in range(12):
        moved = jnp.where(slot == k, roll(matrices, (128 - k) % 128), moved)
    common = jnp.zeros((16, 128), F32)
    for n in range(5):
        for start, offset, count in ((20 + 2 * n, 0, 2), (30 + 3 * n, 3, 3)):
            hit = (lane16 >= start) & (lane16 < start + count)
            common = jnp.where(hit, roll(moved, (start - offset - 24 * n) % 128), common)
    lines = []
    diagonal = lanes((32, 128)) == lax.broadcasted_iota(jnp.int32, (32, 128), 0)
    for total in sums:
        column = jnp.sum(total, axis=1, keepdims=True)
        lines.append(jnp.sum(jnp.where(diagonal, column, 0.0), axis=0, keepdims=True))
    row4, lane4 = lax.broadcasted_iota(jnp.int32, (4, 128), 0), lanes((4, 128))
    for d in range(8):
        message = common
        for n, (x, z) in enumerate(((w0, 0), (w0, 48), (w0, 96), (zr, 0), (t0, 96))):
            hit = (lane16 >= 4 * n) & (lane16 < 4 * n + 4)
            message = jnp.where(hit, roll(x, (4 * n - z - 4 * d) % 128), message)
        middle, last = roll(message, 45), roll(message, 90)
        sent = jnp.where(lane4 < 45, message[0:4], jnp.where(lane4 < 90, middle[4:8], last[8:12]))
        line = jnp.zeros((1, 128), F32)
        for n in range(4):
            start = 120 + 4 * n if n < 2 else 112 + 4 * n
            line = jnp.where((lane1 >= start) & (lane1 < start + 4), roll(lines[n], (start - 4 * d) % 128), line)
            if n == 1:
                first_two, line = line, jnp.zeros((1, 128), F32)
        total = jnp.where(row4 == 0, first_two, jnp.where(row4 == 1, line, 0.0))
        out_ref[4 * d : 4 * d + 4] = jnp.where(lane4 < 120, sent, total)


def batched_inverse(a, lane, row, size):
    base = lane - lane % size
    for k in range(0, size, 2):
        at_k, at_n = lane % size == k, lane % size == k + 1
        left = jnp.take_along_axis(a, base + k, axis=1)
        right = jnp.take_along_axis(a, base + k + 1, axis=1)
        p, q, r, t = left[k : k + 1], right[k : k + 1], left[k + 1 : k + 2], right[k + 1 : k + 2]
        inverse = 1.0 / (p * t - q * r)
        upper = jnp.where(at_k[0:1], 1.0, jnp.where(at_n[0:1], 0.0, a[k : k + 1]))
        lower = jnp.where(at_n[0:1], 1.0, jnp.where(at_k[0:1], 0.0, a[k + 1 : k + 2]))
        first = (t * upper - q * lower) * inverse
        second = (p * lower - r * upper) * inverse
        rest = jnp.where(at_k | at_n, 0.0, a) - left * first - right * second
        a = jnp.where(row == k, first, jnp.where(row == k + 1, second, rest))
    return a


def block_inverse(matrix, low, high, size=16):
    lane = lanes((size, 128))
    row = lax.broadcasted_iota(jnp.int32, (size, 128), 0)
    compact = jnp.where(lane % size == row, 1.0, 0.0)
    for n in range(low // size, high // size):
        compact = jnp.where(lane // size == n, matrix[size * n : size * n + size], compact)
    compact = batched_inverse(compact, lane, row, size)
    parts = []
    for n in range(128 // size):
        active = low <= size * n < high
        parts.append(jnp.where(lane // size == n, compact, 0.0) if active else jnp.zeros((size, 128), F32))
    return jnp.concatenate(parts, axis=0)


def coarse_kernel(place_ref, in_ref, out_ref, g, e, ei, first, second, near):
    pr, pc = place_ref[0], place_ref[1]
    sub8 = lax.broadcasted_iota(jnp.int32, (8, 128), 0)

    lane8 = lanes((8, 128))
    for p in range(16):
        even, odd = jnp.zeros((8, 128), F32), jnp.zeros((8, 128), F32)
        for dr in range(3):
            r = p + 1 - dr
            if not 0 <= r < 16:
                continue
            at = [in_ref[pl.ds(32 * r + dq, 8, stride=4), :] for dq in range(4)]
            pair = (
                at[1] + jnp.where(sub8 >= 1, roll(at[3], 1, 0), 0.0),
                at[2] + jnp.where(sub8 < 7, roll(at[0], 7, 0), 0.0),
            )
            hit = lane8 < (30 if dr == 2 else 45)
            even, odd = (
                old + jnp.where(hit, roll(new, (128 - 45 * dr) % 128) if dr else new, 0.0)
                for old, new in zip((even, odd), pair)
            )
        g[pl.ds(16 * p, 8, stride=2), :] = even
        g[pl.ds(16 * p + 1, 8, stride=2), :] = odd
    tally = [
        roll(jnp.sum(in_ref[pl.ds(n, 128, stride=4), :], axis=0, keepdims=True), 8 + 8 * n) for n in range(2)
    ]
    tally = jnp.where(lanes((1, 128)) < 8, tally[0], tally[1])
    tally = jnp.broadcast_to(tally, (128, 128)).T
    bb, bu, uu, uuu = (tally[4 * n : 4 * n + 4, 0:1] for n in range(4))
    by_lane = jnp.concatenate([g[0:128].T, g[128:256].T], axis=1)

    lane16, row16 = lanes((16, 128)), lax.broadcasted_iota(jnp.int32, (16, 128), 0)
    for p in range(16):
        own = g[16 * p : 16 * p + 16]
        terms = [(own, d, dp, dq) for d, dp, dq in ((0, 0, 0), (1, 0, 1))]
        terms.append((roll(own, 1, 0), 1, 0, -1))
        if p < 15:
            terms += [(own, d, 1, dq) for d, dq in ((3, -1), (4, 0), (5, 1))]
        if p > 0:
            last = g[16 * p - 16 : 16 * p]
            terms += [(roll(last, 15, 0), 3, -1, 1), (last, 4, -1, 0), (roll(last, 1, 0), 5, -1, -1)]
        halves = [jnp.zeros((16, 128), F32), jnp.zeros((16, 128), F32)]
        for x, d, dp, dq in terms:
            target = POS[p + dp] * 16
            h, off = target // 128, target % 128
            q = row16 + dq
            hit = (lane16 == off + q) & (q >= 0) & (q < 16)
            at = 26 + d if d < 2 else 36 + d
            value = jnp.broadcast_to(x[:, at : at + 1], (16, 128))
            halves[h] = jnp.where(hit, value, halves[h])
        at = POS[p] * 16
        e[at : at + 16, 0:128] = halves[0]
        e[at : at + 16, 128:256] = halves[1]

    lane = lanes((128, 128))
    row = lax.broadcasted_iota(jnp.int32, (128, 128), 0)
    outer = block_inverse(e[0:128, 0:128], 0, 128)
    across = dot(outer, e[0:128, 128:256])
    schur = e[128:256, 128:256] - dot(e[128:256, 0:128], across)
    steps = []
    for low, high in ((0, 64), (64, 96)):
        inv = block_inverse(schur, low, high)
        link = jnp.where((row >= low) & (row < high) & (lane >= high), schur, 0.0)
        x = dot(inv, link)
        keep = jnp.where((row >= high) & (lane >= high), schur, 0.0)
        schur = keep - dot(link, x, TN)
        steps.append((inv, jnp.where((row == lane) & (row >= high), 1.0, 0.0) - x))
    inner = block_inverse(schur, 96, 128, 32)
    for inv, y in reversed(steps):
        inner = inv + dot(dot(y, inner), y, NT)
    half = dot(across, inner)
    near_diag = outer + dot(half, across, NT)

    def ordered(top_half, bottom_half):
        blocks = [top_half[16 * n : 16 * n + 16] for n in range(8)]
        blocks += [bottom_half[16 * n : 16 * n + 16] for n in range(8)]
        blocks = [blocks[POS[p]] for p in range(16)]
        return jnp.concatenate(blocks[:8], axis=0), jnp.concatenate(blocks[8:], axis=0)

    left_top, left_bottom = ordered(near_diag, -half.T)
    right_top, right_bottom = ordered(-half, inner)
    top_left, bottom_left = ordered(left_top.T, right_top.T)
    top_right, bottom_right = ordered(left_bottom.T, right_bottom.T)
    inverse = jnp.concatenate(
        [jnp.concatenate([top_left, bottom_left], axis=0), jnp.concatenate([top_right, bottom_right], axis=0)],
        axis=1,
    )
    for n, part in enumerate(parts_of(inverse, 3)):
        ei[n] = part

    def solve(z):
        rows = [part.astype(F32) for part in parts_of(z, 3)]
        rows = jnp.concatenate(rows + [jnp.zeros_like(z)], axis=0).astype(jnp.bfloat16)
        a, b, c = (fast_dot(rows, ei[n]) for n in range(3))
        return a[0:4] + (a[4:8] + b[0:4]) + (a[8:12] + b[4:8] + c[0:4])

    def apply(n, v):
        c = {d: by_lane[at : at + 1] for d, at in enumerate((20 + 2 * n, 21 + 2 * n, 0, 30 + 3 * n, 31 + 3 * n, 32 + 3 * n))}
        total = c[0] * v
        for d, step in ((1, 1), (3, 15), (4, 16), (5, 17)):
            total = total + c[d] * roll(v, 256 - step) + roll(c[d] * v, step)
        return total

    def inner_product(a, b):
        return jnp.sum(a * b, axis=1, keepdims=True)

    wb, wu, wuu, zb, tuu = (by_lane[4 * n : 4 * n + 4] for n in range(5))
    c0 = solve(zb)
    f_c, g_c, h_c, k_c = apply(0, c0), apply(1, c0), apply(2, c0), apply(4, c0)
    grad0 = wb - f_c
    k0 = solve(grad0)
    f_k, g_k = apply(0, k0), apply(1, k0)
    rho0 = bb - 2.0 * inner_product(c0, wb) + inner_product(c0, f_c)
    energy0 = bu - 2.0 * inner_product(c0, wu) + inner_product(c0, g_c)
    curve0 = energy0 - inner_product(k0, grad0)
    a0 = rho0 / curve0
    e1 = c0 - a0 * k0
    f_e = f_c - a0 * f_k
    g_e = g_c - a0 * g_k
    grad1 = wb - f_e + a0 * (g_c - wu)
    k1 = solve(grad1)

    def second_norm(m0, m1, m2, v0, v1, v2, e_image, c_image, last):
        own = m0 - 2.0 * inner_product(e1, v0) + inner_product(e1, e_image)
        mixed = m1 - inner_product(c0, v1) - inner_product(e1, v1) + inner_product(e1, c_image)
        far = m2 - 2.0 * inner_product(c0, v2) + inner_product(c0, last)
        return own - 2.0 * a0 * mixed + a0 * a0 * far

    rho1 = second_norm(bb, bu, uu, wb, wu, wuu, f_e, g_c, h_c)
    energy1 = second_norm(bu, uu, uuu, wu, wuu, tuu, g_e, h_c, k_c)
    beta = rho1 / rho0
    cross = (
        bu
        - inner_product(c0, wu)
        - inner_product(e1, wu)
        + inner_product(e1, g_c)
        - a0 * (uu - 2.0 * inner_product(c0, wuu) + inner_product(c0, h_c))
        - inner_product(k0, grad1)
    )
    curve1 = energy1 - inner_product(k1, grad1) + 2.0 * beta * cross + beta * beta * curve0
    a1 = rho1 / curve1

    mine = lax.broadcasted_iota(jnp.int32, (32, 256), 0) // 4 == pc

    def zone(value):
        value = jnp.broadcast_to(value, (4, 256))
        return jnp.where(mine, jnp.concatenate([value] * 8, axis=0), 0.0)

    ab = a1 * beta
    stacks = (
        (
            zone(a1 * k1 + ab * k0 - e1),
            zone(-(a0 + ab) * c0 - a1 * e1),
            zone((a0 + ab) * c0 + a1 * e1),
            zone((a1 * a0) * c0),
        ),
        (
            zone(-(a1 * a0) * c0),
            zone(c0 - (a0 + ab) * k0 - a1 * k1),
            zone(-a0 - a1 - ab),
            zone(a1 * a0),
        ),
    )
    out_ref[...] = jnp.zeros((256, 128), F32)
    for n, (ref, stack) in enumerate(((first, stacks[0]), (second, stacks[1]))):
        stack = jnp.concatenate(stack, axis=0)
        ref[0:8] = jnp.zeros((8, 128), F32)
        ref[8:136] = stack[:, 0:128].T
        ref[136:264] = stack[:, 128:256].T
        ref[264:272] = jnp.zeros((8, 128), F32)
        for dr in range(3):
            p = jnp.clip(pr - 1 + dr, 0, 15)
            near[...] = ref[pl.ds(pl.multiple_of(16 * p, 16), 32), :]
            for dq in range(4):
                out_ref[pl.ds(16 * n + 4 * dr + dq, 8, stride=32), :] = near[pl.ds(7 + dq, 8, stride=2), :]


def outputs_kernel(
    place_ref, rows_ref, first_ref, second_ref, w_ref, grid_ref, coef_ref, m_ref, sol_ref, res_ref,
    left_ref, step_ref, window_ref,
):
    block = pl.program_id(0)

    @pl.when(block == 0)
    def _():
        pr, pc = place_ref[0], place_ref[1]
        slot = lax.broadcasted_iota(jnp.int32, (16, 128), 0)
        region_row = pr - 1 + slot // 4
        region_col = 2 * pc - 1 + slot % 4
        inside = (slot < 12) & (region_row >= 0) & (region_row < REG) & (region_col >= 0) & (region_col < REG)
        window_ref[...] = jnp.where(inside, region_row * REG + region_col, -1).astype(F32)
        total = m_ref[0:32]
        for n in range(1, 8):
            total = total + m_ref[32 * n : 32 * n + 32]
        top, bottom = total[0:16], total[16:32]
        lane = lanes((16, 128))
        steps = jnp.where(slot == 0, roll(bottom[5:6], 64), jnp.where(slot == 1, roll(bottom[5:6], 32), 0.0))
        m = jnp.concatenate(
            [
                jnp.where((lane >= 64) & (lane < 96), roll(bottom, 32), 0.0),
                jnp.where(lane < 64, top, 0.0),
                jnp.where(lane < 64, roll(top, 64), 0.0),
                jnp.where(lane < 32, bottom, 0.0),
                steps,
                jnp.zeros((48, 128), F32),
            ],
            axis=0,
        ).T
        c1, c2, c3 = parts_of(m[0:96, 0:64], 3)
        left_ref[...] = jnp.concatenate([c1, c1, c2, c2, c1, c3], axis=1)
        for n in range(2):
            step_ref[n] = jnp.broadcast_to(m[0:32, 64 + n : 65 + n], (32, 128))

    left, window = left_ref[...], window_ref[...]
    for part in range(2):
        rows = []
        for n in range(8):
            r = 16 * block + 8 * part + n
            z = jnp.where(grid_ref[pl.ds(r, 1), :] == window, grid_ref[pl.ds(128 + r, 1), :], 0.0)
            rows.append(jnp.concatenate([z, w_ref[r], first_ref[r, 32:48], second_ref[r, 32:48]], axis=0))
        r1, r2, r3 = parts_of(jnp.concatenate(rows, axis=1), 3)
        d = fast_dot(left, jnp.concatenate([r1, r2, r1, r2, r3, r1], axis=0))
        for n in range(8):
            r = 16 * block + 8 * part + n
            b, u, uu = rows_ref[r], first_ref[r, 0:32], second_ref[r, 0:32]
            e = d[:, 128 * n : 128 * n + 128]
            inv = coef_ref[5, pl.ds(r + 16, 1), :]
            p1, p2 = step_ref[0], step_ref[1]
            res_ref[:, 8 * part + n] = b + p1 * u + p2 * uu + e[0:32]
            sol_ref[:, 8 * part + n] = inv * (e[32:64] - p1 * b - p2 * u) + e[64:96]


def swapped(value, axis, start):
    pairs = [(i, i + 1) for i in range(start, lax.axis_size(axis) - 1, 2)]
    return lax.ppermute(value, axis, pairs + [(b, a) for a, b in pairs])


def shape_of(*dims):
    return jax.ShapeDtypeStruct(dims, F32)


def kept(*dims):
    return pltpu.VMEM(dims, F32)


def vmem(*dims):
    return pltpu.VMEM(dims, F32)


def body(load_currents, labels, bump_height, horizontal_class, vertical_class, pad_class, edge_table, pad_table):
    pr, pc = lax.axis_index(ROW), lax.axis_index(COL)
    rows, cols = lax.axis_size(ROW), lax.axis_size(COL)
    place = jnp.stack([pr, pc]).astype(jnp.int32)
    loads = load_currents.reshape(-1, 128)
    grid, far_rows, near_rows = pl.pallas_call(
        prepare_kernel,
        out_shape=(kept(1024, 128), shape_of(HALO, SUB, 128), shape_of(HALO, SUB, 128)),
        compiler_params=limited,
        in_specs=[scalars] + [outside] * 8,
        out_specs=(whole,) * 3,
        scratch_shapes=[pltpu.SMEM((8,), F32), pltpu.SMEM((8,), F32), vmem(32, 8, 128), vmem(32, 8, 128)]
        + [pltpu.VMEM((128, 128), jnp.int32)] * 4
        + [pltpu.SemaphoreType.DMA((9,))],
    )(
        place,
        *(
            pltpu.with_memory_space_constraint(x, pltpu.HBM)
            for x in (
                edge_table, pad_table, load_currents, labels, bump_height,
                horizontal_class, vertical_class, pad_class,
            )
        ),
    )
    far_rows = swapped(far_rows, ROW, 1)
    near_rows = swapped(near_rows, ROW, 0)
    by_rows, own = pl.pallas_call(
        pack_kernel,
        out_shape=(kept(128, 32, 128), kept(GROUPS, SUB, 128)),
        compiler_params=limited,
        in_specs=[whole] * 2,
        out_specs=(whole,) * 2,
    )(loads, grid)
    own, top, bottom = pl.pallas_call(
        corner_kernel,
        out_shape=(shape_of(GROUPS, SUB, 128), kept(HALO, SUB, 128), kept(HALO, SUB, 128)),
        compiler_params=limited,
        in_specs=[scalars] + [whole] * 3,
        out_specs=(whole,) * 3,
    )(place, own, far_rows, near_rows)
    near_columns = swapped(own, COL, 0)
    far_columns = swapped(own, COL, 1)
    first, second, w, coef, payload = pl.pallas_call(
        fields_kernel,
        out_shape=(
            kept(128, 48, 128),
            kept(128, 48, 128),
            kept(128, 16, 128),
            kept(6, 160, 128),
            shape_of(32, 128),
        ),
        compiler_params=limited,
        in_specs=[scalars] + [whole] * 7,
        out_specs=(whole,) * 5,
        scratch_shapes=[
            vmem(5, 160, 128),
            vmem(GROUPS + 2, SUB, 128),
            vmem(GROUPS + 2, SUB, 128),
            vmem(GROUPS + 2, 16, 128),
            vmem(GROUPS + 2, 16, 128),
            vmem(GROUPS + 2, 48, 128),
            vmem(GROUPS + 2, 48, 128),
            vmem(2 * GROUPS, 16, 128),
            vmem(2 * GROUPS, 48, 128),
            vmem(2 * GROUPS, 48, 128),
            vmem(2, GROUPS, 8, 128),
            vmem(144, 48, 128),
            vmem(144, 48, 128),
            vmem(96, 256),
        ],
    )(place, by_rows, grid, top, bottom, own, far_columns, near_columns)
    sent = jnp.broadcast_to(payload.reshape(1, cols, 4, 128), (rows, cols, 4, 128)).reshape(-1, 4, 128)
    everything = lax.all_to_all(sent, ROW + COL, 0, 0, tiled=True).reshape(-1, 128)
    found = pl.pallas_call(
        coarse_kernel,
        out_shape=shape_of(256, 128),
        compiler_params=limited,
        in_specs=[scalars, whole],
        out_specs=whole,
        scratch_shapes=[
            vmem(256, 128),
            vmem(256, 256),
            pltpu.VMEM((3, 256, 256), jnp.bfloat16),
            vmem(272, 128),
            vmem(272, 128),
            vmem(32, 128),
        ],
    )(place, everything)
    matrix = lax.all_to_all(found.reshape(cols, 32, 128), COL, 0, 0, tiled=True).reshape(-1, 128)
    by_block = pl.BlockSpec((32, 16, 128), lambda k: (0, k, 0))
    return pl.pallas_call(
        outputs_kernel,
        grid=(8,),
        out_shape=(shape_of(32, 128, 128), shape_of(32, 128, 128)),
        compiler_params=limited,
        in_specs=[scalars] + [whole] * 7,
        out_specs=(by_block, by_block),
        scratch_shapes=[pltpu.VMEM((96, 384), jnp.bfloat16), vmem(2, 32, 128), vmem(16, 128)],
    )(place, by_rows, first, second, w, grid, coef, matrix)


def solution(mesh):
    finer = Mesh(mesh.devices.reshape(4, 4, 4, 2), ("row_0", "row_1", "col_0", "col_1"))
    grid = P(ROW, COL)
    return jax.shard_map(
        body,
        mesh=finer,
        in_specs=(P(None, ROW, COL), grid, grid, grid, grid, grid, P(), P()),
        out_specs=(P(None, ROW, COL), P(None, ROW, COL)),
        check_vma=False,
    )
```

```python
import jax
import jax.numpy as jnp
from jax import lax
from jax.experimental import pallas as pl
from jax.experimental.pallas import tpu as pltpu
from jax.sharding import Mesh
from jax.sharding import PartitionSpec as P

REG = 16
ROW = ("row_0", "row_1")
COL = ("col_0", "col_1")
F32 = jnp.float32
precise = lax.Precision.HIGHEST

LAB, BUMP, RIGHT, DOWN, PAD = 32, 33, 34, 35, 36
SUB = 40
HALO = 3
GROUPS = 9
ORDER = (1, 3, 5, 7, 9, 11, 13, 15, 2, 6, 10, 14, 4, 12, 8, 0)
POS = tuple(ORDER.index(p) for p in range(16))
NT = (((1,), (1,)), ((), ()))
NN = (((1,), (0,)), ((), ()))
TN = (((0,), (0,)), ((), ()))
whole = pl.BlockSpec(memory_space=pltpu.VMEM)
outside = pl.BlockSpec(memory_space=pltpu.HBM)
limited = pltpu.CompilerParams(vmem_limit_bytes=32 * 2**20)
scalars = pl.BlockSpec(memory_space=pltpu.SMEM)


def dot(a, b, dims=NN):
    return lax.dot_general(a, b, dims, precision=precise, preferred_element_type=F32)


def parts_of(x, count):
    parts = []
    for n in range(count):
        parts.append(x.astype(jnp.bfloat16))
        if n + 1 < count:
            x = x - parts[-1].astype(F32)
    return parts


def fast_dot(a, b, dims=NN):
    return lax.dot_general(a, b, dims, preferred_element_type=F32)


def lanes(shape):
    return lax.broadcasted_iota(jnp.int32, shape, len(shape) - 1)


def roll(x, shift, axis=1):
    return pltpu.roll(x, shift, axis)


def prepare_kernel(
    edge_hbm, pad_hbm, load_hbm, label_hbm, bump_hbm, across_hbm, down_hbm, pad_class_hbm,
    grid_ref, far_ref, near_ref, edge_ref, pad_ref, load_ref, load_end_ref, label_ref, across_ref, down_ref, pad_class_ref, done,
):
    copies = [
        pltpu.make_async_copy(source, target, done.at[n])
        for n, (source, target) in enumerate(
            (
                (edge_hbm, edge_ref),
                (pad_hbm, pad_ref),
                (across_hbm, across_ref),
                (down_hbm, down_ref),
                (pad_class_hbm, pad_class_ref),
                (label_hbm, label_ref),
                (bump_hbm, grid_ref.at[pl.ds(128, 128)]),
                (load_hbm.at[:, pl.ds(0, 8)], load_ref),
                (load_hbm.at[:, pl.ds(120, 8)], load_end_ref),
            )
        )
    ]
    for copy in copies:
        copy.start()
    for copy in copies:
        copy.wait()
    pr, pc = lax.axis_index(ROW), lax.axis_index(COL)
    shape = (128, 128)
    row, lane = lax.broadcasted_iota(jnp.int32, shape, 0), lanes(shape)

    def lookup(table, classes):
        found = jnp.zeros(shape, F32)
        for n in range(8):
            found = jnp.where(classes == n, table[n], found)
        return found

    right = lookup(edge_ref, across_ref[...])
    down = lookup(edge_ref, down_ref[...])
    grid_ref[0:128] = label_ref[...].astype(F32)
    grid_ref[256:384] = jnp.where((lane == 127) & (pc == 7), 0.0, right)
    grid_ref[384:512] = jnp.where((row == 127) & (pr == 15), 0.0, down)
    grid_ref[512:640] = lookup(pad_ref, pad_class_ref[...])
    grid_ref[640:1024] = jnp.zeros((384, 128), F32)
    for n in range(HALO):
        even = pr % 2 == 0
        first, last = load_ref[:, n], load_end_ref[:, 8 - HALO + n]
        far_ref[n, 0:32] = jnp.where(even, first, last)
        near_ref[n, 0:32] = jnp.where(even, last, first)
        first = grid_ref[pl.ds(n, 8, stride=128), :]
        last = grid_ref[pl.ds(128 - HALO + n, 8, stride=128), :]
        far_ref[n, 32:40] = jnp.where(even, first, last)
        near_ref[n, 32:40] = jnp.where(even, last, first)


def pack_kernel(load_ref, grid_ref, rows_ref, own_ref):
    lane = lanes((32, 128)) // 8

    def group(g, slots):
        loads, rest = jnp.zeros((32, 128), F32), jnp.zeros((8, 128), F32)
        for s in slots:
            r = 16 * g - 8 + s
            b = load_ref[pl.ds(r, 32, stride=128), :]
            rows_ref[r] = b
            loads = jnp.where(lane == s, roll(b, (8 * s + 3) % 128), loads)
            rest = jnp.where(lane[0:8] == s, roll(grid_ref[pl.ds(r, 8, stride=128), :], (8 * s + 3) % 128), rest)
        own_ref[g, 0:32] = loads
        own_ref[g, 32:40] = rest

    group(0, range(8, 16))
    group(8, range(8))

    def step(g, _):
        group(g, range(16))
        return 0

    lax.fori_loop(1, 8, step, 0)


def corner_kernel(
    own_ref, far_ref, near_ref, out_ref, top_ref, bottom_ref, far_out_ref, near_out_ref
):
    lane = lanes((SUB, 128)) // 8
    even = lax.axis_index(ROW) % 2 == 0
    top_ref[...] = jnp.where(even, far_ref[...], near_ref[...])
    bottom_ref[...] = jnp.where(even, near_ref[...], far_ref[...])
    for g in range(GROUPS):
        out_ref[g] = own_ref[g]
    start, end = own_ref[0], own_ref[8]
    for n in range(HALO):
        s = 8 - HALO + n
        start = jnp.where(lane == s, roll(top_ref[n], (8 * s + 3) % 128), start)
        s = 8 + n
        end = jnp.where(lane == s, roll(bottom_ref[n], (8 * s + 3) % 128), end)
    out_ref[0] = start
    out_ref[8] = end
    low = lanes((SUB, 128)) % 8 < 4
    to_right_first = lax.axis_index(COL) % 2 == 1
    for h in range(5):
        here = out_ref[2 * h]
        after = out_ref[2 * h + 1] if h < 4 else here
        right = jnp.where(low, here, roll(after, 4))
        left = jnp.where(low, roll(here, 125), roll(after, 1))
        far_out_ref[h] = jnp.where(to_right_first, right, left)
        near_out_ref[h] = jnp.where(to_right_first, left, right)


def fields_kernel(
    rows_ref, grid_ref, top_ref, bottom_ref, own_ref, far_ref, near_ref,
    first_ref, second_ref, w_ref, coef_ref, out_ref,
    ext, so, ss, sz_o, sz_s, y0_o, y0_s, qz, q0, q1, sc, y0, y1, gram,
):
    pr, pc = lax.axis_index(ROW), lax.axis_index(COL)
    lane1 = lanes((1, 128))
    lane16 = lanes((16, 128))
    lane48 = lanes((48, 128))

    for n in range(5):
        ext[n, 0:16] = jnp.zeros((16, 128), F32)
        ext[n, 16:144] = grid_ref[128 * n : 128 * n + 128]
        ext[n, 144:160] = jnp.zeros((16, 128), F32)
        for k in range(HALO):
            ext[n, 16 - HALO + k : 17 - HALO + k] = top_ref[k, 32 + n : 33 + n]
            ext[n, 144 + k : 145 + k] = bottom_ref[k, 32 + n : 33 + n]

    slot = lax.broadcasted_iota(jnp.int32, (16, 128), 0)
    region_row = pr - 1 + slot // 4
    region_col = 2 * pc - 1 + slot % 4
    inside = (slot < 12) & (region_row >= 0) & (region_row < REG) & (region_col >= 0) & (region_col < REG)
    window = jnp.where(inside, region_row * REG + region_col, -1).astype(F32)

    for ref in (so, ss, sz_o, sz_s, y0_o, y0_s):
        ref[0] = jnp.zeros(ref.shape[1:], F32)
        ref[GROUPS + 1] = jnp.zeros(ref.shape[1:], F32)

    def pair_left(o, s, lane):
        j = lane % 8
        return roll(jnp.where(j == 2, s, o), 1), roll(jnp.where(j == 2, o, s), 1)

    def pair_right(o, s, lane):
        j = lane % 8
        return roll(jnp.where(j == 3, s, o), 127), roll(jnp.where(j == 3, o, s), 127)

    def above(before, here, lane):
        return roll(jnp.where(lane >= 120, before, here), 8)

    def below(here, after, lane):
        return roll(jnp.where(lane < 8, after, here), 120)

    even = pc % 2 == 0

    def strips(g, _):
        o_row = own_ref[g]
        far, near = far_ref[g // 2], near_ref[g // 2]
        on_left, on_right = jnp.where(even, far, near), jnp.where(even, near, far)
        turn = 124 * (g % 2)
        s_row = jnp.where(lanes((SUB, 128)) % 8 < 3, roll(on_left, turn), roll(on_right, 3 + turn))
        so[g + 1], ss[g + 1] = o_row, s_row
        lefts = pair_left(o_row[RIGHT : RIGHT + 1], s_row[RIGHT : RIGHT + 1], lane1)
        for side, (row, ref, ll) in enumerate(((o_row, so, lefts[0]), (s_row, ss, lefts[1]))):
            rl, dl = row[RIGHT : RIGHT + 1], row[DOWN : DOWN + 1]
            ul = above(ref[g, DOWN : DOWN + 1], dl, lane1)
            diag = row[PAD : PAD + 1] + rl + ll + dl + ul
            inv = jnp.where(diag > 0, 1.0 / diag, 0.0)
            for n, value in enumerate((diag, rl, ll, dl, ul, inv)):
                sc[side, g, n : n + 1] = value
            z = jnp.where(row[LAB : LAB + 1] == window, row[BUMP : BUMP + 1], 0.0)
            (sz_s if side else sz_o)[g + 1] = z
            if side:
                qz[2 * g] = z
                qz[2 * g + 1] = roll(z, 64)

        at = pl.multiple_of(16 * g + 8, 8)
        beside = jnp.zeros((16, 128), F32)
        for s in range(16):
            beside = jnp.where(slot == s, roll(s_row[RIGHT : RIGHT + 1], 125 - 8 * s), beside)
        rl, dl = ext[2, pl.ds(at, 16)], ext[3, pl.ds(at, 16)]
        ll = roll(jnp.where(lane16 == 127, beside, rl), 1)
        last = ext[3, pl.ds(pl.multiple_of(at - 8, 8), 8)]
        ul = jnp.where(slot == 0, last[7:8], roll(dl, 1, 0))
        diag = ext[4, pl.ds(at, 16)] + rl + ll + dl + ul
        inv = jnp.where(diag > 0, 1.0 / diag, 0.0)
        for n, value in enumerate((diag, rl, ll, dl, ul, inv)):
            coef_ref[n, pl.ds(at, 16)] = value
        return 0

    lax.fori_loop(0, GROUPS, strips, 0, unroll=3)

    def strip_image(ref_o, ref_s, g, lane, sides):
        o, s = ref_o[g + 1], ref_s[g + 1]
        lefts, rights = pair_left(o, s, lane), pair_right(o, s, lane)
        done = []
        for side in sides:
            ref, here = (ref_s, s) if side else (ref_o, o)
            up = above(ref[g], here, lane)
            down = below(here, ref[g + 2], lane)
            c = [sc[side, g, n : n + 1] for n in range(5)]
            done.append(c[0] * here - c[1] * rights[side] - c[2] * lefts[side] - c[3] * down - c[4] * up)
        return done

    def strip_first(g, _):
        w = strip_image(sz_o, sz_s, g, lane16, (0, 1))
        for side, (source, ref) in enumerate(((so, y0_o), (ss, y0_s))):
            inv = sc[side, g, 5:6]
            ref[g + 1, 0:32] = inv * source[g + 1, 0:32]
            ref[g + 1, 32:48] = inv * w[side]
        y = y0_s[g + 1]
        q0[2 * g] = y
        q0[2 * g + 1] = roll(y, 64)
        return 0

    lax.fori_loop(0, GROUPS, strip_first, 0, unroll=3)

    def strip_second(g, _):
        (u,) = strip_image(y0_o, y0_s, g, lane48, (1,))
        y = sc[1, g, 5:6] * u
        q1[2 * g] = y
        q1[2 * g + 1] = roll(y, 64)
        return 0

    lax.fori_loop(0, GROUPS, strip_second, 0, unroll=3)

    def owned(g):
        return not isinstance(g, int)

    def coef(n, g, s):
        return coef_ref[n, pl.ds(8 * g + 8 + s, 1), :]

    def image(here, up, down, strip, g, s, lane):
        other = roll(strip[g], 125 - 8 * s)
        left = roll(jnp.where(lane == 127, other, here), 1)
        right = roll(jnp.where(lane == 0, other, here), 127)
        return (
            coef(0, g, s) * here
            - coef(1, g, s) * right
            - coef(2, g, s) * left
            - coef(3, g, s) * down
            - coef(4, g, s) * up
        )

    def basis(j):
        return jnp.where(ext[0, pl.ds(j, 1), :] == window, ext[1, pl.ds(j, 1), :], 0.0)

    def first_image(g, s):
        r, j = 8 * g - 8 + s, 8 * g + 8 + s
        w = image(basis(j), basis(j - 1), basis(j + 1), qz, g, s, lane16)
        if owned(g):
            b = rows_ref[r]
            w_ref[r] = w
        else:
            b = top_ref[r + HALO, 0:32] if r < 0 else bottom_ref[r - 128, 0:32]
        inv = coef(5, g, s)
        y0[8 * g + s, 0:32] = inv * b
        y0[8 * g + s, 32:48] = inv * w

    def second_image(g, s):
        i = 8 * g + s
        f1 = image(y0[i], y0[i - 1], y0[i + 1], q0, g, s, lane48)
        if owned(g):
            first_ref[8 * g - 8 + s] = f1
        y1[i] = coef(5, g, s) * f1

    def only(work):
        def step(g, _):
            for s in range(8):
                work(g, s)
            return 0

        return step

    for s in (6, 7):
        first_image(0, s)
    lax.fori_loop(1, 17, only(first_image), 0)
    for s in (0, 1):
        first_image(17, s)
    second_image(0, 7)
    lax.fori_loop(1, 17, only(second_image), 0)
    second_image(17, 0)

    gram[...] = jnp.zeros((96, 256), F32)

    def third_image(g, s):
        i = 8 * g + s
        second_ref[i - 8] = image(y1[i], y1[i - 1], y1[i + 1], q1, g, s, lane48)

    def products(g, sums):
        left, every = [], []
        sums = list(sums)
        for s in range(8):
            i = 8 * g + s
            r = i - 8
            b, f1, f2, y0r, y1r = rows_ref[r], first_ref[r], second_ref[r], y0[i], y1[i]
            left.append(jnp.concatenate([basis(i + 8), y0r[32:48], y1r[32:48]], axis=0))
            every.append(jnp.concatenate([b, w_ref[r], f1, f2], axis=0))
            pairs = ((y0r, b), (y0r, f1), (y1r, f1), (y1r, f2))
            sums = [t + p[0:32] * q[0:32] for t, (p, q) in zip(sums, pairs)]
        left = jnp.concatenate(parts_of(jnp.concatenate(left, axis=1), 2), axis=0)
        high, low = parts_of(jnp.concatenate(every, axis=1), 2)
        gram[:, 0:144] += fast_dot(left, high, NT) + fast_dot(left, low, NT)
        return tuple(sums)

    def last_stage(g, sums):
        sums = products(g - 1, sums)
        for s in range(8):
            third_image(g, s)
        return sums

    zero = jnp.zeros((32, 128), F32)
    lax.fori_loop(1, 2, only(third_image), 0)
    sums = lax.fori_loop(2, 17, last_stage, (zero, zero, zero, zero))
    sums = lax.fori_loop(16, 17, products, sums)

    a0, a1 = gram[0:48, 0:128] + gram[48:96, 0:128], gram[0:48, 128:256] + gram[48:96, 128:256]
    zr, w0, t0, w1, t1 = a0[0:16], a0[16:32], a0[32:48], a1[16:32], a1[32:48]
    matrices = jnp.zeros((16, 128), F32)
    for n, (x, z) in enumerate(((w0, 32), (w0, 80), (w1, 0), (zr, 32), (t1, 0))):
        start = 24 * n
        matrices = jnp.where((lane16 >= start) & (lane16 < start + 16), roll(x, (start - z) % 128), matrices)
    moved = jnp.zeros((16, 128), F32)
    for k in range(12):
        moved = jnp.where(slot == k, roll(matrices, (128 - k) % 128), moved)
    common = jnp.zeros((16, 128), F32)
    for n in range(5):
        for start, offset, count in ((20 + 2 * n, 0, 2), (30 + 3 * n, 3, 3)):
            hit = (lane16 >= start) & (lane16 < start + count)
            common = jnp.where(hit, roll(moved, (start - offset - 24 * n) % 128), common)
    lines = []
    diagonal = lanes((32, 128)) == lax.broadcasted_iota(jnp.int32, (32, 128), 0)
    for total in sums:
        column = jnp.sum(total, axis=1, keepdims=True)
        lines.append(jnp.sum(jnp.where(diagonal, column, 0.0), axis=0, keepdims=True))
    row4, lane4 = lax.broadcasted_iota(jnp.int32, (4, 128), 0), lanes((4, 128))
    for d in range(8):
        message = common
        for n, (x, z) in enumerate(((w0, 0), (w0, 48), (w0, 96), (zr, 0), (t0, 96))):
            hit = (lane16 >= 4 * n) & (lane16 < 4 * n + 4)
            message = jnp.where(hit, roll(x, (4 * n - z - 4 * d) % 128), message)
        middle, last = roll(message, 45), roll(message, 90)
        sent = jnp.where(lane4 < 45, message[0:4], jnp.where(lane4 < 90, middle[4:8], last[8:12]))
        line = jnp.zeros((1, 128), F32)
        for n in range(4):
            start = 120 + 4 * n if n < 2 else 112 + 4 * n
            line = jnp.where((lane1 >= start) & (lane1 < start + 4), roll(lines[n], (start - 4 * d) % 128), line)
            if n == 1:
                first_two, line = line, jnp.zeros((1, 128), F32)
        total = jnp.where(row4 == 0, first_two, jnp.where(row4 == 1, line, 0.0))
        out_ref[4 * d : 4 * d + 4] = jnp.where(lane4 < 120, sent, total)


def batched_inverse(a, lane, row, size):
    base = lane - lane % size
    for k in range(0, size, 2):
        at_k, at_n = lane % size == k, lane % size == k + 1
        left = jnp.take_along_axis(a, base + k, axis=1)
        right = jnp.take_along_axis(a, base + k + 1, axis=1)
        p, q, r, t = left[k : k + 1], right[k : k + 1], left[k + 1 : k + 2], right[k + 1 : k + 2]
        inverse = 1.0 / (p * t - q * r)
        upper = jnp.where(at_k[0:1], 1.0, jnp.where(at_n[0:1], 0.0, a[k : k + 1]))
        lower = jnp.where(at_n[0:1], 1.0, jnp.where(at_k[0:1], 0.0, a[k + 1 : k + 2]))
        first = (t * upper - q * lower) * inverse
        second = (p * lower - r * upper) * inverse
        rest = jnp.where(at_k | at_n, 0.0, a) - left * first - right * second
        a = jnp.where(row == k, first, jnp.where(row == k + 1, second, rest))
    return a


def block_inverse(matrix, low, high, size=16):
    lane = lanes((size, 128))
    row = lax.broadcasted_iota(jnp.int32, (size, 128), 0)
    compact = jnp.where(lane % size == row, 1.0, 0.0)
    for n in range(low // size, high // size):
        compact = jnp.where(lane // size == n, matrix[size * n : size * n + size], compact)
    compact = batched_inverse(compact, lane, row, size)
    parts = []
    for n in range(128 // size):
        active = low <= size * n < high
        parts.append(jnp.where(lane // size == n, compact, 0.0) if active else jnp.zeros((size, 128), F32))
    return jnp.concatenate(parts, axis=0)


def coarse_kernel(in_ref, out_ref, g, e, ei, first, second, near):
    pr, pc = lax.axis_index(ROW), lax.axis_index(COL)
    sub8 = lax.broadcasted_iota(jnp.int32, (8, 128), 0)

    lane8 = lanes((8, 128))
    for p in range(16):
        even, odd = jnp.zeros((8, 128), F32), jnp.zeros((8, 128), F32)
        for dr in range(3):
            r = p + 1 - dr
            if not 0 <= r < 16:
                continue
            at = [in_ref[pl.ds(32 * r + dq, 8, stride=4), :] for dq in range(4)]
            pair = (
                at[1] + jnp.where(sub8 >= 1, roll(at[3], 1, 0), 0.0),
                at[2] + jnp.where(sub8 < 7, roll(at[0], 7, 0), 0.0),
            )
            hit = lane8 < (30 if dr == 2 else 45)
            even, odd = (
                old + jnp.where(hit, roll(new, (128 - 45 * dr) % 128) if dr else new, 0.0)
                for old, new in zip((even, odd), pair)
            )
        g[pl.ds(16 * p, 8, stride=2), :] = even
        g[pl.ds(16 * p + 1, 8, stride=2), :] = odd
    tally = [
        roll(jnp.sum(in_ref[pl.ds(n, 128, stride=4), :], axis=0, keepdims=True), 8 + 8 * n) for n in range(2)
    ]
    tally = jnp.where(lanes((1, 128)) < 8, tally[0], tally[1])
    tally = jnp.broadcast_to(tally, (128, 128)).T
    bb, bu, uu, uuu = (tally[4 * n : 4 * n + 4, 0:1] for n in range(4))
    by_lane = jnp.concatenate([g[0:128].T, g[128:256].T], axis=1)

    lane16, row16 = lanes((16, 128)), lax.broadcasted_iota(jnp.int32, (16, 128), 0)
    for p in range(16):
        own = g[16 * p : 16 * p + 16]
        terms = [(own, d, dp, dq) for d, dp, dq in ((0, 0, 0), (1, 0, 1))]
        terms.append((roll(own, 1, 0), 1, 0, -1))
        if p < 15:
            terms += [(own, d, 1, dq) for d, dq in ((3, -1), (4, 0), (5, 1))]
        if p > 0:
            last = g[16 * p - 16 : 16 * p]
            terms += [(roll(last, 15, 0), 3, -1, 1), (last, 4, -1, 0), (roll(last, 1, 0), 5, -1, -1)]
        halves = [jnp.zeros((16, 128), F32), jnp.zeros((16, 128), F32)]
        for x, d, dp, dq in terms:
            target = POS[p + dp] * 16
            h, off = target // 128, target % 128
            q = row16 + dq
            hit = (lane16 == off + q) & (q >= 0) & (q < 16)
            at = 26 + d if d < 2 else 36 + d
            value = jnp.broadcast_to(x[:, at : at + 1], (16, 128))
            halves[h] = jnp.where(hit, value, halves[h])
        at = POS[p] * 16
        e[at : at + 16, 0:128] = halves[0]
        e[at : at + 16, 128:256] = halves[1]

    lane = lanes((128, 128))
    row = lax.broadcasted_iota(jnp.int32, (128, 128), 0)
    outer = block_inverse(e[0:128, 0:128], 0, 128)
    across = dot(outer, e[0:128, 128:256])
    schur = e[128:256, 128:256] - dot(e[128:256, 0:128], across)
    steps = []
    for low, high in ((0, 64), (64, 96)):
        inv = block_inverse(schur, low, high)
        link = jnp.where((row >= low) & (row < high) & (lane >= high), schur, 0.0)
        x = dot(inv, link)
        keep = jnp.where((row >= high) & (lane >= high), schur, 0.0)
        schur = keep - dot(link, x, TN)
        steps.append((inv, jnp.where((row == lane) & (row >= high), 1.0, 0.0) - x))
    inner = block_inverse(schur, 96, 128, 32)
    for inv, y in reversed(steps):
        inner = inv + dot(dot(y, inner), y, NT)
    half = dot(across, inner)
    near_diag = outer + dot(half, across, NT)

    def ordered(top_half, bottom_half):
        blocks = [top_half[16 * n : 16 * n + 16] for n in range(8)]
        blocks += [bottom_half[16 * n : 16 * n + 16] for n in range(8)]
        blocks = [blocks[POS[p]] for p in range(16)]
        return jnp.concatenate(blocks[:8], axis=0), jnp.concatenate(blocks[8:], axis=0)

    left_top, left_bottom = ordered(near_diag, -half.T)
    right_top, right_bottom = ordered(-half, inner)
    top_left, bottom_left = ordered(left_top.T, right_top.T)
    top_right, bottom_right = ordered(left_bottom.T, right_bottom.T)
    inverse = jnp.concatenate(
        [jnp.concatenate([top_left, bottom_left], axis=0), jnp.concatenate([top_right, bottom_right], axis=0)],
        axis=1,
    )
    for n, part in enumerate(parts_of(inverse, 3)):
        ei[n] = part

    def solve(z):
        rows = [part.astype(F32) for part in parts_of(z, 3)]
        rows = jnp.concatenate(rows + [jnp.zeros_like(z)], axis=0).astype(jnp.bfloat16)
        a, b, c = (fast_dot(rows, ei[n]) for n in range(3))
        return a[0:4] + (a[4:8] + b[0:4]) + (a[8:12] + b[4:8] + c[0:4])

    def apply(n, v):
        c = {d: by_lane[at : at + 1] for d, at in enumerate((20 + 2 * n, 21 + 2 * n, 0, 30 + 3 * n, 31 + 3 * n, 32 + 3 * n))}
        total = c[0] * v
        for d, step in ((1, 1), (3, 15), (4, 16), (5, 17)):
            total = total + c[d] * roll(v, 256 - step) + roll(c[d] * v, step)
        return total

    def inner_product(a, b):
        return jnp.sum(a * b, axis=1, keepdims=True)

    wb, wu, wuu, zb, tuu = (by_lane[4 * n : 4 * n + 4] for n in range(5))
    c0 = solve(zb)
    f_c, g_c, h_c, k_c = apply(0, c0), apply(1, c0), apply(2, c0), apply(4, c0)
    grad0 = wb - f_c
    k0 = solve(grad0)
    f_k, g_k = apply(0, k0), apply(1, k0)
    rho0 = bb - 2.0 * inner_product(c0, wb) + inner_product(c0, f_c)
    energy0 = bu - 2.0 * inner_product(c0, wu) + inner_product(c0, g_c)
    curve0 = energy0 - inner_product(k0, grad0)
    a0 = rho0 / curve0
    e1 = c0 - a0 * k0
    f_e = f_c - a0 * f_k
    g_e = g_c - a0 * g_k
    grad1 = wb - f_e + a0 * (g_c - wu)
    k1 = solve(grad1)

    def second_norm(m0, m1, m2, v0, v1, v2, e_image, c_image, last):
        own = m0 - 2.0 * inner_product(e1, v0) + inner_product(e1, e_image)
        mixed = m1 - inner_product(c0, v1) - inner_product(e1, v1) + inner_product(e1, c_image)
        far = m2 - 2.0 * inner_product(c0, v2) + inner_product(c0, last)
        return own - 2.0 * a0 * mixed + a0 * a0 * far

    rho1 = second_norm(bb, bu, uu, wb, wu, wuu, f_e, g_c, h_c)
    energy1 = second_norm(bu, uu, uuu, wu, wuu, tuu, g_e, h_c, k_c)
    beta = rho1 / rho0
    cross = (
        bu
        - inner_product(c0, wu)
        - inner_product(e1, wu)
        + inner_product(e1, g_c)
        - a0 * (uu - 2.0 * inner_product(c0, wuu) + inner_product(c0, h_c))
        - inner_product(k0, grad1)
    )
    curve1 = energy1 - inner_product(k1, grad1) + 2.0 * beta * cross + beta * beta * curve0
    a1 = rho1 / curve1

    mine = lax.broadcasted_iota(jnp.int32, (32, 256), 0) // 4 == pc

    def zone(value):
        value = jnp.broadcast_to(value, (4, 256))
        return jnp.where(mine, jnp.concatenate([value] * 8, axis=0), 0.0)

    ab = a1 * beta
    stacks = (
        (
            zone(a1 * k1 + ab * k0 - e1),
            zone(-(a0 + ab) * c0 - a1 * e1),
            zone((a0 + ab) * c0 + a1 * e1),
            zone((a1 * a0) * c0),
        ),
        (
            zone(-(a1 * a0) * c0),
            zone(c0 - (a0 + ab) * k0 - a1 * k1),
            zone(-a0 - a1 - ab),
            zone(a1 * a0),
        ),
    )
    out_ref[...] = jnp.zeros((256, 128), F32)
    for n, (ref, stack) in enumerate(((first, stacks[0]), (second, stacks[1]))):
        stack = jnp.concatenate(stack, axis=0)
        ref[0:8] = jnp.zeros((8, 128), F32)
        ref[8:136] = stack[:, 0:128].T
        ref[136:264] = stack[:, 128:256].T
        ref[264:272] = jnp.zeros((8, 128), F32)
        for dr in range(3):
            p = jnp.clip(pr - 1 + dr, 0, 15)
            near[...] = ref[pl.ds(pl.multiple_of(16 * p, 16), 32), :]
            for dq in range(4):
                out_ref[pl.ds(16 * n + 4 * dr + dq, 8, stride=32), :] = near[pl.ds(7 + dq, 8, stride=2), :]


def outputs_kernel(
    rows_ref, first_ref, second_ref, w_ref, grid_ref, coef_ref, m_ref, sol_ref, res_ref,
    left_ref, step_ref, window_ref,
):
    block = pl.program_id(0)

    @pl.when(block == 0)
    def _():
        pr, pc = lax.axis_index(ROW), lax.axis_index(COL)
        slot = lax.broadcasted_iota(jnp.int32, (16, 128), 0)
        region_row = pr - 1 + slot // 4
        region_col = 2 * pc - 1 + slot % 4
        inside = (slot < 12) & (region_row >= 0) & (region_row < REG) & (region_col >= 0) & (region_col < REG)
        window_ref[...] = jnp.where(inside, region_row * REG + region_col, -1).astype(F32)
        total = m_ref[0:32]
        for n in range(1, 8):
            total = total + m_ref[32 * n : 32 * n + 32]
        top, bottom = total[0:16], total[16:32]
        lane = lanes((16, 128))
        steps = jnp.where(slot == 0, roll(bottom[5:6], 64), jnp.where(slot == 1, roll(bottom[5:6], 32), 0.0))
        m = jnp.concatenate(
            [
                jnp.where((lane >= 64) & (lane < 96), roll(bottom, 32), 0.0),
                jnp.where(lane < 64, top, 0.0),
                jnp.where(lane < 64, roll(top, 64), 0.0),
                jnp.where(lane < 32, bottom, 0.0),
                steps,
                jnp.zeros((48, 128), F32),
            ],
            axis=0,
        ).T
        c1, c2, c3 = parts_of(m[0:96, 0:64], 3)
        left_ref[...] = jnp.concatenate([c1, c1, c2, c2, c1, c3], axis=1)
        for n in range(2):
            step_ref[n] = jnp.broadcast_to(m[0:32, 64 + n : 65 + n], (32, 128))

    left, window = left_ref[...], window_ref[...]
    for part in range(4):
        rows = []
        for n in range(8):
            r = 32 * block + 8 * part + n
            z = jnp.where(grid_ref[pl.ds(r, 1), :] == window, grid_ref[pl.ds(128 + r, 1), :], 0.0)
            rows.append(jnp.concatenate([z, w_ref[r], first_ref[r, 32:48], second_ref[r, 32:48]], axis=0))
        r1, r2, r3 = parts_of(jnp.concatenate(rows, axis=1), 3)
        d = fast_dot(left, jnp.concatenate([r1, r2, r1, r2, r3, r1], axis=0))
        for n in range(8):
            r = 32 * block + 8 * part + n
            b, u, uu = rows_ref[r], first_ref[r, 0:32], second_ref[r, 0:32]
            e = d[:, 128 * n : 128 * n + 128]
            inv = coef_ref[5, pl.ds(r + 16, 1), :]
            p1, p2 = step_ref[0], step_ref[1]
            res_ref[:, 8 * part + n] = b + p1 * u + p2 * uu + e[0:32]
            sol_ref[:, 8 * part + n] = inv * (e[32:64] - p1 * b - p2 * u) + e[64:96]


def swapped(value, axis, start):
    pairs = [(i, i + 1) for i in range(start, lax.axis_size(axis) - 1, 2)]
    return lax.ppermute(value, axis, pairs + [(b, a) for a, b in pairs])


def shape_of(*dims):
    return jax.ShapeDtypeStruct(dims, F32)


def kept(*dims):
    return pltpu.VMEM(dims, F32)


def vmem(*dims):
    return pltpu.VMEM(dims, F32)


def body(load_currents, labels, bump_height, horizontal_class, vertical_class, pad_class, edge_table, pad_table):
    rows, cols = lax.axis_size(ROW), lax.axis_size(COL)
    loads = load_currents.reshape(-1, 128)
    grid, far_rows, near_rows = pl.pallas_call(
        prepare_kernel,
        out_shape=(kept(1024, 128), shape_of(HALO, SUB, 128), shape_of(HALO, SUB, 128)),
        compiler_params=limited,
        in_specs=[outside] * 8,
        out_specs=(whole,) * 3,
        scratch_shapes=[pltpu.SMEM((8,), F32), pltpu.SMEM((8,), F32), vmem(32, 8, 128), vmem(32, 8, 128)]
        + [pltpu.VMEM((128, 128), jnp.int32)] * 4
        + [pltpu.SemaphoreType.DMA((9,))],
    )(
        *(
            pltpu.with_memory_space_constraint(x, pltpu.HBM)
            for x in (
                edge_table, pad_table, load_currents, labels, bump_height,
                horizontal_class, vertical_class, pad_class,
            )
        ),
    )
    far_rows = swapped(far_rows, ROW, 1)
    near_rows = swapped(near_rows, ROW, 0)
    by_rows, own = pl.pallas_call(
        pack_kernel,
        out_shape=(kept(128, 32, 128), kept(GROUPS, SUB, 128)),
        compiler_params=limited,
        in_specs=[whole] * 2,
        out_specs=(whole,) * 2,
    )(loads, grid)
    own, top, bottom, far_columns, near_columns = pl.pallas_call(
        corner_kernel,
        out_shape=(kept(GROUPS, SUB, 128), kept(HALO, SUB, 128), kept(HALO, SUB, 128))
        + (shape_of(5, SUB, 128),) * 2,
        compiler_params=limited,
        in_specs=[whole] * 3,
        out_specs=(whole,) * 5,
    )(own, far_rows, near_rows)
    far_columns = swapped(far_columns, COL, 1)
    near_columns = swapped(near_columns, COL, 0)
    first, second, w, coef, payload = pl.pallas_call(
        fields_kernel,
        out_shape=(
            kept(128, 48, 128),
            kept(128, 48, 128),
            kept(128, 16, 128),
            kept(6, 160, 128),
            shape_of(32, 128),
        ),
        compiler_params=limited,
        in_specs=[whole] * 7,
        out_specs=(whole,) * 5,
        scratch_shapes=[
            vmem(5, 160, 128),
            vmem(GROUPS + 2, SUB, 128),
            vmem(GROUPS + 2, SUB, 128),
            vmem(GROUPS + 2, 16, 128),
            vmem(GROUPS + 2, 16, 128),
            vmem(GROUPS + 2, 48, 128),
            vmem(GROUPS + 2, 48, 128),
            vmem(2 * GROUPS, 16, 128),
            vmem(2 * GROUPS, 48, 128),
            vmem(2 * GROUPS, 48, 128),
            vmem(2, GROUPS, 8, 128),
            vmem(144, 48, 128),
            vmem(144, 48, 128),
            vmem(96, 256),
        ],
    )(by_rows, grid, top, bottom, own, far_columns, near_columns)
    sent = jnp.broadcast_to(payload.reshape(1, cols, 4, 128), (rows, cols, 4, 128)).reshape(-1, 4, 128)
    everything = lax.all_to_all(sent, ROW + COL, 0, 0, tiled=True).reshape(-1, 128)
    found = pl.pallas_call(
        coarse_kernel,
        out_shape=shape_of(256, 128),
        compiler_params=limited,
        in_specs=[whole],
        out_specs=whole,
        scratch_shapes=[
            vmem(256, 128),
            vmem(256, 256),
            pltpu.VMEM((3, 256, 256), jnp.bfloat16),
            vmem(272, 128),
            vmem(272, 128),
            vmem(32, 128),
        ],
    )(everything)
    matrix = lax.all_to_all(found.reshape(cols, 32, 128), COL, 0, 0, tiled=True).reshape(-1, 128)
    by_block = pl.BlockSpec((32, 32, 128), lambda k: (0, k, 0))
    return pl.pallas_call(
        outputs_kernel,
        grid=(4,),
        out_shape=(shape_of(32, 128, 128), shape_of(32, 128, 128)),
        compiler_params=limited,
        in_specs=[whole] * 7,
        out_specs=(by_block, by_block),
        scratch_shapes=[pltpu.VMEM((96, 384), jnp.bfloat16), vmem(2, 32, 128), vmem(16, 128)],
    )(by_rows, first, second, w, grid, coef, matrix)


def solution(mesh):
    finer = Mesh(mesh.devices.reshape(4, 4, 4, 2), ("row_0", "row_1", "col_0", "col_1"))
    grid = P(ROW, COL)
    return jax.shard_map(
        body,
        mesh=finer,
        in_specs=(P(None, ROW, COL), grid, grid, grid, grid, grid, P(), P()),
        out_specs=(P(None, ROW, COL), P(None, ROW, COL)),
        check_vma=False,
    )
```

```python
import jax
import jax.numpy as jnp
from jax import lax
from jax.experimental import pallas as pl
from jax.experimental.pallas import tpu as pltpu
from jax.sharding import Mesh
from jax.sharding import PartitionSpec as P

REG = 16
ROW = ("row_0", "row_1")
COL = ("col_0", "col_1")
F32 = jnp.float32

LAB, BUMP, RIGHT, DOWN, PAD = 32, 33, 34, 35, 36
SUB = 40
HALO = 3
GROUPS = 9
ORDER = (1, 3, 5, 7, 9, 11, 13, 15, 2, 6, 10, 14, 4, 12, 8, 0)
POS = tuple(ORDER.index(p) for p in range(16))
NT = (((1,), (1,)), ((), ()))
NN = (((1,), (0,)), ((), ()))
TN = (((0,), (0,)), ((), ()))
whole = pl.BlockSpec(memory_space=pltpu.VMEM)
outside = pl.BlockSpec(memory_space=pltpu.HBM)
limited = pltpu.CompilerParams(vmem_limit_bytes=32 * 2**20)


def parts_of(x, count):
    parts = []
    for n in range(count):
        parts.append(x.astype(jnp.bfloat16))
        if n + 1 < count:
            x = x - parts[-1].astype(F32)
    return parts


def fast_dot(a, b, dims=NN):
    return lax.dot_general(a, b, dims, preferred_element_type=F32)


def dot(a, b, dims=NN):
    (at_a,), (at_b,) = dims[0]
    a1, a2, a3 = parts_of(a, 3)
    b1, b2, b3 = parts_of(b, 3)
    return fast_dot(
        jnp.concatenate([a3, a1, a2, a2, a1, a1], axis=at_a),
        jnp.concatenate([b1, b3, b2, b1, b2, b1], axis=at_b),
        dims,
    )


def lanes(shape):
    return lax.broadcasted_iota(jnp.int32, shape, len(shape) - 1)


def roll(x, shift, axis=1):
    return pltpu.roll(x, shift, axis)


def prepare_kernel(
    edge_hbm, pad_hbm, load_hbm, label_hbm, bump_hbm, across_hbm, down_hbm, pad_class_hbm,
    grid_ref, far_ref, near_ref, edge_ref, pad_ref, load_ref, load_end_ref, label_ref, across_ref, down_ref, pad_class_ref, done,
):
    copies = [
        pltpu.make_async_copy(source, target, done.at[n])
        for n, (source, target) in enumerate(
            (
                (edge_hbm, edge_ref),
                (pad_hbm, pad_ref),
                (across_hbm, across_ref),
                (down_hbm, down_ref),
                (pad_class_hbm, pad_class_ref),
                (label_hbm, label_ref),
                (bump_hbm, grid_ref.at[pl.ds(128, 128)]),
                (load_hbm.at[:, pl.ds(0, 8)], load_ref),
                (load_hbm.at[:, pl.ds(120, 8)], load_end_ref),
            )
        )
    ]
    for copy in copies:
        copy.start()
    for copy in copies:
        copy.wait()
    pr, pc = lax.axis_index(ROW), lax.axis_index(COL)
    shape = (128, 128)
    row, lane = lax.broadcasted_iota(jnp.int32, shape, 0), lanes(shape)

    def lookup(table, classes):
        found = jnp.zeros(shape, F32)
        for n in range(8):
            found = jnp.where(classes == n, table[n], found)
        return found

    right = lookup(edge_ref, across_ref[...])
    down = lookup(edge_ref, down_ref[...])
    grid_ref[0:128] = label_ref[...].astype(F32)
    grid_ref[256:384] = jnp.where((lane == 127) & (pc == 7), 0.0, right)
    grid_ref[384:512] = jnp.where((row == 127) & (pr == 15), 0.0, down)
    grid_ref[512:640] = lookup(pad_ref, pad_class_ref[...])
    grid_ref[640:1024] = jnp.zeros((384, 128), F32)
    for n in range(HALO):
        even = pr % 2 == 0
        first, last = load_ref[:, n], load_end_ref[:, 8 - HALO + n]
        far_ref[n, 0:32] = jnp.where(even, first, last)
        near_ref[n, 0:32] = jnp.where(even, last, first)
        first = grid_ref[pl.ds(n, 8, stride=128), :]
        last = grid_ref[pl.ds(128 - HALO + n, 8, stride=128), :]
        far_ref[n, 32:40] = jnp.where(even, first, last)
        near_ref[n, 32:40] = jnp.where(even, last, first)


def pack_kernel(load_ref, grid_ref, rows_ref, own_ref):
    lane = lanes((32, 128)) // 8

    def group(g, slots):
        loads, rest = jnp.zeros((32, 128), F32), jnp.zeros((8, 128), F32)
        for s in slots:
            r = 16 * g - 8 + s
            b = load_ref[pl.ds(r, 32, stride=128), :]
            rows_ref[r] = b
            loads = jnp.where(lane == s, roll(b, (8 * s + 3) % 128), loads)
            rest = jnp.where(lane[0:8] == s, roll(grid_ref[pl.ds(r, 8, stride=128), :], (8 * s + 3) % 128), rest)
        own_ref[g, 0:32] = loads
        own_ref[g, 32:40] = rest

    group(0, range(8, 16))
    group(8, range(8))

    def step(g, _):
        group(g, range(16))
        return 0

    lax.fori_loop(1, 8, step, 0)


def corner_kernel(
    own_ref, far_ref, near_ref, out_ref, top_ref, bottom_ref, far_out_ref, near_out_ref
):
    lane = lanes((SUB, 128)) // 8
    even = lax.axis_index(ROW) % 2 == 0
    top_ref[...] = jnp.where(even, far_ref[...], near_ref[...])
    bottom_ref[...] = jnp.where(even, near_ref[...], far_ref[...])
    for g in range(GROUPS):
        out_ref[g] = own_ref[g]
    start, end = own_ref[0], own_ref[8]
    for n in range(HALO):
        s = 8 - HALO + n
        start = jnp.where(lane == s, roll(top_ref[n], (8 * s + 3) % 128), start)
        s = 8 + n
        end = jnp.where(lane == s, roll(bottom_ref[n], (8 * s + 3) % 128), end)
    out_ref[0] = start
    out_ref[8] = end
    low = lanes((SUB, 128)) % 8 < 4
    to_right_first = lax.axis_index(COL) % 2 == 1
    for h in range(5):
        here = out_ref[2 * h]
        after = out_ref[2 * h + 1] if h < 4 else here
        right = jnp.where(low, here, roll(after, 4))
        left = jnp.where(low, roll(here, 125), roll(after, 1))
        far_out_ref[h] = jnp.where(to_right_first, right, left)
        near_out_ref[h] = jnp.where(to_right_first, left, right)


def fields_kernel(
    rows_ref, grid_ref, top_ref, bottom_ref, own_ref, far_ref, near_ref,
    first_ref, second_ref, w_ref, coef_ref, out_ref,
    ext, so, ss, sz_o, sz_s, y0_o, y0_s, qz, q0, q1, u0, u1, sc, y0, y1, gram,
):
    pr, pc = lax.axis_index(ROW), lax.axis_index(COL)
    lane1 = lanes((1, 128))
    lane16 = lanes((16, 128))
    lane48 = lanes((48, 128))

    for n in range(5):
        ext[n, 0:16] = jnp.zeros((16, 128), F32)
        ext[n, 16:144] = grid_ref[128 * n : 128 * n + 128]
        ext[n, 144:160] = jnp.zeros((16, 128), F32)
        for k in range(HALO):
            ext[n, 16 - HALO + k : 17 - HALO + k] = top_ref[k, 32 + n : 33 + n]
            ext[n, 144 + k : 145 + k] = bottom_ref[k, 32 + n : 33 + n]

    slot = lax.broadcasted_iota(jnp.int32, (16, 128), 0)
    region_row = pr - 1 + slot // 4
    region_col = 2 * pc - 1 + slot % 4
    inside = (slot < 12) & (region_row >= 0) & (region_row < REG) & (region_col >= 0) & (region_col < REG)
    window = jnp.where(inside, region_row * REG + region_col, -1).astype(F32)

    for ref in (so, ss, sz_o, sz_s, y0_o, y0_s):
        ref[0] = jnp.zeros(ref.shape[1:], F32)
        ref[GROUPS + 1] = jnp.zeros(ref.shape[1:], F32)

    def pair_left(o, s, lane):
        j = lane % 8
        return roll(jnp.where(j == 2, s, o), 1), roll(jnp.where(j == 2, o, s), 1)

    def pair_right(o, s, lane):
        j = lane % 8
        return roll(jnp.where(j == 3, s, o), 127), roll(jnp.where(j == 3, o, s), 127)

    def above(before, here, lane):
        return roll(jnp.where(lane >= 120, before, here), 8)

    def below(here, after, lane):
        return roll(jnp.where(lane < 8, after, here), 120)

    even = pc % 2 == 0

    def strips(g, _):
        o_row = own_ref[g]
        far, near = far_ref[g // 2], near_ref[g // 2]
        on_left, on_right = jnp.where(even, far, near), jnp.where(even, near, far)
        turn = 124 * (g % 2)
        s_row = jnp.where(lanes((SUB, 128)) % 8 < 3, roll(on_left, turn), roll(on_right, 3 + turn))
        so[g + 1], ss[g + 1] = o_row, s_row
        lefts = pair_left(o_row[RIGHT : RIGHT + 1], s_row[RIGHT : RIGHT + 1], lane1)
        for side, (row, ref, ll) in enumerate(((o_row, so, lefts[0]), (s_row, ss, lefts[1]))):
            rl, dl = row[RIGHT : RIGHT + 1], row[DOWN : DOWN + 1]
            ul = above(ref[g, DOWN : DOWN + 1], dl, lane1)
            diag = row[PAD : PAD + 1] + rl + ll + dl + ul
            inv = jnp.where(diag > 0, 1.0 / diag, 0.0)
            for n, value in enumerate((diag, rl, ll, dl, ul, inv)):
                sc[side, g, n : n + 1] = value
            z = jnp.where(row[LAB : LAB + 1] == window, row[BUMP : BUMP + 1], 0.0)
            (sz_s if side else sz_o)[g + 1] = z
            if side:
                qz[2 * g] = z
                qz[2 * g + 1] = roll(z, 64)

        at = pl.multiple_of(16 * g + 8, 8)
        beside = jnp.zeros((16, 128), F32)
        for s in range(16):
            beside = jnp.where(slot == s, roll(s_row[RIGHT : RIGHT + 1], 125 - 8 * s), beside)
        rl, dl = ext[2, pl.ds(at, 16)], ext[3, pl.ds(at, 16)]
        ll = roll(jnp.where(lane16 == 127, beside, rl), 1)
        last = ext[3, pl.ds(pl.multiple_of(at - 8, 8), 8)]
        ul = jnp.where(slot == 0, last[7:8], roll(dl, 1, 0))
        diag = ext[4, pl.ds(at, 16)] + rl + ll + dl + ul
        inv = jnp.where(diag > 0, 1.0 / diag, 0.0)
        for n, value in enumerate((diag, rl, ll, dl, ul, inv)):
            coef_ref[n, pl.ds(at, 16)] = value
        return 0

    lax.fori_loop(0, GROUPS, strips, 0, unroll=3)

    def strip_image(ref_o, ref_s, g, lane, sides):
        o, s = ref_o[g + 1], ref_s[g + 1]
        lefts, rights = pair_left(o, s, lane), pair_right(o, s, lane)
        done = []
        for side in sides:
            ref, here = (ref_s, s) if side else (ref_o, o)
            up = above(ref[g], here, lane)
            down = below(here, ref[g + 2], lane)
            c = [sc[side, g, n : n + 1] for n in range(5)]
            done.append(c[0] * here - c[1] * rights[side] - c[2] * lefts[side] - c[3] * down - c[4] * up)
        return done

    def strip_first(g, _):
        w = strip_image(sz_o, sz_s, g, lane16, (0, 1))
        for side, (source, ref) in enumerate(((so, y0_o), (ss, y0_s))):
            inv = sc[side, g, 5:6]
            ref[g + 1, 0:32] = inv * source[g + 1, 0:32]
            ref[g + 1, 32:48] = inv * w[side]
        y = y0_s[g + 1]
        q0[2 * g] = y
        q0[2 * g + 1] = roll(y, 64)
        return 0

    lax.fori_loop(0, GROUPS, strip_first, 0, unroll=3)

    def strip_second(g, _):
        (u,) = strip_image(y0_o, y0_s, g, lane48, (1,))
        y = sc[1, g, 5:6] * u
        q1[2 * g] = y
        q1[2 * g + 1] = roll(y, 64)
        return 0

    lax.fori_loop(0, GROUPS, strip_second, 0, unroll=3)

    def owned(g):
        return not isinstance(g, int)

    def coef(n, g, s):
        return coef_ref[n, pl.ds(8 * g + 8 + s, 1), :]

    def unpacked(strip, g, s):
        return roll(strip[g], 125 - 8 * s)

    def image(here, up, down, other, g, s, lane):
        left = roll(jnp.where(lane == 127, other, here), 1)
        right = roll(jnp.where(lane == 0, other, here), 127)
        return (
            coef(0, g, s) * here
            - coef(1, g, s) * right
            - coef(2, g, s) * left
            - coef(3, g, s) * down
            - coef(4, g, s) * up
        )

    def basis(j):
        return jnp.where(ext[0, pl.ds(j, 1), :] == window, ext[1, pl.ds(j, 1), :], 0.0)

    def first_image(g, s):
        r, j = 8 * g - 8 + s, 8 * g + 8 + s
        w = image(basis(j), basis(j - 1), basis(j + 1), unpacked(qz, g, s), g, s, lane16)
        if owned(g):
            b = rows_ref[r]
            w_ref[r] = w
        else:
            b = top_ref[r + HALO, 0:32] if r < 0 else bottom_ref[r - 128, 0:32]
        inv = coef(5, g, s)
        y0[8 * g + s, 0:32] = inv * b
        y0[8 * g + s, 32:48] = inv * w
        u0[8 * g + s] = unpacked(q0, g, s)
        u1[8 * g + s] = unpacked(q1, g, s)

    def second_image(g, s):
        i = 8 * g + s
        f1 = image(y0[i], y0[i - 1], y0[i + 1], u0[i], g, s, lane48)
        if owned(g):
            first_ref[8 * g - 8 + s] = f1
        y1[i] = coef(5, g, s) * f1

    def only(work):
        def step(g, _):
            for s in range(8):
                work(g, s)
            return 0

        return step

    for s in (6, 7):
        first_image(0, s)
    lax.fori_loop(1, 17, only(first_image), 0)
    for s in (0, 1):
        first_image(17, s)
    second_image(0, 7)

    def second_pair(t, _):
        for s in range(16):
            second_image(2 * t + 1 + s // 8, s % 8)
        return 0

    lax.fori_loop(0, 8, second_pair, 0)
    second_image(17, 0)

    gram[...] = jnp.zeros((96, 256), F32)

    def third_image(g, s):
        i = 8 * g + s
        second_ref[i - 8] = image(y1[i], y1[i - 1], y1[i + 1], u1[i], g, s, lane48)

    def products(g, sums):
        left, every = [], []
        sums = list(sums)
        for s in range(8):
            i = 8 * g + s
            r = i - 8
            b, f1, f2, y0r, y1r = rows_ref[r], first_ref[r], second_ref[r], y0[i], y1[i]
            left.append(jnp.concatenate([basis(i + 8), y0r[32:48], y1r[32:48]], axis=0))
            every.append(jnp.concatenate([b, w_ref[r], f1, f2], axis=0))
            pairs = ((y0r, b), (y0r, f1), (y1r, f1), (y1r, f2))
            sums = [t + p[0:32] * q[0:32] for t, (p, q) in zip(sums, pairs)]
        left = jnp.concatenate(parts_of(jnp.concatenate(left, axis=1), 2), axis=0)
        high, low = parts_of(jnp.concatenate(every, axis=1), 2)
        gram[:, 0:144] += fast_dot(left, high, NT) + fast_dot(left, low, NT)
        return tuple(sums)

    def last_stage(g, sums):
        sums = products(g - 1, sums)
        for s in range(8):
            third_image(g, s)
        return sums

    zero = jnp.zeros((32, 128), F32)
    lax.fori_loop(1, 2, only(third_image), 0)
    sums = lax.fori_loop(2, 17, last_stage, (zero, zero, zero, zero))
    sums = lax.fori_loop(16, 17, products, sums)

    a0, a1 = gram[0:48, 0:128] + gram[48:96, 0:128], gram[0:48, 128:256] + gram[48:96, 128:256]
    zr, w0, t0, w1, t1 = a0[0:16], a0[16:32], a0[32:48], a1[16:32], a1[32:48]
    matrices = jnp.zeros((16, 128), F32)
    for n, (x, z) in enumerate(((w0, 32), (w0, 80), (w1, 0), (zr, 32), (t1, 0))):
        start = 24 * n
        matrices = jnp.where((lane16 >= start) & (lane16 < start + 16), roll(x, (start - z) % 128), matrices)
    moved = jnp.zeros((16, 128), F32)
    for k in range(12):
        moved = jnp.where(slot == k, roll(matrices, (128 - k) % 128), moved)
    common = jnp.zeros((16, 128), F32)
    for n in range(5):
        for start, offset, count in ((20 + 2 * n, 0, 2), (30 + 3 * n, 3, 3)):
            hit = (lane16 >= start) & (lane16 < start + count)
            common = jnp.where(hit, roll(moved, (start - offset - 24 * n) % 128), common)
    lines = []
    diagonal = lanes((32, 128)) == lax.broadcasted_iota(jnp.int32, (32, 128), 0)
    for total in sums:
        column = jnp.sum(total, axis=1, keepdims=True)
        lines.append(jnp.sum(jnp.where(diagonal, column, 0.0), axis=0, keepdims=True))
    row4, lane4 = lax.broadcasted_iota(jnp.int32, (4, 128), 0), lanes((4, 128))
    for d in range(8):
        message = common
        for n, (x, z) in enumerate(((w0, 0), (w0, 48), (w0, 96), (zr, 0), (t0, 96))):
            hit = (lane16 >= 4 * n) & (lane16 < 4 * n + 4)
            message = jnp.where(hit, roll(x, (4 * n - z - 4 * d) % 128), message)
        middle, last = roll(message, 45), roll(message, 90)
        sent = jnp.where(lane4 < 45, message[0:4], jnp.where(lane4 < 90, middle[4:8], last[8:12]))
        line = jnp.zeros((1, 128), F32)
        for n in range(4):
            start = 120 + 4 * n if n < 2 else 112 + 4 * n
            line = jnp.where((lane1 >= start) & (lane1 < start + 4), roll(lines[n], (start - 4 * d) % 128), line)
            if n == 1:
                first_two, line = line, jnp.zeros((1, 128), F32)
        total = jnp.where(row4 == 0, first_two, jnp.where(row4 == 1, line, 0.0))
        sent = jnp.where(lane4 < 120, sent, total)
        if d % 2 == 0:
            before = sent
            continue
        pair = jnp.concatenate([before, sent], axis=0)
        for r in range(16):
            out_ref[32 * r + 4 * d - 4 : 32 * r + 4 * d + 4] = pair


def batched_inverse(a, lane, row, size):
    base = lane - lane % size
    for k in range(0, size, 2):
        at_k, at_n = lane % size == k, lane % size == k + 1
        left = jnp.take_along_axis(a, base + k, axis=1)
        right = jnp.take_along_axis(a, base + k + 1, axis=1)
        p, q, r, t = left[k : k + 1], right[k : k + 1], left[k + 1 : k + 2], right[k + 1 : k + 2]
        inverse = 1.0 / (p * t - q * r)
        upper = jnp.where(at_k[0:1], 1.0, jnp.where(at_n[0:1], 0.0, a[k : k + 1]))
        lower = jnp.where(at_n[0:1], 1.0, jnp.where(at_k[0:1], 0.0, a[k + 1 : k + 2]))
        first = (t * upper - q * lower) * inverse
        second = (p * lower - r * upper) * inverse
        rest = jnp.where(at_k | at_n, 0.0, a) - left * first - right * second
        a = jnp.where(row == k, first, jnp.where(row == k + 1, second, rest))
    return a


def block_inverse(matrix, low, high, size=16):
    lane = lanes((size, 128))
    row = lax.broadcasted_iota(jnp.int32, (size, 128), 0)
    compact = jnp.where(lane % size == row, 1.0, 0.0)
    for n in range(low // size, high // size):
        compact = jnp.where(lane // size == n, matrix[size * n : size * n + size], compact)
    compact = batched_inverse(compact, lane, row, size)
    parts = []
    for n in range(128 // size):
        active = low <= size * n < high
        parts.append(jnp.where(lane // size == n, compact, 0.0) if active else jnp.zeros((size, 128), F32))
    return jnp.concatenate(parts, axis=0)


def coarse_kernel(in_ref, out_ref, g, e, ei, first, second, near):
    pr, pc = lax.axis_index(ROW), lax.axis_index(COL)
    sub8 = lax.broadcasted_iota(jnp.int32, (8, 128), 0)

    lane8 = lanes((8, 128))
    for p in range(16):
        even, odd = jnp.zeros((8, 128), F32), jnp.zeros((8, 128), F32)
        for dr in range(3):
            r = p + 1 - dr
            if not 0 <= r < 16:
                continue
            at = [in_ref[pl.ds(32 * r + dq, 8, stride=4), :] for dq in range(4)]
            pair = (
                at[1] + jnp.where(sub8 >= 1, roll(at[3], 1, 0), 0.0),
                at[2] + jnp.where(sub8 < 7, roll(at[0], 7, 0), 0.0),
            )
            hit = lane8 < (30 if dr == 2 else 45)
            even, odd = (
                old + jnp.where(hit, roll(new, (128 - 45 * dr) % 128) if dr else new, 0.0)
                for old, new in zip((even, odd), pair)
            )
        g[pl.ds(16 * p, 8, stride=2), :] = even
        g[pl.ds(16 * p + 1, 8, stride=2), :] = odd
    tally = [
        roll(jnp.sum(in_ref[pl.ds(n, 128, stride=4), :], axis=0, keepdims=True), 8 + 8 * n) for n in range(2)
    ]
    tally = jnp.where(lanes((1, 128)) < 8, tally[0], tally[1])
    tally = jnp.broadcast_to(tally, (128, 128)).T
    bb, bu, uu, uuu = (tally[4 * n : 4 * n + 4, 0:1] for n in range(4))
    by_lane = jnp.concatenate([g[0:128].T, g[128:256].T], axis=1)

    lane16, row16 = lanes((16, 128)), lax.broadcasted_iota(jnp.int32, (16, 128), 0)
    for p in range(16):
        own = g[16 * p : 16 * p + 16]
        terms = [(own, d, dp, dq) for d, dp, dq in ((0, 0, 0), (1, 0, 1))]
        terms.append((roll(own, 1, 0), 1, 0, -1))
        if p < 15:
            terms += [(own, d, 1, dq) for d, dq in ((3, -1), (4, 0), (5, 1))]
        if p > 0:
            last = g[16 * p - 16 : 16 * p]
            terms += [(roll(last, 15, 0), 3, -1, 1), (last, 4, -1, 0), (roll(last, 1, 0), 5, -1, -1)]
        halves = [jnp.zeros((16, 128), F32), jnp.zeros((16, 128), F32)]
        for x, d, dp, dq in terms:
            target = POS[p + dp] * 16
            h, off = target // 128, target % 128
            q = row16 + dq
            hit = (lane16 == off + q) & (q >= 0) & (q < 16)
            at = 26 + d if d < 2 else 36 + d
            value = jnp.broadcast_to(x[:, at : at + 1], (16, 128))
            halves[h] = jnp.where(hit, value, halves[h])
        at = POS[p] * 16
        e[at : at + 16, 0:128] = halves[0]
        e[at : at + 16, 128:256] = halves[1]

    lane = lanes((128, 128))
    row = lax.broadcasted_iota(jnp.int32, (128, 128), 0)
    outer = block_inverse(e[0:128, 0:128], 0, 128)
    across = dot(outer, e[0:128, 128:256])
    schur = e[128:256, 128:256] - dot(e[128:256, 0:128], across)
    steps = []
    for low, high in ((0, 64), (64, 96)):
        inv = block_inverse(schur, low, high)
        link = jnp.where((row >= low) & (row < high) & (lane >= high), schur, 0.0)
        x = dot(inv, link)
        keep = jnp.where((row >= high) & (lane >= high), schur, 0.0)
        schur = keep - dot(link, x, TN)
        steps.append((inv, jnp.where((row == lane) & (row >= high), 1.0, 0.0) - x))
    inner = block_inverse(schur, 96, 128, 32)
    for inv, y in reversed(steps):
        inner = inv + dot(dot(y, inner), y, NT)
    half = dot(across, inner)
    near_diag = outer + dot(half, across, NT)

    def ordered(top_half, bottom_half):
        blocks = [top_half[16 * n : 16 * n + 16] for n in range(8)]
        blocks += [bottom_half[16 * n : 16 * n + 16] for n in range(8)]
        blocks = [blocks[POS[p]] for p in range(16)]
        return jnp.concatenate(blocks[:8], axis=0), jnp.concatenate(blocks[8:], axis=0)

    left_top, left_bottom = ordered(near_diag, -half.T)
    right_top, right_bottom = ordered(-half, inner)
    top_left, bottom_left = ordered(left_top.T, right_top.T)
    top_right, bottom_right = ordered(left_bottom.T, right_bottom.T)
    inverse = jnp.concatenate(
        [jnp.concatenate([top_left, bottom_left], axis=0), jnp.concatenate([top_right, bottom_right], axis=0)],
        axis=1,
    )
    for n, part in enumerate(parts_of(inverse, 3)):
        ei[n] = part

    def solve(z):
        rows = [part.astype(F32) for part in parts_of(z, 3)]
        rows = jnp.concatenate(rows + [jnp.zeros_like(z)], axis=0).astype(jnp.bfloat16)
        a, b, c = (fast_dot(rows, ei[n]) for n in range(3))
        return a[0:4] + (a[4:8] + b[0:4]) + (a[8:12] + b[4:8] + c[0:4])

    def apply(n, v):
        c = {d: by_lane[at : at + 1] for d, at in enumerate((20 + 2 * n, 21 + 2 * n, 0, 30 + 3 * n, 31 + 3 * n, 32 + 3 * n))}
        total = c[0] * v
        for d, step in ((1, 1), (3, 15), (4, 16), (5, 17)):
            total = total + c[d] * roll(v, 256 - step) + roll(c[d] * v, step)
        return total

    def inner_product(a, b):
        return jnp.sum(a * b, axis=1, keepdims=True)

    wb, wu, wuu, zb, tuu = (by_lane[4 * n : 4 * n + 4] for n in range(5))
    c0 = solve(zb)
    f_c, g_c, h_c, k_c = apply(0, c0), apply(1, c0), apply(2, c0), apply(4, c0)
    grad0 = wb - f_c
    k0 = solve(grad0)
    f_k, g_k = apply(0, k0), apply(1, k0)
    rho0 = bb - 2.0 * inner_product(c0, wb) + inner_product(c0, f_c)
    energy0 = bu - 2.0 * inner_product(c0, wu) + inner_product(c0, g_c)
    curve0 = energy0 - inner_product(k0, grad0)
    a0 = rho0 / curve0
    e1 = c0 - a0 * k0
    f_e = f_c - a0 * f_k
    g_e = g_c - a0 * g_k
    grad1 = wb - f_e + a0 * (g_c - wu)
    k1 = solve(grad1)

    def second_norm(m0, m1, m2, v0, v1, v2, e_image, c_image, last):
        own = m0 - 2.0 * inner_product(e1, v0) + inner_product(e1, e_image)
        mixed = m1 - inner_product(c0, v1) - inner_product(e1, v1) + inner_product(e1, c_image)
        far = m2 - 2.0 * inner_product(c0, v2) + inner_product(c0, last)
        return own - 2.0 * a0 * mixed + a0 * a0 * far

    rho1 = second_norm(bb, bu, uu, wb, wu, wuu, f_e, g_c, h_c)
    energy1 = second_norm(bu, uu, uuu, wu, wuu, tuu, g_e, h_c, k_c)
    beta = rho1 / rho0
    cross = (
        bu
        - inner_product(c0, wu)
        - inner_product(e1, wu)
        + inner_product(e1, g_c)
        - a0 * (uu - 2.0 * inner_product(c0, wuu) + inner_product(c0, h_c))
        - inner_product(k0, grad1)
    )
    curve1 = energy1 - inner_product(k1, grad1) + 2.0 * beta * cross + beta * beta * curve0
    a1 = rho1 / curve1

    mine = lax.broadcasted_iota(jnp.int32, (32, 256), 0) // 4 == pc

    def zone(value):
        value = jnp.broadcast_to(value, (4, 256))
        return jnp.where(mine, jnp.concatenate([value] * 8, axis=0), 0.0)

    ab = a1 * beta
    stacks = (
        (
            zone(a1 * k1 + ab * k0 - e1),
            zone(-(a0 + ab) * c0 - a1 * e1),
            zone((a0 + ab) * c0 + a1 * e1),
            zone((a1 * a0) * c0),
        ),
        (
            zone(-(a1 * a0) * c0),
            zone(c0 - (a0 + ab) * k0 - a1 * k1),
            zone(-a0 - a1 - ab),
            zone(a1 * a0),
        ),
    )
    out_ref[...] = jnp.zeros((256, 128), F32)
    for n, (ref, stack) in enumerate(((first, stacks[0]), (second, stacks[1]))):
        stack = jnp.concatenate(stack, axis=0)
        ref[0:8] = jnp.zeros((8, 128), F32)
        ref[8:136] = stack[:, 0:128].T
        ref[136:264] = stack[:, 128:256].T
        ref[264:272] = jnp.zeros((8, 128), F32)
        for dr in range(3):
            p = jnp.clip(pr - 1 + dr, 0, 15)
            near[...] = ref[pl.ds(pl.multiple_of(16 * p, 16), 32), :]
            for dq in range(4):
                out_ref[pl.ds(16 * n + 4 * dr + dq, 8, stride=32), :] = near[pl.ds(7 + dq, 8, stride=2), :]


def outputs_kernel(
    rows_ref, first_ref, second_ref, w_ref, grid_ref, coef_ref, m_ref, sol_ref, res_ref,
    left_ref, step_ref, window_ref,
):
    block = pl.program_id(0)

    @pl.when(block == 0)
    def _():
        pr, pc = lax.axis_index(ROW), lax.axis_index(COL)
        slot = lax.broadcasted_iota(jnp.int32, (16, 128), 0)
        region_row = pr - 1 + slot // 4
        region_col = 2 * pc - 1 + slot % 4
        inside = (slot < 12) & (region_row >= 0) & (region_row < REG) & (region_col >= 0) & (region_col < REG)
        window_ref[...] = jnp.where(inside, region_row * REG + region_col, -1).astype(F32)
        total = m_ref[0:32]
        for n in range(1, 8):
            total = total + m_ref[32 * n : 32 * n + 32]
        top, bottom = total[0:16], total[16:32]
        lane = lanes((16, 128))
        steps = jnp.where(slot == 0, roll(bottom[5:6], 64), jnp.where(slot == 1, roll(bottom[5:6], 32), 0.0))
        m = jnp.concatenate(
            [
                jnp.where((lane >= 64) & (lane < 96), roll(bottom, 32), 0.0),
                jnp.where(lane < 64, top, 0.0),
                jnp.where(lane < 64, roll(top, 64), 0.0),
                jnp.where(lane < 32, bottom, 0.0),
                steps,
                jnp.zeros((48, 128), F32),
            ],
            axis=0,
        ).T
        c1, c2, c3 = parts_of(m[0:96, 0:64], 3)
        left_ref[...] = jnp.concatenate([c1, c1, c2, c2, c1, c3], axis=1)
        for n in range(2):
            step_ref[n] = jnp.broadcast_to(m[0:32, 64 + n : 65 + n], (32, 128))

    left, window = left_ref[...], window_ref[...]
    for part in range(4):
        rows = []
        for n in range(8):
            r = 32 * block + 8 * part + n
            z = jnp.where(grid_ref[pl.ds(r, 1), :] == window, grid_ref[pl.ds(128 + r, 1), :], 0.0)
            rows.append(jnp.concatenate([z, w_ref[r], first_ref[r, 32:48], second_ref[r, 32:48]], axis=0))
        r1, r2, r3 = parts_of(jnp.concatenate(rows, axis=1), 3)
        d = fast_dot(left, jnp.concatenate([r1, r2, r1, r2, r3, r1], axis=0))
        for n in range(8):
            r = 32 * block + 8 * part + n
            b, u, uu = rows_ref[r], first_ref[r, 0:32], second_ref[r, 0:32]
            e = d[:, 128 * n : 128 * n + 128]
            inv = coef_ref[5, pl.ds(r + 16, 1), :]
            p1, p2 = step_ref[0], step_ref[1]
            res_ref[:, 8 * part + n] = b + p1 * u + p2 * uu + e[0:32]
            sol_ref[:, 8 * part + n] = inv * (e[32:64] - p1 * b - p2 * u) + e[64:96]


def swapped(value, axis, start):
    pairs = [(i, i + 1) for i in range(start, lax.axis_size(axis) - 1, 2)]
    return lax.ppermute(value, axis, pairs + [(b, a) for a, b in pairs])


def shape_of(*dims):
    return jax.ShapeDtypeStruct(dims, F32)


def kept(*dims):
    return pltpu.VMEM(dims, F32)


def vmem(*dims):
    return pltpu.VMEM(dims, F32)


def body(load_currents, labels, bump_height, horizontal_class, vertical_class, pad_class, edge_table, pad_table):
    rows, cols = lax.axis_size(ROW), lax.axis_size(COL)
    loads = load_currents.reshape(-1, 128)
    grid, far_rows, near_rows = pl.pallas_call(
        prepare_kernel,
        out_shape=(kept(1024, 128), shape_of(HALO, SUB, 128), shape_of(HALO, SUB, 128)),
        compiler_params=limited,
        in_specs=[outside] * 8,
        out_specs=(whole,) * 3,
        scratch_shapes=[pltpu.SMEM((8,), F32), pltpu.SMEM((8,), F32), vmem(32, 8, 128), vmem(32, 8, 128)]
        + [pltpu.VMEM((128, 128), jnp.int32)] * 4
        + [pltpu.SemaphoreType.DMA((9,))],
    )(
        *(
            pltpu.with_memory_space_constraint(x, pltpu.HBM)
            for x in (
                edge_table, pad_table, load_currents, labels, bump_height,
                horizontal_class, vertical_class, pad_class,
            )
        ),
    )
    far_rows = swapped(far_rows, ROW, 1)
    near_rows = swapped(near_rows, ROW, 0)
    by_rows, own = pl.pallas_call(
        pack_kernel,
        out_shape=(kept(128, 32, 128), kept(GROUPS, SUB, 128)),
        compiler_params=limited,
        in_specs=[whole] * 2,
        out_specs=(whole,) * 2,
    )(loads, grid)
    own, top, bottom, far_columns, near_columns = pl.pallas_call(
        corner_kernel,
        out_shape=(kept(GROUPS, SUB, 128), kept(HALO, SUB, 128), kept(HALO, SUB, 128))
        + (shape_of(5, SUB, 128),) * 2,
        compiler_params=limited,
        in_specs=[whole] * 3,
        out_specs=(whole,) * 5,
    )(own, far_rows, near_rows)
    far_columns = swapped(far_columns, COL, 1)
    near_columns = swapped(near_columns, COL, 0)
    first, second, w, coef, payload = pl.pallas_call(
        fields_kernel,
        out_shape=(
            kept(128, 48, 128),
            kept(128, 48, 128),
            kept(128, 16, 128),
            kept(6, 160, 128),
            shape_of(512, 128),
        ),
        compiler_params=limited,
        in_specs=[whole] * 7,
        out_specs=(whole,) * 5,
        scratch_shapes=[
            vmem(5, 160, 128),
            vmem(GROUPS + 2, SUB, 128),
            vmem(GROUPS + 2, SUB, 128),
            vmem(GROUPS + 2, 16, 128),
            vmem(GROUPS + 2, 16, 128),
            vmem(GROUPS + 2, 48, 128),
            vmem(GROUPS + 2, 48, 128),
            vmem(2 * GROUPS, 16, 128),
            vmem(2 * GROUPS, 48, 128),
            vmem(2 * GROUPS, 48, 128),
            vmem(144, 48, 128),
            vmem(144, 48, 128),
            vmem(2, GROUPS, 8, 128),
            vmem(144, 48, 128),
            vmem(144, 48, 128),
            vmem(96, 256),
        ],
    )(by_rows, grid, top, bottom, own, far_columns, near_columns)
    sent = payload.reshape(-1, 4, 128)
    everything = lax.all_to_all(sent, ROW + COL, 0, 0, tiled=True).reshape(-1, 128)
    found = pl.pallas_call(
        coarse_kernel,
        out_shape=shape_of(256, 128),
        compiler_params=limited,
        in_specs=[whole],
        out_specs=whole,
        scratch_shapes=[
            vmem(256, 128),
            vmem(256, 256),
            pltpu.VMEM((3, 256, 256), jnp.bfloat16),
            vmem(272, 128),
            vmem(272, 128),
            vmem(32, 128),
        ],
    )(everything)
    matrix = lax.all_to_all(found.reshape(cols, 32, 128), COL, 0, 0, tiled=True).reshape(-1, 128)
    by_block = pl.BlockSpec((32, 32, 128), lambda k: (0, k, 0))
    return pl.pallas_call(
        outputs_kernel,
        grid=(4,),
        out_shape=(shape_of(32, 128, 128), shape_of(32, 128, 128)),
        compiler_params=limited,
        in_specs=[whole] * 7,
        out_specs=(by_block, by_block),
        scratch_shapes=[pltpu.VMEM((96, 384), jnp.bfloat16), vmem(2, 32, 128), vmem(16, 128)],
    )(by_rows, first, second, w, grid, coef, matrix)


def solution(mesh):
    finer = Mesh(mesh.devices.reshape(4, 4, 4, 2), ("row_0", "row_1", "col_0", "col_1"))
    grid = P(ROW, COL)
    return jax.shard_map(
        body,
        mesh=finer,
        in_specs=(P(None, ROW, COL), grid, grid, grid, grid, grid, P(), P()),
        out_specs=(P(None, ROW, COL), P(None, ROW, COL)),
        check_vma=False,
    )
```

```python
import jax
import jax.numpy as jnp
from jax import lax
from jax.experimental import pallas as pl
from jax.experimental.pallas import tpu as pltpu
from jax.sharding import Mesh
from jax.sharding import PartitionSpec as P

REG = 16
ROW = ("row_0", "row_1")
COL = ("col_0", "col_1")
F32 = jnp.float32

LAB, BUMP, RIGHT, DOWN, PAD = 32, 33, 34, 35, 36
SUB = 40
HALO = 3
GROUPS = 9
ORDER = (1, 3, 5, 7, 9, 11, 13, 15, 2, 6, 10, 14, 4, 12, 8, 0)
POS = tuple(ORDER.index(p) for p in range(16))
NT = (((1,), (1,)), ((), ()))
NN = (((1,), (0,)), ((), ()))
TN = (((0,), (0,)), ((), ()))
whole = pl.BlockSpec(memory_space=pltpu.VMEM)
outside = pl.BlockSpec(memory_space=pltpu.HBM)
limited = pltpu.CompilerParams(vmem_limit_bytes=32 * 2**20)


def parts_of(x, count):
    parts = []
    for n in range(count):
        parts.append(x.astype(jnp.bfloat16))
        if n + 1 < count:
            x = x - parts[-1].astype(F32)
    return parts


def fast_dot(a, b, dims=NN):
    return lax.dot_general(a, b, dims, preferred_element_type=F32)


def dot(a, b, dims=NN):
    (at_a,), (at_b,) = dims[0]
    a1, a2, a3 = parts_of(a, 3)
    b1, b2, b3 = parts_of(b, 3)
    return fast_dot(
        jnp.concatenate([a3, a1, a2, a2, a1, a1], axis=at_a),
        jnp.concatenate([b1, b3, b2, b1, b2, b1], axis=at_b),
        dims,
    )


def lanes(shape):
    return lax.broadcasted_iota(jnp.int32, shape, len(shape) - 1)


def roll(x, shift, axis=1):
    return pltpu.roll(x, shift, axis)


def prepare_kernel(
    edge_hbm, pad_hbm, load_hbm, label_hbm, bump_hbm, across_hbm, down_hbm, pad_class_hbm,
    grid_ref, far_ref, near_ref, edge_ref, pad_ref, load_ref, load_end_ref, label_ref, across_ref, down_ref, pad_class_ref, done,
):
    copies = [
        pltpu.make_async_copy(source, target, done.at[n])
        for n, (source, target) in enumerate(
            (
                (edge_hbm, edge_ref),
                (pad_hbm, pad_ref),
                (across_hbm, across_ref),
                (down_hbm, down_ref),
                (pad_class_hbm, pad_class_ref),
                (label_hbm, label_ref),
                (bump_hbm, grid_ref.at[pl.ds(128, 128)]),
                (load_hbm.at[:, pl.ds(0, 8)], load_ref),
                (load_hbm.at[:, pl.ds(120, 8)], load_end_ref),
            )
        )
    ]
    for copy in copies:
        copy.start()
    for copy in copies:
        copy.wait()
    pr, pc = lax.axis_index(ROW), lax.axis_index(COL)
    shape = (128, 128)
    row, lane = lax.broadcasted_iota(jnp.int32, shape, 0), lanes(shape)

    def lookup(table, classes):
        found = jnp.zeros(shape, F32)
        for n in range(8):
            found = jnp.where(classes == n, table[n], found)
        return found

    right = lookup(edge_ref, across_ref[...])
    down = lookup(edge_ref, down_ref[...])
    grid_ref[0:128] = label_ref[...].astype(F32)
    grid_ref[256:384] = jnp.where((lane == 127) & (pc == 7), 0.0, right)
    grid_ref[384:512] = jnp.where((row == 127) & (pr == 15), 0.0, down)
    grid_ref[512:640] = lookup(pad_ref, pad_class_ref[...])
    grid_ref[640:1024] = jnp.zeros((384, 128), F32)
    for n in range(HALO):
        even = pr % 2 == 0
        first, last = load_ref[:, n], load_end_ref[:, 8 - HALO + n]
        far_ref[n, 0:32] = jnp.where(even, first, last)
        near_ref[n, 0:32] = jnp.where(even, last, first)
        first = grid_ref[pl.ds(n, 8, stride=128), :]
        last = grid_ref[pl.ds(128 - HALO + n, 8, stride=128), :]
        far_ref[n, 32:40] = jnp.where(even, first, last)
        near_ref[n, 32:40] = jnp.where(even, last, first)


def pack_kernel(load_ref, grid_ref, rows_ref, own_ref):
    lane = lanes((32, 128)) // 8

    def group(g, slots):
        loads, rest = jnp.zeros((32, 128), F32), jnp.zeros((8, 128), F32)
        for s in slots:
            r = 16 * g - 8 + s
            b = load_ref[pl.ds(r, 32, stride=128), :]
            rows_ref[r] = b
            loads = jnp.where(lane == s, roll(b, (8 * s + 3) % 128), loads)
            rest = jnp.where(lane[0:8] == s, roll(grid_ref[pl.ds(r, 8, stride=128), :], (8 * s + 3) % 128), rest)
        own_ref[g, 0:32] = loads
        own_ref[g, 32:40] = rest

    group(0, range(8, 16))
    group(8, range(8))

    def step(g, _):
        group(g, range(16))
        return 0

    lax.fori_loop(1, 8, step, 0)


def corner_kernel(
    own_ref, far_ref, near_ref, out_ref, top_ref, bottom_ref, far_out_ref, near_out_ref
):
    lane = lanes((SUB, 128)) // 8
    even = lax.axis_index(ROW) % 2 == 0
    top_ref[...] = jnp.where(even, far_ref[...], near_ref[...])
    bottom_ref[...] = jnp.where(even, near_ref[...], far_ref[...])
    for g in range(GROUPS):
        out_ref[g] = own_ref[g]
    start, end = own_ref[0], own_ref[8]
    for n in range(HALO):
        s = 8 - HALO + n
        start = jnp.where(lane == s, roll(top_ref[n], (8 * s + 3) % 128), start)
        s = 8 + n
        end = jnp.where(lane == s, roll(bottom_ref[n], (8 * s + 3) % 128), end)
    out_ref[0] = start
    out_ref[8] = end
    low = lanes((SUB, 128)) % 8 < 4
    to_right_first = lax.axis_index(COL) % 2 == 1
    for h in range(5):
        here = out_ref[2 * h]
        after = out_ref[2 * h + 1] if h < 4 else here
        right = jnp.where(low, here, roll(after, 4))
        left = jnp.where(low, roll(here, 125), roll(after, 1))
        far_out_ref[h] = jnp.where(to_right_first, right, left)
        near_out_ref[h] = jnp.where(to_right_first, left, right)


def fields_kernel(
    rows_ref, grid_ref, top_ref, bottom_ref, own_ref, far_ref, near_ref,
    first_ref, second_ref, w_ref, coef_ref, out_ref,
    ext, so, ss, sz_o, sz_s, y0_o, y0_s, qz, q0, q1, u0, u1, sc, y0, y1, gram,
):
    pr, pc = lax.axis_index(ROW), lax.axis_index(COL)
    lane1 = lanes((1, 128))
    lane16 = lanes((16, 128))
    lane48 = lanes((48, 128))

    for n in range(5):
        ext[n, 0:16] = jnp.zeros((16, 128), F32)
        ext[n, 16:144] = grid_ref[128 * n : 128 * n + 128]
        ext[n, 144:160] = jnp.zeros((16, 128), F32)
        for k in range(HALO):
            ext[n, 16 - HALO + k : 17 - HALO + k] = top_ref[k, 32 + n : 33 + n]
            ext[n, 144 + k : 145 + k] = bottom_ref[k, 32 + n : 33 + n]

    slot = lax.broadcasted_iota(jnp.int32, (16, 128), 0)
    region_row = pr - 1 + slot // 4
    region_col = 2 * pc - 1 + slot % 4
    inside = (slot < 12) & (region_row >= 0) & (region_row < REG) & (region_col >= 0) & (region_col < REG)
    window = jnp.where(inside, region_row * REG + region_col, -1).astype(F32)

    for ref in (so, ss, sz_o, sz_s, y0_o, y0_s):
        ref[0] = jnp.zeros(ref.shape[1:], F32)
        ref[GROUPS + 1] = jnp.zeros(ref.shape[1:], F32)

    def pair_left(o, s, lane):
        j = lane % 8
        return roll(jnp.where(j == 2, s, o), 1), roll(jnp.where(j == 2, o, s), 1)

    def pair_right(o, s, lane):
        j = lane % 8
        return roll(jnp.where(j == 3, s, o), 127), roll(jnp.where(j == 3, o, s), 127)

    def above(before, here, lane):
        return roll(jnp.where(lane >= 120, before, here), 8)

    def below(here, after, lane):
        return roll(jnp.where(lane < 8, after, here), 120)

    even = pc % 2 == 0

    def strips(g, _):
        o_row = own_ref[g]
        far, near = far_ref[g // 2], near_ref[g // 2]
        on_left, on_right = jnp.where(even, far, near), jnp.where(even, near, far)
        turn = 124 * (g % 2)
        s_row = jnp.where(lanes((SUB, 128)) % 8 < 3, roll(on_left, turn), roll(on_right, 3 + turn))
        so[g + 1], ss[g + 1] = o_row, s_row
        lefts = pair_left(o_row[RIGHT : RIGHT + 1], s_row[RIGHT : RIGHT + 1], lane1)
        for side, (row, ref, ll) in enumerate(((o_row, so, lefts[0]), (s_row, ss, lefts[1]))):
            rl, dl = row[RIGHT : RIGHT + 1], row[DOWN : DOWN + 1]
            ul = above(ref[g, DOWN : DOWN + 1], dl, lane1)
            diag = row[PAD : PAD + 1] + rl + ll + dl + ul
            inv = jnp.where(diag > 0, 1.0 / diag, 0.0)
            for n, value in enumerate((diag, rl, ll, dl, ul, inv)):
                sc[side, g, n : n + 1] = value
            z = jnp.where(row[LAB : LAB + 1] == window, row[BUMP : BUMP + 1], 0.0)
            (sz_s if side else sz_o)[g + 1] = z
            if side:
                qz[2 * g] = z
                qz[2 * g + 1] = roll(z, 64)

        at = pl.multiple_of(16 * g + 8, 8)
        beside = jnp.zeros((16, 128), F32)
        for s in range(16):
            beside = jnp.where(slot == s, roll(s_row[RIGHT : RIGHT + 1], 125 - 8 * s), beside)
        rl, dl = ext[2, pl.ds(at, 16)], ext[3, pl.ds(at, 16)]
        ll = roll(jnp.where(lane16 == 127, beside, rl), 1)
        last = ext[3, pl.ds(pl.multiple_of(at - 8, 8), 8)]
        ul = jnp.where(slot == 0, last[7:8], roll(dl, 1, 0))
        diag = ext[4, pl.ds(at, 16)] + rl + ll + dl + ul
        inv = jnp.where(diag > 0, 1.0 / diag, 0.0)
        for n, value in enumerate((diag, rl, ll, dl, ul, inv)):
            coef_ref[n, pl.ds(at, 16)] = value
        return 0

    lax.fori_loop(0, GROUPS, strips, 0, unroll=3)

    def strip_image(ref_o, ref_s, g, lane, sides):
        o, s = ref_o[g + 1], ref_s[g + 1]
        lefts, rights = pair_left(o, s, lane), pair_right(o, s, lane)
        done = []
        for side in sides:
            ref, here = (ref_s, s) if side else (ref_o, o)
            up = above(ref[g], here, lane)
            down = below(here, ref[g + 2], lane)
            c = [sc[side, g, n : n + 1] for n in range(5)]
            done.append(c[0] * here - c[1] * rights[side] - c[2] * lefts[side] - c[3] * down - c[4] * up)
        return done

    def strip_first(g, _):
        w = strip_image(sz_o, sz_s, g, lane16, (0, 1))
        for side, (source, ref) in enumerate(((so, y0_o), (ss, y0_s))):
            inv = sc[side, g, 5:6]
            ref[g + 1, 0:32] = inv * source[g + 1, 0:32]
            ref[g + 1, 32:48] = inv * w[side]
        y = y0_s[g + 1]
        q0[2 * g] = y
        q0[2 * g + 1] = roll(y, 64)
        return 0

    lax.fori_loop(0, GROUPS, strip_first, 0, unroll=3)

    def strip_second(g, _):
        (u,) = strip_image(y0_o, y0_s, g, lane48, (1,))
        y = sc[1, g, 5:6] * u
        q1[2 * g] = y
        q1[2 * g + 1] = roll(y, 64)
        return 0

    lax.fori_loop(0, GROUPS, strip_second, 0, unroll=3)

    def owned(g):
        return not isinstance(g, int)

    def coef(n, g, s):
        return coef_ref[n, pl.ds(8 * g + 8 + s, 1), :]

    def unpacked(strip, g, s):
        return roll(strip[g], 125 - 8 * s)

    def image(here, up, down, other, g, s, lane):
        left = roll(jnp.where(lane == 127, other, here), 1)
        right = roll(jnp.where(lane == 0, other, here), 127)
        return (
            coef(0, g, s) * here
            - coef(1, g, s) * right
            - coef(2, g, s) * left
            - coef(3, g, s) * down
            - coef(4, g, s) * up
        )

    def basis(j):
        return jnp.where(ext[0, pl.ds(j, 1), :] == window, ext[1, pl.ds(j, 1), :], 0.0)

    def first_image(g, s):
        r, j = 8 * g - 8 + s, 8 * g + 8 + s
        w = image(basis(j), basis(j - 1), basis(j + 1), unpacked(qz, g, s), g, s, lane16)
        if owned(g):
            b = rows_ref[r]
            w_ref[r] = w
        else:
            b = top_ref[r + HALO, 0:32] if r < 0 else bottom_ref[r - 128, 0:32]
        inv = coef(5, g, s)
        y0[8 * g + s, 0:32] = inv * b
        y0[8 * g + s, 32:48] = inv * w
        u0[8 * g + s] = unpacked(q0, g, s)
        u1[8 * g + s] = unpacked(q1, g, s)

    def second_image(g, s):
        i = 8 * g + s
        f1 = image(y0[i], y0[i - 1], y0[i + 1], u0[i], g, s, lane48)
        if owned(g):
            first_ref[8 * g - 8 + s] = f1
        y1[i] = coef(5, g, s) * f1

    def only(work):
        def step(g, _):
            for s in range(8):
                work(g, s)
            return 0

        return step

    for s in (6, 7):
        first_image(0, s)
    lax.fori_loop(1, 17, only(first_image), 0)
    for s in (0, 1):
        first_image(17, s)
    second_image(0, 7)

    def second_pair(t, _):
        for s in range(16):
            second_image(2 * t + 1 + s // 8, s % 8)
        return 0

    lax.fori_loop(0, 8, second_pair, 0)
    second_image(17, 0)

    gram[...] = jnp.zeros((96, 256), F32)

    def third_image(g, s):
        i = 8 * g + s
        second_ref[i - 8] = image(y1[i], y1[i - 1], y1[i + 1], u1[i], g, s, lane48)

    def products(g, sums):
        left, every = [], []
        sums = list(sums)
        for s in range(16):
            i = 16 * g + 8 + s
            r = i - 8
            b, f1, f2, y0r, y1r = rows_ref[r], first_ref[r], second_ref[r], y0[i], y1[i]
            left.append(jnp.concatenate([basis(i + 8), y0r[32:48], y1r[32:48]], axis=0))
            every.append(jnp.concatenate([b, w_ref[r], f1, f2], axis=0))
            pairs = ((y0r, b), (y0r, f1), (y1r, f1), (y1r, f2))
            sums = [t + p[0:32] * q[0:32] for t, (p, q) in zip(sums, pairs)]
        left = jnp.concatenate(parts_of(jnp.concatenate(left, axis=1), 2), axis=0)
        high, low = parts_of(jnp.concatenate(every, axis=1), 2)
        gram[:, 0:144] += fast_dot(left, high, NT) + fast_dot(left, low, NT)
        return tuple(sums)

    def third_pair(t, _):
        for s in range(16):
            third_image(2 * t + 1 + s // 8, s % 8)
        return 0

    def last_stage(t, sums):
        sums = products(t - 1, sums)
        third_pair(t, 0)
        return sums

    zero = jnp.zeros((32, 128), F32)
    lax.fori_loop(0, 1, third_pair, 0)
    sums = lax.fori_loop(1, 8, last_stage, (zero, zero, zero, zero))
    sums = lax.fori_loop(7, 8, products, sums)

    a0, a1 = gram[0:48, 0:128] + gram[48:96, 0:128], gram[0:48, 128:256] + gram[48:96, 128:256]
    zr, w0, t0, w1, t1 = a0[0:16], a0[16:32], a0[32:48], a1[16:32], a1[32:48]
    matrices = jnp.zeros((16, 128), F32)
    for n, (x, z) in enumerate(((w0, 32), (w0, 80), (w1, 0), (zr, 32), (t1, 0))):
        start = 24 * n
        matrices = jnp.where((lane16 >= start) & (lane16 < start + 16), roll(x, (start - z) % 128), matrices)
    moved = jnp.zeros((16, 128), F32)
    for k in range(12):
        moved = jnp.where(slot == k, roll(matrices, (128 - k) % 128), moved)
    common = jnp.zeros((16, 128), F32)
    for n in range(5):
        for start, offset, count in ((20 + 2 * n, 0, 2), (30 + 3 * n, 3, 3)):
            hit = (lane16 >= start) & (lane16 < start + count)
            common = jnp.where(hit, roll(moved, (start - offset - 24 * n) % 128), common)
    lines = []
    diagonal = lanes((32, 128)) == lax.broadcasted_iota(jnp.int32, (32, 128), 0)
    for total in sums:
        column = jnp.sum(total, axis=1, keepdims=True)
        lines.append(jnp.sum(jnp.where(diagonal, column, 0.0), axis=0, keepdims=True))
    row4, lane4 = lax.broadcasted_iota(jnp.int32, (4, 128), 0), lanes((4, 128))
    for d in range(8):
        message = common
        for n, (x, z) in enumerate(((w0, 0), (w0, 48), (w0, 96), (zr, 0), (t0, 96))):
            hit = (lane16 >= 4 * n) & (lane16 < 4 * n + 4)
            message = jnp.where(hit, roll(x, (4 * n - z - 4 * d) % 128), message)
        middle, last = roll(message, 45), roll(message, 90)
        sent = jnp.where(lane4 < 45, message[0:4], jnp.where(lane4 < 90, middle[4:8], last[8:12]))
        line = jnp.zeros((1, 128), F32)
        for n in range(4):
            start = 120 + 4 * n if n < 2 else 112 + 4 * n
            line = jnp.where((lane1 >= start) & (lane1 < start + 4), roll(lines[n], (start - 4 * d) % 128), line)
            if n == 1:
                first_two, line = line, jnp.zeros((1, 128), F32)
        total = jnp.where(row4 == 0, first_two, jnp.where(row4 == 1, line, 0.0))
        sent = jnp.where(lane4 < 120, sent, total)
        if d % 2 == 0:
            before = sent
            continue
        pair = jnp.concatenate([before, sent], axis=0)
        for r in range(16):
            out_ref[32 * r + 4 * d - 4 : 32 * r + 4 * d + 4] = pair


def batched_inverse(a, lane, row, size):
    base = lane - lane % size
    for k in range(0, size, 2):
        at_k, at_n = lane % size == k, lane % size == k + 1
        left = jnp.take_along_axis(a, base + k, axis=1)
        right = jnp.take_along_axis(a, base + k + 1, axis=1)
        p, q, r, t = left[k : k + 1], right[k : k + 1], left[k + 1 : k + 2], right[k + 1 : k + 2]
        inverse = 1.0 / (p * t - q * r)
        upper = jnp.where(at_k[0:1], 1.0, jnp.where(at_n[0:1], 0.0, a[k : k + 1]))
        lower = jnp.where(at_n[0:1], 1.0, jnp.where(at_k[0:1], 0.0, a[k + 1 : k + 2]))
        first = (t * upper - q * lower) * inverse
        second = (p * lower - r * upper) * inverse
        rest = jnp.where(at_k | at_n, 0.0, a) - left * first - right * second
        a = jnp.where(row == k, first, jnp.where(row == k + 1, second, rest))
    return a


def block_inverse(matrix, low, high, size=16):
    lane = lanes((size, 128))
    row = lax.broadcasted_iota(jnp.int32, (size, 128), 0)
    compact = jnp.where(lane % size == row, 1.0, 0.0)
    for n in range(low // size, high // size):
        compact = jnp.where(lane // size == n, matrix[size * n : size * n + size], compact)
    compact = batched_inverse(compact, lane, row, size)
    parts = []
    for n in range(128 // size):
        active = low <= size * n < high
        parts.append(jnp.where(lane // size == n, compact, 0.0) if active else jnp.zeros((size, 128), F32))
    return jnp.concatenate(parts, axis=0)


def coarse_kernel(in_ref, out_ref, g, e, ei, first, second, near):
    pr, pc = lax.axis_index(ROW), lax.axis_index(COL)
    sub8 = lax.broadcasted_iota(jnp.int32, (8, 128), 0)

    lane8 = lanes((8, 128))
    for p in range(16):
        even, odd = jnp.zeros((8, 128), F32), jnp.zeros((8, 128), F32)
        for dr in range(3):
            r = p + 1 - dr
            if not 0 <= r < 16:
                continue
            at = [in_ref[pl.ds(32 * r + dq, 8, stride=4), :] for dq in range(4)]
            pair = (
                at[1] + jnp.where(sub8 >= 1, roll(at[3], 1, 0), 0.0),
                at[2] + jnp.where(sub8 < 7, roll(at[0], 7, 0), 0.0),
            )
            hit = lane8 < (30 if dr == 2 else 45)
            even, odd = (
                old + jnp.where(hit, roll(new, (128 - 45 * dr) % 128) if dr else new, 0.0)
                for old, new in zip((even, odd), pair)
            )
        g[pl.ds(16 * p, 8, stride=2), :] = even
        g[pl.ds(16 * p + 1, 8, stride=2), :] = odd
    tally = [
        roll(jnp.sum(in_ref[pl.ds(n, 128, stride=4), :], axis=0, keepdims=True), 8 + 8 * n) for n in range(2)
    ]
    tally = jnp.where(lanes((1, 128)) < 8, tally[0], tally[1])
    tally = jnp.broadcast_to(tally, (128, 128)).T
    bb, bu, uu, uuu = (tally[4 * n : 4 * n + 4, 0:1] for n in range(4))
    by_lane = jnp.concatenate([g[0:128].T, g[128:256].T], axis=1)

    lane16, row16 = lanes((16, 128)), lax.broadcasted_iota(jnp.int32, (16, 128), 0)
    for p in range(16):
        own = g[16 * p : 16 * p + 16]
        terms = [(own, d, dp, dq) for d, dp, dq in ((0, 0, 0), (1, 0, 1))]
        terms.append((roll(own, 1, 0), 1, 0, -1))
        if p < 15:
            terms += [(own, d, 1, dq) for d, dq in ((3, -1), (4, 0), (5, 1))]
        if p > 0:
            last = g[16 * p - 16 : 16 * p]
            terms += [(roll(last, 15, 0), 3, -1, 1), (last, 4, -1, 0), (roll(last, 1, 0), 5, -1, -1)]
        halves = [jnp.zeros((16, 128), F32), jnp.zeros((16, 128), F32)]
        for x, d, dp, dq in terms:
            target = POS[p + dp] * 16
            h, off = target // 128, target % 128
            q = row16 + dq
            hit = (lane16 == off + q) & (q >= 0) & (q < 16)
            at = 26 + d if d < 2 else 36 + d
            value = jnp.broadcast_to(x[:, at : at + 1], (16, 128))
            halves[h] = jnp.where(hit, value, halves[h])
        at = POS[p] * 16
        e[at : at + 16, 0:128] = halves[0]
        e[at : at + 16, 128:256] = halves[1]

    lane = lanes((128, 128))
    row = lax.broadcasted_iota(jnp.int32, (128, 128), 0)
    outer = block_inverse(e[0:128, 0:128], 0, 128)
    across = dot(outer, e[0:128, 128:256])
    schur = e[128:256, 128:256] - dot(e[128:256, 0:128], across)
    steps = []
    for low, high in ((0, 64), (64, 96)):
        inv = block_inverse(schur, low, high)
        link = jnp.where((row >= low) & (row < high) & (lane >= high), schur, 0.0)
        x = dot(inv, link)
        keep = jnp.where((row >= high) & (lane >= high), schur, 0.0)
        schur = keep - dot(link, x, TN)
        steps.append((inv, jnp.where((row == lane) & (row >= high), 1.0, 0.0) - x))
    inner = block_inverse(schur, 96, 128, 32)
    for inv, y in reversed(steps):
        inner = inv + dot(dot(y, inner), y, NT)
    half = dot(across, inner)
    near_diag = outer + dot(half, across, NT)

    def ordered(top_half, bottom_half):
        blocks = [top_half[16 * n : 16 * n + 16] for n in range(8)]
        blocks += [bottom_half[16 * n : 16 * n + 16] for n in range(8)]
        blocks = [blocks[POS[p]] for p in range(16)]
        return jnp.concatenate(blocks[:8], axis=0), jnp.concatenate(blocks[8:], axis=0)

    left_top, left_bottom = ordered(near_diag, -half.T)
    right_top, right_bottom = ordered(-half, inner)
    top_left, bottom_left = ordered(left_top.T, right_top.T)
    top_right, bottom_right = ordered(left_bottom.T, right_bottom.T)
    inverse = jnp.concatenate(
        [jnp.concatenate([top_left, bottom_left], axis=0), jnp.concatenate([top_right, bottom_right], axis=0)],
        axis=1,
    )
    for n, part in enumerate(parts_of(inverse, 3)):
        ei[n] = part

    def solve(z):
        rows = [part.astype(F32) for part in parts_of(z, 3)]
        rows = jnp.concatenate(rows + [jnp.zeros_like(z)], axis=0).astype(jnp.bfloat16)
        a, b, c = (fast_dot(rows, ei[n]) for n in range(3))
        return a[0:4] + (a[4:8] + b[0:4]) + (a[8:12] + b[4:8] + c[0:4])

    def apply(n, v):
        c = {d: by_lane[at : at + 1] for d, at in enumerate((20 + 2 * n, 21 + 2 * n, 0, 30 + 3 * n, 31 + 3 * n, 32 + 3 * n))}
        total = c[0] * v
        for d, step in ((1, 1), (3, 15), (4, 16), (5, 17)):
            total = total + c[d] * roll(v, 256 - step) + roll(c[d] * v, step)
        return total

    def inner_product(a, b):
        return jnp.sum(a * b, axis=1, keepdims=True)

    wb, wu, wuu, zb, tuu = (by_lane[4 * n : 4 * n + 4] for n in range(5))
    c0 = solve(zb)
    f_c, g_c, h_c, k_c = apply(0, c0), apply(1, c0), apply(2, c0), apply(4, c0)
    grad0 = wb - f_c
    k0 = solve(grad0)
    f_k, g_k = apply(0, k0), apply(1, k0)
    rho0 = bb - 2.0 * inner_product(c0, wb) + inner_product(c0, f_c)
    energy0 = bu - 2.0 * inner_product(c0, wu) + inner_product(c0, g_c)
    curve0 = energy0 - inner_product(k0, grad0)
    a0 = rho0 / curve0
    e1 = c0 - a0 * k0
    f_e = f_c - a0 * f_k
    g_e = g_c - a0 * g_k
    grad1 = wb - f_e + a0 * (g_c - wu)
    k1 = solve(grad1)

    def second_norm(m0, m1, m2, v0, v1, v2, e_image, c_image, last):
        own = m0 - 2.0 * inner_product(e1, v0) + inner_product(e1, e_image)
        mixed = m1 - inner_product(c0, v1) - inner_product(e1, v1) + inner_product(e1, c_image)
        far = m2 - 2.0 * inner_product(c0, v2) + inner_product(c0, last)
        return own - 2.0 * a0 * mixed + a0 * a0 * far

    rho1 = second_norm(bb, bu, uu, wb, wu, wuu, f_e, g_c, h_c)
    energy1 = second_norm(bu, uu, uuu, wu, wuu, tuu, g_e, h_c, k_c)
    beta = rho1 / rho0
    cross = (
        bu
        - inner_product(c0, wu)
        - inner_product(e1, wu)
        + inner_product(e1, g_c)
        - a0 * (uu - 2.0 * inner_product(c0, wuu) + inner_product(c0, h_c))
        - inner_product(k0, grad1)
    )
    curve1 = energy1 - inner_product(k1, grad1) + 2.0 * beta * cross + beta * beta * curve0
    a1 = rho1 / curve1

    mine = lax.broadcasted_iota(jnp.int32, (32, 256), 0) // 4 == pc

    def zone(value):
        value = jnp.broadcast_to(value, (4, 256))
        return jnp.where(mine, jnp.concatenate([value] * 8, axis=0), 0.0)

    ab = a1 * beta
    stacks = (
        (
            zone(a1 * k1 + ab * k0 - e1),
            zone(-(a0 + ab) * c0 - a1 * e1),
            zone((a0 + ab) * c0 + a1 * e1),
            zone((a1 * a0) * c0),
        ),
        (
            zone(-(a1 * a0) * c0),
            zone(c0 - (a0 + ab) * k0 - a1 * k1),
            zone(-a0 - a1 - ab),
            zone(a1 * a0),
        ),
    )
    out_ref[...] = jnp.zeros((256, 128), F32)
    for n, (ref, stack) in enumerate(((first, stacks[0]), (second, stacks[1]))):
        stack = jnp.concatenate(stack, axis=0)
        ref[0:8] = jnp.zeros((8, 128), F32)
        ref[8:136] = stack[:, 0:128].T
        ref[136:264] = stack[:, 128:256].T
        ref[264:272] = jnp.zeros((8, 128), F32)
        for dr in range(3):
            p = jnp.clip(pr - 1 + dr, 0, 15)
            near[...] = ref[pl.ds(pl.multiple_of(16 * p, 16), 32), :]
            for dq in range(4):
                out_ref[pl.ds(16 * n + 4 * dr + dq, 8, stride=32), :] = near[pl.ds(7 + dq, 8, stride=2), :]


def outputs_kernel(
    rows_ref, first_ref, second_ref, w_ref, grid_ref, coef_ref, m_ref, sol_ref, res_ref,
    left_ref, step_ref, window_ref,
):
    block = pl.program_id(0)

    @pl.when(block == 0)
    def _():
        pr, pc = lax.axis_index(ROW), lax.axis_index(COL)
        slot = lax.broadcasted_iota(jnp.int32, (16, 128), 0)
        region_row = pr - 1 + slot // 4
        region_col = 2 * pc - 1 + slot % 4
        inside = (slot < 12) & (region_row >= 0) & (region_row < REG) & (region_col >= 0) & (region_col < REG)
        window_ref[...] = jnp.where(inside, region_row * REG + region_col, -1).astype(F32)
        total = m_ref[0:32]
        for n in range(1, 8):
            total = total + m_ref[32 * n : 32 * n + 32]
        top, bottom = total[0:16], total[16:32]
        lane = lanes((16, 128))
        steps = jnp.where(slot == 0, roll(bottom[5:6], 64), jnp.where(slot == 1, roll(bottom[5:6], 32), 0.0))
        m = jnp.concatenate(
            [
                jnp.where((lane >= 64) & (lane < 96), roll(bottom, 32), 0.0),
                jnp.where(lane < 64, top, 0.0),
                jnp.where(lane < 64, roll(top, 64), 0.0),
                jnp.where(lane < 32, bottom, 0.0),
                steps,
                jnp.zeros((48, 128), F32),
            ],
            axis=0,
        ).T
        c1, c2, c3 = parts_of(m[0:96, 0:64], 3)
        left_ref[...] = jnp.concatenate([c1, c1, c2, c2, c1, c3], axis=1)
        for n in range(2):
            step_ref[n] = jnp.broadcast_to(m[0:32, 64 + n : 65 + n], (32, 128))

    left, window = left_ref[...], window_ref[...]
    for part in range(4):
        rows = []
        for n in range(8):
            r = 32 * block + 8 * part + n
            z = jnp.where(grid_ref[pl.ds(r, 1), :] == window, grid_ref[pl.ds(128 + r, 1), :], 0.0)
            rows.append(jnp.concatenate([z, w_ref[r], first_ref[r, 32:48], second_ref[r, 32:48]], axis=0))
        r1, r2, r3 = parts_of(jnp.concatenate(rows, axis=1), 3)
        d = fast_dot(left, jnp.concatenate([r1, r2, r1, r2, r3, r1], axis=0))
        for n in range(8):
            r = 32 * block + 8 * part + n
            b, u, uu = rows_ref[r], first_ref[r, 0:32], second_ref[r, 0:32]
            e = d[:, 128 * n : 128 * n + 128]
            inv = coef_ref[5, pl.ds(r + 16, 1), :]
            p1, p2 = step_ref[0], step_ref[1]
            res_ref[:, 8 * part + n] = b + p1 * u + p2 * uu + e[0:32]
            sol_ref[:, 8 * part + n] = inv * (e[32:64] - p1 * b - p2 * u) + e[64:96]


def swapped(value, axis, start):
    pairs = [(i, i + 1) for i in range(start, lax.axis_size(axis) - 1, 2)]
    return lax.ppermute(value, axis, pairs + [(b, a) for a, b in pairs])


def shape_of(*dims):
    return jax.ShapeDtypeStruct(dims, F32)


def kept(*dims):
    return pltpu.VMEM(dims, F32)


def vmem(*dims):
    return pltpu.VMEM(dims, F32)


def body(load_currents, labels, bump_height, horizontal_class, vertical_class, pad_class, edge_table, pad_table):
    rows, cols = lax.axis_size(ROW), lax.axis_size(COL)
    loads = load_currents.reshape(-1, 128)
    grid, far_rows, near_rows = pl.pallas_call(
        prepare_kernel,
        out_shape=(kept(1024, 128), shape_of(HALO, SUB, 128), shape_of(HALO, SUB, 128)),
        compiler_params=limited,
        in_specs=[outside] * 8,
        out_specs=(whole,) * 3,
        scratch_shapes=[pltpu.SMEM((8,), F32), pltpu.SMEM((8,), F32), vmem(32, 8, 128), vmem(32, 8, 128)]
        + [pltpu.VMEM((128, 128), jnp.int32)] * 4
        + [pltpu.SemaphoreType.DMA((9,))],
    )(
        *(
            pltpu.with_memory_space_constraint(x, pltpu.HBM)
            for x in (
                edge_table, pad_table, load_currents, labels, bump_height,
                horizontal_class, vertical_class, pad_class,
            )
        ),
    )
    far_rows = swapped(far_rows, ROW, 1)
    near_rows = swapped(near_rows, ROW, 0)
    by_rows, own = pl.pallas_call(
        pack_kernel,
        out_shape=(kept(128, 32, 128), kept(GROUPS, SUB, 128)),
        compiler_params=limited,
        in_specs=[whole] * 2,
        out_specs=(whole,) * 2,
    )(loads, grid)
    own, top, bottom, far_columns, near_columns = pl.pallas_call(
        corner_kernel,
        out_shape=(kept(GROUPS, SUB, 128), kept(HALO, SUB, 128), kept(HALO, SUB, 128))
        + (shape_of(5, SUB, 128),) * 2,
        compiler_params=limited,
        in_specs=[whole] * 3,
        out_specs=(whole,) * 5,
    )(own, far_rows, near_rows)
    far_columns = swapped(far_columns, COL, 1)
    near_columns = swapped(near_columns, COL, 0)
    first, second, w, coef, payload = pl.pallas_call(
        fields_kernel,
        out_shape=(
            kept(128, 48, 128),
            kept(128, 48, 128),
            kept(128, 16, 128),
            kept(6, 160, 128),
            shape_of(512, 128),
        ),
        compiler_params=limited,
        in_specs=[whole] * 7,
        out_specs=(whole,) * 5,
        scratch_shapes=[
            vmem(5, 160, 128),
            vmem(GROUPS + 2, SUB, 128),
            vmem(GROUPS + 2, SUB, 128),
            vmem(GROUPS + 2, 16, 128),
            vmem(GROUPS + 2, 16, 128),
            vmem(GROUPS + 2, 48, 128),
            vmem(GROUPS + 2, 48, 128),
            vmem(2 * GROUPS, 16, 128),
            vmem(2 * GROUPS, 48, 128),
            vmem(2 * GROUPS, 48, 128),
            vmem(144, 48, 128),
            vmem(144, 48, 128),
            vmem(2, GROUPS, 8, 128),
            vmem(144, 48, 128),
            vmem(144, 48, 128),
            vmem(96, 256),
        ],
    )(by_rows, grid, top, bottom, own, far_columns, near_columns)
    sent = payload.reshape(-1, 4, 128)
    everything = lax.all_to_all(sent, ROW + COL, 0, 0, tiled=True).reshape(-1, 128)
    found = pl.pallas_call(
        coarse_kernel,
        out_shape=shape_of(256, 128),
        compiler_params=limited,
        in_specs=[whole],
        out_specs=whole,
        scratch_shapes=[
            vmem(256, 128),
            vmem(256, 256),
            pltpu.VMEM((3, 256, 256), jnp.bfloat16),
            vmem(272, 128),
            vmem(272, 128),
            vmem(32, 128),
        ],
    )(everything)
    matrix = lax.all_to_all(found.reshape(cols, 32, 128), COL, 0, 0, tiled=True).reshape(-1, 128)
    by_block = pl.BlockSpec((32, 32, 128), lambda k: (0, k, 0))
    return pl.pallas_call(
        outputs_kernel,
        grid=(4,),
        out_shape=(shape_of(32, 128, 128), shape_of(32, 128, 128)),
        compiler_params=limited,
        in_specs=[whole] * 7,
        out_specs=(by_block, by_block),
        scratch_shapes=[pltpu.VMEM((96, 384), jnp.bfloat16), vmem(2, 32, 128), vmem(16, 128)],
    )(by_rows, first, second, w, grid, coef, matrix)


def solution(mesh):
    finer = Mesh(mesh.devices.reshape(4, 4, 4, 2), ("row_0", "row_1", "col_0", "col_1"))
    grid = P(ROW, COL)
    return jax.shard_map(
        body,
        mesh=finer,
        in_specs=(P(None, ROW, COL), grid, grid, grid, grid, grid, P(), P()),
        out_specs=(P(None, ROW, COL), P(None, ROW, COL)),
        check_vma=False,
    )
```

```python
import jax
import jax.numpy as jnp
from jax import lax
from jax.experimental import pallas as pl
from jax.experimental.pallas import tpu as pltpu
from jax.sharding import Mesh
from jax.sharding import PartitionSpec as P

REG = 16
ROW = ("row_0", "row_1")
COL = ("col_0", "col_1")
F32 = jnp.float32

LAB, BUMP, RIGHT, DOWN, PAD = 32, 33, 34, 35, 36
SUB = 40
HALO = 3
GROUPS = 9
ORDER = (1, 3, 5, 7, 9, 11, 13, 15, 2, 6, 10, 14, 4, 12, 8, 0)
POS = tuple(ORDER.index(p) for p in range(16))
NT = (((1,), (1,)), ((), ()))
NN = (((1,), (0,)), ((), ()))
TN = (((0,), (0,)), ((), ()))
whole = pl.BlockSpec(memory_space=pltpu.VMEM)
outside = pl.BlockSpec(memory_space=pltpu.HBM)
limited = pltpu.CompilerParams(vmem_limit_bytes=32 * 2**20)


def parts_of(x, count):
    parts = []
    for n in range(count):
        parts.append(x.astype(jnp.bfloat16))
        if n + 1 < count:
            x = x - parts[-1].astype(F32)
    return parts


def fast_dot(a, b, dims=NN):
    return lax.dot_general(a, b, dims, preferred_element_type=F32)


def dot(a, b, dims=NN):
    (at_a,), (at_b,) = dims[0]
    a1, a2, a3 = parts_of(a, 3)
    b1, b2, b3 = parts_of(b, 3)
    return fast_dot(
        jnp.concatenate([a3, a1, a2, a2, a1, a1], axis=at_a),
        jnp.concatenate([b1, b3, b2, b1, b2, b1], axis=at_b),
        dims,
    )


def lanes(shape):
    return lax.broadcasted_iota(jnp.int32, shape, len(shape) - 1)


def roll(x, shift, axis=1):
    return pltpu.roll(x, shift, axis)


def prepare_kernel(
    edge_hbm, pad_hbm, load_hbm, label_hbm, bump_hbm, across_hbm, down_hbm, pad_class_hbm,
    grid_ref, far_ref, near_ref, edge_ref, pad_ref, load_ref, load_end_ref, label_ref, across_ref, down_ref, pad_class_ref, done,
):
    copies = [
        pltpu.make_async_copy(source, target, done.at[n])
        for n, (source, target) in enumerate(
            (
                (edge_hbm, edge_ref),
                (pad_hbm, pad_ref),
                (across_hbm, across_ref),
                (down_hbm, down_ref),
                (pad_class_hbm, pad_class_ref),
                (label_hbm, label_ref),
                (bump_hbm, grid_ref.at[pl.ds(128, 128)]),
                (load_hbm.at[:, pl.ds(0, 8)], load_ref),
                (load_hbm.at[:, pl.ds(120, 8)], load_end_ref),
            )
        )
    ]
    for copy in copies:
        copy.start()
    for copy in copies:
        copy.wait()
    pr, pc = lax.axis_index(ROW), lax.axis_index(COL)
    shape = (128, 128)
    row, lane = lax.broadcasted_iota(jnp.int32, shape, 0), lanes(shape)

    def lookup(table, classes):
        found = jnp.zeros(shape, F32)
        for n in range(8):
            found = jnp.where(classes == n, table[n], found)
        return found

    right = lookup(edge_ref, across_ref[...])
    down = lookup(edge_ref, down_ref[...])
    grid_ref[0:128] = label_ref[...].astype(F32)
    grid_ref[256:384] = jnp.where((lane == 127) & (pc == 7), 0.0, right)
    grid_ref[384:512] = jnp.where((row == 127) & (pr == 15), 0.0, down)
    grid_ref[512:640] = lookup(pad_ref, pad_class_ref[...])
    grid_ref[640:1024] = jnp.zeros((384, 128), F32)
    for n in range(HALO):
        even = pr % 2 == 0
        first, last = load_ref[:, n], load_end_ref[:, 8 - HALO + n]
        far_ref[n, 0:32] = jnp.where(even, first, last)
        near_ref[n, 0:32] = jnp.where(even, last, first)
        first = grid_ref[pl.ds(n, 8, stride=128), :]
        last = grid_ref[pl.ds(128 - HALO + n, 8, stride=128), :]
        far_ref[n, 32:40] = jnp.where(even, first, last)
        near_ref[n, 32:40] = jnp.where(even, last, first)


def pack_kernel(load_ref, grid_ref, rows_ref, own_ref):
    lane = lanes((32, 128)) // 8

    def group(g, slots):
        loads, rest = jnp.zeros((32, 128), F32), jnp.zeros((8, 128), F32)
        for s in slots:
            r = 16 * g - 8 + s
            b = load_ref[pl.ds(r, 32, stride=128), :]
            rows_ref[r] = b
            loads = jnp.where(lane == s, roll(b, (8 * s + 3) % 128), loads)
            rest = jnp.where(lane[0:8] == s, roll(grid_ref[pl.ds(r, 8, stride=128), :], (8 * s + 3) % 128), rest)
        own_ref[g, 0:32] = loads
        own_ref[g, 32:40] = rest

    group(0, range(8, 16))
    group(8, range(8))

    def step(g, _):
        group(g, range(16))
        return 0

    lax.fori_loop(1, 8, step, 0)


def corner_kernel(
    own_ref, far_ref, near_ref, out_ref, top_ref, bottom_ref, far_out_ref, near_out_ref
):
    lane = lanes((SUB, 128)) // 8
    even = lax.axis_index(ROW) % 2 == 0
    top_ref[...] = jnp.where(even, far_ref[...], near_ref[...])
    bottom_ref[...] = jnp.where(even, near_ref[...], far_ref[...])
    for g in range(GROUPS):
        out_ref[g] = own_ref[g]
    start, end = own_ref[0], own_ref[8]
    for n in range(HALO):
        s = 8 - HALO + n
        start = jnp.where(lane == s, roll(top_ref[n], (8 * s + 3) % 128), start)
        s = 8 + n
        end = jnp.where(lane == s, roll(bottom_ref[n], (8 * s + 3) % 128), end)
    out_ref[0] = start
    out_ref[8] = end
    low = lanes((SUB, 128)) % 8 < 4
    to_right_first = lax.axis_index(COL) % 2 == 1
    for h in range(5):
        here = out_ref[2 * h]
        after = out_ref[2 * h + 1] if h < 4 else here
        right = jnp.where(low, here, roll(after, 4))
        left = jnp.where(low, roll(here, 125), roll(after, 1))
        far_out_ref[h] = jnp.where(to_right_first, right, left)
        near_out_ref[h] = jnp.where(to_right_first, left, right)


def fields_kernel(
    rows_ref, grid_ref, top_ref, bottom_ref, own_ref, far_ref, near_ref,
    first_ref, second_ref, w_ref, coef_ref, out_ref,
    ext, so, ss, sz_o, sz_s, y0_o, y0_s, qz, q0, q1, u0, u1, sc, y0, y1, gram,
):
    pr, pc = lax.axis_index(ROW), lax.axis_index(COL)
    lane1 = lanes((1, 128))
    lane16 = lanes((16, 128))
    lane48 = lanes((48, 128))

    for n in range(5):
        ext[n, 0:16] = jnp.zeros((16, 128), F32)
        ext[n, 16:144] = grid_ref[128 * n : 128 * n + 128]
        ext[n, 144:160] = jnp.zeros((16, 128), F32)
        for k in range(HALO):
            ext[n, 16 - HALO + k : 17 - HALO + k] = top_ref[k, 32 + n : 33 + n]
            ext[n, 144 + k : 145 + k] = bottom_ref[k, 32 + n : 33 + n]

    slot = lax.broadcasted_iota(jnp.int32, (16, 128), 0)
    region_row = pr - 1 + slot // 4
    region_col = 2 * pc - 1 + slot % 4
    inside = (slot < 12) & (region_row >= 0) & (region_row < REG) & (region_col >= 0) & (region_col < REG)
    window = jnp.where(inside, region_row * REG + region_col, -1).astype(F32)

    for ref in (so, ss, sz_o, sz_s, y0_o, y0_s):
        ref[0] = jnp.zeros(ref.shape[1:], F32)
        ref[GROUPS + 1] = jnp.zeros(ref.shape[1:], F32)

    def pair_left(o, s, lane):
        j = lane % 8
        return roll(jnp.where(j == 2, s, o), 1), roll(jnp.where(j == 2, o, s), 1)

    def pair_right(o, s, lane):
        j = lane % 8
        return roll(jnp.where(j == 3, s, o), 127), roll(jnp.where(j == 3, o, s), 127)

    def above(before, here, lane):
        return roll(jnp.where(lane >= 120, before, here), 8)

    def below(here, after, lane):
        return roll(jnp.where(lane < 8, after, here), 120)

    even = pc % 2 == 0

    def strips(g, _):
        o_row = own_ref[g]
        far, near = far_ref[g // 2], near_ref[g // 2]
        on_left, on_right = jnp.where(even, far, near), jnp.where(even, near, far)
        turn = 124 * (g % 2)
        s_row = jnp.where(lanes((SUB, 128)) % 8 < 3, roll(on_left, turn), roll(on_right, 3 + turn))
        so[g + 1], ss[g + 1] = o_row, s_row
        lefts = pair_left(o_row[RIGHT : RIGHT + 1], s_row[RIGHT : RIGHT + 1], lane1)
        for side, (row, ref, ll) in enumerate(((o_row, so, lefts[0]), (s_row, ss, lefts[1]))):
            rl, dl = row[RIGHT : RIGHT + 1], row[DOWN : DOWN + 1]
            ul = above(ref[g, DOWN : DOWN + 1], dl, lane1)
            diag = row[PAD : PAD + 1] + rl + ll + dl + ul
            inv = jnp.where(diag > 0, 1.0 / diag, 0.0)
            for n, value in enumerate((diag, rl, ll, dl, ul, inv)):
                sc[side, g, n : n + 1] = value
            z = jnp.where(row[LAB : LAB + 1] == window, row[BUMP : BUMP + 1], 0.0)
            (sz_s if side else sz_o)[g + 1] = z
            if side:
                qz[2 * g] = z
                qz[2 * g + 1] = roll(z, 64)

        at = pl.multiple_of(16 * g + 8, 8)
        beside = jnp.zeros((16, 128), F32)
        for s in range(16):
            beside = jnp.where(slot == s, roll(s_row[RIGHT : RIGHT + 1], 125 - 8 * s), beside)
        rl, dl = ext[2, pl.ds(at, 16)], ext[3, pl.ds(at, 16)]
        ll = roll(jnp.where(lane16 == 127, beside, rl), 1)
        last = ext[3, pl.ds(pl.multiple_of(at - 8, 8), 8)]
        ul = jnp.where(slot == 0, last[7:8], roll(dl, 1, 0))
        diag = ext[4, pl.ds(at, 16)] + rl + ll + dl + ul
        inv = jnp.where(diag > 0, 1.0 / diag, 0.0)
        for n, value in enumerate((diag, rl, ll, dl, ul, inv)):
            coef_ref[n, pl.ds(at, 16)] = value
        return 0

    lax.fori_loop(0, GROUPS, strips, 0, unroll=3)

    def strip_image(ref_o, ref_s, g, lane, sides):
        o, s = ref_o[g + 1], ref_s[g + 1]
        lefts, rights = pair_left(o, s, lane), pair_right(o, s, lane)
        done = []
        for side in sides:
            ref, here = (ref_s, s) if side else (ref_o, o)
            up = above(ref[g], here, lane)
            down = below(here, ref[g + 2], lane)
            c = [sc[side, g, n : n + 1] for n in range(5)]
            done.append(c[0] * here - c[1] * rights[side] - c[2] * lefts[side] - c[3] * down - c[4] * up)
        return done

    def strip_first(g, _):
        w = strip_image(sz_o, sz_s, g, lane16, (0, 1))
        for side, (source, ref) in enumerate(((so, y0_o), (ss, y0_s))):
            inv = sc[side, g, 5:6]
            ref[g + 1, 0:32] = inv * source[g + 1, 0:32]
            ref[g + 1, 32:48] = inv * w[side]
        y = y0_s[g + 1]
        q0[2 * g] = y
        q0[2 * g + 1] = roll(y, 64)
        return 0

    lax.fori_loop(0, GROUPS, strip_first, 0, unroll=3)

    def strip_second(g, _):
        (u,) = strip_image(y0_o, y0_s, g, lane48, (1,))
        y = sc[1, g, 5:6] * u
        q1[2 * g] = y
        q1[2 * g + 1] = roll(y, 64)
        return 0

    lax.fori_loop(0, GROUPS, strip_second, 0, unroll=3)

    def owned(g):
        return not isinstance(g, int)

    def coef(n, g, s):
        return coef_ref[n, pl.ds(8 * g + 8 + s, 1), :]

    def unpacked(strip, g, s):
        return roll(strip[g], 125 - 8 * s)

    def image(here, up, down, other, g, s, lane):
        left = roll(jnp.where(lane == 127, other, here), 1)
        right = roll(jnp.where(lane == 0, other, here), 127)
        return (
            coef(0, g, s) * here
            - coef(1, g, s) * right
            - coef(2, g, s) * left
            - coef(3, g, s) * down
            - coef(4, g, s) * up
        )

    def basis(j):
        return jnp.where(ext[0, pl.ds(j, 1), :] == window, ext[1, pl.ds(j, 1), :], 0.0)

    def first_image(g, s):
        r, j = 8 * g - 8 + s, 8 * g + 8 + s
        w = image(basis(j), basis(j - 1), basis(j + 1), unpacked(qz, g, s), g, s, lane16)
        if owned(g):
            b = rows_ref[r]
            w_ref[r] = w
        else:
            b = top_ref[r + HALO, 0:32] if r < 0 else bottom_ref[r - 128, 0:32]
        inv = coef(5, g, s)
        y0[8 * g + s, 0:32] = inv * b
        y0[8 * g + s, 32:48] = inv * w
        u0[8 * g + s] = unpacked(q0, g, s)

    def second_image(g, s):
        i = 8 * g + s
        f1 = image(y0[i], y0[i - 1], y0[i + 1], u0[i], g, s, lane48)
        if owned(g):
            first_ref[8 * g - 8 + s] = f1
            u1[i] = unpacked(q1, g, s)
        y1[i] = coef(5, g, s) * f1

    def only(work):
        def step(g, _):
            for s in range(8):
                work(g, s)
            return 0

        return step

    for s in (6, 7):
        first_image(0, s)
    lax.fori_loop(1, 17, only(first_image), 0)
    for s in (0, 1):
        first_image(17, s)
    second_image(0, 7)

    def second_pair(t, _):
        for s in range(16):
            second_image(2 * t + 1 + s // 8, s % 8)
        return 0

    lax.fori_loop(0, 8, second_pair, 0)
    second_image(17, 0)

    gram[...] = jnp.zeros((96, 256), F32)

    def third_image(g, s):
        i = 8 * g + s
        second_ref[i - 8] = image(y1[i], y1[i - 1], y1[i + 1], u1[i], g, s, lane48)

    def products(g, sums):
        left, every = [], []
        sums = list(sums)
        for s in range(16):
            i = 16 * g + 8 + s
            r = i - 8
            b, f1, f2, y0r, y1r = rows_ref[r], first_ref[r], second_ref[r], y0[i], y1[i]
            left.append(jnp.concatenate([basis(i + 8), y0r[32:48], y1r[32:48]], axis=0))
            every.append(jnp.concatenate([b, w_ref[r], f1, f2], axis=0))
            pairs = ((y0r, b), (y0r, f1), (y1r, f1), (y1r, f2))
            sums = [t + p[0:32] * q[0:32] for t, (p, q) in zip(sums, pairs)]
        left = jnp.concatenate(parts_of(jnp.concatenate(left, axis=1), 2), axis=0)
        high, low = parts_of(jnp.concatenate(every, axis=1), 2)
        gram[:, 0:144] += fast_dot(left, high, NT) + fast_dot(left, low, NT)
        return tuple(sums)

    def third_pair(t, _):
        for s in range(16):
            third_image(2 * t + 1 + s // 8, s % 8)
        return 0

    def last_stage(t, sums):
        sums = products(t - 1, sums)
        third_pair(t, 0)
        return sums

    zero = jnp.zeros((32, 128), F32)
    lax.fori_loop(0, 1, third_pair, 0)
    sums = lax.fori_loop(1, 8, last_stage, (zero, zero, zero, zero))
    sums = lax.fori_loop(7, 8, products, sums)

    a0, a1 = gram[0:48, 0:128] + gram[48:96, 0:128], gram[0:48, 128:256] + gram[48:96, 128:256]
    zr, w0, t0, w1, t1 = a0[0:16], a0[16:32], a0[32:48], a1[16:32], a1[32:48]
    matrices = jnp.zeros((16, 128), F32)
    for n, (x, z) in enumerate(((w0, 32), (w0, 80), (w1, 0), (zr, 32), (t1, 0))):
        start = 24 * n
        matrices = jnp.where((lane16 >= start) & (lane16 < start + 16), roll(x, (start - z) % 128), matrices)
    moved = jnp.zeros((16, 128), F32)
    for k in range(12):
        moved = jnp.where(slot == k, roll(matrices, (128 - k) % 128), moved)
    common = jnp.zeros((16, 128), F32)
    for n in range(5):
        for start, offset, count in ((20 + 2 * n, 0, 2), (30 + 3 * n, 3, 3)):
            hit = (lane16 >= start) & (lane16 < start + count)
            common = jnp.where(hit, roll(moved, (start - offset - 24 * n) % 128), common)
    lines = []
    diagonal = lanes((32, 128)) == lax.broadcasted_iota(jnp.int32, (32, 128), 0)
    for total in sums:
        column = jnp.sum(total, axis=1, keepdims=True)
        lines.append(jnp.sum(jnp.where(diagonal, column, 0.0), axis=0, keepdims=True))
    row4, lane4 = lax.broadcasted_iota(jnp.int32, (4, 128), 0), lanes((4, 128))
    for d in range(8):
        message = common
        for n, (x, z) in enumerate(((w0, 0), (w0, 48), (w0, 96), (zr, 0), (t0, 96))):
            hit = (lane16 >= 4 * n) & (lane16 < 4 * n + 4)
            message = jnp.where(hit, roll(x, (4 * n - z - 4 * d) % 128), message)
        middle, last = roll(message, 45), roll(message, 90)
        sent = jnp.where(lane4 < 45, message[0:4], jnp.where(lane4 < 90, middle[4:8], last[8:12]))
        line = jnp.zeros((1, 128), F32)
        for n in range(4):
            start = 120 + 4 * n if n < 2 else 112 + 4 * n
            line = jnp.where((lane1 >= start) & (lane1 < start + 4), roll(lines[n], (start - 4 * d) % 128), line)
            if n == 1:
                first_two, line = line, jnp.zeros((1, 128), F32)
        total = jnp.where(row4 == 0, first_two, jnp.where(row4 == 1, line, 0.0))
        sent = jnp.where(lane4 < 120, sent, total)
        if d % 2 == 0:
            before = sent
            continue
        pair = jnp.concatenate([before, sent], axis=0)
        for r in range(16):
            out_ref[32 * r + 4 * d - 4 : 32 * r + 4 * d + 4] = pair


def batched_inverse(a, lane, row, size):
    base = lane - lane % size
    for k in range(0, size, 2):
        at_k, at_n = lane % size == k, lane % size == k + 1
        left = jnp.take_along_axis(a, base + k, axis=1)
        right = jnp.take_along_axis(a, base + k + 1, axis=1)
        p, q, r, t = left[k : k + 1], right[k : k + 1], left[k + 1 : k + 2], right[k + 1 : k + 2]
        inverse = 1.0 / (p * t - q * r)
        upper = jnp.where(at_k[0:1], 1.0, jnp.where(at_n[0:1], 0.0, a[k : k + 1]))
        lower = jnp.where(at_n[0:1], 1.0, jnp.where(at_k[0:1], 0.0, a[k + 1 : k + 2]))
        first = (t * upper - q * lower) * inverse
        second = (p * lower - r * upper) * inverse
        rest = jnp.where(at_k | at_n, 0.0, a) - left * first - right * second
        a = jnp.where(row == k, first, jnp.where(row == k + 1, second, rest))
    return a


def block_inverse(matrix, low, high, size=16):
    lane = lanes((size, 128))
    row = lax.broadcasted_iota(jnp.int32, (size, 128), 0)
    compact = jnp.where(lane % size == row, 1.0, 0.0)
    for n in range(low // size, high // size):
        compact = jnp.where(lane // size == n, matrix[size * n : size * n + size], compact)
    compact = batched_inverse(compact, lane, row, size)
    parts = []
    for n in range(128 // size):
        active = low <= size * n < high
        parts.append(jnp.where(lane // size == n, compact, 0.0) if active else jnp.zeros((size, 128), F32))
    return jnp.concatenate(parts, axis=0)


def coarse_kernel(in_ref, out_ref, g, e, ei, first, second, near):
    pr, pc = lax.axis_index(ROW), lax.axis_index(COL)
    sub8 = lax.broadcasted_iota(jnp.int32, (8, 128), 0)

    lane8 = lanes((8, 128))
    for p in range(16):
        even, odd = jnp.zeros((8, 128), F32), jnp.zeros((8, 128), F32)
        for dr in range(3):
            r = p + 1 - dr
            if not 0 <= r < 16:
                continue
            at = [in_ref[pl.ds(32 * r + dq, 8, stride=4), :] for dq in range(4)]
            pair = (
                at[1] + jnp.where(sub8 >= 1, roll(at[3], 1, 0), 0.0),
                at[2] + jnp.where(sub8 < 7, roll(at[0], 7, 0), 0.0),
            )
            hit = lane8 < (30 if dr == 2 else 45)
            even, odd = (
                old + jnp.where(hit, roll(new, (128 - 45 * dr) % 128) if dr else new, 0.0)
                for old, new in zip((even, odd), pair)
            )
        g[pl.ds(16 * p, 8, stride=2), :] = even
        g[pl.ds(16 * p + 1, 8, stride=2), :] = odd
    tally = [
        roll(jnp.sum(in_ref[pl.ds(n, 128, stride=4), :], axis=0, keepdims=True), 8 + 8 * n) for n in range(2)
    ]
    tally = jnp.where(lanes((1, 128)) < 8, tally[0], tally[1])
    tally = jnp.broadcast_to(tally, (128, 128)).T
    bb, bu, uu, uuu = (tally[4 * n : 4 * n + 4, 0:1] for n in range(4))
    by_lane = jnp.concatenate([g[0:128].T, g[128:256].T], axis=1)

    lane16, row16 = lanes((16, 128)), lax.broadcasted_iota(jnp.int32, (16, 128), 0)
    for p in range(16):
        own = g[16 * p : 16 * p + 16]
        terms = [(own, d, dp, dq) for d, dp, dq in ((0, 0, 0), (1, 0, 1))]
        terms.append((roll(own, 1, 0), 1, 0, -1))
        if p < 15:
            terms += [(own, d, 1, dq) for d, dq in ((3, -1), (4, 0), (5, 1))]
        if p > 0:
            last = g[16 * p - 16 : 16 * p]
            terms += [(roll(last, 15, 0), 3, -1, 1), (last, 4, -1, 0), (roll(last, 1, 0), 5, -1, -1)]
        halves = [jnp.zeros((16, 128), F32), jnp.zeros((16, 128), F32)]
        for x, d, dp, dq in terms:
            target = POS[p + dp] * 16
            h, off = target // 128, target % 128
            q = row16 + dq
            hit = (lane16 == off + q) & (q >= 0) & (q < 16)
            at = 26 + d if d < 2 else 36 + d
            value = jnp.broadcast_to(x[:, at : at + 1], (16, 128))
            halves[h] = jnp.where(hit, value, halves[h])
        at = POS[p] * 16
        e[at : at + 16, 0:128] = halves[0]
        e[at : at + 16, 128:256] = halves[1]

    lane = lanes((128, 128))
    row = lax.broadcasted_iota(jnp.int32, (128, 128), 0)
    outer = block_inverse(e[0:128, 0:128], 0, 128)
    across = dot(outer, e[0:128, 128:256])
    schur = e[128:256, 128:256] - dot(e[128:256, 0:128], across)
    steps = []
    for low, high in ((0, 64), (64, 96)):
        inv = block_inverse(schur, low, high)
        link = jnp.where((row >= low) & (row < high) & (lane >= high), schur, 0.0)
        x = dot(inv, link)
        keep = jnp.where((row >= high) & (lane >= high), schur, 0.0)
        schur = keep - dot(link, x, TN)
        steps.append((inv, jnp.where((row == lane) & (row >= high), 1.0, 0.0) - x))
    inner = block_inverse(schur, 96, 128, 32)
    for inv, y in reversed(steps):
        inner = inv + dot(dot(y, inner), y, NT)
    half = dot(across, inner)
    near_diag = outer + dot(half, across, NT)

    def ordered(top_half, bottom_half):
        blocks = [top_half[16 * n : 16 * n + 16] for n in range(8)]
        blocks += [bottom_half[16 * n : 16 * n + 16] for n in range(8)]
        blocks = [blocks[POS[p]] for p in range(16)]
        return jnp.concatenate(blocks[:8], axis=0), jnp.concatenate(blocks[8:], axis=0)

    left_top, left_bottom = ordered(near_diag, -half.T)
    right_top, right_bottom = ordered(-half, inner)
    top_left, bottom_left = ordered(left_top.T, right_top.T)
    top_right, bottom_right = ordered(left_bottom.T, right_bottom.T)
    inverse = jnp.concatenate(
        [jnp.concatenate([top_left, bottom_left], axis=0), jnp.concatenate([top_right, bottom_right], axis=0)],
        axis=1,
    )
    for n, part in enumerate(parts_of(inverse, 3)):
        ei[n] = part

    def solve(z):
        rows = [part.astype(F32) for part in parts_of(z, 3)]
        rows = jnp.concatenate(rows + [jnp.zeros_like(z)], axis=0).astype(jnp.bfloat16)
        a, b, c = (fast_dot(rows, ei[n]) for n in range(3))
        return a[0:4] + (a[4:8] + b[0:4]) + (a[8:12] + b[4:8] + c[0:4])

    def apply(n, v):
        c = {d: by_lane[at : at + 1] for d, at in enumerate((20 + 2 * n, 21 + 2 * n, 0, 30 + 3 * n, 31 + 3 * n, 32 + 3 * n))}
        total = c[0] * v
        for d, step in ((1, 1), (3, 15), (4, 16), (5, 17)):
            total = total + c[d] * roll(v, 256 - step) + roll(c[d] * v, step)
        return total

    def inner_product(a, b):
        return jnp.sum(a * b, axis=1, keepdims=True)

    wb, wu, wuu, zb, tuu = (by_lane[4 * n : 4 * n + 4] for n in range(5))
    c0 = solve(zb)
    f_c, g_c, h_c, k_c = apply(0, c0), apply(1, c0), apply(2, c0), apply(4, c0)
    grad0 = wb - f_c
    k0 = solve(grad0)
    f_k, g_k = apply(0, k0), apply(1, k0)
    rho0 = bb - 2.0 * inner_product(c0, wb) + inner_product(c0, f_c)
    energy0 = bu - 2.0 * inner_product(c0, wu) + inner_product(c0, g_c)
    curve0 = energy0 - inner_product(k0, grad0)
    a0 = rho0 / curve0
    e1 = c0 - a0 * k0
    f_e = f_c - a0 * f_k
    g_e = g_c - a0 * g_k
    grad1 = wb - f_e + a0 * (g_c - wu)
    k1 = solve(grad1)

    def second_norm(m0, m1, m2, v0, v1, v2, e_image, c_image, last):
        own = m0 - 2.0 * inner_product(e1, v0) + inner_product(e1, e_image)
        mixed = m1 - inner_product(c0, v1) - inner_product(e1, v1) + inner_product(e1, c_image)
        far = m2 - 2.0 * inner_product(c0, v2) + inner_product(c0, last)
        return own - 2.0 * a0 * mixed + a0 * a0 * far

    rho1 = second_norm(bb, bu, uu, wb, wu, wuu, f_e, g_c, h_c)
    energy1 = second_norm(bu, uu, uuu, wu, wuu, tuu, g_e, h_c, k_c)
    beta = rho1 / rho0
    cross = (
        bu
        - inner_product(c0, wu)
        - inner_product(e1, wu)
        + inner_product(e1, g_c)
        - a0 * (uu - 2.0 * inner_product(c0, wuu) + inner_product(c0, h_c))
        - inner_product(k0, grad1)
    )
    curve1 = energy1 - inner_product(k1, grad1) + 2.0 * beta * cross + beta * beta * curve0
    a1 = rho1 / curve1

    mine = lax.broadcasted_iota(jnp.int32, (32, 256), 0) // 4 == pc

    def zone(value):
        value = jnp.broadcast_to(value, (4, 256))
        return jnp.where(mine, jnp.concatenate([value] * 8, axis=0), 0.0)

    ab = a1 * beta
    stacks = (
        (
            zone(a1 * k1 + ab * k0 - e1),
            zone(-(a0 + ab) * c0 - a1 * e1),
            zone((a0 + ab) * c0 + a1 * e1),
            zone((a1 * a0) * c0),
        ),
        (
            zone(-(a1 * a0) * c0),
            zone(c0 - (a0 + ab) * k0 - a1 * k1),
            zone(-a0 - a1 - ab),
            zone(a1 * a0),
        ),
    )
    out_ref[...] = jnp.zeros((256, 128), F32)
    for n, (ref, stack) in enumerate(((first, stacks[0]), (second, stacks[1]))):
        stack = jnp.concatenate(stack, axis=0)
        ref[0:8] = jnp.zeros((8, 128), F32)
        ref[8:136] = stack[:, 0:128].T
        ref[136:264] = stack[:, 128:256].T
        ref[264:272] = jnp.zeros((8, 128), F32)
        for dr in range(3):
            p = jnp.clip(pr - 1 + dr, 0, 15)
            near[...] = ref[pl.ds(pl.multiple_of(16 * p, 16), 32), :]
            for dq in range(4):
                out_ref[pl.ds(16 * n + 4 * dr + dq, 8, stride=32), :] = near[pl.ds(7 + dq, 8, stride=2), :]


def outputs_kernel(
    rows_ref, first_ref, second_ref, w_ref, grid_ref, coef_ref, m_ref, sol_ref, res_ref,
    left_ref, step_ref, window_ref,
):
    block = pl.program_id(0)

    @pl.when(block == 0)
    def _():
        pr, pc = lax.axis_index(ROW), lax.axis_index(COL)
        slot = lax.broadcasted_iota(jnp.int32, (16, 128), 0)
        region_row = pr - 1 + slot // 4
        region_col = 2 * pc - 1 + slot % 4
        inside = (slot < 12) & (region_row >= 0) & (region_row < REG) & (region_col >= 0) & (region_col < REG)
        window_ref[...] = jnp.where(inside, region_row * REG + region_col, -1).astype(F32)
        total = m_ref[0:32]
        for n in range(1, 8):
            total = total + m_ref[32 * n : 32 * n + 32]
        top, bottom = total[0:16], total[16:32]
        lane = lanes((16, 128))
        steps = jnp.where(slot == 0, roll(bottom[5:6], 64), jnp.where(slot == 1, roll(bottom[5:6], 32), 0.0))
        m = jnp.concatenate(
            [
                jnp.where((lane >= 64) & (lane < 96), roll(bottom, 32), 0.0),
                jnp.where(lane < 64, top, 0.0),
                jnp.where(lane < 64, roll(top, 64), 0.0),
                jnp.where(lane < 32, bottom, 0.0),
                steps,
                jnp.zeros((48, 128), F32),
            ],
            axis=0,
        ).T
        c1, c2, c3 = parts_of(m[0:96, 0:64], 3)
        left_ref[...] = jnp.concatenate([c1, c1, c2, c2, c1, c3], axis=1)
        for n in range(2):
            step_ref[n] = jnp.broadcast_to(m[0:32, 64 + n : 65 + n], (32, 128))

    left, window = left_ref[...], window_ref[...]
    for part in range(4):
        rows = []
        for n in range(8):
            r = 32 * block + 8 * part + n
            z = jnp.where(grid_ref[pl.ds(r, 1), :] == window, grid_ref[pl.ds(128 + r, 1), :], 0.0)
            rows.append(jnp.concatenate([z, w_ref[r], first_ref[r, 32:48], second_ref[r, 32:48]], axis=0))
        r1, r2, r3 = parts_of(jnp.concatenate(rows, axis=1), 3)
        d = fast_dot(left, jnp.concatenate([r1, r2, r1, r2, r3, r1], axis=0))
        for n in range(8):
            r = 32 * block + 8 * part + n
            b, u, uu = rows_ref[r], first_ref[r, 0:32], second_ref[r, 0:32]
            e = d[:, 128 * n : 128 * n + 128]
            inv = coef_ref[5, pl.ds(r + 16, 1), :]
            p1, p2 = step_ref[0], step_ref[1]
            res_ref[:, 8 * part + n] = b + p1 * u + p2 * uu + e[0:32]
            sol_ref[:, 8 * part + n] = inv * (e[32:64] - p1 * b - p2 * u) + e[64:96]


def swapped(value, axis, start):
    pairs = [(i, i + 1) for i in range(start, lax.axis_size(axis) - 1, 2)]
    return lax.ppermute(value, axis, pairs + [(b, a) for a, b in pairs])


def shape_of(*dims):
    return jax.ShapeDtypeStruct(dims, F32)


def kept(*dims):
    return pltpu.VMEM(dims, F32)


def vmem(*dims):
    return pltpu.VMEM(dims, F32)


def body(load_currents, labels, bump_height, horizontal_class, vertical_class, pad_class, edge_table, pad_table):
    rows, cols = lax.axis_size(ROW), lax.axis_size(COL)
    loads = load_currents.reshape(-1, 128)
    grid, far_rows, near_rows = pl.pallas_call(
        prepare_kernel,
        out_shape=(kept(1024, 128), shape_of(HALO, SUB, 128), shape_of(HALO, SUB, 128)),
        compiler_params=limited,
        in_specs=[outside] * 8,
        out_specs=(whole,) * 3,
        scratch_shapes=[pltpu.SMEM((8,), F32), pltpu.SMEM((8,), F32), vmem(32, 8, 128), vmem(32, 8, 128)]
        + [pltpu.VMEM((128, 128), jnp.int32)] * 4
        + [pltpu.SemaphoreType.DMA((9,))],
    )(
        *(
            pltpu.with_memory_space_constraint(x, pltpu.HBM)
            for x in (
                edge_table, pad_table, load_currents, labels, bump_height,
                horizontal_class, vertical_class, pad_class,
            )
        ),
    )
    far_rows = swapped(far_rows, ROW, 1)
    near_rows = swapped(near_rows, ROW, 0)
    by_rows, own = pl.pallas_call(
        pack_kernel,
        out_shape=(kept(128, 32, 128), kept(GROUPS, SUB, 128)),
        compiler_params=limited,
        in_specs=[whole] * 2,
        out_specs=(whole,) * 2,
    )(loads, grid)
    own, top, bottom, far_columns, near_columns = pl.pallas_call(
        corner_kernel,
        out_shape=(kept(GROUPS, SUB, 128), kept(HALO, SUB, 128), kept(HALO, SUB, 128))
        + (shape_of(5, SUB, 128),) * 2,
        compiler_params=limited,
        in_specs=[whole] * 3,
        out_specs=(whole,) * 5,
    )(own, far_rows, near_rows)
    far_columns = swapped(far_columns, COL, 1)
    near_columns = swapped(near_columns, COL, 0)
    first, second, w, coef, payload = pl.pallas_call(
        fields_kernel,
        out_shape=(
            kept(128, 48, 128),
            kept(128, 48, 128),
            kept(128, 16, 128),
            kept(6, 160, 128),
            shape_of(512, 128),
        ),
        compiler_params=limited,
        in_specs=[whole] * 7,
        out_specs=(whole,) * 5,
        scratch_shapes=[
            vmem(5, 160, 128),
            vmem(GROUPS + 2, SUB, 128),
            vmem(GROUPS + 2, SUB, 128),
            vmem(GROUPS + 2, 16, 128),
            vmem(GROUPS + 2, 16, 128),
            vmem(GROUPS + 2, 48, 128),
            vmem(GROUPS + 2, 48, 128),
            vmem(2 * GROUPS, 16, 128),
            vmem(2 * GROUPS, 48, 128),
            vmem(2 * GROUPS, 48, 128),
            vmem(144, 48, 128),
            vmem(144, 48, 128),
            vmem(2, GROUPS, 8, 128),
            vmem(144, 48, 128),
            vmem(144, 48, 128),
            vmem(96, 256),
        ],
    )(by_rows, grid, top, bottom, own, far_columns, near_columns)
    sent = payload.reshape(-1, 4, 128)
    everything = lax.all_to_all(sent, ROW + COL, 0, 0, tiled=True).reshape(-1, 128)
    found = pl.pallas_call(
        coarse_kernel,
        out_shape=shape_of(256, 128),
        compiler_params=limited,
        in_specs=[whole],
        out_specs=whole,
        scratch_shapes=[
            vmem(256, 128),
            vmem(256, 256),
            pltpu.VMEM((3, 256, 256), jnp.bfloat16),
            vmem(272, 128),
            vmem(272, 128),
            vmem(32, 128),
        ],
    )(everything)
    matrix = lax.all_to_all(found.reshape(cols, 32, 128), COL, 0, 0, tiled=True).reshape(-1, 128)
    by_block = pl.BlockSpec((32, 32, 128), lambda k: (0, k, 0))
    return pl.pallas_call(
        outputs_kernel,
        grid=(4,),
        out_shape=(shape_of(32, 128, 128), shape_of(32, 128, 128)),
        compiler_params=limited,
        in_specs=[whole] * 7,
        out_specs=(by_block, by_block),
        scratch_shapes=[pltpu.VMEM((96, 384), jnp.bfloat16), vmem(2, 32, 128), vmem(16, 128)],
    )(by_rows, first, second, w, grid, coef, matrix)


def solution(mesh):
    finer = Mesh(mesh.devices.reshape(4, 4, 4, 2), ("row_0", "row_1", "col_0", "col_1"))
    grid = P(ROW, COL)
    return jax.shard_map(
        body,
        mesh=finer,
        in_specs=(P(None, ROW, COL), grid, grid, grid, grid, grid, P(), P()),
        out_specs=(P(None, ROW, COL), P(None, ROW, COL)),
        check_vma=False,
    )
```

```python
import jax
import jax.numpy as jnp
from jax import lax
from jax.experimental import pallas as pl
from jax.experimental.pallas import tpu as pltpu
from jax.sharding import Mesh
from jax.sharding import PartitionSpec as P

REG = 16
ROW = ("row_0", "row_1")
COL = ("col_0", "col_1")
F32 = jnp.float32

LAB, BUMP, RIGHT, DOWN, PAD = 32, 33, 34, 35, 36
SUB = 40
HALO = 3
GROUPS = 9
ORDER = (1, 3, 5, 7, 9, 11, 13, 15, 2, 6, 10, 14, 4, 12, 8, 0)
POS = tuple(ORDER.index(p) for p in range(16))
NT = (((1,), (1,)), ((), ()))
NN = (((1,), (0,)), ((), ()))
TN = (((0,), (0,)), ((), ()))
whole = pl.BlockSpec(memory_space=pltpu.VMEM)
outside = pl.BlockSpec(memory_space=pltpu.HBM)
limited = pltpu.CompilerParams(vmem_limit_bytes=32 * 2**20)


def parts_of(x, count):
    parts = []
    for n in range(count):
        parts.append(x.astype(jnp.bfloat16))
        if n + 1 < count:
            x = x - parts[-1].astype(F32)
    return parts


def fast_dot(a, b, dims=NN):
    return lax.dot_general(a, b, dims, preferred_element_type=F32)


def dot(a, b, dims=NN):
    (at_a,), (at_b,) = dims[0]
    a1, a2, a3 = parts_of(a, 3)
    b1, b2, b3 = parts_of(b, 3)
    return fast_dot(
        jnp.concatenate([a3, a1, a2, a2, a1, a1], axis=at_a),
        jnp.concatenate([b1, b3, b2, b1, b2, b1], axis=at_b),
        dims,
    )


def lanes(shape):
    return lax.broadcasted_iota(jnp.int32, shape, len(shape) - 1)


def roll(x, shift, axis=1):
    return pltpu.roll(x, shift, axis)


def prepare_kernel(
    edge_hbm, pad_hbm, load_hbm, label_hbm, bump_hbm, across_hbm, down_hbm, pad_class_hbm,
    grid_ref, far_ref, near_ref, edge_ref, pad_ref, load_ref, load_end_ref, label_ref, across_ref, down_ref, pad_class_ref, done,
):
    copies = [
        pltpu.make_async_copy(source, target, done.at[n])
        for n, (source, target) in enumerate(
            (
                (edge_hbm, edge_ref),
                (pad_hbm, pad_ref),
                (across_hbm, across_ref),
                (down_hbm, down_ref),
                (pad_class_hbm, pad_class_ref),
                (label_hbm, label_ref),
                (bump_hbm, grid_ref.at[pl.ds(128, 128)]),
                (load_hbm.at[:, pl.ds(0, 8)], load_ref),
                (load_hbm.at[:, pl.ds(120, 8)], load_end_ref),
            )
        )
    ]
    for copy in copies:
        copy.start()
    for copy in copies:
        copy.wait()
    pr, pc = lax.axis_index(ROW), lax.axis_index(COL)
    shape = (128, 128)
    row, lane = lax.broadcasted_iota(jnp.int32, shape, 0), lanes(shape)

    def lookup(table, classes):
        found = jnp.zeros(shape, F32)
        for n in range(8):
            found = jnp.where(classes == n, table[n], found)
        return found

    right = lookup(edge_ref, across_ref[...])
    down = lookup(edge_ref, down_ref[...])
    grid_ref[0:128] = label_ref[...].astype(F32)
    grid_ref[256:384] = jnp.where((lane == 127) & (pc == 7), 0.0, right)
    grid_ref[384:512] = jnp.where((row == 127) & (pr == 15), 0.0, down)
    grid_ref[512:640] = lookup(pad_ref, pad_class_ref[...])
    grid_ref[640:1024] = jnp.zeros((384, 128), F32)
    for n in range(HALO):
        even = pr % 2 == 0
        first, last = load_ref[:, n], load_end_ref[:, 8 - HALO + n]
        far_ref[n, 0:32] = jnp.where(even, first, last)
        near_ref[n, 0:32] = jnp.where(even, last, first)
        first = grid_ref[pl.ds(n, 8, stride=128), :]
        last = grid_ref[pl.ds(128 - HALO + n, 8, stride=128), :]
        far_ref[n, 32:40] = jnp.where(even, first, last)
        near_ref[n, 32:40] = jnp.where(even, last, first)


def pack_kernel(load_ref, grid_ref, rows_ref, own_ref):
    lane = lanes((32, 128)) // 8

    def group(g, slots):
        loads, rest = jnp.zeros((32, 128), F32), jnp.zeros((8, 128), F32)
        for s in slots:
            r = 16 * g - 8 + s
            b = load_ref[pl.ds(r, 32, stride=128), :]
            rows_ref[r] = b
            loads = jnp.where(lane == s, roll(b, (8 * s + 3) % 128), loads)
            rest = jnp.where(lane[0:8] == s, roll(grid_ref[pl.ds(r, 8, stride=128), :], (8 * s + 3) % 128), rest)
        own_ref[g, 0:32] = loads
        own_ref[g, 32:40] = rest

    group(0, range(8, 16))
    group(8, range(8))

    def step(g, _):
        group(g, range(16))
        return 0

    lax.fori_loop(1, 8, step, 0)


def corner_kernel(
    own_ref, far_ref, near_ref, out_ref, top_ref, bottom_ref, far_out_ref, near_out_ref
):
    lane = lanes((SUB, 128)) // 8
    even = lax.axis_index(ROW) % 2 == 0
    top_ref[...] = jnp.where(even, far_ref[...], near_ref[...])
    bottom_ref[...] = jnp.where(even, near_ref[...], far_ref[...])
    for g in range(GROUPS):
        out_ref[g] = own_ref[g]
    start, end = own_ref[0], own_ref[8]
    for n in range(HALO):
        s = 8 - HALO + n
        start = jnp.where(lane == s, roll(top_ref[n], (8 * s + 3) % 128), start)
        s = 8 + n
        end = jnp.where(lane == s, roll(bottom_ref[n], (8 * s + 3) % 128), end)
    out_ref[0] = start
    out_ref[8] = end
    low = lanes((SUB, 128)) % 8 < 4
    to_right_first = lax.axis_index(COL) % 2 == 1
    for h in range(5):
        here = out_ref[2 * h]
        after = out_ref[2 * h + 1] if h < 4 else here
        right = jnp.where(low, here, roll(after, 4))
        left = jnp.where(low, roll(here, 125), roll(after, 1))
        far_out_ref[h] = jnp.where(to_right_first, right, left)
        near_out_ref[h] = jnp.where(to_right_first, left, right)


def fields_kernel(
    rows_ref, grid_ref, top_ref, bottom_ref, own_ref, far_ref, near_ref,
    first_ref, second_ref, w_ref, coef_ref, out_ref,
    ext, so, ss, sz_o, sz_s, y0_o, y0_s, qz, q0, q1, u0, u1, sc, y0, y1, gram,
):
    pr, pc = lax.axis_index(ROW), lax.axis_index(COL)
    lane1 = lanes((1, 128))
    lane16 = lanes((16, 128))
    lane48 = lanes((48, 128))

    for n in range(5):
        ext[n, 0:16] = jnp.zeros((16, 128), F32)
        ext[n, 16:144] = grid_ref[128 * n : 128 * n + 128]
        ext[n, 144:160] = jnp.zeros((16, 128), F32)
        for k in range(HALO):
            ext[n, 16 - HALO + k : 17 - HALO + k] = top_ref[k, 32 + n : 33 + n]
            ext[n, 144 + k : 145 + k] = bottom_ref[k, 32 + n : 33 + n]

    slot = lax.broadcasted_iota(jnp.int32, (16, 128), 0)
    region_row = pr - 1 + slot // 4
    region_col = 2 * pc - 1 + slot % 4
    inside = (slot < 12) & (region_row >= 0) & (region_row < REG) & (region_col >= 0) & (region_col < REG)
    window = jnp.where(inside, region_row * REG + region_col, -1).astype(F32)

    for ref in (so, ss, sz_o, sz_s, y0_o, y0_s):
        ref[0] = jnp.zeros(ref.shape[1:], F32)
        ref[GROUPS + 1] = jnp.zeros(ref.shape[1:], F32)

    def pair_left(o, s, lane):
        j = lane % 8
        return roll(jnp.where(j == 2, s, o), 1), roll(jnp.where(j == 2, o, s), 1)

    def pair_right(o, s, lane):
        j = lane % 8
        return roll(jnp.where(j == 3, s, o), 127), roll(jnp.where(j == 3, o, s), 127)

    def above(before, here, lane):
        return roll(jnp.where(lane >= 120, before, here), 8)

    def below(here, after, lane):
        return roll(jnp.where(lane < 8, after, here), 120)

    even = pc % 2 == 0

    def strips(g, _):
        o_row = own_ref[g]
        far, near = far_ref[g // 2], near_ref[g // 2]
        on_left, on_right = jnp.where(even, far, near), jnp.where(even, near, far)
        turn = 124 * (g % 2)
        s_row = jnp.where(lanes((SUB, 128)) % 8 < 3, roll(on_left, turn), roll(on_right, 3 + turn))
        so[g + 1], ss[g + 1] = o_row, s_row
        lefts = pair_left(o_row[RIGHT : RIGHT + 1], s_row[RIGHT : RIGHT + 1], lane1)
        for side, (row, ref, ll) in enumerate(((o_row, so, lefts[0]), (s_row, ss, lefts[1]))):
            rl, dl = row[RIGHT : RIGHT + 1], row[DOWN : DOWN + 1]
            ul = above(ref[g, DOWN : DOWN + 1], dl, lane1)
            diag = row[PAD : PAD + 1] + rl + ll + dl + ul
            inv = jnp.where(diag > 0, 1.0 / diag, 0.0)
            for n, value in enumerate((diag, rl, ll, dl, ul, inv)):
                sc[side, g, n : n + 1] = value
            z = jnp.where(row[LAB : LAB + 1] == window, row[BUMP : BUMP + 1], 0.0)
            (sz_s if side else sz_o)[g + 1] = z
            if side:
                qz[2 * g] = z
                qz[2 * g + 1] = roll(z, 64)

        at = pl.multiple_of(16 * g + 8, 8)
        beside = jnp.zeros((16, 128), F32)
        for s in range(16):
            beside = jnp.where(slot == s, roll(s_row[RIGHT : RIGHT + 1], 125 - 8 * s), beside)
        rl, dl = ext[2, pl.ds(at, 16)], ext[3, pl.ds(at, 16)]
        ll = roll(jnp.where(lane16 == 127, beside, rl), 1)
        last = ext[3, pl.ds(pl.multiple_of(at - 8, 8), 8)]
        ul = jnp.where(slot == 0, last[7:8], roll(dl, 1, 0))
        diag = ext[4, pl.ds(at, 16)] + rl + ll + dl + ul
        inv = jnp.where(diag > 0, 1.0 / diag, 0.0)
        for n, value in enumerate((diag, rl, ll, dl, ul, inv)):
            coef_ref[n, pl.ds(at, 16)] = value
        return 0

    lax.fori_loop(0, GROUPS, strips, 0, unroll=3)

    def strip_image(ref_o, ref_s, g, lane, sides):
        o, s = ref_o[g + 1], ref_s[g + 1]
        lefts, rights = pair_left(o, s, lane), pair_right(o, s, lane)
        done = []
        for side in sides:
            ref, here = (ref_s, s) if side else (ref_o, o)
            up = above(ref[g], here, lane)
            down = below(here, ref[g + 2], lane)
            c = [sc[side, g, n : n + 1] for n in range(5)]
            done.append(c[0] * here - c[1] * rights[side] - c[2] * lefts[side] - c[3] * down - c[4] * up)
        return done

    def strip_first(g, _):
        w = strip_image(sz_o, sz_s, g, lane16, (0, 1))
        for side, (source, ref) in enumerate(((so, y0_o), (ss, y0_s))):
            inv = sc[side, g, 5:6]
            ref[g + 1, 0:32] = inv * source[g + 1, 0:32]
            ref[g + 1, 32:48] = inv * w[side]
        y = y0_s[g + 1]
        for s in range(16):
            u0[16 * g + s] = roll(y, (125 - 8 * s) % 128)
        return 0

    lax.fori_loop(0, GROUPS, strip_first, 0, unroll=3)

    def strip_second(g, _):
        (u,) = strip_image(y0_o, y0_s, g, lane48, (1,))
        y = sc[1, g, 5:6] * u
        q1[2 * g] = y
        q1[2 * g + 1] = roll(y, 64)
        return 0

    lax.fori_loop(0, GROUPS, strip_second, 0, unroll=3)

    def owned(g):
        return not isinstance(g, int)

    def coef(n, g, s):
        return coef_ref[n, pl.ds(8 * g + 8 + s, 1), :]

    def unpacked(strip, g, s):
        return roll(strip[g], 125 - 8 * s)

    def image(here, up, down, other, g, s, lane):
        left = roll(jnp.where(lane == 127, other, here), 1)
        right = roll(jnp.where(lane == 0, other, here), 127)
        return (
            coef(0, g, s) * here
            - coef(1, g, s) * right
            - coef(2, g, s) * left
            - coef(3, g, s) * down
            - coef(4, g, s) * up
        )

    def basis(j):
        return jnp.where(ext[0, pl.ds(j, 1), :] == window, ext[1, pl.ds(j, 1), :], 0.0)

    def first_image(g, s):
        r, j = 8 * g - 8 + s, 8 * g + 8 + s
        w = image(basis(j), basis(j - 1), basis(j + 1), unpacked(qz, g, s), g, s, lane16)
        if owned(g):
            b = rows_ref[r]
            w_ref[r] = w
        else:
            b = top_ref[r + HALO, 0:32] if r < 0 else bottom_ref[r - 128, 0:32]
        inv = coef(5, g, s)
        y0[8 * g + s, 0:32] = inv * b
        y0[8 * g + s, 32:48] = inv * w

    def second_image(g, s):
        i = 8 * g + s
        f1 = image(y0[i], y0[i - 1], y0[i + 1], u0[i], g, s, lane48)
        if owned(g):
            first_ref[8 * g - 8 + s] = f1
            u1[i] = unpacked(q1, g, s)
        y1[i] = coef(5, g, s) * f1

    def only(work):
        def step(g, _):
            for s in range(8):
                work(g, s)
            return 0

        return step

    for s in (6, 7):
        first_image(0, s)
    lax.fori_loop(1, 17, only(first_image), 0)
    for s in (0, 1):
        first_image(17, s)
    second_image(0, 7)

    def second_pair(t, _):
        for s in range(16):
            second_image(2 * t + 1 + s // 8, s % 8)
        return 0

    lax.fori_loop(0, 8, second_pair, 0)
    second_image(17, 0)

    gram[...] = jnp.zeros((96, 256), F32)

    def third_image(g, s):
        i = 8 * g + s
        second_ref[i - 8] = image(y1[i], y1[i - 1], y1[i + 1], u1[i], g, s, lane48)

    def products(g, sums):
        left, every = [], []
        sums = list(sums)
        for s in range(16):
            i = 16 * g + 8 + s
            r = i - 8
            b, f1, f2, y0r, y1r = rows_ref[r], first_ref[r], second_ref[r], y0[i], y1[i]
            left.append(jnp.concatenate([basis(i + 8), y0r[32:48], y1r[32:48]], axis=0))
            every.append(jnp.concatenate([b, w_ref[r], f1, f2], axis=0))
            pairs = ((y0r, b), (y0r, f1), (y1r, f1), (y1r, f2))
            sums = [t + p[0:32] * q[0:32] for t, (p, q) in zip(sums, pairs)]
        left = jnp.concatenate(parts_of(jnp.concatenate(left, axis=1), 2), axis=0)
        high, low = parts_of(jnp.concatenate(every, axis=1), 2)
        gram[:, 0:144] += fast_dot(left, high, NT) + fast_dot(left, low, NT)
        return tuple(sums)

    def third_pair(t, _):
        for s in range(16):
            third_image(2 * t + 1 + s // 8, s % 8)
        return 0

    def last_stage(t, sums):
        sums = products(t - 1, sums)
        third_pair(t, 0)
        return sums

    zero = jnp.zeros((32, 128), F32)
    lax.fori_loop(0, 1, third_pair, 0)
    sums = lax.fori_loop(1, 8, last_stage, (zero, zero, zero, zero))
    sums = lax.fori_loop(7, 8, products, sums)

    a0, a1 = gram[0:48, 0:128] + gram[48:96, 0:128], gram[0:48, 128:256] + gram[48:96, 128:256]
    zr, w0, t0, w1, t1 = a0[0:16], a0[16:32], a0[32:48], a1[16:32], a1[32:48]
    matrices = jnp.zeros((16, 128), F32)
    for n, (x, z) in enumerate(((w0, 32), (w0, 80), (w1, 0), (zr, 32), (t1, 0))):
        start = 24 * n
        matrices = jnp.where((lane16 >= start) & (lane16 < start + 16), roll(x, (start - z) % 128), matrices)
    moved = jnp.zeros((16, 128), F32)
    for k in range(12):
        moved = jnp.where(slot == k, roll(matrices, (128 - k) % 128), moved)
    common = jnp.zeros((16, 128), F32)
    for n in range(5):
        for start, offset, count in ((20 + 2 * n, 0, 2), (30 + 3 * n, 3, 3)):
            hit = (lane16 >= start) & (lane16 < start + count)
            common = jnp.where(hit, roll(moved, (start - offset - 24 * n) % 128), common)
    lines = []
    diagonal = lanes((32, 128)) == lax.broadcasted_iota(jnp.int32, (32, 128), 0)
    for total in sums:
        column = jnp.sum(total, axis=1, keepdims=True)
        lines.append(jnp.sum(jnp.where(diagonal, column, 0.0), axis=0, keepdims=True))
    row4, lane4 = lax.broadcasted_iota(jnp.int32, (4, 128), 0), lanes((4, 128))
    for d in range(8):
        message = common
        for n, (x, z) in enumerate(((w0, 0), (w0, 48), (w0, 96), (zr, 0), (t0, 96))):
            hit = (lane16 >= 4 * n) & (lane16 < 4 * n + 4)
            message = jnp.where(hit, roll(x, (4 * n - z - 4 * d) % 128), message)
        middle, last = roll(message, 45), roll(message, 90)
        sent = jnp.where(lane4 < 45, message[0:4], jnp.where(lane4 < 90, middle[4:8], last[8:12]))
        line = jnp.zeros((1, 128), F32)
        for n in range(4):
            start = 120 + 4 * n if n < 2 else 112 + 4 * n
            line = jnp.where((lane1 >= start) & (lane1 < start + 4), roll(lines[n], (start - 4 * d) % 128), line)
            if n == 1:
                first_two, line = line, jnp.zeros((1, 128), F32)
        total = jnp.where(row4 == 0, first_two, jnp.where(row4 == 1, line, 0.0))
        sent = jnp.where(lane4 < 120, sent, total)
        if d % 2 == 0:
            before = sent
            continue
        pair = jnp.concatenate([before, sent], axis=0)
        for r in range(16):
            out_ref[32 * r + 4 * d - 4 : 32 * r + 4 * d + 4] = pair


def batched_inverse(a, lane, row, size):
    base = lane - lane % size
    for k in range(0, size, 2):
        at_k, at_n = lane % size == k, lane % size == k + 1
        left = jnp.take_along_axis(a, base + k, axis=1)
        right = jnp.take_along_axis(a, base + k + 1, axis=1)
        p, q, r, t = left[k : k + 1], right[k : k + 1], left[k + 1 : k + 2], right[k + 1 : k + 2]
        inverse = 1.0 / (p * t - q * r)
        upper = jnp.where(at_k[0:1], 1.0, jnp.where(at_n[0:1], 0.0, a[k : k + 1]))
        lower = jnp.where(at_n[0:1], 1.0, jnp.where(at_k[0:1], 0.0, a[k + 1 : k + 2]))
        first = (t * upper - q * lower) * inverse
        second = (p * lower - r * upper) * inverse
        rest = jnp.where(at_k | at_n, 0.0, a) - left * first - right * second
        a = jnp.where(row == k, first, jnp.where(row == k + 1, second, rest))
    return a


def block_inverse(matrix, low, high, size=16):
    lane = lanes((size, 128))
    row = lax.broadcasted_iota(jnp.int32, (size, 128), 0)
    compact = jnp.where(lane % size == row, 1.0, 0.0)
    for n in range(low // size, high // size):
        compact = jnp.where(lane // size == n, matrix[size * n : size * n + size], compact)
    compact = batched_inverse(compact, lane, row, size)
    parts = []
    for n in range(128 // size):
        active = low <= size * n < high
        parts.append(jnp.where(lane // size == n, compact, 0.0) if active else jnp.zeros((size, 128), F32))
    return jnp.concatenate(parts, axis=0)


def coarse_kernel(in_ref, out_ref, g, e, ei, first, second, near):
    pr, pc = lax.axis_index(ROW), lax.axis_index(COL)
    sub8 = lax.broadcasted_iota(jnp.int32, (8, 128), 0)

    lane8 = lanes((8, 128))
    for p in range(16):
        even, odd = jnp.zeros((8, 128), F32), jnp.zeros((8, 128), F32)
        for dr in range(3):
            r = p + 1 - dr
            if not 0 <= r < 16:
                continue
            at = [in_ref[pl.ds(32 * r + dq, 8, stride=4), :] for dq in range(4)]
            pair = (
                at[1] + jnp.where(sub8 >= 1, roll(at[3], 1, 0), 0.0),
                at[2] + jnp.where(sub8 < 7, roll(at[0], 7, 0), 0.0),
            )
            hit = lane8 < (30 if dr == 2 else 45)
            even, odd = (
                old + jnp.where(hit, roll(new, (128 - 45 * dr) % 128) if dr else new, 0.0)
                for old, new in zip((even, odd), pair)
            )
        g[pl.ds(16 * p, 8, stride=2), :] = even
        g[pl.ds(16 * p + 1, 8, stride=2), :] = odd
    tally = [
        roll(jnp.sum(in_ref[pl.ds(n, 128, stride=4), :], axis=0, keepdims=True), 8 + 8 * n) for n in range(2)
    ]
    tally = jnp.where(lanes((1, 128)) < 8, tally[0], tally[1])
    tally = jnp.broadcast_to(tally, (128, 128)).T
    bb, bu, uu, uuu = (tally[4 * n : 4 * n + 4, 0:1] for n in range(4))
    by_lane = jnp.concatenate([g[0:128].T, g[128:256].T], axis=1)

    lane16, row16 = lanes((16, 128)), lax.broadcasted_iota(jnp.int32, (16, 128), 0)
    for p in range(16):
        own = g[16 * p : 16 * p + 16]
        terms = [(own, d, dp, dq) for d, dp, dq in ((0, 0, 0), (1, 0, 1))]
        terms.append((roll(own, 1, 0), 1, 0, -1))
        if p < 15:
            terms += [(own, d, 1, dq) for d, dq in ((3, -1), (4, 0), (5, 1))]
        if p > 0:
            last = g[16 * p - 16 : 16 * p]
            terms += [(roll(last, 15, 0), 3, -1, 1), (last, 4, -1, 0), (roll(last, 1, 0), 5, -1, -1)]
        halves = [jnp.zeros((16, 128), F32), jnp.zeros((16, 128), F32)]
        for x, d, dp, dq in terms:
            target = POS[p + dp] * 16
            h, off = target // 128, target % 128
            q = row16 + dq
            hit = (lane16 == off + q) & (q >= 0) & (q < 16)
            at = 26 + d if d < 2 else 36 + d
            value = jnp.broadcast_to(x[:, at : at + 1], (16, 128))
            halves[h] = jnp.where(hit, value, halves[h])
        at = POS[p] * 16
        e[at : at + 16, 0:128] = halves[0]
        e[at : at + 16, 128:256] = halves[1]

    lane = lanes((128, 128))
    row = lax.broadcasted_iota(jnp.int32, (128, 128), 0)
    outer = block_inverse(e[0:128, 0:128], 0, 128)
    across = dot(outer, e[0:128, 128:256])
    schur = e[128:256, 128:256] - dot(e[128:256, 0:128], across)
    steps = []
    for low, high in ((0, 64), (64, 96)):
        inv = block_inverse(schur, low, high)
        link = jnp.where((row >= low) & (row < high) & (lane >= high), schur, 0.0)
        x = dot(inv, link)
        keep = jnp.where((row >= high) & (lane >= high), schur, 0.0)
        schur = keep - dot(link, x, TN)
        steps.append((inv, jnp.where((row == lane) & (row >= high), 1.0, 0.0) - x))
    inner = block_inverse(schur, 96, 128, 32)
    for inv, y in reversed(steps):
        inner = inv + dot(dot(y, inner), y, NT)
    half = dot(across, inner)
    near_diag = outer + dot(half, across, NT)

    def ordered(top_half, bottom_half):
        blocks = [top_half[16 * n : 16 * n + 16] for n in range(8)]
        blocks += [bottom_half[16 * n : 16 * n + 16] for n in range(8)]
        blocks = [blocks[POS[p]] for p in range(16)]
        return jnp.concatenate(blocks[:8], axis=0), jnp.concatenate(blocks[8:], axis=0)

    left_top, left_bottom = ordered(near_diag, -half.T)
    right_top, right_bottom = ordered(-half, inner)
    top_left, bottom_left = ordered(left_top.T, right_top.T)
    top_right, bottom_right = ordered(left_bottom.T, right_bottom.T)
    inverse = jnp.concatenate(
        [jnp.concatenate([top_left, bottom_left], axis=0), jnp.concatenate([top_right, bottom_right], axis=0)],
        axis=1,
    )
    for n, part in enumerate(parts_of(inverse, 3)):
        ei[n] = part

    def solve(z):
        rows = [part.astype(F32) for part in parts_of(z, 3)]
        rows = jnp.concatenate(rows + [jnp.zeros_like(z)], axis=0).astype(jnp.bfloat16)
        a, b, c = (fast_dot(rows, ei[n]) for n in range(3))
        return a[0:4] + (a[4:8] + b[0:4]) + (a[8:12] + b[4:8] + c[0:4])

    def apply(n, v):
        c = {d: by_lane[at : at + 1] for d, at in enumerate((20 + 2 * n, 21 + 2 * n, 0, 30 + 3 * n, 31 + 3 * n, 32 + 3 * n))}
        total = c[0] * v
        for d, step in ((1, 1), (3, 15), (4, 16), (5, 17)):
            total = total + c[d] * roll(v, 256 - step) + roll(c[d] * v, step)
        return total

    def inner_product(a, b):
        return jnp.sum(a * b, axis=1, keepdims=True)

    wb, wu, wuu, zb, tuu = (by_lane[4 * n : 4 * n + 4] for n in range(5))
    c0 = solve(zb)
    f_c, g_c, h_c, k_c = apply(0, c0), apply(1, c0), apply(2, c0), apply(4, c0)
    grad0 = wb - f_c
    k0 = solve(grad0)
    f_k, g_k = apply(0, k0), apply(1, k0)
    rho0 = bb - 2.0 * inner_product(c0, wb) + inner_product(c0, f_c)
    energy0 = bu - 2.0 * inner_product(c0, wu) + inner_product(c0, g_c)
    curve0 = energy0 - inner_product(k0, grad0)
    a0 = rho0 / curve0
    e1 = c0 - a0 * k0
    f_e = f_c - a0 * f_k
    g_e = g_c - a0 * g_k
    grad1 = wb - f_e + a0 * (g_c - wu)
    k1 = solve(grad1)

    def second_norm(m0, m1, m2, v0, v1, v2, e_image, c_image, last):
        own = m0 - 2.0 * inner_product(e1, v0) + inner_product(e1, e_image)
        mixed = m1 - inner_product(c0, v1) - inner_product(e1, v1) + inner_product(e1, c_image)
        far = m2 - 2.0 * inner_product(c0, v2) + inner_product(c0, last)
        return own - 2.0 * a0 * mixed + a0 * a0 * far

    rho1 = second_norm(bb, bu, uu, wb, wu, wuu, f_e, g_c, h_c)
    energy1 = second_norm(bu, uu, uuu, wu, wuu, tuu, g_e, h_c, k_c)
    beta = rho1 / rho0
    cross = (
        bu
        - inner_product(c0, wu)
        - inner_product(e1, wu)
        + inner_product(e1, g_c)
        - a0 * (uu - 2.0 * inner_product(c0, wuu) + inner_product(c0, h_c))
        - inner_product(k0, grad1)
    )
    curve1 = energy1 - inner_product(k1, grad1) + 2.0 * beta * cross + beta * beta * curve0
    a1 = rho1 / curve1

    mine = lax.broadcasted_iota(jnp.int32, (32, 256), 0) // 4 == pc

    def zone(value):
        value = jnp.broadcast_to(value, (4, 256))
        return jnp.where(mine, jnp.concatenate([value] * 8, axis=0), 0.0)

    ab = a1 * beta
    stacks = (
        (
            zone(a1 * k1 + ab * k0 - e1),
            zone(-(a0 + ab) * c0 - a1 * e1),
            zone((a0 + ab) * c0 + a1 * e1),
            zone((a1 * a0) * c0),
        ),
        (
            zone(-(a1 * a0) * c0),
            zone(c0 - (a0 + ab) * k0 - a1 * k1),
            zone(-a0 - a1 - ab),
            zone(a1 * a0),
        ),
    )
    out_ref[...] = jnp.zeros((256, 128), F32)
    for n, (ref, stack) in enumerate(((first, stacks[0]), (second, stacks[1]))):
        stack = jnp.concatenate(stack, axis=0)
        ref[0:8] = jnp.zeros((8, 128), F32)
        ref[8:136] = stack[:, 0:128].T
        ref[136:264] = stack[:, 128:256].T
        ref[264:272] = jnp.zeros((8, 128), F32)
        for dr in range(3):
            p = jnp.clip(pr - 1 + dr, 0, 15)
            near[...] = ref[pl.ds(pl.multiple_of(16 * p, 16), 32), :]
            for dq in range(4):
                out_ref[pl.ds(16 * n + 4 * dr + dq, 8, stride=32), :] = near[pl.ds(7 + dq, 8, stride=2), :]


def outputs_kernel(
    rows_ref, first_ref, second_ref, w_ref, grid_ref, coef_ref, m_ref, sol_ref, res_ref,
    left_ref, step_ref, window_ref,
):
    block = pl.program_id(0)

    @pl.when(block == 0)
    def _():
        pr, pc = lax.axis_index(ROW), lax.axis_index(COL)
        slot = lax.broadcasted_iota(jnp.int32, (16, 128), 0)
        region_row = pr - 1 + slot // 4
        region_col = 2 * pc - 1 + slot % 4
        inside = (slot < 12) & (region_row >= 0) & (region_row < REG) & (region_col >= 0) & (region_col < REG)
        window_ref[...] = jnp.where(inside, region_row * REG + region_col, -1).astype(F32)
        total = m_ref[0:32]
        for n in range(1, 8):
            total = total + m_ref[32 * n : 32 * n + 32]
        top, bottom = total[0:16], total[16:32]
        lane = lanes((16, 128))
        steps = jnp.where(slot == 0, roll(bottom[5:6], 64), jnp.where(slot == 1, roll(bottom[5:6], 32), 0.0))
        m = jnp.concatenate(
            [
                jnp.where((lane >= 64) & (lane < 96), roll(bottom, 32), 0.0),
                jnp.where(lane < 64, top, 0.0),
                jnp.where(lane < 64, roll(top, 64), 0.0),
                jnp.where(lane < 32, bottom, 0.0),
                steps,
                jnp.zeros((48, 128), F32),
            ],
            axis=0,
        ).T
        c1, c2, c3 = parts_of(m[0:96, 0:64], 3)
        left_ref[...] = jnp.concatenate([c1, c1, c2, c2, c1, c3], axis=1)
        for n in range(2):
            step_ref[n] = jnp.broadcast_to(m[0:32, 64 + n : 65 + n], (32, 128))

    left, window = left_ref[...], window_ref[...]
    for part in range(4):
        rows = []
        for n in range(8):
            r = 32 * block + 8 * part + n
            z = jnp.where(grid_ref[pl.ds(r, 1), :] == window, grid_ref[pl.ds(128 + r, 1), :], 0.0)
            rows.append(jnp.concatenate([z, w_ref[r], first_ref[r, 32:48], second_ref[r, 32:48]], axis=0))
        r1, r2, r3 = parts_of(jnp.concatenate(rows, axis=1), 3)
        d = fast_dot(left, jnp.concatenate([r1, r2, r1, r2, r3, r1], axis=0))
        for n in range(8):
            r = 32 * block + 8 * part + n
            b, u, uu = rows_ref[r], first_ref[r, 0:32], second_ref[r, 0:32]
            e = d[:, 128 * n : 128 * n + 128]
            inv = coef_ref[5, pl.ds(r + 16, 1), :]
            p1, p2 = step_ref[0], step_ref[1]
            res_ref[:, 8 * part + n] = b + p1 * u + p2 * uu + e[0:32]
            sol_ref[:, 8 * part + n] = inv * (e[32:64] - p1 * b - p2 * u) + e[64:96]


def swapped(value, axis, start):
    pairs = [(i, i + 1) for i in range(start, lax.axis_size(axis) - 1, 2)]
    return lax.ppermute(value, axis, pairs + [(b, a) for a, b in pairs])


def shape_of(*dims):
    return jax.ShapeDtypeStruct(dims, F32)


def kept(*dims):
    return pltpu.VMEM(dims, F32)


def vmem(*dims):
    return pltpu.VMEM(dims, F32)


def body(load_currents, labels, bump_height, horizontal_class, vertical_class, pad_class, edge_table, pad_table):
    rows, cols = lax.axis_size(ROW), lax.axis_size(COL)
    loads = load_currents.reshape(-1, 128)
    grid, far_rows, near_rows = pl.pallas_call(
        prepare_kernel,
        out_shape=(kept(1024, 128), shape_of(HALO, SUB, 128), shape_of(HALO, SUB, 128)),
        compiler_params=limited,
        in_specs=[outside] * 8,
        out_specs=(whole,) * 3,
        scratch_shapes=[pltpu.SMEM((8,), F32), pltpu.SMEM((8,), F32), vmem(32, 8, 128), vmem(32, 8, 128)]
        + [pltpu.VMEM((128, 128), jnp.int32)] * 4
        + [pltpu.SemaphoreType.DMA((9,))],
    )(
        *(
            pltpu.with_memory_space_constraint(x, pltpu.HBM)
            for x in (
                edge_table, pad_table, load_currents, labels, bump_height,
                horizontal_class, vertical_class, pad_class,
            )
        ),
    )
    far_rows = swapped(far_rows, ROW, 1)
    near_rows = swapped(near_rows, ROW, 0)
    by_rows, own = pl.pallas_call(
        pack_kernel,
        out_shape=(kept(128, 32, 128), kept(GROUPS, SUB, 128)),
        compiler_params=limited,
        in_specs=[whole] * 2,
        out_specs=(whole,) * 2,
    )(loads, grid)
    own, top, bottom, far_columns, near_columns = pl.pallas_call(
        corner_kernel,
        out_shape=(kept(GROUPS, SUB, 128), kept(HALO, SUB, 128), kept(HALO, SUB, 128))
        + (shape_of(5, SUB, 128),) * 2,
        compiler_params=limited,
        in_specs=[whole] * 3,
        out_specs=(whole,) * 5,
    )(own, far_rows, near_rows)
    far_columns = swapped(far_columns, COL, 1)
    near_columns = swapped(near_columns, COL, 0)
    first, second, w, coef, payload = pl.pallas_call(
        fields_kernel,
        out_shape=(
            kept(128, 48, 128),
            kept(128, 48, 128),
            kept(128, 16, 128),
            kept(6, 160, 128),
            shape_of(512, 128),
        ),
        compiler_params=limited,
        in_specs=[whole] * 7,
        out_specs=(whole,) * 5,
        scratch_shapes=[
            vmem(5, 160, 128),
            vmem(GROUPS + 2, SUB, 128),
            vmem(GROUPS + 2, SUB, 128),
            vmem(GROUPS + 2, 16, 128),
            vmem(GROUPS + 2, 16, 128),
            vmem(GROUPS + 2, 48, 128),
            vmem(GROUPS + 2, 48, 128),
            vmem(2 * GROUPS, 16, 128),
            vmem(2 * GROUPS, 48, 128),
            vmem(2 * GROUPS, 48, 128),
            vmem(144, 48, 128),
            vmem(144, 48, 128),
            vmem(2, GROUPS, 8, 128),
            vmem(144, 48, 128),
            vmem(144, 48, 128),
            vmem(96, 256),
        ],
    )(by_rows, grid, top, bottom, own, far_columns, near_columns)
    sent = payload.reshape(-1, 4, 128)
    everything = lax.all_to_all(sent, ROW + COL, 0, 0, tiled=True).reshape(-1, 128)
    found = pl.pallas_call(
        coarse_kernel,
        out_shape=shape_of(256, 128),
        compiler_params=limited,
        in_specs=[whole],
        out_specs=whole,
        scratch_shapes=[
            vmem(256, 128),
            vmem(256, 256),
            pltpu.VMEM((3, 256, 256), jnp.bfloat16),
            vmem(272, 128),
            vmem(272, 128),
            vmem(32, 128),
        ],
    )(everything)
    matrix = lax.all_to_all(found.reshape(cols, 32, 128), COL, 0, 0, tiled=True).reshape(-1, 128)
    by_block = pl.BlockSpec((32, 32, 128), lambda k: (0, k, 0))
    return pl.pallas_call(
        outputs_kernel,
        grid=(4,),
        out_shape=(shape_of(32, 128, 128), shape_of(32, 128, 128)),
        compiler_params=limited,
        in_specs=[whole] * 7,
        out_specs=(by_block, by_block),
        scratch_shapes=[pltpu.VMEM((96, 384), jnp.bfloat16), vmem(2, 32, 128), vmem(16, 128)],
    )(by_rows, first, second, w, grid, coef, matrix)


def solution(mesh):
    finer = Mesh(mesh.devices.reshape(4, 4, 4, 2), ("row_0", "row_1", "col_0", "col_1"))
    grid = P(ROW, COL)
    return jax.shard_map(
        body,
        mesh=finer,
        in_specs=(P(None, ROW, COL), grid, grid, grid, grid, grid, P(), P()),
        out_specs=(P(None, ROW, COL), P(None, ROW, COL)),
        check_vma=False,
    )
```

```python
import jax
import jax.numpy as jnp
from jax import lax
from jax.experimental import pallas as pl
from jax.experimental.pallas import tpu as pltpu
from jax.sharding import Mesh
from jax.sharding import PartitionSpec as P

REG = 16
ROW = ("row_0", "row_1")
COL = ("col_0", "col_1")
F32 = jnp.float32

LAB, BUMP, RIGHT, DOWN, PAD = 32, 33, 34, 35, 36
SUB = 40
HALO = 3
GROUPS = 9
ORDER = (1, 3, 5, 7, 9, 11, 13, 15, 2, 6, 10, 14, 4, 12, 8, 0)
POS = tuple(ORDER.index(p) for p in range(16))
NT = (((1,), (1,)), ((), ()))
NN = (((1,), (0,)), ((), ()))
TN = (((0,), (0,)), ((), ()))
whole = pl.BlockSpec(memory_space=pltpu.VMEM)
outside = pl.BlockSpec(memory_space=pltpu.HBM)
limited = pltpu.CompilerParams(vmem_limit_bytes=32 * 2**20)


def parts_of(x, count):
    parts = []
    for n in range(count):
        parts.append(x.astype(jnp.bfloat16))
        if n + 1 < count:
            x = x - parts[-1].astype(F32)
    return parts


def fast_dot(a, b, dims=NN):
    return lax.dot_general(a, b, dims, preferred_element_type=F32)


def dot(a, b, dims=NN):
    (at_a,), (at_b,) = dims[0]
    a1, a2, a3 = parts_of(a, 3)
    b1, b2, b3 = parts_of(b, 3)
    return fast_dot(
        jnp.concatenate([a3, a1, a2, a2, a1, a1], axis=at_a),
        jnp.concatenate([b1, b3, b2, b1, b2, b1], axis=at_b),
        dims,
    )


def lanes(shape):
    return lax.broadcasted_iota(jnp.int32, shape, len(shape) - 1)


def roll(x, shift, axis=1):
    return pltpu.roll(x, shift, axis)


def prepare_kernel(
    edge_hbm, pad_hbm, load_hbm, label_hbm, bump_hbm, across_hbm, down_hbm, pad_class_hbm,
    grid_ref, far_ref, near_ref, edge_ref, pad_ref, load_ref, load_end_ref, label_ref, across_ref, down_ref, pad_class_ref, done,
):
    copies = [
        pltpu.make_async_copy(source, target, done.at[n])
        for n, (source, target) in enumerate(
            (
                (edge_hbm, edge_ref),
                (pad_hbm, pad_ref),
                (across_hbm, across_ref),
                (down_hbm, down_ref),
                (pad_class_hbm, pad_class_ref),
                (label_hbm, label_ref),
                (bump_hbm, grid_ref.at[pl.ds(128, 128)]),
                (load_hbm.at[:, pl.ds(0, 8)], load_ref),
                (load_hbm.at[:, pl.ds(120, 8)], load_end_ref),
            )
        )
    ]
    for copy in copies:
        copy.start()
    for copy in copies:
        copy.wait()
    pr, pc = lax.axis_index(ROW), lax.axis_index(COL)
    shape = (128, 128)
    row, lane = lax.broadcasted_iota(jnp.int32, shape, 0), lanes(shape)

    def lookup(table, classes):
        found = jnp.zeros(shape, F32)
        for n in range(8):
            found = jnp.where(classes == n, table[n], found)
        return found

    right = lookup(edge_ref, across_ref[...])
    down = lookup(edge_ref, down_ref[...])
    grid_ref[0:128] = label_ref[...].astype(F32)
    grid_ref[256:384] = jnp.where((lane == 127) & (pc == 7), 0.0, right)
    grid_ref[384:512] = jnp.where((row == 127) & (pr == 15), 0.0, down)
    grid_ref[512:640] = lookup(pad_ref, pad_class_ref[...])
    grid_ref[640:1024] = jnp.zeros((384, 128), F32)
    for n in range(HALO):
        even = pr % 2 == 0
        first, last = load_ref[:, n], load_end_ref[:, 8 - HALO + n]
        far_ref[n, 0:32] = jnp.where(even, first, last)
        near_ref[n, 0:32] = jnp.where(even, last, first)
        first = grid_ref[pl.ds(n, 8, stride=128), :]
        last = grid_ref[pl.ds(128 - HALO + n, 8, stride=128), :]
        far_ref[n, 32:40] = jnp.where(even, first, last)
        near_ref[n, 32:40] = jnp.where(even, last, first)


def pack_kernel(load_ref, grid_ref, rows_ref, own_ref):
    lane = lanes((32, 128)) // 8

    def group(g, slots):
        loads, rest = jnp.zeros((32, 128), F32), jnp.zeros((8, 128), F32)
        for s in slots:
            r = 16 * g - 8 + s
            b = load_ref[pl.ds(r, 32, stride=128), :]
            rows_ref[r] = b
            loads = jnp.where(lane == s, roll(b, (8 * s + 3) % 128), loads)
            rest = jnp.where(lane[0:8] == s, roll(grid_ref[pl.ds(r, 8, stride=128), :], (8 * s + 3) % 128), rest)
        own_ref[g, 0:32] = loads
        own_ref[g, 32:40] = rest

    group(0, range(8, 16))
    group(8, range(8))

    def step(g, _):
        group(g, range(16))
        return 0

    lax.fori_loop(1, 8, step, 0)


def corner_kernel(
    own_ref, far_ref, near_ref, out_ref, top_ref, bottom_ref, far_out_ref, near_out_ref
):
    lane = lanes((SUB, 128)) // 8
    even = lax.axis_index(ROW) % 2 == 0
    top_ref[...] = jnp.where(even, far_ref[...], near_ref[...])
    bottom_ref[...] = jnp.where(even, near_ref[...], far_ref[...])
    for g in range(GROUPS):
        out_ref[g] = own_ref[g]
    start, end = own_ref[0], own_ref[8]
    for n in range(HALO):
        s = 8 - HALO + n
        start = jnp.where(lane == s, roll(top_ref[n], (8 * s + 3) % 128), start)
        s = 8 + n
        end = jnp.where(lane == s, roll(bottom_ref[n], (8 * s + 3) % 128), end)
    out_ref[0] = start
    out_ref[8] = end
    low = lanes((SUB, 128)) % 8 < 4
    to_right_first = lax.axis_index(COL) % 2 == 1
    for h in range(5):
        here = out_ref[2 * h]
        after = out_ref[2 * h + 1] if h < 4 else here
        right = jnp.where(low, here, roll(after, 4))
        left = jnp.where(low, roll(here, 125), roll(after, 1))
        far_out_ref[h] = jnp.where(to_right_first, right, left)
        near_out_ref[h] = jnp.where(to_right_first, left, right)


def fields_kernel(
    rows_ref, grid_ref, top_ref, bottom_ref, own_ref, far_ref, near_ref,
    first_ref, second_ref, w_ref, coef_ref, out_ref,
    ext, so, ss, sz_o, sz_s, y0_o, y0_s, qz, q0, q1, u0, u1, sc, y0, y1, gram,
):
    pr, pc = lax.axis_index(ROW), lax.axis_index(COL)
    lane1 = lanes((1, 128))
    lane16 = lanes((16, 128))
    lane48 = lanes((48, 128))

    for n in range(5):
        ext[n, 0:16] = jnp.zeros((16, 128), F32)
        ext[n, 16:144] = grid_ref[128 * n : 128 * n + 128]
        ext[n, 144:160] = jnp.zeros((16, 128), F32)
        for k in range(HALO):
            ext[n, 16 - HALO + k : 17 - HALO + k] = top_ref[k, 32 + n : 33 + n]
            ext[n, 144 + k : 145 + k] = bottom_ref[k, 32 + n : 33 + n]

    slot = lax.broadcasted_iota(jnp.int32, (16, 128), 0)
    region_row = pr - 1 + slot // 4
    region_col = 2 * pc - 1 + slot % 4
    inside = (slot < 12) & (region_row >= 0) & (region_row < REG) & (region_col >= 0) & (region_col < REG)
    window = jnp.where(inside, region_row * REG + region_col, -1).astype(F32)

    for ref in (so, ss, sz_o, sz_s, y0_o, y0_s):
        ref[0] = jnp.zeros(ref.shape[1:], F32)
        ref[GROUPS + 1] = jnp.zeros(ref.shape[1:], F32)

    def pair_left(o, s, lane):
        j = lane % 8
        return roll(jnp.where(j == 2, s, o), 1), roll(jnp.where(j == 2, o, s), 1)

    def pair_right(o, s, lane):
        j = lane % 8
        return roll(jnp.where(j == 3, s, o), 127), roll(jnp.where(j == 3, o, s), 127)

    def above(before, here, lane):
        return roll(jnp.where(lane >= 120, before, here), 8)

    def below(here, after, lane):
        return roll(jnp.where(lane < 8, after, here), 120)

    even = pc % 2 == 0

    def strips(g, _):
        o_row = own_ref[g]
        far, near = far_ref[g // 2], near_ref[g // 2]
        on_left, on_right = jnp.where(even, far, near), jnp.where(even, near, far)
        turn = 124 * (g % 2)
        s_row = jnp.where(lanes((SUB, 128)) % 8 < 3, roll(on_left, turn), roll(on_right, 3 + turn))
        so[g + 1], ss[g + 1] = o_row, s_row
        lefts = pair_left(o_row[RIGHT : RIGHT + 1], s_row[RIGHT : RIGHT + 1], lane1)
        for side, (row, ref, ll) in enumerate(((o_row, so, lefts[0]), (s_row, ss, lefts[1]))):
            rl, dl = row[RIGHT : RIGHT + 1], row[DOWN : DOWN + 1]
            ul = above(ref[g, DOWN : DOWN + 1], dl, lane1)
            diag = row[PAD : PAD + 1] + rl + ll + dl + ul
            inv = jnp.where(diag > 0, 1.0 / diag, 0.0)
            for n, value in enumerate((diag, rl, ll, dl, ul, inv)):
                sc[side, g, n : n + 1] = value
            z = jnp.where(row[LAB : LAB + 1] == window, row[BUMP : BUMP + 1], 0.0)
            (sz_s if side else sz_o)[g + 1] = z
            if side:
                qz[2 * g] = z
                qz[2 * g + 1] = roll(z, 64)

        at = pl.multiple_of(16 * g + 8, 8)
        beside = jnp.zeros((16, 128), F32)
        for s in range(16):
            beside = jnp.where(slot == s, roll(s_row[RIGHT : RIGHT + 1], 125 - 8 * s), beside)
        rl, dl = ext[2, pl.ds(at, 16)], ext[3, pl.ds(at, 16)]
        ll = roll(jnp.where(lane16 == 127, beside, rl), 1)
        last = ext[3, pl.ds(pl.multiple_of(at - 8, 8), 8)]
        ul = jnp.where(slot == 0, last[7:8], roll(dl, 1, 0))
        diag = ext[4, pl.ds(at, 16)] + rl + ll + dl + ul
        inv = jnp.where(diag > 0, 1.0 / diag, 0.0)
        for n, value in enumerate((diag, rl, ll, dl, ul, inv)):
            coef_ref[n, pl.ds(at, 16)] = value
        return 0

    lax.fori_loop(0, GROUPS, strips, 0, unroll=3)

    def strip_image(ref_o, ref_s, g, lane, sides):
        o, s = ref_o[g + 1], ref_s[g + 1]
        lefts, rights = pair_left(o, s, lane), pair_right(o, s, lane)
        done = []
        for side in sides:
            ref, here = (ref_s, s) if side else (ref_o, o)
            up = above(ref[g], here, lane)
            down = below(here, ref[g + 2], lane)
            c = [sc[side, g, n : n + 1] for n in range(5)]
            done.append(c[0] * here - c[1] * rights[side] - c[2] * lefts[side] - c[3] * down - c[4] * up)
        return done

    def strip_first(g, _):
        w = strip_image(sz_o, sz_s, g, lane16, (0, 1))
        for side, (source, ref) in enumerate(((so, y0_o), (ss, y0_s))):
            inv = sc[side, g, 5:6]
            ref[g + 1, 0:32] = inv * source[g + 1, 0:32]
            ref[g + 1, 32:48] = inv * w[side]
        y = y0_s[g + 1]
        q0[2 * g] = y
        q0[2 * g + 1] = roll(y, 64)
        return 0

    lax.fori_loop(0, GROUPS, strip_first, 0, unroll=9)

    def strip_second(g, _):
        (u,) = strip_image(y0_o, y0_s, g, lane48, (1,))
        y = sc[1, g, 5:6] * u
        q1[2 * g] = y
        q1[2 * g + 1] = roll(y, 64)
        return 0

    lax.fori_loop(0, GROUPS, strip_second, 0, unroll=9)

    def owned(g):
        return not isinstance(g, int)

    def coef(n, g, s):
        return coef_ref[n, pl.ds(8 * g + 8 + s, 1), :]

    def unpacked(strip, g, s):
        return roll(strip[g], 125 - 8 * s)

    def image(here, up, down, other, g, s, lane):
        left = roll(jnp.where(lane == 127, other, here), 1)
        right = roll(jnp.where(lane == 0, other, here), 127)
        return (
            coef(0, g, s) * here
            - coef(1, g, s) * right
            - coef(2, g, s) * left
            - coef(3, g, s) * down
            - coef(4, g, s) * up
        )

    def basis(j):
        return jnp.where(ext[0, pl.ds(j, 1), :] == window, ext[1, pl.ds(j, 1), :], 0.0)

    def first_image(g, s):
        r, j = 8 * g - 8 + s, 8 * g + 8 + s
        w = image(basis(j), basis(j - 1), basis(j + 1), unpacked(qz, g, s), g, s, lane16)
        if owned(g):
            b = rows_ref[r]
            w_ref[r] = w
        else:
            b = top_ref[r + HALO, 0:32] if r < 0 else bottom_ref[r - 128, 0:32]
        inv = coef(5, g, s)
        y0[8 * g + s, 0:32] = inv * b
        y0[8 * g + s, 32:48] = inv * w
        u0[8 * g + s] = unpacked(q0, g, s)

    def second_image(g, s):
        i = 8 * g + s
        f1 = image(y0[i], y0[i - 1], y0[i + 1], u0[i], g, s, lane48)
        if owned(g):
            first_ref[8 * g - 8 + s] = f1
            u1[i] = unpacked(q1, g, s)
        y1[i] = coef(5, g, s) * f1

    def only(work):
        def step(g, _):
            for s in range(8):
                work(g, s)
            return 0

        return step

    for s in (6, 7):
        first_image(0, s)
    lax.fori_loop(1, 17, only(first_image), 0)
    for s in (0, 1):
        first_image(17, s)
    second_image(0, 7)

    def second_pair(t, _):
        for s in range(16):
            second_image(2 * t + 1 + s // 8, s % 8)
        return 0

    lax.fori_loop(0, 8, second_pair, 0)
    second_image(17, 0)

    gram[...] = jnp.zeros((96, 256), F32)

    def third_image(g, s):
        i = 8 * g + s
        second_ref[i - 8] = image(y1[i], y1[i - 1], y1[i + 1], u1[i], g, s, lane48)

    def products(g, sums):
        left, every = [], []
        sums = list(sums)
        for s in range(16):
            i = 16 * g + 8 + s
            r = i - 8
            b, f1, f2, y0r, y1r = rows_ref[r], first_ref[r], second_ref[r], y0[i], y1[i]
            left.append(jnp.concatenate([basis(i + 8), y0r[32:48], y1r[32:48]], axis=0))
            every.append(jnp.concatenate([b, w_ref[r], f1, f2], axis=0))
            pairs = ((y0r, b), (y0r, f1), (y1r, f1), (y1r, f2))
            sums = [t + p[0:32] * q[0:32] for t, (p, q) in zip(sums, pairs)]
        left = jnp.concatenate(parts_of(jnp.concatenate(left, axis=1), 2), axis=0)
        high, low = parts_of(jnp.concatenate(every, axis=1), 2)
        gram[:, 0:144] += fast_dot(left, high, NT) + fast_dot(left, low, NT)
        return tuple(sums)

    def third_pair(t, _):
        for s in range(16):
            third_image(2 * t + 1 + s // 8, s % 8)
        return 0

    def last_stage(t, sums):
        sums = products(t - 1, sums)
        third_pair(t, 0)
        return sums

    zero = jnp.zeros((32, 128), F32)
    lax.fori_loop(0, 1, third_pair, 0)
    sums = lax.fori_loop(1, 8, last_stage, (zero, zero, zero, zero))
    sums = lax.fori_loop(7, 8, products, sums)

    a0, a1 = gram[0:48, 0:128] + gram[48:96, 0:128], gram[0:48, 128:256] + gram[48:96, 128:256]
    zr, w0, t0, w1, t1 = a0[0:16], a0[16:32], a0[32:48], a1[16:32], a1[32:48]
    matrices = jnp.zeros((16, 128), F32)
    for n, (x, z) in enumerate(((w0, 32), (w0, 80), (w1, 0), (zr, 32), (t1, 0))):
        start = 24 * n
        matrices = jnp.where((lane16 >= start) & (lane16 < start + 16), roll(x, (start - z) % 128), matrices)
    moved = jnp.zeros((16, 128), F32)
    for k in range(12):
        moved = jnp.where(slot == k, roll(matrices, (128 - k) % 128), moved)
    common = jnp.zeros((16, 128), F32)
    for n in range(5):
        for start, offset, count in ((20 + 2 * n, 0, 2), (30 + 3 * n, 3, 3)):
            hit = (lane16 >= start) & (lane16 < start + count)
            common = jnp.where(hit, roll(moved, (start - offset - 24 * n) % 128), common)
    lines = []
    diagonal = lanes((32, 128)) == lax.broadcasted_iota(jnp.int32, (32, 128), 0)
    for total in sums:
        column = jnp.sum(total, axis=1, keepdims=True)
        lines.append(jnp.sum(jnp.where(diagonal, column, 0.0), axis=0, keepdims=True))
    row4, lane4 = lax.broadcasted_iota(jnp.int32, (4, 128), 0), lanes((4, 128))
    for d in range(8):
        message = common
        for n, (x, z) in enumerate(((w0, 0), (w0, 48), (w0, 96), (zr, 0), (t0, 96))):
            hit = (lane16 >= 4 * n) & (lane16 < 4 * n + 4)
            message = jnp.where(hit, roll(x, (4 * n - z - 4 * d) % 128), message)
        middle, last = roll(message, 45), roll(message, 90)
        sent = jnp.where(lane4 < 45, message[0:4], jnp.where(lane4 < 90, middle[4:8], last[8:12]))
        line = jnp.zeros((1, 128), F32)
        for n in range(4):
            start = 120 + 4 * n if n < 2 else 112 + 4 * n
            line = jnp.where((lane1 >= start) & (lane1 < start + 4), roll(lines[n], (start - 4 * d) % 128), line)
            if n == 1:
                first_two, line = line, jnp.zeros((1, 128), F32)
        total = jnp.where(row4 == 0, first_two, jnp.where(row4 == 1, line, 0.0))
        sent = jnp.where(lane4 < 120, sent, total)
        if d % 2 == 0:
            before = sent
            continue
        pair = jnp.concatenate([before, sent], axis=0)
        for r in range(16):
            out_ref[32 * r + 4 * d - 4 : 32 * r + 4 * d + 4] = pair


def batched_inverse(a, lane, row, size):
    base = lane - lane % size
    for k in range(0, size, 2):
        at_k, at_n = lane % size == k, lane % size == k + 1
        left = jnp.take_along_axis(a, base + k, axis=1)
        right = jnp.take_along_axis(a, base + k + 1, axis=1)
        p, q, r, t = left[k : k + 1], right[k : k + 1], left[k + 1 : k + 2], right[k + 1 : k + 2]
        inverse = 1.0 / (p * t - q * r)
        upper = jnp.where(at_k[0:1], 1.0, jnp.where(at_n[0:1], 0.0, a[k : k + 1]))
        lower = jnp.where(at_n[0:1], 1.0, jnp.where(at_k[0:1], 0.0, a[k + 1 : k + 2]))
        first = (t * upper - q * lower) * inverse
        second = (p * lower - r * upper) * inverse
        rest = jnp.where(at_k | at_n, 0.0, a) - left * first - right * second
        a = jnp.where(row == k, first, jnp.where(row == k + 1, second, rest))
    return a


def block_inverse(matrix, low, high, size=16):
    lane = lanes((size, 128))
    row = lax.broadcasted_iota(jnp.int32, (size, 128), 0)
    compact = jnp.where(lane % size == row, 1.0, 0.0)
    for n in range(low // size, high // size):
        compact = jnp.where(lane // size == n, matrix[size * n : size * n + size], compact)
    compact = batched_inverse(compact, lane, row, size)
    parts = []
    for n in range(128 // size):
        active = low <= size * n < high
        parts.append(jnp.where(lane // size == n, compact, 0.0) if active else jnp.zeros((size, 128), F32))
    return jnp.concatenate(parts, axis=0)


def coarse_kernel(in_ref, out_ref, g, e, ei, first, second, near):
    pr, pc = lax.axis_index(ROW), lax.axis_index(COL)
    sub8 = lax.broadcasted_iota(jnp.int32, (8, 128), 0)

    lane8 = lanes((8, 128))
    for p in range(16):
        even, odd = jnp.zeros((8, 128), F32), jnp.zeros((8, 128), F32)
        for dr in range(3):
            r = p + 1 - dr
            if not 0 <= r < 16:
                continue
            at = [in_ref[pl.ds(32 * r + dq, 8, stride=4), :] for dq in range(4)]
            pair = (
                at[1] + jnp.where(sub8 >= 1, roll(at[3], 1, 0), 0.0),
                at[2] + jnp.where(sub8 < 7, roll(at[0], 7, 0), 0.0),
            )
            hit = lane8 < (30 if dr == 2 else 45)
            even, odd = (
                old + jnp.where(hit, roll(new, (128 - 45 * dr) % 128) if dr else new, 0.0)
                for old, new in zip((even, odd), pair)
            )
        g[pl.ds(16 * p, 8, stride=2), :] = even
        g[pl.ds(16 * p + 1, 8, stride=2), :] = odd
    tally = [
        roll(jnp.sum(in_ref[pl.ds(n, 128, stride=4), :], axis=0, keepdims=True), 8 + 8 * n) for n in range(2)
    ]
    tally = jnp.where(lanes((1, 128)) < 8, tally[0], tally[1])
    tally = jnp.broadcast_to(tally, (128, 128)).T
    bb, bu, uu, uuu = (tally[4 * n : 4 * n + 4, 0:1] for n in range(4))
    by_lane = jnp.concatenate([g[0:128].T, g[128:256].T], axis=1)

    lane16, row16 = lanes((16, 128)), lax.broadcasted_iota(jnp.int32, (16, 128), 0)
    for p in range(16):
        own = g[16 * p : 16 * p + 16]
        terms = [(own, d, dp, dq) for d, dp, dq in ((0, 0, 0), (1, 0, 1))]
        terms.append((roll(own, 1, 0), 1, 0, -1))
        if p < 15:
            terms += [(own, d, 1, dq) for d, dq in ((3, -1), (4, 0), (5, 1))]
        if p > 0:
            last = g[16 * p - 16 : 16 * p]
            terms += [(roll(last, 15, 0), 3, -1, 1), (last, 4, -1, 0), (roll(last, 1, 0), 5, -1, -1)]
        halves = [jnp.zeros((16, 128), F32), jnp.zeros((16, 128), F32)]
        for x, d, dp, dq in terms:
            target = POS[p + dp] * 16
            h, off = target // 128, target % 128
            q = row16 + dq
            hit = (lane16 == off + q) & (q >= 0) & (q < 16)
            at = 26 + d if d < 2 else 36 + d
            value = jnp.broadcast_to(x[:, at : at + 1], (16, 128))
            halves[h] = jnp.where(hit, value, halves[h])
        at = POS[p] * 16
        e[at : at + 16, 0:128] = halves[0]
        e[at : at + 16, 128:256] = halves[1]

    lane = lanes((128, 128))
    row = lax.broadcasted_iota(jnp.int32, (128, 128), 0)
    outer = block_inverse(e[0:128, 0:128], 0, 128)
    across = dot(outer, e[0:128, 128:256])
    schur = e[128:256, 128:256] - dot(e[128:256, 0:128], across)
    steps = []
    for low, high in ((0, 64), (64, 96)):
        inv = block_inverse(schur, low, high)
        link = jnp.where((row >= low) & (row < high) & (lane >= high), schur, 0.0)
        x = dot(inv, link)
        keep = jnp.where((row >= high) & (lane >= high), schur, 0.0)
        schur = keep - dot(link, x, TN)
        steps.append((inv, jnp.where((row == lane) & (row >= high), 1.0, 0.0) - x))
    inner = block_inverse(schur, 96, 128, 32)
    for inv, y in reversed(steps):
        inner = inv + dot(dot(y, inner), y, NT)
    half = dot(across, inner)
    near_diag = outer + dot(half, across, NT)

    def ordered(top_half, bottom_half):
        blocks = [top_half[16 * n : 16 * n + 16] for n in range(8)]
        blocks += [bottom_half[16 * n : 16 * n + 16] for n in range(8)]
        blocks = [blocks[POS[p]] for p in range(16)]
        return jnp.concatenate(blocks[:8], axis=0), jnp.concatenate(blocks[8:], axis=0)

    left_top, left_bottom = ordered(near_diag, -half.T)
    right_top, right_bottom = ordered(-half, inner)
    top_left, bottom_left = ordered(left_top.T, right_top.T)
    top_right, bottom_right = ordered(left_bottom.T, right_bottom.T)
    inverse = jnp.concatenate(
        [jnp.concatenate([top_left, bottom_left], axis=0), jnp.concatenate([top_right, bottom_right], axis=0)],
        axis=1,
    )
    for n, part in enumerate(parts_of(inverse, 3)):
        ei[n] = part

    def solve(z):
        rows = [part.astype(F32) for part in parts_of(z, 3)]
        rows = jnp.concatenate(rows + [jnp.zeros_like(z)], axis=0).astype(jnp.bfloat16)
        a, b, c = (fast_dot(rows, ei[n]) for n in range(3))
        return a[0:4] + (a[4:8] + b[0:4]) + (a[8:12] + b[4:8] + c[0:4])

    def apply(n, v):
        c = {d: by_lane[at : at + 1] for d, at in enumerate((20 + 2 * n, 21 + 2 * n, 0, 30 + 3 * n, 31 + 3 * n, 32 + 3 * n))}
        total = c[0] * v
        for d, step in ((1, 1), (3, 15), (4, 16), (5, 17)):
            total = total + c[d] * roll(v, 256 - step) + roll(c[d] * v, step)
        return total

    def inner_product(a, b):
        return jnp.sum(a * b, axis=1, keepdims=True)

    wb, wu, wuu, zb, tuu = (by_lane[4 * n : 4 * n + 4] for n in range(5))
    c0 = solve(zb)
    f_c, g_c, h_c, k_c = apply(0, c0), apply(1, c0), apply(2, c0), apply(4, c0)
    grad0 = wb - f_c
    k0 = solve(grad0)
    f_k, g_k = apply(0, k0), apply(1, k0)
    rho0 = bb - 2.0 * inner_product(c0, wb) + inner_product(c0, f_c)
    energy0 = bu - 2.0 * inner_product(c0, wu) + inner_product(c0, g_c)
    curve0 = energy0 - inner_product(k0, grad0)
    a0 = rho0 / curve0
    e1 = c0 - a0 * k0
    f_e = f_c - a0 * f_k
    g_e = g_c - a0 * g_k
    grad1 = wb - f_e + a0 * (g_c - wu)
    k1 = solve(grad1)

    def second_norm(m0, m1, m2, v0, v1, v2, e_image, c_image, last):
        own = m0 - 2.0 * inner_product(e1, v0) + inner_product(e1, e_image)
        mixed = m1 - inner_product(c0, v1) - inner_product(e1, v1) + inner_product(e1, c_image)
        far = m2 - 2.0 * inner_product(c0, v2) + inner_product(c0, last)
        return own - 2.0 * a0 * mixed + a0 * a0 * far

    rho1 = second_norm(bb, bu, uu, wb, wu, wuu, f_e, g_c, h_c)
    energy1 = second_norm(bu, uu, uuu, wu, wuu, tuu, g_e, h_c, k_c)
    beta = rho1 / rho0
    cross = (
        bu
        - inner_product(c0, wu)
        - inner_product(e1, wu)
        + inner_product(e1, g_c)
        - a0 * (uu - 2.0 * inner_product(c0, wuu) + inner_product(c0, h_c))
        - inner_product(k0, grad1)
    )
    curve1 = energy1 - inner_product(k1, grad1) + 2.0 * beta * cross + beta * beta * curve0
    a1 = rho1 / curve1

    mine = lax.broadcasted_iota(jnp.int32, (32, 256), 0) // 4 == pc

    def zone(value):
        value = jnp.broadcast_to(value, (4, 256))
        return jnp.where(mine, jnp.concatenate([value] * 8, axis=0), 0.0)

    ab = a1 * beta
    stacks = (
        (
            zone(a1 * k1 + ab * k0 - e1),
            zone(-(a0 + ab) * c0 - a1 * e1),
            zone((a0 + ab) * c0 + a1 * e1),
            zone((a1 * a0) * c0),
        ),
        (
            zone(-(a1 * a0) * c0),
            zone(c0 - (a0 + ab) * k0 - a1 * k1),
            zone(-a0 - a1 - ab),
            zone(a1 * a0),
        ),
    )
    out_ref[...] = jnp.zeros((256, 128), F32)
    for n, (ref, stack) in enumerate(((first, stacks[0]), (second, stacks[1]))):
        stack = jnp.concatenate(stack, axis=0)
        ref[0:8] = jnp.zeros((8, 128), F32)
        ref[8:136] = stack[:, 0:128].T
        ref[136:264] = stack[:, 128:256].T
        ref[264:272] = jnp.zeros((8, 128), F32)
        for dr in range(3):
            p = jnp.clip(pr - 1 + dr, 0, 15)
            near[...] = ref[pl.ds(pl.multiple_of(16 * p, 16), 32), :]
            for dq in range(4):
                out_ref[pl.ds(16 * n + 4 * dr + dq, 8, stride=32), :] = near[pl.ds(7 + dq, 8, stride=2), :]


def outputs_kernel(
    rows_ref, first_ref, second_ref, w_ref, grid_ref, coef_ref, m_ref, sol_ref, res_ref,
    left_ref, step_ref, window_ref,
):
    block = pl.program_id(0)

    @pl.when(block == 0)
    def _():
        pr, pc = lax.axis_index(ROW), lax.axis_index(COL)
        slot = lax.broadcasted_iota(jnp.int32, (16, 128), 0)
        region_row = pr - 1 + slot // 4
        region_col = 2 * pc - 1 + slot % 4
        inside = (slot < 12) & (region_row >= 0) & (region_row < REG) & (region_col >= 0) & (region_col < REG)
        window_ref[...] = jnp.where(inside, region_row * REG + region_col, -1).astype(F32)
        total = m_ref[0:32]
        for n in range(1, 8):
            total = total + m_ref[32 * n : 32 * n + 32]
        top, bottom = total[0:16], total[16:32]
        lane = lanes((16, 128))
        steps = jnp.where(slot == 0, roll(bottom[5:6], 64), jnp.where(slot == 1, roll(bottom[5:6], 32), 0.0))
        m = jnp.concatenate(
            [
                jnp.where((lane >= 64) & (lane < 96), roll(bottom, 32), 0.0),
                jnp.where(lane < 64, top, 0.0),
                jnp.where(lane < 64, roll(top, 64), 0.0),
                jnp.where(lane < 32, bottom, 0.0),
                steps,
                jnp.zeros((48, 128), F32),
            ],
            axis=0,
        ).T
        c1, c2, c3 = parts_of(m[0:96, 0:64], 3)
        left_ref[...] = jnp.concatenate([c1, c1, c2, c2, c1, c3], axis=1)
        for n in range(2):
            step_ref[n] = jnp.broadcast_to(m[0:32, 64 + n : 65 + n], (32, 128))

    left, window = left_ref[...], window_ref[...]
    for part in range(4):
        rows = []
        for n in range(8):
            r = 32 * block + 8 * part + n
            z = jnp.where(grid_ref[pl.ds(r, 1), :] == window, grid_ref[pl.ds(128 + r, 1), :], 0.0)
            rows.append(jnp.concatenate([z, w_ref[r], first_ref[r, 32:48], second_ref[r, 32:48]], axis=0))
        r1, r2, r3 = parts_of(jnp.concatenate(rows, axis=1), 3)
        d = fast_dot(left, jnp.concatenate([r1, r2, r1, r2, r3, r1], axis=0))
        for n in range(8):
            r = 32 * block + 8 * part + n
            b, u, uu = rows_ref[r], first_ref[r, 0:32], second_ref[r, 0:32]
            e = d[:, 128 * n : 128 * n + 128]
            inv = coef_ref[5, pl.ds(r + 16, 1), :]
            p1, p2 = step_ref[0], step_ref[1]
            res_ref[:, 8 * part + n] = b + p1 * u + p2 * uu + e[0:32]
            sol_ref[:, 8 * part + n] = inv * (e[32:64] - p1 * b - p2 * u) + e[64:96]


def swapped(value, axis, start):
    pairs = [(i, i + 1) for i in range(start, lax.axis_size(axis) - 1, 2)]
    return lax.ppermute(value, axis, pairs + [(b, a) for a, b in pairs])


def shape_of(*dims):
    return jax.ShapeDtypeStruct(dims, F32)


def kept(*dims):
    return pltpu.VMEM(dims, F32)


def vmem(*dims):
    return pltpu.VMEM(dims, F32)


def body(load_currents, labels, bump_height, horizontal_class, vertical_class, pad_class, edge_table, pad_table):
    rows, cols = lax.axis_size(ROW), lax.axis_size(COL)
    loads = load_currents.reshape(-1, 128)
    grid, far_rows, near_rows = pl.pallas_call(
        prepare_kernel,
        out_shape=(kept(1024, 128), shape_of(HALO, SUB, 128), shape_of(HALO, SUB, 128)),
        compiler_params=limited,
        in_specs=[outside] * 8,
        out_specs=(whole,) * 3,
        scratch_shapes=[pltpu.SMEM((8,), F32), pltpu.SMEM((8,), F32), vmem(32, 8, 128), vmem(32, 8, 128)]
        + [pltpu.VMEM((128, 128), jnp.int32)] * 4
        + [pltpu.SemaphoreType.DMA((9,))],
    )(
        *(
            pltpu.with_memory_space_constraint(x, pltpu.HBM)
            for x in (
                edge_table, pad_table, load_currents, labels, bump_height,
                horizontal_class, vertical_class, pad_class,
            )
        ),
    )
    far_rows = swapped(far_rows, ROW, 1)
    near_rows = swapped(near_rows, ROW, 0)
    by_rows, own = pl.pallas_call(
        pack_kernel,
        out_shape=(kept(128, 32, 128), kept(GROUPS, SUB, 128)),
        compiler_params=limited,
        in_specs=[whole] * 2,
        out_specs=(whole,) * 2,
    )(loads, grid)
    own, top, bottom, far_columns, near_columns = pl.pallas_call(
        corner_kernel,
        out_shape=(kept(GROUPS, SUB, 128), kept(HALO, SUB, 128), kept(HALO, SUB, 128))
        + (shape_of(5, SUB, 128),) * 2,
        compiler_params=limited,
        in_specs=[whole] * 3,
        out_specs=(whole,) * 5,
    )(own, far_rows, near_rows)
    far_columns = swapped(far_columns, COL, 1)
    near_columns = swapped(near_columns, COL, 0)
    first, second, w, coef, payload = pl.pallas_call(
        fields_kernel,
        out_shape=(
            kept(128, 48, 128),
            kept(128, 48, 128),
            kept(128, 16, 128),
            kept(6, 160, 128),
            shape_of(512, 128),
        ),
        compiler_params=limited,
        in_specs=[whole] * 7,
        out_specs=(whole,) * 5,
        scratch_shapes=[
            vmem(5, 160, 128),
            vmem(GROUPS + 2, SUB, 128),
            vmem(GROUPS + 2, SUB, 128),
            vmem(GROUPS + 2, 16, 128),
            vmem(GROUPS + 2, 16, 128),
            vmem(GROUPS + 2, 48, 128),
            vmem(GROUPS + 2, 48, 128),
            vmem(2 * GROUPS, 16, 128),
            vmem(2 * GROUPS, 48, 128),
            vmem(2 * GROUPS, 48, 128),
            vmem(144, 48, 128),
            vmem(144, 48, 128),
            vmem(2, GROUPS, 8, 128),
            vmem(144, 48, 128),
            vmem(144, 48, 128),
            vmem(96, 256),
        ],
    )(by_rows, grid, top, bottom, own, far_columns, near_columns)
    sent = payload.reshape(-1, 4, 128)
    everything = lax.all_to_all(sent, ROW + COL, 0, 0, tiled=True).reshape(-1, 128)
    found = pl.pallas_call(
        coarse_kernel,
        out_shape=shape_of(256, 128),
        compiler_params=limited,
        in_specs=[whole],
        out_specs=whole,
        scratch_shapes=[
            vmem(256, 128),
            vmem(256, 256),
            pltpu.VMEM((3, 256, 256), jnp.bfloat16),
            vmem(272, 128),
            vmem(272, 128),
            vmem(32, 128),
        ],
    )(everything)
    matrix = lax.all_to_all(found.reshape(cols, 32, 128), COL, 0, 0, tiled=True).reshape(-1, 128)
    by_block = pl.BlockSpec((32, 32, 128), lambda k: (0, k, 0))
    return pl.pallas_call(
        outputs_kernel,
        grid=(4,),
        out_shape=(shape_of(32, 128, 128), shape_of(32, 128, 128)),
        compiler_params=limited,
        in_specs=[whole] * 7,
        out_specs=(by_block, by_block),
        scratch_shapes=[pltpu.VMEM((96, 384), jnp.bfloat16), vmem(2, 32, 128), vmem(16, 128)],
    )(by_rows, first, second, w, grid, coef, matrix)


def solution(mesh):
    finer = Mesh(mesh.devices.reshape(4, 4, 4, 2), ("row_0", "row_1", "col_0", "col_1"))
    grid = P(ROW, COL)
    return jax.shard_map(
        body,
        mesh=finer,
        in_specs=(P(None, ROW, COL), grid, grid, grid, grid, grid, P(), P()),
        out_specs=(P(None, ROW, COL), P(None, ROW, COL)),
        check_vma=False,
    )
```
